32 devices in a mesh: wide: 16 (over z, y, core), narrow: 2 (over x).
Axes of the slice: x: 2, y: 2, z: 4, core: 2. Of those that a mesh axis runs over, the one named last changes fastest.
Arguments:
- tokens: bfloat16 [16384, 768], P('wide', 'narrow'), may hold values from -6 to 6
- lengths: int32 [16], P('wide'), may hold values from 1 to 1024, as said below
- qkv_weight: bfloat16 [768, 3, 768], P(None, None, 'narrow'), may hold values from -0.21875 to 0.21875
- qv_bias: bfloat16 [2, 768], P(None, 'narrow'), may hold values from -1 to 1
- proj_weight: bfloat16 [768, 768], P('narrow'), may hold values from -0.875 to 0.875
- proj_bias: bfloat16 [768], replicated, may hold values from -3 to 3
- up_weight: bfloat16 [768, 3072], P(None, 'narrow'), may hold values from -0.21875 to 0.21875
- up_bias: bfloat16 [3072], P('narrow'), may hold values from -3 to 3
- down_weight: bfloat16 [3072, 768], P('narrow'), may hold values from -0.109375 to 0.109375
- down_bias: bfloat16 [768], replicated, may hold values from -3 to 3
- first_gain: bfloat16 [768], replicated, may hold values from 0.099609375 to 1.8984375
- first_shift: bfloat16 [768], replicated, may hold values from -2 to 2
- second_gain: bfloat16 [768], replicated, may hold values from 0.099609375 to 1.8984375
- second_shift: bfloat16 [768], replicated, may hold values from -2 to 2
- cotangent: bfloat16 [16384, 768], P('wide', 'narrow'), may hold values from -6 to 6
Outputs:
- layer_out: bfloat16 [16384, 768], P('wide', 'narrow')
- input_grad: bfloat16 [16384, 768], P('wide', 'narrow')
- grad_qkv_weight: float32 [768, 3, 768], P(None, None, 'narrow')
- grad_qv_bias: float32 [2, 768], P(None, 'narrow')
- grad_proj_weight: float32 [768, 768], P('narrow')
- grad_proj_bias: float32 [768], replicated
- grad_up_weight: float32 [768, 3072], P(None, 'narrow')
- grad_up_bias: float32 [3072], P('narrow')
- grad_down_weight: float32 [3072, 768], P('narrow')
- grad_down_bias: float32 [768], replicated
- grad_first_gain: float32 [768], replicated
- grad_first_shift: float32 [768], replicated
- grad_second_gain: float32 [768], replicated
- grad_second_shift: float32 [768], replicated
The draws below stay inside these ranges and needn't reach their ends.
Inputs may be any that keep to these rules, and one draw needn't show every extreme that they name: `lengths`: some sequence has exactly 1024 live tokens.
All inputs are finite; a program needn't handle non-finite values.
Results may differ from the reference program's by a relative error of at most 0.0097.
Values may be sent and summed in bfloat16 or wider, within the bound.
A program may use at most 192 MiB of HBM per device.

```python
import jax
import jax.numpy as jnp
from jax import lax

D = 768
HEADS = 12
FF = 3072
LEN = 1024
SEQS = 16
TOKENS = 16384


def draw_lengths(key, part):
    first_key, second_key = jax.random.split(jax.random.fold_in(key, 17))
    picks = jax.random.randint(first_key, (3, SEQS), 1, LEN + 1)
    shortest = jnp.min(picks, axis=0)
    based = LEN + 1 - shortest
    chosen = jax.random.randint(second_key, (), 0, SEQS)
    return jnp.where(jnp.arange(SEQS) == chosen, LEN, based).astype(jnp.int32)


def shard_levels(rng, extent, shards, low, top_value):
    level, own = 1.0, jax.random.fold_in(rng, 6)
    for axis_at, shards_of in shards:
        draws = jnp.exp(jax.random.uniform(jax.random.fold_in(own, axis_at), (shards_of,), jnp.float32, low / len(shards), top_value / len(shards)))
        level = level * jnp.repeat(draws, extent[axis_at] // shards_of).reshape([-1 if axis == axis_at else 1 for axis in range(len(extent))])
    return level


def gaussian(own_key, shape, scale, bound, pieces=(), kind=jnp.bfloat16):
    entries = scale * jax.random.normal(own_key, shape, jnp.float32)
    if pieces:
        entries = entries * shard_levels(own_key, shape, pieces, -0.22, 0.18)
    return jnp.clip(entries, -bound, bound).astype(kind)


def setup_inputs(seed: int = 0) -> dict:
    key_of = jax.random.split(jax.random.key(seed), 16)
    tokens = gaussian(key_of[0], (TOKENS, D), 1.0, 6.0, ((0, 16), (1, 2)))
    lengths = draw_lengths(jax.random.fold_in(key_of[15], 71), 0)
    qkv_weight = gaussian(key_of[2], (D, 3, D), D ** -0.5, 0.21875, ((2, 2),))
    qv_bias = gaussian(key_of[3], (2, D), 0.2, 1.0, ((1, 2),))
    proj_weight = gaussian(key_of[4], (D, D), (D // 16) ** -0.5, 0.875, ((0, 2),))
    proj_bias = gaussian(key_of[5], (D,), 0.5, 3.0)
    up_weight = gaussian(key_of[6], (D, FF), D ** -0.5, 0.21875, ((1, 2),))
    up_bias = gaussian(key_of[7], (FF,), 0.5, 3.0, ((0, 2),))
    down_weight = gaussian(key_of[8], (FF, D), FF ** -0.5, 0.109375, ((0, 2),))
    down_bias = gaussian(key_of[9], (D,), 0.5, 3.0)
    first_gain = jnp.clip(1.0 + 0.18 * jax.random.normal(key_of[10], (D,), jnp.float32), 0.099609375, 1.8984375).astype(jnp.bfloat16)
    first_shift = gaussian(key_of[11], (D,), 0.3, 2.0)
    second_gain = jnp.clip(1.0 + 0.18 * jax.random.normal(key_of[12], (D,), jnp.float32), 0.099609375, 1.8984375).astype(jnp.bfloat16)
    second_shift = gaussian(key_of[13], (D,), 0.3, 2.0)
    cotangent = gaussian(key_of[14], (TOKENS, D), 1.0, 6.0, ((0, 16), (1, 2)))
    return dict(tokens=tokens, lengths=lengths, qkv_weight=qkv_weight, qv_bias=qv_bias, proj_weight=proj_weight, proj_bias=proj_bias, up_weight=up_weight, up_bias=up_bias, down_weight=down_weight, down_bias=down_bias, first_gain=first_gain, first_shift=first_shift, second_gain=second_gain, second_shift=second_shift, cotangent=cotangent)


EPS = 1e-05
PRECISE = lax.Precision.HIGHEST

@jax.custom_vjp
def low(v):
    return lax.optimization_barrier(v.astype(jnp.bfloat16)).astype(jnp.float32)

@jax.custom_vjp
def low_back(v):
    return v

def low_keep(v):
    return (low(v), None)

def low_pass(kept, grad):
    return (grad,)

def back_keep(v):
    return (v, None)

def back_low(kept, grad):
    return (low(grad),)
low.defvjp(low_keep, low_pass)
low_back.defvjp(back_keep, back_low)

def layer_norm(values, norm_gain, norm_shift):
    row_mean = lax.optimization_barrier(jnp.mean(values, axis=-1, keepdims=True))
    centred = values - row_mean
    spread = lax.optimization_barrier(jnp.mean(centred * centred, axis=-1, keepdims=True))
    return centred * lax.rsqrt(spread + EPS) * norm_gain + norm_shift

def attention(queries, key_rows, value_rows, length):
    seq_len = queries.shape[0]
    block_rows = min(512, seq_len)
    score_scale = queries.shape[2] ** (-0.5)
    key_pos = jnp.arange(seq_len, dtype=jnp.int32)

    def one_block(begin_row):
        block_q = lax.dynamic_slice_in_dim(queries, begin_row, block_rows, 0)
        raw_scores = jnp.einsum('qhe,khe->hqk', block_q, key_rows, precision=PRECISE) * score_scale
        row_pos = begin_row + jnp.arange(block_rows, dtype=jnp.int32)
        allowed = (key_pos[None, :] <= row_pos[:, None]) & (key_pos[None, :] < length)
        scores = low_back(jnp.where(allowed[None], raw_scores, -1e+30))
        weights = low(jax.nn.softmax(scores, axis=-1))
        return jnp.einsum('hqk,khe->qhe', weights, value_rows, precision=PRECISE)
    starts = jnp.arange(seq_len // block_rows, dtype=jnp.int32) * block_rows
    blocks = lax.map(jax.checkpoint(one_block), starts)
    return blocks.reshape(seq_len, queries.shape[1] * queries.shape[2])

def forward(seq_tokens, qkv_weight, qv_bias, proj_weight, proj_bias, up_weight, up_bias, down_weight, down_bias, first_gain, first_shift, second_gain, second_shift, length):
    seq_len = seq_tokens.shape[0]
    normed = low(layer_norm(seq_tokens, first_gain, first_shift))
    projected = jnp.einsum('td,dcf->tcf', normed, qkv_weight, precision=PRECISE)
    queries = low(low_back(projected[:, 0] + qv_bias[0]))
    key_rows = low(low_back(projected[:, 1]))
    value_rows = low(low_back(projected[:, 2] + qv_bias[1]))
    split_shape = (seq_len, HEADS, D // HEADS)
    mixed_rows = attention(queries.reshape(split_shape), key_rows.reshape(split_shape), value_rows.reshape(split_shape), length)
    mixed_rows = low(low_back(mixed_rows))
    branch_out = low_back(jnp.dot(mixed_rows, proj_weight, precision=PRECISE))
    middle = seq_tokens + branch_out + proj_bias
    second = low(layer_norm(middle, second_gain, second_shift))
    hidden = low_back(jnp.dot(second, up_weight, precision=PRECISE) + up_bias)
    active = low(jax.nn.gelu(hidden, approximate=True))
    return middle + jnp.dot(active, down_weight, precision=PRECISE) + down_bias

def reference(tokens, lengths, qkv_weight, qv_bias, proj_weight, proj_bias, up_weight, up_bias, down_weight, down_bias, first_gain, first_shift, second_gain, second_shift, cotangent):
    parameters = tuple((sequence_entry.astype(jnp.float32) for sequence_entry in (qkv_weight, qv_bias, proj_weight, proj_bias, up_weight, up_bias, down_weight, down_bias, first_gain, first_shift, second_gain, second_shift)))
    input_batch = tokens.astype(jnp.float32).reshape(SEQS, LEN, D)
    upstream_gradient = cotangent.astype(jnp.float32).reshape(SEQS, LEN, D)
    positions = jnp.arange(LEN, dtype=jnp.int32)

    def single_sequence(gradient_totals, seq_item):
        seq_tokens, seq_grad, length = seq_item
        valid_rows = (positions < length).astype(jnp.float32)[:, None]

        def run_layer(layer_in, *weight_list):
            return forward(layer_in, *weight_list, length)
        seq_out, pull_back = jax.vjp(run_layer, seq_tokens, *parameters)
        grad_list = pull_back(seq_grad * valid_rows)
        gradient_totals = tuple((running + update for running, update in zip(gradient_totals, grad_list[1:])))
        return (gradient_totals, (seq_out.astype(jnp.bfloat16), grad_list[0].astype(jnp.bfloat16)))
    blank_slots = tuple((jnp.zeros(sequence_entry.shape, jnp.float32) for sequence_entry in parameters))
    gradient_totals, (output_batch, incoming_gradients) = lax.scan(single_sequence, blank_slots, (input_batch, upstream_gradient, lengths))
    factor = 1.0 / SEQS
    return (output_batch.reshape(TOKENS, D), incoming_gradients.reshape(TOKENS, D), gradient_totals[0] * factor, gradient_totals[1] * factor, gradient_totals[2] * factor, gradient_totals[3] * factor, gradient_totals[4] * factor, gradient_totals[5] * factor, gradient_totals[6] * factor, gradient_totals[7] * factor, gradient_totals[8] * factor, gradient_totals[9] * factor, gradient_totals[10] * factor, gradient_totals[11] * factor)
```

```python
import functools

import jax
import jax.numpy as jnp
from jax import lax
from jax.experimental import pallas as pl
from jax.experimental.pallas import tpu as pltpu
from jax.sharding import PartitionSpec as P

EPS = 1e-05
HEAD = 64
F32, BF16 = jnp.float32, jnp.bfloat16
NT = (((1,), (1,)), ((), ()))
TN = (((0,), (0,)), ((), ()))
GELU_A, GELU_B = 0.7978845608028654, 0.044715
VMEM_LIMIT = 56 * 1024 * 1024


def dot(a, b):
    return jnp.dot(a, b, preferred_element_type=F32)


def dot_nt(a, b):
    return lax.dot_general(a, b, NT, preferred_element_type=F32)


def dot_tn(a, b):
    return lax.dot_general(a, b, TN, preferred_element_type=F32)


def params(**more):
    return pltpu.CompilerParams(vmem_limit_bytes=VMEM_LIMIT, **more)


def cost(flops, size, trans=0):
    return pl.CostEstimate(flops=int(flops), bytes_accessed=int(size), transcendentals=int(trans))


def lane_part(which, width):
    return pl.ds(pl.multiple_of(which * width, 128), width)


def norm_rows(x):
    mean = jnp.mean(x, axis=-1, keepdims=True)
    cen = x - mean
    var = jnp.mean(cen * cen, axis=-1, keepdims=True)
    r = lax.rsqrt(var + EPS)
    return cen * r, r


def add_rows(ref, first, value):
    total = jnp.sum(value, axis=0, keepdims=True)

    @pl.when(first)
    def _():
        ref[...] = total

    @pl.when(jnp.logical_not(first))
    def _():
        ref[...] += total


def rows_spec(rows, cols, base=0):
    return pl.BlockSpec((rows, cols), lambda i, *_: (i + base, 0))


def whole_spec(shape):
    zeros = (0,) * len(shape)
    return pl.BlockSpec(shape, lambda i, *_: zeros)


def qkv_body(n_ref, own, got, w, bias, gain, shift, xf, low, q, k, v):
    n = n_ref[0]
    cw = own.shape[1]
    xf[:, lane_part(n, cw)] = own[...]
    xf[:, lane_part(1 - n, cw)] = got[...]
    xhat, _ = norm_rows(xf[...].astype(F32))
    y = (xhat * gain[...] + shift[...]).astype(BF16)
    low[...] = y
    q[...] = (dot(y, w[0]) + bias[0:1, :]).astype(BF16) * jnp.asarray(HEAD**-0.5, BF16)
    k[...] = dot(y, w[1]).astype(BF16)
    v[...] = (dot(y, w[2]) + bias[1:2, :]).astype(BF16)


def qkv_call(n, own, got, w, bias, gain, shift, block=256):
    rows, cw = own.shape
    d, lw = w.shape[1], w.shape[2]
    sd = jax.ShapeDtypeStruct
    return pl.pallas_call(
        qkv_body,
        out_shape=(sd((rows, d), BF16), sd((rows, d), BF16)) + (sd((rows, lw), BF16),) * 3,
        grid_spec=pltpu.PrefetchScalarGridSpec(
            num_scalar_prefetch=1,
            grid=(rows // block,),
            in_specs=[rows_spec(block, cw), rows_spec(block, cw)]
            + [whole_spec(a.shape) for a in (w, bias, gain, shift)],
            out_specs=[rows_spec(block, d)] * 2 + [rows_spec(block, lw)] * 3,
        ),
        compiler_params=params(),
        cost_estimate=cost(2 * rows * d * 3 * lw, 2 * (rows * d * 5 + w.size)),
        name="norm_qkv",
    )(n, own, got, w, bias, gain, shift)


def three(x):
    hi = x.astype(BF16).astype(F32)
    mid = (x - hi).astype(BF16).astype(F32)
    return hi, mid, x - hi - mid


def lanes_of(par):
    lane = lax.broadcasted_iota(jnp.int32, (1, 2 * HEAD), 1)
    mine = (lane // HEAD) == par
    return lane, mine, (1 - par) * HEAD


def place(lane, mine, at, base, terms):
    out = jnp.where(mine, base, 0.0)
    for i, term in enumerate(terms):
        out = jnp.where(lane == at + i, term, out)
    return out


def fwd_body(len_ref, q, k, v, o, qa_out, ka, va, *, r0, bq):
    par = pl.program_id(0) % 2
    lane, mine, at = lanes_of(par)
    keys = k.shape[0]
    kpos = lax.broadcasted_iota(jnp.int32, (keys, 1), 0)
    kbias = jnp.where(kpos < len_ref[0], 0.0, -1e30)
    ka[...] = place(lane, mine, at, k[...].astype(F32), [kbias]).astype(BF16)
    va[...] = place(lane, mine, at, v[...].astype(F32), [1.0]).astype(BF16)
    tri = lax.broadcasted_iota(jnp.int32, (bq, bq), 1) <= lax.broadcasted_iota(jnp.int32, (bq, bq), 0)
    for i in range(q.shape[0] // bq):
        nk = r0 + (i + 1) * bq
        rows = pl.ds(i * bq, bq)
        qf = q[rows, :].astype(F32)
        qa = place(lane, mine, at, qf, [1.0])
        s = dot_nt(qa.astype(BF16), ka[0:nk, :])
        edge = jnp.where(tri, s[:, nk - bq :], -1e30)
        m = jnp.max(edge, axis=1, keepdims=True)
        if nk > bq:
            m = jnp.maximum(m, jnp.max(s[:, : nk - bq], axis=1, keepdims=True))
        pv = dot(jnp.exp(edge - m).astype(BF16), va[nk - bq : nk, :])
        if nk > bq:
            pv += dot(jnp.exp(s[:, : nk - bq] - m).astype(BF16), va[0 : nk - bq, :])
        total = jnp.sum(jnp.where(lane == at, pv, 0.0), axis=1, keepdims=True)
        out = (pv / total).astype(BF16).astype(F32)
        old = o[rows, :].astype(F32)
        o[rows, :] = jnp.where(mine, out, jnp.where(par == 0, 0.0, old)).astype(BF16)
        lse = m + jnp.log(total)
        qa_out[0, rows, :] = place(lane, mine, at, qf, [1.0, *three(lse)]).astype(BF16)


def attend_forward(length, q, k, v, r0, rows, bq=256):
    width = q.shape[1]
    heads, pair = width // HEAD, 2 * HEAD
    keys = r0 + rows
    half = lambda h, *_: (0, h // 2)
    sd = jax.ShapeDtypeStruct
    work = 4 * heads * rows * (keys - rows // 2) * HEAD
    return pl.pallas_call(
        functools.partial(fwd_body, r0=r0, bq=bq),
        out_shape=(sd((rows, width), BF16), sd((heads, rows, pair), BF16)),
        grid_spec=pltpu.PrefetchScalarGridSpec(
            num_scalar_prefetch=1,
            grid=(heads,),
            in_specs=[
                pl.BlockSpec((rows, pair), lambda h, *_: (r0 // rows, h // 2)),
                pl.BlockSpec((keys, pair), half),
                pl.BlockSpec((keys, pair), half),
            ],
            out_specs=[
                pl.BlockSpec((rows, pair), half),
                pl.BlockSpec((1, rows, pair), lambda h, *_: (h, 0, 0)),
            ],
            scratch_shapes=[pltpu.VMEM((keys, pair), BF16)] * 2,
        ),
        compiler_params=params(),
        cost_estimate=cost(4 * work, 2 * rows * width * 6, work // 256),
        name="attend_fwd",
    )(length, q, k, v)


def bwd_body(len_ref, qa, k, v, do, o, dq, dk, dv, ka, va, dk_acc, dv_acc, *, r0, bq):
    par = pl.program_id(0) % 2
    lane, mine, at = lanes_of(par)
    keys = k.shape[0]
    kpos = lax.broadcasted_iota(jnp.int32, (keys, 1), 0)
    kbias = jnp.where(kpos < len_ref[0], 0.0, -1e30)
    ka[...] = place(lane, mine, at, k[...].astype(F32), [kbias, -1.0, -1.0, -1.0]).astype(BF16)
    va[...] = place(lane, mine, at, v[...].astype(F32), [-1.0, -1.0, -1.0]).astype(BF16)
    dk_acc[...] = jnp.zeros_like(dk_acc)
    dv_acc[...] = jnp.zeros_like(dv_acc)
    tri = lax.broadcasted_iota(jnp.int32, (bq, bq), 0) <= lax.broadcasted_iota(jnp.int32, (bq, bq), 1)

    def put(ref, rows, new):
        old = ref[rows, :].astype(F32)
        ref[rows, :] = jnp.where(mine, new, jnp.where(par == 0, 0.0, old)).astype(BF16)

    for i in range(qa.shape[1] // bq):
        rows = pl.ds(i * bq, bq)
        qb = qa[0, rows, :]
        df = do[rows, :].astype(F32)
        delta = jnp.sum(jnp.where(mine, df * o[rows, :].astype(F32), 0.0), axis=1, keepdims=True)
        db = place(lane, mine, at, df, three(delta)).astype(BF16)
        dqs = None
        for j in range((r0 + i * bq) // bq + 1):
            cols = pl.ds(j * bq, bq)
            kb, vb = ka[cols, :], va[cols, :]
            s = dot_nt(kb, qb)
            if j * bq == r0 + i * bq:
                s = jnp.where(tri, s, -1e30)
            p = jnp.exp(s)
            ds = (p * dot_nt(vb, db)).astype(BF16)
            dv_acc[cols, :] += dot(p.astype(BF16), db)
            dk_acc[cols, :] += dot(ds, qb)
            part = dot_tn(ds, kb)
            dqs = part if dqs is None else dqs + part
        put(dq, rows, dqs * HEAD**-0.5)
    put(dk, pl.ds(0, keys), dk_acc[...])
    put(dv, pl.ds(0, keys), dv_acc[...])


def attend_backward(length, qa, k, v, do, o, r0, rows, bq=256):
    width = k.shape[1]
    heads, pair = width // HEAD, 2 * HEAD
    keys = r0 + rows
    half = lambda h, *_: (0, h // 2)
    sd = jax.ShapeDtypeStruct
    work = 4 * heads * rows * (keys - rows // 2) * HEAD
    return pl.pallas_call(
        functools.partial(bwd_body, r0=r0, bq=bq),
        out_shape=(sd((rows, width), BF16), sd((keys, width), BF16), sd((keys, width), BF16)),
        grid_spec=pltpu.PrefetchScalarGridSpec(
            num_scalar_prefetch=1,
            grid=(heads,),
            in_specs=[
                pl.BlockSpec((1, rows, pair), lambda h, *_: (h, 0, 0)),
                pl.BlockSpec((keys, pair), half),
                pl.BlockSpec((keys, pair), half),
                pl.BlockSpec((rows, pair), half),
                pl.BlockSpec((rows, pair), half),
            ],
            out_specs=[
                pl.BlockSpec((rows, pair), half),
                pl.BlockSpec((keys, pair), half),
                pl.BlockSpec((keys, pair), half),
            ],
            scratch_shapes=[pltpu.VMEM((keys, pair), BF16)] * 2 + [pltpu.VMEM((keys, pair), F32)] * 2,
        ),
        compiler_params=params(),
        cost_estimate=cost(10 * work, 2 * rows * width * 9, work // 256),
        name="attend_bwd",
    )(length, qa, k, v, do, o)


def mlp_body(
    s_ref, xf, mo, mr, pwo, pwr, pb, gain, shift, up, ub, down, db, co, cr,
    mid, second, active, gh, cf, lo, send, gs, sum_ub, sum_db,
    *, r0,
):
    n, length = s_ref[0], s_ref[1]
    i = pl.program_id(0)
    rows, cw = co.shape
    m = xf[...].astype(F32) + (dot(mo[...], pwo[...]) + dot(mr[...], pwr[...])) + pb[...]
    mid[...] = m
    xhat, _ = norm_rows(m)
    sec = (xhat * gain[...] + shift[...]).astype(BF16)
    second[...] = sec
    hid = dot(sec, up[...]) + ub[...]
    sq = hid * hid
    t = jnp.tanh(GELU_A * (hid + GELU_B * (sq * hid)))
    half = 0.5 * (1.0 + t)
    act = (hid * half).astype(BF16)
    active[...] = act
    slope = half + (0.5 * hid) * (1.0 - t * t) * (GELU_A + (3.0 * GELU_A * GELU_B) * sq)
    mine, other = lane_part(n, cw), lane_part(1 - n, cw)
    lo[...] = mid[:, mine] + dot(act, down[:, mine]) + db[:, mine]
    send[...] = dot(act, down[:, other]).astype(BF16)
    pos = r0 + i * rows + lax.broadcasted_iota(jnp.int32, (rows, 1), 0)
    live = (pos < length).astype(F32)
    cf[:, mine] = (co[...].astype(F32) * live).astype(BF16)
    cf[:, other] = (cr[...].astype(F32) * live).astype(BF16)
    cot = cf[...]
    ghid = (dot_nt(cot, down[...]) * slope).astype(BF16)
    gh[...] = ghid
    gs[...] = dot_nt(ghid, up[...]).astype(BF16)
    add_rows(sum_ub, i == 0, ghid.astype(F32))
    add_rows(sum_db, i == 0, cot.astype(F32))


def mlp_call(scal, xf, mo, mr, pwo, pwr, pb, gain, shift, up, ub, down, db, co, cr, r0, block=256):
    rows, lw = mo.shape
    d, f = up.shape
    cw = co.shape[1]
    b0 = r0 // block
    sd = jax.ShapeDtypeStruct
    return pl.pallas_call(
        functools.partial(mlp_body, r0=r0),
        out_shape=(
            sd((rows, d), F32), sd((rows, d), BF16), sd((rows, f), BF16), sd((rows, f), BF16),
            sd((rows, d), BF16), sd((rows, cw), F32), sd((rows, cw), BF16), sd((rows, d), BF16),
            sd((1, f), F32), sd((1, d), F32),
        ),
        grid_spec=pltpu.PrefetchScalarGridSpec(
            num_scalar_prefetch=1,
            grid=(rows // block,),
            in_specs=[rows_spec(block, d, b0), rows_spec(block, lw), rows_spec(block, lw)]
            + [whole_spec(a.shape) for a in (pwo, pwr, pb, gain, shift, up, ub, down, db)]
            + [rows_spec(block, cw, b0), rows_spec(block, cw, b0)],
            out_specs=[
                rows_spec(block, d), rows_spec(block, d), rows_spec(block, f), rows_spec(block, f),
                rows_spec(block, d), rows_spec(block, cw), rows_spec(block, cw), rows_spec(block, d),
                whole_spec((1, f)), whole_spec((1, d)),
            ],
        ),
        compiler_params=params(),
        cost_estimate=cost(2 * rows * d * (d + 4 * f), 2 * (rows * d * 8 + rows * f * 2 + 2 * d * f), rows * f),
        name="mlp",
    )(scal, xf, mo, mr, pwo, pwr, pb, gain, shift, up, ub, down, db, co, cr)


def mid_body(s_ref, go, gr, mid, cf, gain, pwo, low, gm_own, gmix, sum_gain, sum_shift, sum_pb):
    n = s_ref[0]
    i = pl.program_id(0)
    cw = gm_own.shape[1]
    g = go[...].astype(F32) + gr[...].astype(F32)
    xhat, r = norm_rows(mid[...])
    gg = g * gain[...]
    m1 = jnp.mean(gg, axis=-1, keepdims=True)
    m2 = jnp.mean(gg * xhat, axis=-1, keepdims=True)
    gm = cf[...].astype(F32) + r * (gg - m1 - xhat * m2)
    mid[...] = gm
    gm_own[...] = mid[:, lane_part(n, cw)]
    gl = gm.astype(BF16)
    low[...] = gl
    gmix[...] = dot_nt(gl, pwo[...]).astype(BF16)
    add_rows(sum_gain, i == 0, g * xhat)
    add_rows(sum_shift, i == 0, g)
    add_rows(sum_pb, i == 0, gm)


def mid_call(scal, go, gr, mid, cf, gain, pwo, block=256):
    rows, d = mid.shape
    lw = pwo.shape[0]
    cw = d // 2
    sd = jax.ShapeDtypeStruct
    return pl.pallas_call(
        mid_body,
        out_shape=(
            sd((rows, d), BF16), sd((rows, cw), F32), sd((rows, lw), BF16),
            sd((1, d), F32), sd((1, d), F32), sd((1, d), F32),
        ),
        grid_spec=pltpu.PrefetchScalarGridSpec(
            num_scalar_prefetch=1,
            grid=(rows // block,),
            in_specs=[rows_spec(block, d)] * 4 + [whole_spec(gain.shape), whole_spec(pwo.shape)],
            out_specs=[rows_spec(block, d), rows_spec(block, cw), rows_spec(block, lw)] + [whole_spec((1, d))] * 3,
        ),
        compiler_params=params(),
        cost_estimate=cost(2 * rows * d * lw, rows * d * 16),
        name="mid_bwd",
    )(scal, go, gr, mid, cf, gain, pwo)


def part_body(s_ref, dq, dk, dv, w, xf, gain, keep, send, stats, tmp):
    n = s_ref[0]
    cw = keep.shape[1]
    for c in range(2):
        g = dot_nt(dq[...], w[0, c * cw : (c + 1) * cw, :])
        g += dot_nt(dk[...], w[1, c * cw : (c + 1) * cw, :])
        g += dot_nt(dv[...], w[2, c * cw : (c + 1) * cw, :])
        tmp[:, c * cw : (c + 1) * cw] = g
    keep[...] = tmp[:, lane_part(n, cw)]
    send[...] = tmp[:, lane_part(1 - n, cw)].astype(BF16)
    xhat, _ = norm_rows(xf[...].astype(F32))
    gg = tmp[...] * gain[...]
    m1 = jnp.mean(gg, axis=-1, keepdims=True)
    m2 = jnp.mean(gg * xhat, axis=-1, keepdims=True)
    lane = lax.broadcasted_iota(jnp.int32, (1, 128), 1)
    both = jnp.where(lane == 0, m1, jnp.where(lane == 1, m2, 0.0))
    stats[...] = both.T[0:8, :]


def part_call(scal, dq, dk, dv, w, xf, gain, block=256):
    rows, d = xf.shape
    lw = dq.shape[1]
    cw = d // 2
    sd = jax.ShapeDtypeStruct
    return pl.pallas_call(
        part_body,
        out_shape=(sd((rows, cw), F32), sd((rows, cw), BF16), sd((8, rows), F32)),
        grid_spec=pltpu.PrefetchScalarGridSpec(
            num_scalar_prefetch=1,
            grid=(rows // block,),
            in_specs=[rows_spec(block, lw)] * 3 + [whole_spec(w.shape), rows_spec(block, d), whole_spec(gain.shape)],
            out_specs=[
                rows_spec(block, cw), rows_spec(block, cw),
                pl.BlockSpec((8, block), lambda i, *_: (0, i)),
            ],
            scratch_shapes=[pltpu.VMEM((block, d), F32)],
        ),
        compiler_params=params(),
        cost_estimate=cost(6 * rows * d * lw, rows * d * 8),
        name="qkv_bwd",
    )(scal, dq, dk, dv, w, xf, gain)


def in_body(s_ref, keep, got, st_own, st_got, xf, gm, gain, out, sum_gain, sum_shift):
    n = s_ref[0]
    i = pl.program_id(0)
    cw = keep.shape[1]
    x = xf[...].astype(F32)
    mean = jnp.mean(x, axis=-1, keepdims=True)
    cen = x - mean
    r = lax.rsqrt(jnp.mean(cen * cen, axis=-1, keepdims=True) + EPS)
    xhat = (xf[:, lane_part(n, cw)].astype(F32) - mean) * r
    st = (st_own[...] + st_got[...]).T
    g = keep[...] + got[...].astype(F32)
    gg = g * gain[:, lane_part(n, cw)]
    out[...] = (gm[...] + r * (gg - st[:, 0:1] - xhat * st[:, 1:2])).astype(BF16)
    add_rows(sum_gain, i == 0, g * xhat)
    add_rows(sum_shift, i == 0, g)


def in_call(scal, keep, got, st_own, st_got, xf, gm, gain, block=256):
    rows, d = xf.shape
    cw = d // 2
    sd = jax.ShapeDtypeStruct
    stat = pl.BlockSpec((8, block), lambda i, *_: (0, i))
    return pl.pallas_call(
        in_body,
        out_shape=(sd((rows, cw), BF16), sd((1, cw), F32), sd((1, cw), F32)),
        grid_spec=pltpu.PrefetchScalarGridSpec(
            num_scalar_prefetch=1,
            grid=(rows // block,),
            in_specs=[rows_spec(block, cw)] * 2 + [stat, stat, rows_spec(block, d), rows_spec(block, cw), whole_spec(gain.shape)],
            out_specs=[rows_spec(block, cw), whole_spec((1, cw)), whole_spec((1, cw))],
        ),
        compiler_params=params(),
        cost_estimate=cost(rows * d * 16, rows * d * 8),
        name="in_bwd",
    )(scal, keep, got, st_own, st_got, xf, gm, gain)


def on_device(
    tokens, lengths, qkv_weight, qv_bias, proj_weight, proj_bias, up_weight, up_bias,
    down_weight, down_bias, first_gain, first_shift, second_gain, second_shift, cotangent,
):
    rows, cw = tokens.shape
    n = lax.axis_index("narrow").astype(jnp.int32)
    n1 = n.reshape(1)
    scal = jnp.concatenate([n1, lengths.astype(jnp.int32)])
    swap = lambda a: lax.ppermute(a, "narrow", [(0, 1), (1, 0)])
    row = lambda a: a.astype(F32).reshape(1, -1)
    w3 = jnp.transpose(qkv_weight, (1, 0, 2))
    gain1, shift1, gain2, shift2 = map(row, (first_gain, first_shift, second_gain, second_shift))

    got_tokens = swap(tokens)
    got_cot = swap(cotangent)
    got_proj = swap(proj_weight)
    xf, low, q, k, v = qkv_call(n1, tokens, got_tokens, w3, qv_bias.astype(F32), gain1, shift1)
    mixed, qa = attend_forward(lengths, q, k, v, 0, rows)
    got_mixed = swap(mixed)
    mid, second, active, gh, cf, lo, send, gs, sum_ub, sum_db = mlp_call(
        scal, xf, mixed, got_mixed, proj_weight, got_proj, row(proj_bias), gain2, shift2,
        up_weight, row(up_bias), down_weight, row(down_bias), cotangent, got_cot, 0,
    )
    got_gs = swap(gs)
    layer_out = (lo + swap(send).astype(F32)).astype(BF16)
    grad_down = dot_tn(active, cf)
    grad_up = dot_tn(second, gh)
    mlow, gm_own, gmix, sum_g2, sum_s2, sum_pb = mid_call(n1, gs, got_gs, mid, cf, gain2, proj_weight)
    dq, dk, dv = attend_backward(lengths, qa, k, v, gmix, mixed, 0, rows)
    keep, nsend, stats = part_call(n1, dq, dk, dv, w3, xf, gain1)
    input_grad, sum_g1, sum_s1 = in_call(n1, keep, swap(nsend), stats, swap(stats), xf, gm_own, gain1)
    grad_proj = dot_tn(mixed, mlow)
    grad_qkv = jnp.stack([dot_tn(low, a) for a in (dq, dk, dv)])
    bias_sums = jnp.concatenate([jnp.sum(a.astype(F32), axis=0) for a in (dq, dv)])

    spread = lambda a: lax.dynamic_update_slice(jnp.zeros((2 * cw,), F32), a.reshape(-1), (n * cw,))
    both = jnp.concatenate([spread(sum_g1), spread(sum_s1)])
    both = both + swap(both)
    small = jnp.concatenate(
        [both] + [a.reshape(-1) for a in (sum_g2, sum_s2, sum_pb, sum_db, sum_ub, bias_sums)]
    )
    d = 2 * cw
    pad = -small.shape[0] % (16 * d)
    small = jnp.pad(small, (0, pad)).reshape(-1, d)
    proj_small = jnp.concatenate([grad_proj.astype(BF16), small.astype(BF16)], axis=0)
    s_down, s_up, s_proj, s_qkv = lax.psum(
        (grad_down.astype(BF16), grad_up.astype(BF16), proj_small, grad_qkv.astype(BF16)), "wide"
    )
    factor = 1.0 / (lengths.shape[0] * lax.axis_size("wide"))
    fin = lambda a: a.astype(F32) * factor
    flat = fin(s_proj[grad_proj.shape[0] :]).reshape(-1)
    lw, ff = proj_weight.shape[0], up_weight.shape[1]
    cuts = [d, d, d, d, d, d, ff, lw, lw]
    pieces, at = [], 0
    for c in cuts:
        pieces.append(flat[at : at + c])
        at += c
    g1, s1, g2, s2, pb, dbs, ubs, qb, vb = pieces
    return (
        layer_out, input_grad, jnp.transpose(fin(s_qkv), (1, 0, 2)), jnp.stack([qb, vb]),
        fin(s_proj[: grad_proj.shape[0]]), pb, fin(s_up), ubs, fin(s_down), dbs, g1, s1, g2, s2,
    )


def solution(mesh):
    split = P("wide", "narrow")
    none3, cols, rows1 = P(None, None, "narrow"), P(None, "narrow"), P("narrow", None)
    return jax.shard_map(
        on_device,
        mesh=mesh,
        in_specs=(
            split, P("wide"), none3, cols, rows1, P(), cols, P("narrow"), rows1, P(), P(), P(), P(), P(), split,
        ),
        out_specs=(
            split, split, none3, cols, rows1, P(), cols, P("narrow"), rows1, P(), P(), P(), P(), P(),
        ),
        check_vma=False,
    )
```

```python
import functools

import jax
import jax.numpy as jnp
from jax import lax
from jax.experimental import pallas as pl
from jax.experimental.pallas import tpu as pltpu
from jax.sharding import PartitionSpec as P

EPS = 1e-05
HEAD = 64
F32, BF16 = jnp.float32, jnp.bfloat16
NT = (((1,), (1,)), ((), ()))
TN = (((0,), (0,)), ((), ()))
GELU_A, GELU_B = 0.7978845608028654, 0.044715
VMEM_LIMIT = 56 * 1024 * 1024


def dot(a, b):
    return jnp.dot(a, b, preferred_element_type=F32)


def dot_nt(a, b):
    return lax.dot_general(a, b, NT, preferred_element_type=F32)


def dot_tn(a, b):
    return lax.dot_general(a, b, TN, preferred_element_type=F32)


def params(**more):
    return pltpu.CompilerParams(vmem_limit_bytes=VMEM_LIMIT, **more)


def cost(flops, size, trans=0):
    return pl.CostEstimate(flops=int(flops), bytes_accessed=int(size), transcendentals=int(trans))


def lane_part(which, width):
    return pl.ds(pl.multiple_of(which * width, 128), width)


def norm_rows(x):
    mean = jnp.mean(x, axis=-1, keepdims=True)
    cen = x - mean
    var = jnp.mean(cen * cen, axis=-1, keepdims=True)
    r = lax.rsqrt(var + EPS)
    return cen * r, r


def add_rows(ref, first, value):
    total = jnp.sum(value, axis=0, keepdims=True)

    @pl.when(first)
    def _():
        ref[...] = total

    @pl.when(jnp.logical_not(first))
    def _():
        ref[...] += total


def rows_spec(rows, cols, base=0):
    return pl.BlockSpec((rows, cols), lambda i, *_: (i + base, 0))


def whole_spec(shape):
    zeros = (0,) * len(shape)
    return pl.BlockSpec(shape, lambda i, *_: zeros)


def qkv_body(n_ref, own, got, w, bias, gain, shift, xf, low, q, k, v):
    n = n_ref[0]
    cw = own.shape[1]
    xf[:, lane_part(n, cw)] = own[...]
    xf[:, lane_part(1 - n, cw)] = got[...]
    xhat, _ = norm_rows(xf[...].astype(F32))
    y = (xhat * gain[...] + shift[...]).astype(BF16)
    low[...] = y
    q[...] = (dot(y, w[0]) + bias[0:1, :]).astype(BF16) * jnp.asarray(HEAD**-0.5, BF16)
    k[...] = dot(y, w[1]).astype(BF16)
    v[...] = (dot(y, w[2]) + bias[1:2, :]).astype(BF16)


def qkv_call(n, own, got, w, bias, gain, shift, block=256):
    rows, cw = own.shape
    d, lw = w.shape[1], w.shape[2]
    sd = jax.ShapeDtypeStruct
    return pl.pallas_call(
        qkv_body,
        out_shape=(sd((rows, d), BF16), sd((rows, d), BF16)) + (sd((rows, lw), BF16),) * 3,
        grid_spec=pltpu.PrefetchScalarGridSpec(
            num_scalar_prefetch=1,
            grid=(rows // block,),
            in_specs=[rows_spec(block, cw), rows_spec(block, cw)]
            + [whole_spec(a.shape) for a in (w, bias, gain, shift)],
            out_specs=[rows_spec(block, d)] * 2 + [rows_spec(block, lw)] * 3,
        ),
        compiler_params=params(),
        cost_estimate=cost(2 * rows * d * 3 * lw, 2 * (rows * d * 5 + w.size)),
        name="norm_qkv",
    )(n, own, got, w, bias, gain, shift)


def three(x):
    hi = x.astype(BF16).astype(F32)
    mid = (x - hi).astype(BF16).astype(F32)
    return hi, mid, x - hi - mid


def lanes_of(par):
    lane = lax.broadcasted_iota(jnp.int32, (1, 2 * HEAD), 1)
    mine = (lane // HEAD) == par
    return lane, mine, (1 - par) * HEAD


def place(lane, mine, at, base, terms):
    out = jnp.where(mine, base, 0.0)
    for i, term in enumerate(terms):
        out = jnp.where(lane == at + i, term, out)
    return out


def fwd_body(len_ref, q, k, v, o, qa_out, ka, va, *, r0, bq):
    par = pl.program_id(0) % 2
    lane, mine, at = lanes_of(par)
    keys = k.shape[0]
    kpos = lax.broadcasted_iota(jnp.int32, (keys, 1), 0)
    kbias = jnp.where(kpos < len_ref[0], 0.0, -1e30)
    ka[...] = place(lane, mine, at, k[...].astype(F32), [kbias]).astype(BF16)
    va[...] = place(lane, mine, at, v[...].astype(F32), [1.0]).astype(BF16)
    tri = lax.broadcasted_iota(jnp.int32, (bq, bq), 1) <= lax.broadcasted_iota(jnp.int32, (bq, bq), 0)
    for i in range(q.shape[0] // bq):
        nk = r0 + (i + 1) * bq
        rows = pl.ds(i * bq, bq)
        qf = q[rows, :].astype(F32)
        qa = place(lane, mine, at, qf, [1.0])
        s = dot_nt(qa.astype(BF16), ka[0:nk, :])
        edge = jnp.where(tri, s[:, nk - bq :], -1e30)
        m = jnp.max(edge, axis=1, keepdims=True)
        if nk > bq:
            m = jnp.maximum(m, jnp.max(s[:, : nk - bq], axis=1, keepdims=True))
        pv = dot(jnp.exp(edge - m).astype(BF16), va[nk - bq : nk, :])
        if nk > bq:
            pv += dot(jnp.exp(s[:, : nk - bq] - m).astype(BF16), va[0 : nk - bq, :])
        total = jnp.sum(jnp.where(lane == at, pv, 0.0), axis=1, keepdims=True)
        out = (pv / total).astype(BF16).astype(F32)
        old = o[rows, :].astype(F32)
        o[rows, :] = jnp.where(mine, out, jnp.where(par == 0, 0.0, old)).astype(BF16)
        lse = m + jnp.log(total)
        qa_out[0, rows, :] = place(lane, mine, at, qf, [1.0, *three(lse)]).astype(BF16)


def attend_forward(length, q, k, v, r0, rows, bq=256):
    width = q.shape[1]
    heads, pair = width // HEAD, 2 * HEAD
    keys = r0 + rows
    half = lambda h, *_: (0, h // 2)
    sd = jax.ShapeDtypeStruct
    work = 4 * heads * rows * (keys - rows // 2) * HEAD
    return pl.pallas_call(
        functools.partial(fwd_body, r0=r0, bq=bq),
        out_shape=(sd((rows, width), BF16), sd((heads, rows, pair), BF16)),
        grid_spec=pltpu.PrefetchScalarGridSpec(
            num_scalar_prefetch=1,
            grid=(heads,),
            in_specs=[
                pl.BlockSpec((rows, pair), lambda h, *_: (r0 // rows, h // 2)),
                pl.BlockSpec((keys, pair), half),
                pl.BlockSpec((keys, pair), half),
            ],
            out_specs=[
                pl.BlockSpec((rows, pair), half),
                pl.BlockSpec((1, rows, pair), lambda h, *_: (h, 0, 0)),
            ],
            scratch_shapes=[pltpu.VMEM((keys, pair), BF16)] * 2,
        ),
        compiler_params=params(),
        cost_estimate=cost(4 * work, 2 * rows * width * 6, work // 256),
        name="attend_fwd",
    )(length, q, k, v)


def bwd_body(len_ref, qa, k, v, do, o, dq, dk, dv, ka, va, dk_acc, dv_acc, *, r0, bq):
    par = pl.program_id(0) % 2
    lane, mine, at = lanes_of(par)
    keys = k.shape[0]
    kpos = lax.broadcasted_iota(jnp.int32, (keys, 1), 0)
    kbias = jnp.where(kpos < len_ref[0], 0.0, -1e30)
    ka[...] = place(lane, mine, at, k[...].astype(F32), [kbias, -1.0, -1.0, -1.0]).astype(BF16)
    va[...] = place(lane, mine, at, v[...].astype(F32), [-1.0, -1.0, -1.0]).astype(BF16)
    dk_acc[...] = jnp.zeros_like(dk_acc)
    dv_acc[...] = jnp.zeros_like(dv_acc)
    tri = lax.broadcasted_iota(jnp.int32, (bq, bq), 0) <= lax.broadcasted_iota(jnp.int32, (bq, bq), 1)

    def put(ref, rows, new):
        old = ref[rows, :].astype(F32)
        ref[rows, :] = jnp.where(mine, new, jnp.where(par == 0, 0.0, old)).astype(BF16)

    for i in range(qa.shape[1] // bq):
        rows = pl.ds(i * bq, bq)
        qb = qa[0, rows, :]
        df = do[rows, :].astype(F32)
        delta = jnp.sum(jnp.where(mine, df * o[rows, :].astype(F32), 0.0), axis=1, keepdims=True)
        db = place(lane, mine, at, df, three(delta)).astype(BF16)
        dqs = None
        for j in range((r0 + i * bq) // bq + 1):
            cols = pl.ds(j * bq, bq)
            kb, vb = ka[cols, :], va[cols, :]
            s = dot_nt(kb, qb)
            if j * bq == r0 + i * bq:
                s = jnp.where(tri, s, -1e30)
            p = jnp.exp(s)
            ds = (p * dot_nt(vb, db)).astype(BF16)
            dv_acc[cols, :] += dot(p.astype(BF16), db)
            dk_acc[cols, :] += dot(ds, qb)
            part = dot_tn(ds, kb)
            dqs = part if dqs is None else dqs + part
        put(dq, rows, dqs * HEAD**-0.5)
    put(dk, pl.ds(0, keys), dk_acc[...])
    put(dv, pl.ds(0, keys), dv_acc[...])


def attend_backward(length, qa, k, v, do, o, r0, rows, bq=256):
    width = k.shape[1]
    heads, pair = width // HEAD, 2 * HEAD
    keys = r0 + rows
    half = lambda h, *_: (0, h // 2)
    sd = jax.ShapeDtypeStruct
    work = 4 * heads * rows * (keys - rows // 2) * HEAD
    return pl.pallas_call(
        functools.partial(bwd_body, r0=r0, bq=bq),
        out_shape=(sd((rows, width), BF16), sd((keys, width), BF16), sd((keys, width), BF16)),
        grid_spec=pltpu.PrefetchScalarGridSpec(
            num_scalar_prefetch=1,
            grid=(heads,),
            in_specs=[
                pl.BlockSpec((1, rows, pair), lambda h, *_: (h, 0, 0)),
                pl.BlockSpec((keys, pair), half),
                pl.BlockSpec((keys, pair), half),
                pl.BlockSpec((rows, pair), half),
                pl.BlockSpec((rows, pair), half),
            ],
            out_specs=[
                pl.BlockSpec((rows, pair), half),
                pl.BlockSpec((keys, pair), half),
                pl.BlockSpec((keys, pair), half),
            ],
            scratch_shapes=[pltpu.VMEM((keys, pair), BF16)] * 2 + [pltpu.VMEM((keys, pair), F32)] * 2,
        ),
        compiler_params=params(),
        cost_estimate=cost(10 * work, 2 * rows * width * 9, work // 256),
        name="attend_bwd",
    )(length, qa, k, v, do, o)


def mlp_body(
    s_ref, xf, mo, mr, pwo, pwr, pb, gain, shift, up, ub, down, db, co, cr,
    mid, second, active, gh, cf, lo, send, gs, sum_ub, sum_db,
    *, r0,
):
    n, length = s_ref[0], s_ref[1]
    i = pl.program_id(0)
    rows, cw = co.shape
    m = xf[...].astype(F32) + (dot(mo[...], pwo[...]) + dot(mr[...], pwr[...])) + pb[...]
    mid[...] = m
    xhat, _ = norm_rows(m)
    sec = (xhat * gain[...] + shift[...]).astype(BF16)
    second[...] = sec
    hid = dot(sec, up[...]) + ub[...]
    sq = hid * hid
    t = jnp.tanh(GELU_A * (hid + GELU_B * (sq * hid)))
    half = 0.5 * (1.0 + t)
    act = (hid * half).astype(BF16)
    active[...] = act
    slope = half + (0.5 * hid) * (1.0 - t * t) * (GELU_A + (3.0 * GELU_A * GELU_B) * sq)
    mine, other = lane_part(n, cw), lane_part(1 - n, cw)
    lo[...] = mid[:, mine] + dot(act, down[:, mine]) + db[:, mine]
    send[...] = dot(act, down[:, other]).astype(BF16)
    pos = r0 + i * rows + lax.broadcasted_iota(jnp.int32, (rows, 1), 0)
    live = (pos < length).astype(F32)
    cf[:, mine] = (co[...].astype(F32) * live).astype(BF16)
    cf[:, other] = (cr[...].astype(F32) * live).astype(BF16)
    cot = cf[...]
    ghid = (dot_nt(cot, down[...]) * slope).astype(BF16)
    gh[...] = ghid
    gs[...] = dot_nt(ghid, up[...]).astype(BF16)
    add_rows(sum_ub, i == 0, ghid.astype(F32))
    add_rows(sum_db, i == 0, cot.astype(F32))


def mlp_call(scal, xf, mo, mr, pwo, pwr, pb, gain, shift, up, ub, down, db, co, cr, r0, block=256):
    rows, lw = mo.shape
    d, f = up.shape
    cw = co.shape[1]
    b0 = r0 // block
    sd = jax.ShapeDtypeStruct
    return pl.pallas_call(
        functools.partial(mlp_body, r0=r0),
        out_shape=(
            sd((rows, d), F32), sd((rows, d), BF16), sd((rows, f), BF16), sd((rows, f), BF16),
            sd((rows, d), BF16), sd((rows, cw), F32), sd((rows, cw), BF16), sd((rows, d), BF16),
            sd((1, f), F32), sd((1, d), F32),
        ),
        grid_spec=pltpu.PrefetchScalarGridSpec(
            num_scalar_prefetch=1,
            grid=(rows // block,),
            in_specs=[rows_spec(block, d, b0), rows_spec(block, lw), rows_spec(block, lw)]
            + [whole_spec(a.shape) for a in (pwo, pwr, pb, gain, shift, up, ub, down, db)]
            + [rows_spec(block, cw, b0), rows_spec(block, cw, b0)],
            out_specs=[
                rows_spec(block, d), rows_spec(block, d), rows_spec(block, f), rows_spec(block, f),
                rows_spec(block, d), rows_spec(block, cw), rows_spec(block, cw), rows_spec(block, d),
                whole_spec((1, f)), whole_spec((1, d)),
            ],
        ),
        compiler_params=params(),
        cost_estimate=cost(2 * rows * d * (d + 4 * f), 2 * (rows * d * 8 + rows * f * 2 + 2 * d * f), rows * f),
        name="mlp",
    )(scal, xf, mo, mr, pwo, pwr, pb, gain, shift, up, ub, down, db, co, cr)


def mid_body(s_ref, go, gr, mid, cf, gain, pwo, low, gm_own, gmix, sum_gain, sum_shift, sum_pb):
    n = s_ref[0]
    i = pl.program_id(0)
    cw = gm_own.shape[1]
    g = go[...].astype(F32) + gr[...].astype(F32)
    xhat, r = norm_rows(mid[...])
    gg = g * gain[...]
    m1 = jnp.mean(gg, axis=-1, keepdims=True)
    m2 = jnp.mean(gg * xhat, axis=-1, keepdims=True)
    gm = cf[...].astype(F32) + r * (gg - m1 - xhat * m2)
    mid[...] = gm
    gm_own[...] = mid[:, lane_part(n, cw)]
    gl = gm.astype(BF16)
    low[...] = gl
    gmix[...] = dot_nt(gl, pwo[...]).astype(BF16)
    add_rows(sum_gain, i == 0, g * xhat)
    add_rows(sum_shift, i == 0, g)
    add_rows(sum_pb, i == 0, gm)


def mid_call(scal, go, gr, mid, cf, gain, pwo, block=256):
    rows, d = mid.shape
    lw = pwo.shape[0]
    cw = d // 2
    sd = jax.ShapeDtypeStruct
    return pl.pallas_call(
        mid_body,
        out_shape=(
            sd((rows, d), BF16), sd((rows, cw), F32), sd((rows, lw), BF16),
            sd((1, d), F32), sd((1, d), F32), sd((1, d), F32),
        ),
        grid_spec=pltpu.PrefetchScalarGridSpec(
            num_scalar_prefetch=1,
            grid=(rows // block,),
            in_specs=[rows_spec(block, d)] * 4 + [whole_spec(gain.shape), whole_spec(pwo.shape)],
            out_specs=[rows_spec(block, d), rows_spec(block, cw), rows_spec(block, lw)] + [whole_spec((1, d))] * 3,
        ),
        compiler_params=params(),
        cost_estimate=cost(2 * rows * d * lw, rows * d * 16),
        name="mid_bwd",
    )(scal, go, gr, mid, cf, gain, pwo)


def part_body(s_ref, dq, dk, dv, w, xf, gain, keep, send, stats, tmp):
    n = s_ref[0]
    cw = keep.shape[1]
    for c in range(2):
        g = dot_nt(dq[...], w[0, c * cw : (c + 1) * cw, :])
        g += dot_nt(dk[...], w[1, c * cw : (c + 1) * cw, :])
        g += dot_nt(dv[...], w[2, c * cw : (c + 1) * cw, :])
        tmp[:, c * cw : (c + 1) * cw] = g
    keep[...] = tmp[:, lane_part(n, cw)]
    send[...] = tmp[:, lane_part(1 - n, cw)].astype(BF16)
    xhat, _ = norm_rows(xf[...].astype(F32))
    gg = tmp[...] * gain[...]
    m1 = jnp.mean(gg, axis=-1, keepdims=True)
    m2 = jnp.mean(gg * xhat, axis=-1, keepdims=True)
    lane = lax.broadcasted_iota(jnp.int32, (1, 128), 1)
    both = jnp.where(lane == 0, m1, jnp.where(lane == 1, m2, 0.0))
    stats[...] = both.T[0:8, :]


def part_call(scal, dq, dk, dv, w, xf, gain, block=256):
    rows, d = xf.shape
    lw = dq.shape[1]
    cw = d // 2
    sd = jax.ShapeDtypeStruct
    return pl.pallas_call(
        part_body,
        out_shape=(sd((rows, cw), F32), sd((rows, cw), BF16), sd((8, rows), F32)),
        grid_spec=pltpu.PrefetchScalarGridSpec(
            num_scalar_prefetch=1,
            grid=(rows // block,),
            in_specs=[rows_spec(block, lw)] * 3 + [whole_spec(w.shape), rows_spec(block, d), whole_spec(gain.shape)],
            out_specs=[
                rows_spec(block, cw), rows_spec(block, cw),
                pl.BlockSpec((8, block), lambda i, *_: (0, i)),
            ],
            scratch_shapes=[pltpu.VMEM((block, d), F32)],
        ),
        compiler_params=params(),
        cost_estimate=cost(6 * rows * d * lw, rows * d * 8),
        name="qkv_bwd",
    )(scal, dq, dk, dv, w, xf, gain)


def in_body(s_ref, keep, got, st_own, st_got, xf, gm, gain, out, sum_gain, sum_shift):
    n = s_ref[0]
    i = pl.program_id(0)
    cw = keep.shape[1]
    x = xf[...].astype(F32)
    mean = jnp.mean(x, axis=-1, keepdims=True)
    cen = x - mean
    r = lax.rsqrt(jnp.mean(cen * cen, axis=-1, keepdims=True) + EPS)
    xhat = (xf[:, lane_part(n, cw)].astype(F32) - mean) * r
    st = (st_own[...] + st_got[...]).T
    g = keep[...] + got[...].astype(F32)
    gg = g * gain[:, lane_part(n, cw)]
    out[...] = (gm[...] + r * (gg - st[:, 0:1] - xhat * st[:, 1:2])).astype(BF16)
    add_rows(sum_gain, i == 0, g * xhat)
    add_rows(sum_shift, i == 0, g)


def in_call(scal, keep, got, st_own, st_got, xf, gm, gain, block=256):
    rows, d = xf.shape
    cw = d // 2
    sd = jax.ShapeDtypeStruct
    stat = pl.BlockSpec((8, block), lambda i, *_: (0, i))
    return pl.pallas_call(
        in_body,
        out_shape=(sd((rows, cw), BF16), sd((1, cw), F32), sd((1, cw), F32)),
        grid_spec=pltpu.PrefetchScalarGridSpec(
            num_scalar_prefetch=1,
            grid=(rows // block,),
            in_specs=[rows_spec(block, cw)] * 2 + [stat, stat, rows_spec(block, d), rows_spec(block, cw), whole_spec(gain.shape)],
            out_specs=[rows_spec(block, cw), whole_spec((1, cw)), whole_spec((1, cw))],
        ),
        compiler_params=params(),
        cost_estimate=cost(rows * d * 16, rows * d * 8),
        name="in_bwd",
    )(scal, keep, got, st_own, st_got, xf, gm, gain)


def bit_of(index, bit):
    return (index // (1 << bit)) % 2


def flip(index, bit):
    return index + (1 - 2 * bit_of(index, bit)) * (1 << bit)


def greet(peers):
    barrier = pltpu.get_barrier_semaphore()
    for peer in peers:
        pl.semaphore_signal(barrier, inc=1, device_id=peer)
    pl.semaphore_wait(barrier, len(peers))


class Chain:
    def __init__(self, order, src, dst, box, part, send_sem, recv_sem, me):
        self.order, self.src, self.dst, self.box, self.part = order, src, dst, box, part
        self.send_sem, self.recv_sem, self.me = send_sem, recv_sem, me
        self.base, self.size, self.at = 0, src.shape[0], 0
        self.copy = None

    def _start(self, step, bit, src, dst):
        self.copy = pltpu.make_async_remote_copy(
            src_ref=src,
            dst_ref=dst,
            send_sem=self.send_sem.at[step],
            recv_sem=self.recv_sem.at[step],
            device_id={"wide": flip(self.me, bit)},
            device_id_type=pl.DeviceIdType.MESH,
        )
        self.copy.start()

    def scatter_start(self, step):
        bit = self.order[step]
        half = self.size // 2
        mine = bit_of(self.me, bit)
        source = self.src if step == 0 else self.part
        self.keep = self.base + mine * half
        give = self.base + (1 - mine) * half
        self._start(step, bit, source.at[pl.ds(give, half)], self.box.at[pl.ds(self.at, half)])

    def scatter_end(self, step):
        half = self.size // 2
        source = self.src if step == 0 else self.part
        target = self.dst if step == len(self.order) - 1 else self.part
        self.copy.wait()

        def add(i, carry):
            got = self.box[self.at + i].astype(F32) + source[self.keep + i].astype(F32)
            target[self.keep + i] = got.astype(BF16)
            return carry

        lax.fori_loop(0, half, add, 0)
        self.at += half
        self.base, self.size = self.keep, half

    def gather_start(self, step):
        bit = self.order[len(self.order) - 1 - step]
        region = self.dst.at[pl.ds(self.base, self.size)]
        self._start(len(self.order) + step, bit, region, region)

    def gather_end(self, step):
        bit = self.order[len(self.order) - 1 - step]
        self.copy.wait()
        self.base = self.base - bit_of(self.me, bit) * self.size
        self.size *= 2


def sum_body(*refs, orders):
    k = len(orders)
    srcs, dsts = refs[:k], refs[k : 2 * k]
    boxes, parts, send_sem, recv_sem = refs[2 * k : 3 * k], refs[3 * k : 4 * k], refs[4 * k], refs[4 * k + 1]
    me = lax.axis_index("wide")
    steps = len(orders[0])
    greet([{"wide": flip(me, bit)} for bit in range(steps)])
    chains = [
        Chain(orders[i], srcs[i], dsts[i], boxes[i], parts[i], send_sem.at[i], recv_sem.at[i], me) for i in range(k)
    ]
    for chain in chains:
        chain.scatter_start(0)
    for step in range(steps):
        for chain in chains:
            chain.scatter_end(step)
            if step + 1 < steps:
                chain.scatter_start(step + 1)
            else:
                chain.gather_start(0)
    for step in range(steps):
        for chain in chains:
            chain.gather_end(step)
            if step + 1 < steps:
                chain.gather_start(step + 1)


def orders_for(wide):
    steps = wide.bit_length() - 1
    first = list(range(steps))
    second = [0] + first[2:] + first[1:2]
    return first, second


def sum_call(arrays, orders, ident):
    steps = len(orders[0])
    vmem = pl.BlockSpec(memory_space=pltpu.VMEM)
    k = len(arrays)
    size = sum(a.size for a in arrays)
    return pl.pallas_call(
        functools.partial(sum_body, orders=orders),
        out_shape=tuple(jax.ShapeDtypeStruct(a.shape, BF16) for a in arrays),
        in_specs=[vmem] * k,
        out_specs=(vmem,) * k,
        scratch_shapes=[pltpu.VMEM(a.shape, BF16) for a in arrays] * 2
        + [pltpu.SemaphoreType.DMA((k, 2 * steps)), pltpu.SemaphoreType.DMA((k, 2 * steps))],
        compiler_params=params(collective_id=ident, has_side_effects=True),
        cost_estimate=cost(size * 2, size * 8),
        name="sum_wide",
    )(*arrays)


def on_device(
    tokens, lengths, qkv_weight, qv_bias, proj_weight, proj_bias, up_weight, up_bias,
    down_weight, down_bias, first_gain, first_shift, second_gain, second_shift, cotangent,
):
    rows, cw = tokens.shape
    n = lax.axis_index("narrow").astype(jnp.int32)
    n1 = n.reshape(1)
    scal = jnp.concatenate([n1, lengths.astype(jnp.int32)])
    swap = lambda a: lax.ppermute(a, "narrow", [(0, 1), (1, 0)])
    row = lambda a: a.astype(F32).reshape(1, -1)
    w3 = jnp.transpose(qkv_weight, (1, 0, 2))
    gain1, shift1, gain2, shift2 = map(row, (first_gain, first_shift, second_gain, second_shift))

    got_tokens = swap(tokens)
    got_cot = swap(cotangent)
    got_proj = swap(proj_weight)
    xf, low, q, k, v = qkv_call(n1, tokens, got_tokens, w3, qv_bias.astype(F32), gain1, shift1)
    mixed, qa = attend_forward(lengths, q, k, v, 0, rows)
    got_mixed = swap(mixed)
    mid, second, active, gh, cf, lo, send, gs, sum_ub, sum_db = mlp_call(
        scal, xf, mixed, got_mixed, proj_weight, got_proj, row(proj_bias), gain2, shift2,
        up_weight, row(up_bias), down_weight, row(down_bias), cotangent, got_cot, 0,
    )
    got_gs = swap(gs)
    layer_out = (lo + swap(send).astype(F32)).astype(BF16)
    grad_down = dot_tn(active, cf)
    grad_up = dot_tn(second, gh)
    mlow, gm_own, gmix, sum_g2, sum_s2, sum_pb = mid_call(n1, gs, got_gs, mid, cf, gain2, proj_weight)
    dq, dk, dv = attend_backward(lengths, qa, k, v, gmix, mixed, 0, rows)
    keep, nsend, stats = part_call(n1, dq, dk, dv, w3, xf, gain1)
    input_grad, sum_g1, sum_s1 = in_call(n1, keep, swap(nsend), stats, swap(stats), xf, gm_own, gain1)
    grad_proj = dot_tn(mixed, mlow)
    grad_qkv = [dot_tn(low, a) for a in (dq, dk, dv)]
    bias_sums = jnp.concatenate([jnp.sum(a.astype(F32), axis=0) for a in (dq, dv)])

    d, ff, lw = 2 * cw, up_weight.shape[1], proj_weight.shape[0]
    wide = lax.axis_size("wide")
    spread = lambda a: lax.dynamic_update_slice(jnp.zeros((d,), F32), a.reshape(-1), (n * cw,))
    both = jnp.concatenate([spread(sum_g1), spread(sum_s1)])
    both = both + swap(both)
    small = jnp.concatenate(
        [both] + [a.reshape(-1) for a in (sum_g2, sum_s2, sum_pb, sum_db, sum_ub, bias_sums)]
    )
    small = jnp.pad(small, (0, -small.shape[0] % (wide * 16 * 128))).reshape(wide, -1, 128).astype(BF16)
    grad_proj = jnp.stack([grad_proj[:, :cw], grad_proj[:, cw:]])
    arrays = [grad_down, grad_up, grad_qkv[0], grad_qkv[1], grad_qkv[2], grad_proj]
    arrays = [a.astype(BF16).reshape(wide, -1, a.shape[-1]) for a in arrays] + [small]
    first, second_order = orders_for(wide)
    orders = [first, second_order, first, second_order, first, first, first]
    sums = sum_call(arrays, orders, 1)
    factor = 1.0 / (lengths.shape[0] * wide)
    fin = lambda a: a.astype(F32) * factor
    s_down, s_up = fin(sums[0]).reshape(-1, d), fin(sums[1]).reshape(-1, ff)
    s_qkv = jnp.stack([fin(a).reshape(-1, lw) for a in sums[2:5]])
    s_proj = fin(sums[5]).reshape(2, lw, cw)
    s_proj = jnp.concatenate([s_proj[0], s_proj[1]], axis=1)
    flat = fin(sums[6]).reshape(-1)
    cuts = [d, d, d, d, d, d, ff, lw, lw]
    pieces, at = [], 0
    for c in cuts:
        pieces.append(flat[at : at + c])
        at += c
    g1, s1, g2, s2, pb, dbs, ubs, qb, vb = pieces
    return (
        layer_out, input_grad, jnp.transpose(s_qkv, (1, 0, 2)), jnp.stack([qb, vb]),
        s_proj, pb, s_up, ubs, s_down, dbs, g1, s1, g2, s2,
    )


def solution(mesh):
    split = P("wide", "narrow")
    none3, cols, rows1 = P(None, None, "narrow"), P(None, "narrow"), P("narrow", None)
    return jax.shard_map(
        on_device,
        mesh=mesh,
        in_specs=(
            split, P("wide"), none3, cols, rows1, P(), cols, P("narrow"), rows1, P(), P(), P(), P(), P(), split,
        ),
        out_specs=(
            split, split, none3, cols, rows1, P(), cols, P("narrow"), rows1, P(), P(), P(), P(), P(),
        ),
        check_vma=False,
    )
```

```python
import functools

import jax
import jax.numpy as jnp
from jax import lax
from jax.experimental import pallas as pl
from jax.experimental.pallas import tpu as pltpu
from jax.sharding import PartitionSpec as P

EPS = 1e-05
HEAD = 64
F32, BF16 = jnp.float32, jnp.bfloat16
NT = (((1,), (1,)), ((), ()))
TN = (((0,), (0,)), ((), ()))
GELU_A, GELU_B = 0.7978845608028654, 0.044715
VMEM_LIMIT = 63 * 1024 * 1024


def dot(a, b):
    return jnp.dot(a, b, preferred_element_type=F32)


def dot_nt(a, b):
    return lax.dot_general(a, b, NT, preferred_element_type=F32)


def dot_tn(a, b):
    return lax.dot_general(a, b, TN, preferred_element_type=F32)


def params(**more):
    return pltpu.CompilerParams(vmem_limit_bytes=VMEM_LIMIT, **more)


def cost(flops, size, trans=0):
    return pl.CostEstimate(flops=int(flops), bytes_accessed=int(size), transcendentals=int(trans))


def lane_part(which, width):
    return pl.ds(pl.multiple_of(which * width, 128), width)


def norm_rows(x):
    mean = jnp.mean(x, axis=-1, keepdims=True)
    cen = x - mean
    var = jnp.mean(cen * cen, axis=-1, keepdims=True)
    r = lax.rsqrt(var + EPS)
    return cen * r, r


def rows_spec(rows, cols, base=0):
    return pl.BlockSpec((rows, cols), lambda i, *_: (i + base, 0))


def whole_spec(shape):
    zeros = (0,) * len(shape)
    return pl.BlockSpec(shape, lambda i, *_: zeros)


MESH = pl.DeviceIdType.MESH


def bit_of(index, bit):
    return (index // (1 << bit)) % 2


def flip(index, bit):
    return index + (1 - 2 * bit_of(index, bit)) * (1 << bit)


def greet(peers):
    barrier = pltpu.get_barrier_semaphore()
    for peer in peers:
        pl.semaphore_signal(barrier, inc=1, device_id=peer, device_id_type=MESH)
    pl.semaphore_wait(barrier, len(peers))


def remote(src, dst, sems, at, peer):
    return pltpu.make_async_remote_copy(
        src_ref=src, dst_ref=dst, send_sem=sems[0].at[at], recv_sem=sems[1].at[at],
        device_id=peer, device_id_type=MESH,
    )


def block_rows(start, size, unit=16):
    return pl.ds(start if isinstance(start, int) else pl.multiple_of(start, unit), size)


class Chain:
    def __init__(self, me, order, rows):
        self.me, self.steps, self.splits = me, [], []
        base, size, box = 0, rows, 0
        for bit in order:
            if size % 32 == 0:
                half = size // 2
                mine = bit_of(me, bit)
                keep, give = base + mine * half, base + (1 - mine) * half
                self.splits.append((bit, base, keep, half))
            else:
                half, keep, give = size, base, base
            self.steps.append((bit, keep, give, half, box))
            base, size, box = keep, half, box + half
        self.base, self.size, self.box_rows = base, size, box
        self.first = self.steps[0][1]

    def scatter(self, src, box, part, own, sems, at, cols):
        self.src, self.box, self.part, self.own = src, box, part, own
        self.sems, self.at, self.cols = sems, at, cols
        return self

    def _source(self, step):
        if step == 0:
            return self.src, 0
        return self.part, self.first

    def _scatter_copy(self, step):
        bit, _, give, half, box = self.steps[step]
        source, off = self._source(step)
        return remote(
            source.at[block_rows(give - off, half), self.cols],
            self.box.at[pl.ds(box, half), self.cols],
            self.sems, self.at + step, {"wide": flip(self.me, bit)},
        )

    def scatter_start(self, step):
        self._scatter_copy(step).start()

    def scatter_end(self, step):
        self._scatter_copy(step).wait()
        _, keep, _, half, box = self.steps[step]
        source, off = self._source(step)
        last = step == len(self.steps) - 1
        target, out = (self.own, keep) if last else (self.part, self.first)
        unit = next(u for u in (96, 64, 48, 32, 16) if half % u == 0)

        def add(i, carry):
            at = i * unit
            got = self.box[block_rows(box + at, unit), self.cols].astype(F32)
            mine = source[block_rows(keep - off + at, unit), self.cols].astype(F32)
            target[block_rows(keep - out + at, unit), self.cols] = (got + mine).astype(BF16)
            return carry

        lax.fori_loop(0, half // unit, add, 0)

    def gather(self, own, dst, sems, at, cols):
        self.own, self.dst, self.gsems, self.gat, self.gcols = own, dst, sems, at, cols
        return self

    def gather_open(self):
        self.dst[block_rows(self.base, self.size), self.gcols] = self.own[:, self.gcols]

    def gather_copy_open(self, sem, at):
        region = self.dst.at[block_rows(self.base, self.size), self.gcols]
        return pltpu.make_async_copy(self.own.at[:, self.gcols], region, sem.at[at])

    def _gather_copy(self, step):
        bit, _, keep, half = self.splits[len(self.splits) - 1 - step]
        region = self.dst.at[block_rows(keep, half), self.gcols]
        return remote(region, region, self.gsems, self.gat + step, {"wide": flip(self.me, bit)})

    def gather_start(self, step):
        if step < len(self.splits):
            self._gather_copy(step).start()

    def gather_end(self, step):
        if step < len(self.splits):
            self._gather_copy(step).wait()


def bits(wide):
    return wide.bit_length() - 1


def order_of(wide, kind):
    steps = list(range(bits(wide)))
    return steps if kind == 0 else [0] + steps[2:] + steps[1:2]


def thirds(cols):
    w = cols // 3
    return [(0, pl.ds(0, w)), (0, pl.ds(w, w)), (1, pl.ds(2 * w, w))]


def wide_peers(me, wide):
    return [{"wide": flip(me, b)} for b in range(bits(wide))]


def vmem():
    return pl.BlockSpec(memory_space=pltpu.VMEM)


def anywhere():
    return pl.BlockSpec(memory_space=pl.ANY)


def sems(*counts):
    return [pltpu.SemaphoreType.DMA((c,)) for c in counts]


def qkv_body(own_hbm, own, w, bias, gain, shift, xf, low, q, k, v, got, send_sem, recv_sem):
    n = lax.axis_index("narrow")
    i = pl.program_id(0)
    rows, cw = own.shape
    peer = {"narrow": 1 - n}

    def copy(at):
        block = block_rows(at * rows, rows)
        return remote(own_hbm.at[block], got.at[block], (send_sem, recv_sem), at, peer)

    @pl.when(i == 0)
    def _():
        greet([peer])
        for at in range(got.shape[0] // rows):
            copy(at).start()

    xf[:, lane_part(n, cw)] = own[...]
    copy(i).wait()
    xf[:, lane_part(1 - n, cw)] = got[block_rows(i * rows, rows), :]
    xhat, _ = norm_rows(xf[...].astype(F32))
    y = (xhat * gain[...] + shift[...]).astype(BF16)
    low[...] = y
    q[...] = (dot(y, w[0]) + bias[0:1, :]).astype(BF16) * jnp.asarray(HEAD**-0.5, BF16)
    k[...] = dot(y, w[1]).astype(BF16)
    v[...] = (dot(y, w[2]) + bias[1:2, :]).astype(BF16)


def qkv_call(own, w, bias, gain, shift, block=256):
    rows, cw = own.shape
    d, lw = w.shape[1], w.shape[2]
    sd = jax.ShapeDtypeStruct
    return pl.pallas_call(
        qkv_body,
        out_shape=(sd((rows, d), BF16), sd((rows, d), BF16)) + (sd((rows, lw), BF16),) * 3,
        grid_spec=pltpu.PrefetchScalarGridSpec(
            num_scalar_prefetch=0,
            grid=(rows // block,),
            in_specs=[anywhere(), rows_spec(block, cw)] + [whole_spec(a.shape) for a in (w, bias, gain, shift)],
            out_specs=[rows_spec(block, d)] * 2 + [rows_spec(block, lw)] * 3,
            scratch_shapes=[pltpu.VMEM((rows, cw), BF16)] + sems(rows // block, rows // block),
        ),
        compiler_params=params(collective_id=1, has_side_effects=True),
        cost_estimate=cost(2 * rows * d * 3 * lw, 2 * (rows * d * 5 + w.size)),
        name="norm_qkv",
    )(own, own, w, bias, gain, shift)


def three(x):
    hi = x.astype(BF16).astype(F32)
    mid = (x - hi).astype(BF16).astype(F32)
    return hi, mid, x - hi - mid


def lanes_of(par):
    lane = lax.broadcasted_iota(jnp.int32, (1, 2 * HEAD), 1)
    mine = (lane // HEAD) == par
    return lane, mine, (1 - par) * HEAD


def place(lane, mine, at, base, terms):
    out = jnp.where(mine, base, 0.0)
    for i, term in enumerate(terms):
        out = jnp.where(lane == at + i, term, out)
    return out


def fwd_body(
    len_ref, q, k, v, pw, o, qa_out, o_got, pw_got, ka, va, send_sem, recv_sem, *, bq
):
    head = pl.program_id(0)
    par, pair = head % 2, head // 2
    lane, mine, at = lanes_of(par)
    n, me = lax.axis_index("narrow"), lax.axis_index("wide")
    peer, core = {"narrow": 1 - n}, {"wide": flip(me, 0)}
    pairs = pl.num_programs(0) // 2
    both = (send_sem, recv_sem)
    cols = lane_part(pair, 2 * HEAD)
    part = block_rows((me % 2) * (pw.shape[0] // 2), pw.shape[0] // 2)
    npairs = o.shape[1] // (2 * HEAD)
    weights = remote(pw.at[part], pw_got.at[part], both, npairs, peer)
    shared = remote(pw_got.at[part], pw_got.at[part], both, npairs + 1, core)

    @pl.when(head == 0)
    def _():
        greet([peer, core])
        weights.start()

    keys = k.shape[0]
    kpos = lax.broadcasted_iota(jnp.int32, (keys, 1), 0)
    kbias = jnp.where(kpos < len_ref[0], 0.0, -1e30)
    ka[...] = place(lane, mine, at, k[...].astype(F32), [kbias]).astype(BF16)
    va[...] = place(lane, mine, at, v[...].astype(F32), [1.0]).astype(BF16)
    tri = lax.broadcasted_iota(jnp.int32, (bq, bq), 1) <= lax.broadcasted_iota(jnp.int32, (bq, bq), 0)
    for i in range(q.shape[0] // bq):
        nk = (i + 1) * bq
        rows = pl.ds(i * bq, bq)
        qf = q[rows, :].astype(F32)
        qa = place(lane, mine, at, qf, [1.0])
        s = dot_nt(qa.astype(BF16), ka[0:nk, :])
        edge = jnp.where(tri, s[:, nk - bq :], -1e30)
        m = jnp.max(edge, axis=1, keepdims=True)
        if nk > bq:
            m = jnp.maximum(m, jnp.max(s[:, : nk - bq], axis=1, keepdims=True))
        pv = dot(jnp.exp(edge - m).astype(BF16), va[nk - bq : nk, :])
        if nk > bq:
            pv += dot(jnp.exp(s[:, : nk - bq] - m).astype(BF16), va[0 : nk - bq, :])
        total = jnp.sum(jnp.where(lane == at, pv, 0.0), axis=1, keepdims=True)
        out = (pv / total).astype(BF16).astype(F32)
        old = o[rows, cols].astype(F32)
        o[rows, cols] = jnp.where(mine, out, jnp.where(par == 0, 0.0, old)).astype(BF16)
        lse = m + jnp.log(total)
        qa_out[0, rows, :] = place(lane, mine, at, qf, [1.0, *three(lse)]).astype(BF16)

    def mixed(j):
        c = pl.ds(j * 2 * HEAD, 2 * HEAD)
        return remote(o.at[:, c], o_got.at[:, c], both, j, peer)

    for j in range(npairs):

        @pl.when(head == 2 * j + 1)
        def _():
            mixed(j).start()

    @pl.when(head == 3)
    def _():
        weights.wait()
        shared.start()

    @pl.when(head == 2 * npairs - 1)
    def _():
        shared.wait()
        for j in range(npairs):
            mixed(j).wait()


def attend_forward(length, q, k, v, pw, bq=256):
    rows, width = q.shape
    heads, pair = width // HEAD, 2 * HEAD
    half = lambda h, *_: (0, h // 2)
    sd = jax.ShapeDtypeStruct
    work = 2 * heads * rows * rows * HEAD
    return pl.pallas_call(
        functools.partial(fwd_body, bq=bq),
        out_shape=(
            sd((rows, width), BF16), sd((heads, rows, pair), BF16), sd((rows, width), BF16), sd(pw.shape, BF16),
        ),
        grid_spec=pltpu.PrefetchScalarGridSpec(
            num_scalar_prefetch=1,
            grid=(heads,),
            in_specs=[pl.BlockSpec((rows, pair), half)] * 3 + [anywhere()],
            out_specs=[vmem(), pl.BlockSpec((1, rows, pair), lambda h, *_: (h, 0, 0)), anywhere(), anywhere()],
            scratch_shapes=[pltpu.VMEM((rows, pair), BF16)] * 2 + sems(heads // 2 + 2, heads // 2 + 2),
        ),
        compiler_params=params(collective_id=2, has_side_effects=True),
        cost_estimate=cost(4 * work, 2 * rows * width * 6, work // 256),
        name="attend_fwd",
    )(length, q, k, v, pw)


def mlp_body(
    len_ref, xf, mo, mr, pwo, pwr, pb, gain, shift, ub, db, up_hbm, down_hbm, cot,
    lo, lo_send, gmix, gm, gup, down_own, gp_own, gp_other, sum_ub, sum_db, sum_g, sum_s, sum_pb,
    up, down, cot_got, cf, mid, second, active, slope, gh, gs_send, gs_got, gs_own, gdown, box, part,
    glow, gmix_send, load_sem, nsend, nrecv, wsend, wrecv,
    *, wide,
):
    n, me = lax.axis_index("narrow"), lax.axis_index("wide")
    peer = {"narrow": 1 - n}
    rows, cw = cot.shape
    d, f = up.shape
    half, block = rows // 2, min(256, rows // 2)
    each = half // block
    mine, other = lane_part(n, cw), lane_part(1 - n, cw)
    narrow, across = (nsend, nrecv), (wsend, wrecv)
    loads = [
        pltpu.make_async_copy(up_hbm, up, load_sem.at[0]),
        pltpu.make_async_copy(down_hbm, down, load_sem.at[1]),
    ]
    for load in loads:
        load.start()
    greet([peer] + wide_peers(me, wide))

    def cot_copy(side, j):
        r = block_rows(side * half + j * block, block)
        return (cot.at[r], cot_got.at[r])

    for a, side in enumerate((n, 1 - n)):
        for j in range(each):
            src, dst = cot_copy(side, j)
            remote(src, dst, narrow, a * each + j, peer).start()

    def forward(i, carry):
        r = block_rows(i * block, block)
        m = xf[r, :].astype(F32) + (dot(mo[r, :], pwo[...]) + dot(mr[r, :], pwr[...])) + pb[...]
        mid[r, :] = m
        xhat, _ = norm_rows(m)
        sec = (xhat * gain[...] + shift[...]).astype(BF16)
        second[r, :] = sec
        hid = dot(sec, up[...]) + ub[...]
        sq = hid * hid
        t = jnp.tanh(GELU_A * (hid + GELU_B * (sq * hid)))
        hf = 0.5 * (1.0 + t)
        act = (hid * hf).astype(BF16)
        active[r, :] = act
        slope[r, :] = hf + (0.5 * hid) * (1.0 - t * t) * (GELU_A + (3.0 * GELU_A * GELU_B) * sq)
        lo[r, :] = mid[r, mine] + dot(act, down[:, mine]) + db[:, mine]
        lo_send[r, :] = dot(act, down[:, other]).astype(BF16)
        return carry

    for load in loads:
        load.wait()
    lax.fori_loop(0, rows // block, forward, 0)

    def backward(side, j, a):
        src, dst = cot_copy(side, j)
        remote(src, dst, narrow, a * each + j, peer).wait()
        at = side * half + j * block
        r = block_rows(at, block)
        pos = at + lax.broadcasted_iota(jnp.int32, (block, 1), 0)
        live = (pos < len_ref[0]).astype(F32)
        cf[r, mine] = (cot[r, :].astype(F32) * live).astype(BF16)
        cf[r, other] = (cot_got[r, :].astype(F32) * live).astype(BF16)
        ghid = (dot_nt(cf[r, :], down[...]) * slope[r, :]).astype(BF16)
        gh[r, :] = ghid
        return dot_nt(ghid, up[...]), ghid

    def gs_copy(j):
        r = pl.ds(j * block, block)
        return remote(gs_send.at[r], gs_got.at[r], narrow, 2 * each + j, peer)

    sum_ub[...] = jnp.zeros_like(sum_ub)

    def for_peer(j, carry):
        g, ghid = backward(1 - n, j, 0)
        r = block_rows(j * block, block)
        gs_send[r, :] = g.astype(BF16)
        remote(gs_send.at[r], gs_got.at[r], narrow, 2 * each + j, peer).start()
        sum_ub[...] += jnp.sum(ghid.astype(F32), axis=0, keepdims=True)
        return carry

    def for_own(j, carry):
        g, ghid = backward(n, j, 1)
        gs_own[block_rows(j * block, block), :] = g
        sum_ub[...] += jnp.sum(ghid.astype(F32), axis=0, keepdims=True)
        return carry

    lax.fori_loop(0, each, for_peer, 0)
    lax.fori_loop(0, each, for_own, 0)

    chains = []
    for a, (kind, cols) in enumerate(thirds(d)):
        chain = Chain(me, order_of(wide, kind), f)
        chains.append(chain.scatter(gdown, box, part, down_own, across, a * bits(wide), cols))

    def weight_down(i, carry):
        c = block_rows(i * 256, 256, 256)
        gdown[c, :] = dot_tn(active[:, c], cf[...]).astype(BF16)
        return carry

    def weight_up(i, carry):
        c = block_rows(i * 256, 256, 256)
        gup[c, :] = dot_tn(second[:, c], gh[...]).astype(BF16)
        return carry

    lax.fori_loop(0, f // 256, weight_down, 0)
    for chain in chains:
        chain.scatter_start(0)
    lax.fori_loop(0, d // 256, weight_up, 0)

    def advance(step):
        for chain in chains:
            chain.scatter_end(step)
            if step + 1 < bits(wide):
                chain.scatter_start(step + 1)

    advance(0)
    for j in range(each):
        gs_copy(j).wait()
    for ref in (sum_g, sum_s, sum_pb, sum_db):
        ref[...] = jnp.zeros_like(ref)

    def gmix_copy(j):
        r = block_rows(n * half + j * block, block)
        return remote(gmix_send.at[block_rows(j * block, block)], gmix.at[r], narrow, 3 * each + j, peer)

    def back_norm(j, carry):
        r, rh = block_rows(n * half + j * block, block), block_rows(j * block, block)
        g = gs_own[rh, :] + gs_got[rh, :].astype(F32)
        xhat, scale = norm_rows(mid[r, :])
        gg = g * gain[...]
        m1 = jnp.mean(gg, axis=-1, keepdims=True)
        m2 = jnp.mean(gg * xhat, axis=-1, keepdims=True)
        c = cf[r, :].astype(F32)
        grad = c + scale * (gg - m1 - xhat * m2)
        gm[rh, :] = grad
        gl = grad.astype(BF16)
        glow[rh, :] = gl
        gmix_send[rh, :] = dot_nt(gl, pwr[...]).astype(BF16)
        gmix_copy(j).start()
        gmix[r, :] = dot_nt(gl, pwo[...]).astype(BF16)
        sum_g[...] += jnp.sum(g * xhat, axis=0, keepdims=True)
        sum_s[...] += jnp.sum(g, axis=0, keepdims=True)
        sum_pb[...] += jnp.sum(grad, axis=0, keepdims=True)
        sum_db[...] += jnp.sum(c, axis=0, keepdims=True)
        return carry

    lax.fori_loop(0, each, back_norm, 0)
    for step in range(1, bits(wide)):
        advance(step)
        if step == 1:
            own_rows = block_rows(n * half, half)
            lw = mo.shape[1]
            for src, dst in ((mo, gp_own), (mr, gp_other)):
                total = dot_tn(src[own_rows, :], glow[...]).astype(BF16)
                dst[0:lw, :] = total[:, :cw]
                dst[lw : 2 * lw, :] = total[:, cw:]

    def received(j):
        r = block_rows((1 - n) * half + j * block, block)
        return remote(gmix_send.at[block_rows(j * block, block)], gmix.at[r], narrow, 3 * each + j, peer)

    for j in range(each):
        gmix_copy(j).wait()


def mlp_call(length, xf, mo, mr, pwo, pwr, pb, gain, shift, up, ub, down, db, cot, wide):
    rows, d = xf.shape
    f, lw, cw = up.shape[1], mo.shape[1], cot.shape[1]
    half = rows // 2
    chain = Chain(0, order_of(wide, 0), f)
    sd, vm = jax.ShapeDtypeStruct, pltpu.VMEM
    each = half // min(256, half)
    return pl.pallas_call(
        functools.partial(mlp_body, wide=wide),
        out_shape=(
            sd((rows, cw), F32), sd((rows, cw), BF16), sd((rows, lw), BF16), sd((half, d), F32),
            sd((d, f), BF16), sd((chain.size, d), BF16), sd((2 * lw, cw), BF16), sd((2 * lw, cw), BF16),
            sd((1, f), F32), sd((1, d), F32), sd((1, d), F32), sd((1, d), F32), sd((1, d), F32),
        ),
        in_specs=[pl.BlockSpec(memory_space=pltpu.SMEM)] + [vmem()] * 10 + [anywhere(), anywhere(), vmem()],
        out_specs=(vmem(),) * 13,
        scratch_shapes=[
            vm((d, f), BF16), vm((f, d), BF16), vm((rows, cw), BF16), vm((rows, d), BF16), vm((rows, d), F32),
            vm((rows, d), BF16), vm((rows, f), BF16), vm((rows, f), F32), vm((rows, f), BF16),
            vm((half, d), BF16), vm((half, d), BF16), vm((half, d), F32), vm((f, d), BF16),
            vm((chain.box_rows, d), BF16), vm((f // 2, d), BF16), vm((half, d), BF16), vm((half, lw), BF16),
        ]
        + sems(2, 4 * each, 4 * each, 3 * bits(wide), 3 * bits(wide)),
        compiler_params=params(collective_id=3, has_side_effects=True),
        cost_estimate=cost(2 * rows * d * (d + 6 * f), 2 * (rows * d * 8 + 2 * d * f), rows * f),
        name="mlp",
    )(length, xf, mo, mr, pwo, pwr, pb, gain, shift, ub, db, up, down, cot)


def bwd_body(
    len_ref, qa, k, v, do, o, lo_send, gup, down_own, gp_own, gp_other,
    dq, dk, dv, lo_got, gdown, up_own, gp_sum,
    ka, va, dk_acc, dv_acc, up_box, up_part, own_box, own_part, other_box, other_part,
    own_shard, other_shard, peer_shard, open_sem, nsend, nrecv, wsend, wrecv, *, bq, wide,
):
    head = pl.program_id(0)
    heads = 2 * (lo_got.shape[1] // (2 * HEAD))
    n, me = lax.axis_index("narrow"), lax.axis_index("wide")
    peer = {"narrow": 1 - n}
    narrow, across = (nsend, nrecv), (wsend, wrecv)
    steps = bits(wide)
    scatters, gathers = [], []
    for a, (kind, cols) in enumerate(thirds(gup.shape[1])):
        chain = Chain(me, order_of(wide, kind), gup.shape[0])
        scatters.append(chain.scatter(gup, up_box, up_part, up_own, across, a * steps, cols))
    cw = gp_own.shape[1]
    for a, (src, box, part, own) in enumerate(
        ((gp_own, own_box, own_part, own_shard), (gp_other, other_box, other_part, other_shard))
    ):
        chain = Chain(me, order_of(wide, 0), gp_own.shape[0])
        scatters.append(chain.scatter(src, box, part, own, across, (3 + a) * steps, pl.ds(0, cw)))
    for a, (kind, cols) in enumerate(thirds(gdown.shape[1])):
        chain = Chain(me, order_of(wide, kind), gdown.shape[0])
        gathers.append(chain.gather(down_own, gdown, across, (5 + a) * steps, cols))
    layer = remote(lo_send, lo_got, narrow, 0, peer)
    shard = remote(other_shard, peer_shard, narrow, 1, peer)

    @pl.when(head == 0)
    def _():
        greet([peer] + wide_peers(me, wide))
        layer.start()
        for chain in scatters:
            chain.scatter_start(0)
        opens = [chain.gather_copy_open(open_sem, a) for a, chain in enumerate(gathers)]
        for opened in opens:
            opened.start()
        for opened, chain in zip(opens, gathers):
            opened.wait()
            chain.gather_start(0)

    par = head % 2
    lane, mine, at = lanes_of(par)
    keys = k.shape[0]
    kpos = lax.broadcasted_iota(jnp.int32, (keys, 1), 0)
    kbias = jnp.where(kpos < len_ref[0], 0.0, -1e30)
    ka[...] = place(lane, mine, at, k[...].astype(F32), [kbias, -1.0, -1.0, -1.0]).astype(BF16)
    va[...] = place(lane, mine, at, v[...].astype(F32), [-1.0, -1.0, -1.0]).astype(BF16)
    dk_acc[...] = jnp.zeros_like(dk_acc)
    dv_acc[...] = jnp.zeros_like(dv_acc)
    tri = lax.broadcasted_iota(jnp.int32, (bq, bq), 0) <= lax.broadcasted_iota(jnp.int32, (bq, bq), 1)

    def put(ref, rows, new):
        old = ref[rows, :].astype(F32)
        ref[rows, :] = jnp.where(mine, new, jnp.where(par == 0, 0.0, old)).astype(BF16)

    for i in range(qa.shape[1] // bq):
        rows = pl.ds(i * bq, bq)
        qb = qa[0, rows, :]
        df = do[rows, :].astype(F32)
        delta = jnp.sum(jnp.where(mine, df * o[rows, :].astype(F32), 0.0), axis=1, keepdims=True)
        db = place(lane, mine, at, df, three(delta)).astype(BF16)
        dqs = None
        for j in range(i + 1):
            cols = pl.ds(j * bq, bq)
            kb, vb = ka[cols, :], va[cols, :]
            s = dot_nt(kb, qb)
            if j == i:
                s = jnp.where(tri, s, -1e30)
            p = jnp.exp(s)
            ds = (p * dot_nt(vb, db)).astype(BF16)
            dv_acc[cols, :] += dot(p.astype(BF16), db)
            dk_acc[cols, :] += dot(ds, qb)
            part = dot_tn(ds, kb)
            dqs = part if dqs is None else dqs + part
        put(dq, rows, dqs * HEAD**-0.5)
    put(dk, pl.ds(0, keys), dk_acc[...])
    put(dv, pl.ds(0, keys), dv_acc[...])

    def advance(step):
        for chain in scatters:
            chain.scatter_end(step)
            if step + 1 < steps:
                chain.scatter_start(step + 1)
        for chain in gathers:
            chain.gather_end(step)
            chain.gather_start(step + 1)
        if step == steps - 1:
            shard.start()

    for step in range(steps):

        @pl.when(head == min(heads - 1, (step * heads) // steps + (1 if step else 0)))
        def _():
            advance(step)

    @pl.when(head == heads - 1)
    def _():
        shard.wait()
        gp_sum[...] = (own_shard[...].astype(F32) + peer_shard[...].astype(F32)).astype(BF16)
        layer.wait()


def attend_backward(length, qa, k, v, do, o, lo_send, gup, down_own, gp_own, gp_other, wide, bq=256):
    rows, width = k.shape
    heads, pair = width // HEAD, 2 * HEAD
    half = lambda h, *_: (0, h // 2)
    sd, vm = jax.ShapeDtypeStruct, pltpu.VMEM
    work = 2 * heads * rows * rows * HEAD
    d, f = gup.shape
    up_chain = Chain(0, order_of(wide, 0), d)
    gp_rows, cw = gp_own.shape
    gp_chain = Chain(0, order_of(wide, 0), gp_rows)
    pairs = [pl.BlockSpec((rows, pair), half)]
    steps = bits(wide)
    return pl.pallas_call(
        functools.partial(bwd_body, bq=bq, wide=wide),
        out_shape=(
            (sd((rows, width), BF16),) * 3
            + (sd(lo_send.shape, BF16), sd((f, d), BF16), sd((up_chain.size, f), BF16), sd((gp_chain.size, cw), BF16))
        ),
        grid_spec=pltpu.PrefetchScalarGridSpec(
            num_scalar_prefetch=1,
            grid=(heads,),
            in_specs=[pl.BlockSpec((1, rows, pair), lambda h, *_: (h, 0, 0))] + pairs * 4 + [vmem()] * 5,
            out_specs=pairs * 3 + [anywhere()] * 2 + [vmem()] * 2,
            scratch_shapes=[vm((rows, pair), BF16)] * 2 + [vm((rows, pair), F32)] * 2
            + [vm((up_chain.box_rows, f), BF16), vm((d // 2, f), BF16)]
            + [vm((gp_chain.box_rows, cw), BF16), vm((gp_rows // 2, cw), BF16)] * 2
            + [vm((gp_chain.size, cw), BF16)] * 3
            + sems(3, 2, 2, 8 * steps, 8 * steps),
        ),
        compiler_params=params(collective_id=4, has_side_effects=True),
        cost_estimate=cost(10 * work, 2 * rows * width * 9, work // 256),
        name="attend_bwd",
    )(length, qa, k, v, do, o, lo_send, gup, down_own, gp_own, gp_other)


def last_body(
    dq, dk, dv, low_hbm, w_hbm, xf_hbm, gm, gain, up_own, gp_sum, s_ub, s_db, s_g2, s_s2, s_pb,
    ig, gup, gp, gq, gk, gv, small,
    low, w, xf, gn_send, gn_got, gn_own, ig_own, ig_send, src, box, part, own, vec, vec_box,
    load_sem, nsend, nrecv, wsend, wrecv, *, wide,
):
    n, me = lax.axis_index("narrow"), lax.axis_index("wide")
    peer = {"narrow": 1 - n}
    narrow, across = (nsend, nrecv), (wsend, wrecv)
    steps = bits(wide)
    rows, lw = dq.shape
    d = gain.shape[1]
    cw = d // 2
    half, block = rows // 2, min(256, rows // 2)
    each = half // block
    loads = [
        pltpu.make_async_copy(a, b, load_sem.at[i])
        for i, (a, b) in enumerate(((low_hbm, low), (w_hbm, w), (xf_hbm, xf)))
    ]
    for load in loads:
        load.start()
    greet([peer] + wide_peers(me, wide))
    gathers = []
    for a, (kind, cols) in enumerate(thirds(gup.shape[1])):
        chain = Chain(me, order_of(wide, kind), gup.shape[0])
        gathers.append(chain.gather(up_own, gup, across, a * steps, cols))
    chain = Chain(me, order_of(wide, 0), gp.shape[0])
    gathers.append(chain.gather(gp_sum, gp, across, 3 * steps, pl.ds(0, cw)))
    for chain in gathers:
        chain.gather_open()
        chain.gather_start(0)

    grads, outs = (dq, dk, dv), (gq, gk, gv)
    scatters = []
    for c in range(3):
        chain = Chain(me, order_of(wide, 1 if c == 1 else 0), d)
        chain.scatter(src.at[c], box.at[c], part.at[c], own.at[c], across, (4 + c) * steps, pl.ds(0, lw))
        scatters.append(chain.gather(own.at[c], outs[c], across, (7 + c) * steps, pl.ds(0, lw)))

    def scatter_step(step):
        for chain in scatters:
            chain.scatter_end(step)
            if step + 1 < steps:
                chain.scatter_start(step + 1)
            else:
                chain.gather_open()
                chain.gather_start(0)

    def gather_step(chains, step):
        for chain in chains:
            chain.gather_end(step)
            chain.gather_start(step + 1)

    loads[0].wait()
    for c in range(3):
        src[c] = dot_tn(low[...], grads[c][...]).astype(BF16)
        scatters[c].scatter_start(0)
    gather_step(gathers, 0)
    loads[1].wait()

    def gn_part(at, cols):
        r = block_rows(at, block)
        total = dot_nt(dq[r, :], w[0, cols, :])
        total += dot_nt(dk[r, :], w[1, cols, :])
        return total + dot_nt(dv[r, :], w[2, cols, :])

    def gn_copy(j):
        r = pl.ds(j * block, block)
        return remote(gn_send.at[r], gn_got.at[r], narrow, j, peer)

    for j in range(each):
        at = (1 - n) * half + j * block
        for c in range(2):
            cols = slice(c * cw, (c + 1) * cw)
            gn_send[j * block : (j + 1) * block, cols] = gn_part(at, cols).astype(BF16)
        gn_copy(j).start()
    scatter_step(0)
    for j in range(each):
        at = n * half + j * block
        for c in range(2):
            cols = slice(c * cw, (c + 1) * cw)
            gn_own[j * block : (j + 1) * block, cols] = gn_part(at, cols)
    gather_step(gathers, 1)
    loads[2].wait()

    vec[...] = jnp.zeros_like(vec)

    def put(at, value):
        for i in range(value.shape[1] // 128):
            vec[at + i : at + i + 1, :] = value[:, i * 128 : (i + 1) * 128]

    dr, fr, lr = d // 128, s_ub.shape[1] // 128, lw // 128
    shared = -(-6 * dr // 8) * 8
    put(2 * dr, s_g2[...])
    put(3 * dr, s_s2[...])
    put(4 * dr, s_pb[...])
    put(5 * dr, s_db[...])
    put(shared, s_ub[...])
    put(shared + fr, jnp.sum(dq[...].astype(F32), axis=0, keepdims=True))
    put(shared + fr + lr, jnp.sum(dv[...].astype(F32), axis=0, keepdims=True))

    mine, other = lane_part(n, cw), lane_part(1 - n, cw)
    g1 = s1 = 0.0

    def ig_copy(j):
        r = block_rows(n * half + j * block, block)
        return remote(ig_send.at[pl.ds(j * block, block)], ig.at[r], narrow, each + j, peer)

    for j in range(each):
        gn_copy(j).wait()
        rh = pl.ds(j * block, block)
        r = block_rows(n * half + j * block, block)
        g = gn_own[rh, :] + gn_got[rh, :].astype(F32)
        xhat, scale = norm_rows(xf[r, :].astype(F32))
        gg = g * gain[...]
        m1 = jnp.mean(gg, axis=-1, keepdims=True)
        m2 = jnp.mean(gg * xhat, axis=-1, keepdims=True)
        ig_own[...] = gm[rh, :] + scale * (gg - m1 - xhat * m2)
        ig_send[rh, :] = ig_own[:, other].astype(BF16)
        ig_copy(j).start()
        ig[r, :] = ig_own[:, mine].astype(BF16)
        g1 += jnp.sum(g * xhat, axis=0, keepdims=True)
        s1 += jnp.sum(g, axis=0, keepdims=True)
    put(0, g1)
    put(dr, s1)

    def vec_copy(step):
        if step == 0:
            top = pl.ds(0, shared)
            return remote(vec.at[top], vec_box.at[0, top], narrow, 2 * each, peer)
        return remote(vec, vec_box.at[step], across, 10 * steps + step - 1, {"wide": flip(me, step - 1)})

    def vec_end(step):
        vec_copy(step).wait()
        if step == 0:
            vec[0:shared, :] += vec_box[0, 0:shared, :]
        else:
            vec[...] += vec_box[step]
        if step < steps:
            vec_copy(step + 1).start()

    vec_copy(0).start()
    for step in range(1, steps):
        scatter_step(step)
        vec_end(step - 1)
    for step in range(2, steps):
        gather_step(gathers, step)
    vec_end(steps - 1)
    for step in range(steps):
        gather_step(scatters, step)
    vec_end(steps)
    small[...] = vec[...]
    for j in range(each):
        ig_copy(j).wait()


def last_call(dq, dk, dv, low, w, xf, gm, gain, up_own, gp_sum, s_ub, s_db, s_g2, s_s2, s_pb, wide):
    rows, lw = dq.shape
    d, f = xf.shape[1], s_ub.shape[1]
    cw, half = d // 2, rows // 2
    block = min(256, half)
    each, steps = half // block, bits(wide)
    sd, vm = jax.ShapeDtypeStruct, pltpu.VMEM
    chain = Chain(0, order_of(wide, 0), d)
    vec_rows = -(-6 * d // 1024) * 8 + -(-(f + 2 * lw) // 1024) * 8
    return pl.pallas_call(
        functools.partial(last_body, wide=wide),
        out_shape=(sd((rows, cw), BF16), sd((d, f), BF16), sd((2 * lw, cw), BF16))
        + (sd((d, lw), BF16),) * 3 + (sd((vec_rows, 128), F32),),
        in_specs=[vmem()] * 3 + [anywhere()] * 3 + [vmem()] * 9,
        out_specs=(vmem(),) * 7,
        scratch_shapes=[
            vm((rows, d), BF16), vm(w.shape, BF16), vm((rows, d), BF16), vm((half, d), BF16), vm((half, d), BF16),
            vm((half, d), F32), vm((block, d), F32), vm((half, cw), BF16), vm((3, d, lw), BF16),
            vm((3, chain.box_rows, lw), BF16), vm((3, d // 2, lw), BF16), vm((3, chain.size, lw), BF16),
            vm((vec_rows, 128), F32), vm((steps + 1, vec_rows, 128), F32),
        ]
        + sems(3, 2 * each + 1, 2 * each + 1, 11 * steps, 11 * steps),
        compiler_params=params(collective_id=5, has_side_effects=True),
        cost_estimate=cost(2 * rows * d * 6 * lw, 2 * rows * d * 8),
        name="last",
    )(dq, dk, dv, low, w, xf, gm, gain, up_own, gp_sum, s_ub, s_db, s_g2, s_s2, s_pb)


def on_device(
    tokens, lengths, qkv_weight, qv_bias, proj_weight, proj_bias, up_weight, up_bias,
    down_weight, down_bias, first_gain, first_shift, second_gain, second_shift, cotangent,
):
    cw = tokens.shape[1]
    d, ff, lw = 2 * cw, up_weight.shape[1], proj_weight.shape[0]
    wide = lax.axis_size("wide")
    row = lambda a: a.astype(F32).reshape(1, -1)
    w3 = jnp.transpose(qkv_weight, (1, 0, 2))
    gain1, shift1, gain2, shift2 = map(row, (first_gain, first_shift, second_gain, second_shift))

    xf, low, q, k, v = qkv_call(tokens, w3, qv_bias.astype(F32), gain1, shift1)
    mixed, qa, mixed_got, proj_got = attend_forward(lengths, q, k, v, proj_weight)
    lo, lo_send, gmix, gm, gup, down_own, gp_own, gp_other, s_ub, s_db, s_g2, s_s2, s_pb = mlp_call(
        lengths, xf, mixed, mixed_got, proj_weight, proj_got, row(proj_bias), gain2, shift2,
        up_weight, row(up_bias), down_weight, row(down_bias), cotangent, wide,
    )
    dq, dk, dv, lo_got, gdown, up_own, gp_sum = attend_backward(
        lengths, qa, k, v, gmix, mixed, lo_send, gup, down_own, gp_own, gp_other, wide
    )
    ig, gup, gp, gq, gk, gv, small = last_call(
        dq, dk, dv, low, w3, xf, gm, gain1, up_own, gp_sum, s_ub, s_db, s_g2, s_s2, s_pb, wide
    )
    layer_out = (lo + lo_got.astype(F32)).astype(BF16)
    factor = 1.0 / (lengths.shape[0] * wide)
    fin = lambda a: a.astype(F32) * factor
    s_qkv = jnp.stack([fin(a) for a in (gq, gk, gv)])
    s_proj = jnp.concatenate([fin(gp[:lw]), fin(gp[lw:])], axis=1)
    flat = (small * factor).reshape(-1)
    shared = -(-6 * d // 1024) * 1024
    g1, s1, g2, s2, pb, dbs = (flat[i * d : (i + 1) * d] for i in range(6))
    ubs = flat[shared : shared + ff]
    qvb = flat[shared + ff : shared + ff + 2 * lw].reshape(2, lw)
    return (
        layer_out, ig, jnp.transpose(s_qkv, (1, 0, 2)), qvb,
        s_proj, pb, fin(gup), ubs, fin(gdown), dbs, g1, s1, g2, s2,
    )


def solution(mesh):
    split = P("wide", "narrow")
    none3, cols, rows1 = P(None, None, "narrow"), P(None, "narrow"), P("narrow", None)
    return jax.shard_map(
        on_device,
        mesh=mesh,
        in_specs=(
            split, P("wide"), none3, cols, rows1, P(), cols, P("narrow"), rows1, P(), P(), P(), P(), P(), split,
        ),
        out_specs=(
            split, split, none3, cols, rows1, P(), cols, P("narrow"), rows1, P(), P(), P(), P(), P(),
        ),
        check_vma=False,
    )
```

```python
import functools

import jax
import jax.numpy as jnp
from jax import lax
from jax.experimental import pallas as pl
from jax.experimental.pallas import tpu as pltpu
from jax.sharding import PartitionSpec as P

EPS = 1e-05
HEAD = 64
F32, BF16 = jnp.float32, jnp.bfloat16
NT = (((1,), (1,)), ((), ()))
TN = (((0,), (0,)), ((), ()))
GELU_A, GELU_B = 0.7978845608028654, 0.044715
VMEM_LIMIT = 63 * 1024 * 1024


def dot(a, b):
    return jnp.dot(a, b, preferred_element_type=F32)


def dot_nt(a, b):
    return lax.dot_general(a, b, NT, preferred_element_type=F32)


def dot_tn(a, b):
    return lax.dot_general(a, b, TN, preferred_element_type=F32)


def params(**more):
    return pltpu.CompilerParams(vmem_limit_bytes=VMEM_LIMIT, **more)


def cost(flops, size, trans=0):
    return pl.CostEstimate(flops=int(flops), bytes_accessed=int(size), transcendentals=int(trans))


def lane_part(which, width):
    return pl.ds(pl.multiple_of(which * width, 128), width)


def norm_rows(x):
    mean = jnp.mean(x, axis=-1, keepdims=True)
    cen = x - mean
    var = jnp.mean(cen * cen, axis=-1, keepdims=True)
    r = lax.rsqrt(var + EPS)
    return cen * r, r


def rows_spec(rows, cols, base=0):
    return pl.BlockSpec((rows, cols), lambda i, *_: (i + base, 0))


def whole_spec(shape):
    zeros = (0,) * len(shape)
    return pl.BlockSpec(shape, lambda i, *_: zeros)


MESH = pl.DeviceIdType.MESH
scope = jax.named_scope


def vec(ref):
    return ref[...].astype(F32).reshape(1, -1)


def bit_of(index, bit):
    return (index // (1 << bit)) % 2


def flip(index, bit):
    return index + (1 - 2 * bit_of(index, bit)) * (1 << bit)


def greet(peers):
    barrier = pltpu.get_barrier_semaphore()
    for peer in peers:
        pl.semaphore_signal(barrier, inc=1, device_id=peer, device_id_type=MESH)
    pl.semaphore_wait(barrier, len(peers))


def remote(src, dst, sems, at, peer):
    return pltpu.make_async_remote_copy(
        src_ref=src, dst_ref=dst, send_sem=sems[0].at[at], recv_sem=sems[1].at[at],
        device_id=peer, device_id_type=MESH,
    )


def block_rows(start, size, unit=16):
    return pl.ds(start if isinstance(start, int) else pl.multiple_of(start, unit), size)


class Chain:
    def __init__(self, me, order, rows):
        self.me, self.steps, self.splits = me, [], []
        base, size, box = 0, rows, 0
        for bit in order:
            if size % 32 == 0:
                half = size // 2
                mine = bit_of(me, bit)
                keep, give = base + mine * half, base + (1 - mine) * half
                self.splits.append((bit, base, keep, half))
            else:
                half, keep, give = size, base, base
            self.steps.append((bit, keep, give, half, box))
            base, size, box = keep, half, box + half
        self.base, self.size, self.box_rows = base, size, box
        self.first = self.steps[0][1]

    def scatter(self, src, box, part, own, sems, at, cols):
        self.src, self.box, self.part, self.own = src, box, part, own
        self.sems, self.at, self.cols = sems, at, cols
        return self

    def _source(self, step):
        if step == 0:
            return self.src, 0
        return self.part, self.first

    def _scatter_copy(self, step):
        bit, _, give, half, box = self.steps[step]
        source, off = self._source(step)
        return remote(
            source.at[block_rows(give - off, half), self.cols],
            self.box.at[pl.ds(box, half), self.cols],
            self.sems, self.at + step, {"wide": flip(self.me, bit)},
        )

    def scatter_start(self, step):
        self._scatter_copy(step).start()

    def scatter_end(self, step):
        self._scatter_copy(step).wait()
        _, keep, _, half, box = self.steps[step]
        source, off = self._source(step)
        last = step == len(self.steps) - 1
        target, out = (self.own, keep) if last else (self.part, self.first)
        unit = next(u for u in (96, 64, 48, 32, 16) if half % u == 0)

        def add(i, carry):
            at = i * unit
            got = self.box[block_rows(box + at, unit), self.cols].astype(F32)
            mine = source[block_rows(keep - off + at, unit), self.cols].astype(F32)
            target[block_rows(keep - out + at, unit), self.cols] = (got + mine).astype(BF16)
            return carry

        lax.fori_loop(0, half // unit, add, 0)

    def gather(self, own, dst, sems, at, cols):
        self.own, self.dst, self.gsems, self.gat, self.gcols = own, dst, sems, at, cols
        return self

    def gather_open(self):
        self.dst[block_rows(self.base, self.size), self.gcols] = self.own[:, self.gcols]

    def gather_copy_open(self, sem, at):
        region = self.dst.at[block_rows(self.base, self.size), self.gcols]
        return pltpu.make_async_copy(self.own.at[:, self.gcols], region, sem.at[at])

    def _gather_copy(self, step):
        bit, _, keep, half = self.splits[len(self.splits) - 1 - step]
        region = self.dst.at[block_rows(keep, half), self.gcols]
        return remote(region, region, self.gsems, self.gat + step, {"wide": flip(self.me, bit)})

    def gather_start(self, step):
        if step < len(self.splits):
            self._gather_copy(step).start()

    def gather_end(self, step):
        if step < len(self.splits):
            self._gather_copy(step).wait()


def bits(wide):
    return wide.bit_length() - 1


def order_of(wide, kind):
    steps = list(range(bits(wide)))
    return steps if kind == 0 else [0] + steps[2:] + steps[1:2]


def thirds(cols):
    w = cols // 3
    return [(0, pl.ds(0, w)), (0, pl.ds(w, w)), (1, pl.ds(2 * w, w))]


def wide_peers(me, wide):
    return [{"wide": flip(me, b)} for b in range(bits(wide))]


def vmem():
    return pl.BlockSpec(memory_space=pltpu.VMEM)


def anywhere():
    return pl.BlockSpec(memory_space=pl.ANY)


def sems(*counts):
    return [pltpu.SemaphoreType.DMA((c,)) for c in counts]


def qkv_body(own_hbm, own, w, bias, gain, shift, xf, low, q, k, v, got, send_sem, recv_sem):
    n = lax.axis_index("narrow")
    i = pl.program_id(0)
    rows, cw = own.shape
    peer = {"narrow": 1 - n}

    def copy(at):
        block = block_rows(at * rows, rows)
        return remote(own_hbm.at[block], got.at[block], (send_sem, recv_sem), at, peer)

    @pl.when(i == 0)
    def _():
        greet([peer])
        for at in range(got.shape[0] // rows):
            copy(at).start()

    xf[:, lane_part(n, cw)] = own[...]
    with scope("wait"):
        copy(i).wait()
    xf[:, lane_part(1 - n, cw)] = got[block_rows(i * rows, rows), :]
    xhat, _ = norm_rows(xf[...].astype(F32))
    y = (xhat * vec(gain) + vec(shift)).astype(BF16)
    low[...] = y
    q[...] = (dot(y, w[0]) + bias[0:1, :].astype(F32)).astype(BF16) * jnp.asarray(HEAD**-0.5, BF16)
    k[...] = dot(y, w[1]).astype(BF16)
    v[...] = (dot(y, w[2]) + bias[1:2, :].astype(F32)).astype(BF16)


def qkv_call(own, w, bias, gain, shift, block=256):
    rows, cw = own.shape
    d, lw = w.shape[1], w.shape[2]
    sd = jax.ShapeDtypeStruct
    return pl.pallas_call(
        qkv_body,
        out_shape=(sd((rows, d), BF16), sd((rows, d), BF16)) + (sd((rows, lw), BF16),) * 3,
        grid_spec=pltpu.PrefetchScalarGridSpec(
            num_scalar_prefetch=0,
            grid=(rows // block,),
            in_specs=[anywhere(), rows_spec(block, cw)] + [whole_spec(a.shape) for a in (w, bias, gain, shift)],
            out_specs=[rows_spec(block, d)] * 2 + [rows_spec(block, lw)] * 3,
            scratch_shapes=[pltpu.VMEM((rows, cw), BF16)] + sems(rows // block, rows // block),
        ),
        compiler_params=params(collective_id=1, has_side_effects=True),
        cost_estimate=cost(2 * rows * d * 3 * lw, 2 * (rows * d * 5 + w.size)),
        name="norm_qkv",
    )(own, own, w, bias, gain, shift)


def three(x):
    hi = x.astype(BF16).astype(F32)
    mid = (x - hi).astype(BF16).astype(F32)
    return hi, mid, x - hi - mid


def lanes_of(par):
    lane = lax.broadcasted_iota(jnp.int32, (1, 2 * HEAD), 1)
    mine = (lane // HEAD) == par
    return lane, mine, (1 - par) * HEAD


def place(lane, mine, at, base, terms):
    out = jnp.where(mine, base, 0.0)
    for i, term in enumerate(terms):
        out = jnp.where(lane == at + i, term, out)
    return out


def fwd_body(
    len_ref, q, k, v, pw, o, qa_out, o_got, pw_got, ka, va, send_sem, recv_sem, *, bq
):
    head = pl.program_id(0)
    par, pair = head % 2, head // 2
    lane, mine, at = lanes_of(par)
    n, me = lax.axis_index("narrow"), lax.axis_index("wide")
    peer, core = {"narrow": 1 - n}, {"wide": flip(me, 0)}
    pairs = pl.num_programs(0) // 2
    both = (send_sem, recv_sem)
    cols = lane_part(pair, 2 * HEAD)
    part = block_rows((me % 2) * (pw.shape[0] // 2), pw.shape[0] // 2)
    npairs = o.shape[1] // (2 * HEAD)
    weights = remote(pw.at[part], pw_got.at[part], both, npairs, peer)
    shared = remote(pw_got.at[part], pw_got.at[part], both, npairs + 1, core)

    @pl.when(head == 0)
    def _():
        greet([peer, core])
        weights.start()

    keys = k.shape[0]
    kpos = lax.broadcasted_iota(jnp.int32, (keys, 1), 0)
    kbias = jnp.where(kpos < len_ref[0], 0.0, -1e30)
    ka[...] = place(lane, mine, at, k[...].astype(F32), [kbias]).astype(BF16)
    va[...] = place(lane, mine, at, v[...].astype(F32), [1.0]).astype(BF16)
    tri = lax.broadcasted_iota(jnp.int32, (bq, bq), 1) <= lax.broadcasted_iota(jnp.int32, (bq, bq), 0)
    for i in range(q.shape[0] // bq):
        nk = (i + 1) * bq
        rows = pl.ds(i * bq, bq)
        qf = q[rows, :].astype(F32)
        qa = place(lane, mine, at, qf, [1.0])
        s = dot_nt(qa.astype(BF16), ka[0:nk, :])
        edge = jnp.where(tri, s[:, nk - bq :], -1e30)
        m = jnp.max(edge, axis=1, keepdims=True)
        if nk > bq:
            m = jnp.maximum(m, jnp.max(s[:, : nk - bq], axis=1, keepdims=True))
        pv = dot(jnp.exp(edge - m).astype(BF16), va[nk - bq : nk, :])
        if nk > bq:
            pv += dot(jnp.exp(s[:, : nk - bq] - m).astype(BF16), va[0 : nk - bq, :])
        total = jnp.sum(jnp.where(lane == at, pv, 0.0), axis=1, keepdims=True)
        out = (pv / total).astype(BF16).astype(F32)
        old = o[rows, cols].astype(F32)
        o[rows, cols] = jnp.where(mine, out, jnp.where(par == 0, 0.0, old)).astype(BF16)
        lse = m + jnp.log(total)
        qa_out[0, rows, :] = place(lane, mine, at, qf, [1.0, *three(lse)]).astype(BF16)

    def mixed(j):
        c = pl.ds(j * 2 * HEAD, 2 * HEAD)
        return remote(o.at[:, c], o_got.at[:, c], both, j, peer)

    for j in range(npairs):

        @pl.when(head == 2 * j + 1)
        def _():
            mixed(j).start()

    @pl.when(head == 3)
    def _():
        weights.wait()
        shared.start()

    @pl.when(head == 2 * npairs - 1)
    def _():
        shared.wait()
        for j in range(npairs):
            mixed(j).wait()


def attend_forward(length, q, k, v, pw, bq=256):
    rows, width = q.shape
    heads, pair = width // HEAD, 2 * HEAD
    half = lambda h, *_: (0, h // 2)
    sd = jax.ShapeDtypeStruct
    work = 2 * heads * rows * rows * HEAD
    return pl.pallas_call(
        functools.partial(fwd_body, bq=bq),
        out_shape=(
            sd((rows, width), BF16), sd((heads, rows, pair), BF16), sd((rows, width), BF16), sd(pw.shape, BF16),
        ),
        grid_spec=pltpu.PrefetchScalarGridSpec(
            num_scalar_prefetch=1,
            grid=(heads,),
            in_specs=[pl.BlockSpec((rows, pair), half)] * 3 + [anywhere()],
            out_specs=[vmem(), pl.BlockSpec((1, rows, pair), lambda h, *_: (h, 0, 0)), anywhere(), anywhere()],
            scratch_shapes=[pltpu.VMEM((rows, pair), BF16)] * 2 + sems(heads // 2 + 2, heads // 2 + 2),
        ),
        compiler_params=params(collective_id=2, has_side_effects=True),
        cost_estimate=cost(4 * work, 2 * rows * width * 6, work // 256),
        name="attend_fwd",
    )(length, q, k, v, pw)


def mlp_body(
    len_ref, xf, mo, mr, pwo, pwr, pb, gain, shift, ub, up_hbm, down_hbm, cot,
    lo, lo_send, gmix, gm, gup, down_own, gp_own, gp_other, sum_ub, sum_db, sum_g, sum_s, sum_pb,
    up, down, cot_got, cf, mid, second, active, slope, gh, gs_send, gs_got, gs_own, gdown, box, part,
    glow, gmix_send, load_sem, nsend, nrecv, wsend, wrecv,
    *, wide,
):
    n, me = lax.axis_index("narrow"), lax.axis_index("wide")
    peer = {"narrow": 1 - n}
    rows, cw = cot.shape
    d, f = up.shape
    half, block = rows // 2, min(256, rows // 2)
    each = half // block
    mine, other = lane_part(n, cw), lane_part(1 - n, cw)
    narrow, across = (nsend, nrecv), (wsend, wrecv)
    loads = [
        pltpu.make_async_copy(up_hbm, up, load_sem.at[0]),
        pltpu.make_async_copy(down_hbm, down, load_sem.at[1]),
    ]
    for load in loads:
        load.start()
    greet([peer] + wide_peers(me, wide))

    def cot_copy(side, j):
        r = block_rows(side * half + j * block, block)
        return (cot.at[r], cot_got.at[r])

    for a, side in enumerate((n, 1 - n)):
        for j in range(each):
            src, dst = cot_copy(side, j)
            remote(src, dst, narrow, a * each + j, peer).start()

    def forward(i, carry):
        r = block_rows(i * block, block)
        m = xf[r, :].astype(F32) + (dot(mo[r, :], pwo[...]) + dot(mr[r, :], pwr[...])) + vec(pb)
        mid[r, :] = m
        xhat, _ = norm_rows(m)
        sec = (xhat * vec(gain) + vec(shift)).astype(BF16)
        second[r, :] = sec
        hid = dot(sec, up[...]) + vec(ub)
        sq = hid * hid
        t = jnp.tanh(GELU_A * (hid + GELU_B * (sq * hid)))
        hf = 0.5 * (1.0 + t)
        act = (hid * hf).astype(BF16)
        active[r, :] = act
        slope[r, :] = hf + (0.5 * hid) * (1.0 - t * t) * (GELU_A + (3.0 * GELU_A * GELU_B) * sq)
        lo[r, :] = mid[r, mine] + dot(act, down[:, mine])
        lo_send[r, :] = dot(act, down[:, other]).astype(BF16)
        return carry

    with scope("load"):
        for load in loads:
            load.wait()
    with scope("forward"):
        lax.fori_loop(0, rows // block, forward, 0)

    def backward(side, j, a):
        src, dst = cot_copy(side, j)
        remote(src, dst, narrow, a * each + j, peer).wait()
        at = side * half + j * block
        r = block_rows(at, block)
        pos = at + lax.broadcasted_iota(jnp.int32, (block, 1), 0)
        live = (pos < len_ref[0]).astype(F32)
        cf[r, mine] = (cot[r, :].astype(F32) * live).astype(BF16)
        cf[r, other] = (cot_got[r, :].astype(F32) * live).astype(BF16)
        ghid = (dot_nt(cf[r, :], down[...]) * slope[r, :]).astype(BF16)
        gh[r, :] = ghid
        return dot_nt(ghid, up[...]), ghid

    def gs_copy(j):
        r = pl.ds(j * block, block)
        return remote(gs_send.at[r], gs_got.at[r], narrow, 2 * each + j, peer)

    sum_ub[...] = jnp.zeros_like(sum_ub)

    def for_peer(j, carry):
        g, ghid = backward(1 - n, j, 0)
        r = block_rows(j * block, block)
        gs_send[r, :] = g.astype(BF16)
        remote(gs_send.at[r], gs_got.at[r], narrow, 2 * each + j, peer).start()
        sum_ub[...] += jnp.sum(ghid.astype(F32), axis=0, keepdims=True)
        return carry

    def for_own(j, carry):
        g, ghid = backward(n, j, 1)
        gs_own[block_rows(j * block, block), :] = g
        sum_ub[...] += jnp.sum(ghid.astype(F32), axis=0, keepdims=True)
        return carry

    with scope("for_peer"):
        lax.fori_loop(0, each, for_peer, 0)
    with scope("for_own"):
        lax.fori_loop(0, each, for_own, 0)

    chains = []
    for a, (kind, cols) in enumerate(thirds(d)):
        chain = Chain(me, order_of(wide, kind), f)
        chains.append(chain.scatter(gdown, box, part, down_own, across, a * bits(wide), cols))

    def weight_down(i, carry):
        c = block_rows(i * 256, 256, 256)
        gdown[c, :] = dot_tn(active[:, c], cf[...]).astype(BF16)
        return carry

    def weight_up(i, carry):
        c = block_rows(i * 256, 256, 256)
        gup[c, :] = dot_tn(second[:, c], gh[...]).astype(BF16)
        return carry

    with scope("w_down"):
        lax.fori_loop(0, f // 256, weight_down, 0)
    for chain in chains:
        chain.scatter_start(0)
    with scope("w_up"):
        lax.fori_loop(0, d // 256, weight_up, 0)

    def advance(step):
        with scope(f"step{step}"):
            for chain in chains:
                chain.scatter_end(step)
                if step + 1 < bits(wide):
                    chain.scatter_start(step + 1)

    advance(0)
    with scope("gs_wait"):
        for j in range(each):
            gs_copy(j).wait()
    for ref in (sum_g, sum_s, sum_pb, sum_db):
        ref[...] = jnp.zeros_like(ref)

    def gmix_copy(j):
        r = block_rows(n * half + j * block, block)
        return remote(gmix_send.at[block_rows(j * block, block)], gmix.at[r], narrow, 3 * each + j, peer)

    def back_norm(j, carry):
        r, rh = block_rows(n * half + j * block, block), block_rows(j * block, block)
        g = gs_own[rh, :] + gs_got[rh, :].astype(F32)
        xhat, scale = norm_rows(mid[r, :])
        gg = g * vec(gain)
        m1 = jnp.mean(gg, axis=-1, keepdims=True)
        m2 = jnp.mean(gg * xhat, axis=-1, keepdims=True)
        c = cf[r, :].astype(F32)
        grad = c + scale * (gg - m1 - xhat * m2)
        gm[rh, :] = grad
        gl = grad.astype(BF16)
        glow[rh, :] = gl
        gmix_send[rh, :] = dot_nt(gl, pwr[...]).astype(BF16)
        gmix_copy(j).start()
        gmix[r, :] = dot_nt(gl, pwo[...]).astype(BF16)
        sum_g[...] += jnp.sum(g * xhat, axis=0, keepdims=True)
        sum_s[...] += jnp.sum(g, axis=0, keepdims=True)
        sum_pb[...] += jnp.sum(grad, axis=0, keepdims=True)
        sum_db[...] += jnp.sum(c, axis=0, keepdims=True)
        return carry

    with scope("back_norm"):
        lax.fori_loop(0, each, back_norm, 0)
    for step in range(1, bits(wide)):
        advance(step)
        if step == 1:
            own_rows = block_rows(n * half, half)
            lw = mo.shape[1]
            for src, dst in ((mo, gp_own), (mr, gp_other)):
                total = dot_tn(src[own_rows, :], glow[...]).astype(BF16)
                dst[0:lw, :] = total[:, :cw]
                dst[lw : 2 * lw, :] = total[:, cw:]

    with scope("gmix_wait"):
        for j in range(each):
            gmix_copy(j).wait()


def mlp_call(length, xf, mo, mr, pwo, pwr, pb, gain, shift, up, ub, down, cot, wide):
    rows, d = xf.shape
    f, lw, cw = up.shape[1], mo.shape[1], cot.shape[1]
    half = rows // 2
    chain = Chain(0, order_of(wide, 0), f)
    sd, vm = jax.ShapeDtypeStruct, pltpu.VMEM
    each = half // min(256, half)
    return pl.pallas_call(
        functools.partial(mlp_body, wide=wide),
        out_shape=(
            sd((rows, cw), F32), sd((rows, cw), BF16), sd((rows, lw), BF16), sd((half, d), F32),
            sd((d, f), BF16), sd((chain.size, d), BF16), sd((2 * lw, cw), BF16), sd((2 * lw, cw), BF16),
            sd((1, f), F32), sd((1, d), F32), sd((1, d), F32), sd((1, d), F32), sd((1, d), F32),
        ),
        in_specs=[pl.BlockSpec(memory_space=pltpu.SMEM)] + [vmem()] * 9 + [anywhere(), anywhere(), vmem()],
        out_specs=(vmem(),) * 13,
        scratch_shapes=[
            vm((d, f), BF16), vm((f, d), BF16), vm((rows, cw), BF16), vm((rows, d), BF16), vm((rows, d), F32),
            vm((rows, d), BF16), vm((rows, f), BF16), vm((rows, f), F32), vm((rows, f), BF16),
            vm((half, d), BF16), vm((half, d), BF16), vm((half, d), F32), vm((f, d), BF16),
            vm((chain.box_rows, d), BF16), vm((f // 2, d), BF16), vm((half, d), BF16), vm((half, lw), BF16),
        ]
        + sems(2, 4 * each, 4 * each, 3 * bits(wide), 3 * bits(wide)),
        compiler_params=params(collective_id=3, has_side_effects=True),
        cost_estimate=cost(2 * rows * d * (d + 6 * f), 2 * (rows * d * 8 + 2 * d * f), rows * f),
        name="mlp",
    )(length, xf, mo, mr, pwo, pwr, pb, gain, shift, ub, up, down, cot)


def bwd_body(
    len_ref, qa, k, v, do, o, lo_send, gup, down_own, gp_own, gp_other,
    dq, dk, dv, lo_got, gdown, up_own, gp_sum,
    ka, va, dk_acc, dv_acc, up_box, up_part, own_box, own_part, other_box, other_part,
    own_shard, other_shard, peer_shard, open_sem, nsend, nrecv, wsend, wrecv, *, bq, wide,
):
    head = pl.program_id(0)
    heads = 2 * (lo_got.shape[1] // (2 * HEAD))
    n, me = lax.axis_index("narrow"), lax.axis_index("wide")
    peer = {"narrow": 1 - n}
    narrow, across = (nsend, nrecv), (wsend, wrecv)
    steps = bits(wide)
    scatters, gathers = [], []
    for a, (kind, cols) in enumerate(thirds(gup.shape[1])):
        chain = Chain(me, order_of(wide, kind), gup.shape[0])
        scatters.append(chain.scatter(gup, up_box, up_part, up_own, across, a * steps, cols))
    cw = gp_own.shape[1]
    for a, (src, box, part, own) in enumerate(
        ((gp_own, own_box, own_part, own_shard), (gp_other, other_box, other_part, other_shard))
    ):
        chain = Chain(me, order_of(wide, 0), gp_own.shape[0])
        scatters.append(chain.scatter(src, box, part, own, across, (3 + a) * steps, pl.ds(0, cw)))
    for a, (kind, cols) in enumerate(thirds(gdown.shape[1])):
        chain = Chain(me, order_of(wide, kind), gdown.shape[0])
        gathers.append(chain.gather(down_own, gdown, across, (5 + a) * steps, cols))
    layer = remote(lo_send, lo_got, narrow, 0, peer)
    shard = remote(other_shard, peer_shard, narrow, 1, peer)

    @pl.when(head == 0)
    def _():
        greet([peer] + wide_peers(me, wide))
        layer.start()
        for chain in scatters:
            chain.scatter_start(0)
        opens = [chain.gather_copy_open(open_sem, a) for a, chain in enumerate(gathers)]
        for opened in opens:
            opened.start()
        for opened, chain in zip(opens, gathers):
            opened.wait()
            chain.gather_start(0)

    par = head % 2
    lane, mine, at = lanes_of(par)
    keys = k.shape[0]
    kpos = lax.broadcasted_iota(jnp.int32, (keys, 1), 0)
    kbias = jnp.where(kpos < len_ref[0], 0.0, -1e30)
    ka[...] = place(lane, mine, at, k[...].astype(F32), [kbias, -1.0, -1.0, -1.0]).astype(BF16)
    va[...] = place(lane, mine, at, v[...].astype(F32), [-1.0, -1.0, -1.0]).astype(BF16)
    dk_acc[...] = jnp.zeros_like(dk_acc)
    dv_acc[...] = jnp.zeros_like(dv_acc)
    tri = lax.broadcasted_iota(jnp.int32, (bq, bq), 0) <= lax.broadcasted_iota(jnp.int32, (bq, bq), 1)

    def put(ref, rows, new):
        old = ref[rows, :].astype(F32)
        ref[rows, :] = jnp.where(mine, new, jnp.where(par == 0, 0.0, old)).astype(BF16)

    for i in range(qa.shape[1] // bq):
        rows = pl.ds(i * bq, bq)
        qb = qa[0, rows, :]
        df = do[rows, :].astype(F32)
        delta = jnp.sum(jnp.where(mine, df * o[rows, :].astype(F32), 0.0), axis=1, keepdims=True)
        db = place(lane, mine, at, df, three(delta)).astype(BF16)
        dqs = None
        for j in range(i + 1):
            cols = pl.ds(j * bq, bq)
            kb, vb = ka[cols, :], va[cols, :]
            s = dot_nt(kb, qb)
            if j == i:
                s = jnp.where(tri, s, -1e30)
            p = jnp.exp(s)
            ds = (p * dot_nt(vb, db)).astype(BF16)
            dv_acc[cols, :] += dot(p.astype(BF16), db)
            dk_acc[cols, :] += dot(ds, qb)
            part = dot_tn(ds, kb)
            dqs = part if dqs is None else dqs + part
        put(dq, rows, dqs * HEAD**-0.5)
    put(dk, pl.ds(0, keys), dk_acc[...])
    put(dv, pl.ds(0, keys), dv_acc[...])

    def advance(step):
        with scope(f"scatter{step}"):
            for chain in scatters:
                chain.scatter_end(step)
                if step + 1 < steps:
                    chain.scatter_start(step + 1)
        with scope(f"gather{step}"):
            for chain in gathers:
                chain.gather_end(step)
                chain.gather_start(step + 1)
        if step == steps - 1:
            shard.start()

    for step in range(steps):

        @pl.when(head == min(heads - 1, (step * heads) // steps + (1 if step else 0)))
        def _():
            advance(step)

    @pl.when(head == heads - 1)
    def _():
        shard.wait()
        gp_sum[...] = (own_shard[...].astype(F32) + peer_shard[...].astype(F32)).astype(BF16)
        layer.wait()


def attend_backward(length, qa, k, v, do, o, lo_send, gup, down_own, gp_own, gp_other, wide, bq=256):
    rows, width = k.shape
    heads, pair = width // HEAD, 2 * HEAD
    half = lambda h, *_: (0, h // 2)
    sd, vm = jax.ShapeDtypeStruct, pltpu.VMEM
    work = 2 * heads * rows * rows * HEAD
    d, f = gup.shape
    up_chain = Chain(0, order_of(wide, 0), d)
    gp_rows, cw = gp_own.shape
    gp_chain = Chain(0, order_of(wide, 0), gp_rows)
    pairs = [pl.BlockSpec((rows, pair), half)]
    steps = bits(wide)
    return pl.pallas_call(
        functools.partial(bwd_body, bq=bq, wide=wide),
        out_shape=(
            (sd((rows, width), BF16),) * 3
            + (sd(lo_send.shape, BF16), sd((f, d), BF16), sd((up_chain.size, f), BF16), sd((gp_chain.size, cw), BF16))
        ),
        grid_spec=pltpu.PrefetchScalarGridSpec(
            num_scalar_prefetch=1,
            grid=(heads,),
            in_specs=[pl.BlockSpec((1, rows, pair), lambda h, *_: (h, 0, 0))] + pairs * 4 + [vmem()] * 5,
            out_specs=pairs * 3 + [anywhere()] * 2 + [vmem()] * 2,
            scratch_shapes=[vm((rows, pair), BF16)] * 2 + [vm((rows, pair), F32)] * 2
            + [vm((up_chain.box_rows, f), BF16), vm((d // 2, f), BF16)]
            + [vm((gp_chain.box_rows, cw), BF16), vm((gp_rows // 2, cw), BF16)] * 2
            + [vm((gp_chain.size, cw), BF16)] * 3
            + sems(3, 2, 2, 8 * steps, 8 * steps),
        ),
        compiler_params=params(collective_id=4, has_side_effects=True),
        cost_estimate=cost(10 * work, 2 * rows * width * 9, work // 256),
        name="attend_bwd",
    )(length, qa, k, v, do, o, lo_send, gup, down_own, gp_own, gp_other)


def last_body(
    dq, dk, dv, low_hbm, w_hbm, xf_hbm, gm, gain, up_own, gp_sum, s_ub, s_db, s_g2, s_s2, s_pb,
    ig, gup, gp, gq, gk, gv, small,
    low, w, xf, gn_send, gn_got, gn_own, ig_own, ig_send, src, box, part, own, sums, sums_box,
    load_sem, nsend, nrecv, wsend, wrecv, *, wide,
):
    n, me = lax.axis_index("narrow"), lax.axis_index("wide")
    peer = {"narrow": 1 - n}
    narrow, across = (nsend, nrecv), (wsend, wrecv)
    steps = bits(wide)
    rows, lw = dq.shape
    d = gain.shape[0]
    cw = d // 2
    half, block = rows // 2, min(256, rows // 2)
    each = half // block
    loads = [
        pltpu.make_async_copy(a, b, load_sem.at[i])
        for i, (a, b) in enumerate(((low_hbm, low), (w_hbm, w), (xf_hbm, xf)))
    ]
    for load in loads:
        load.start()
    greet([peer] + wide_peers(me, wide))
    gathers = []
    for a, (kind, cols) in enumerate(thirds(gup.shape[1])):
        chain = Chain(me, order_of(wide, kind), gup.shape[0])
        gathers.append(chain.gather(up_own, gup, across, a * steps, cols))
    chain = Chain(me, order_of(wide, 0), gp.shape[0])
    gathers.append(chain.gather(gp_sum, gp, across, 3 * steps, pl.ds(0, cw)))
    for chain in gathers:
        chain.gather_open()
        chain.gather_start(0)

    grads, outs = (dq, dk, dv), (gq, gk, gv)
    scatters = []
    for c in range(3):
        chain = Chain(me, order_of(wide, 1 if c == 1 else 0), d)
        chain.scatter(src.at[c], box.at[c], part.at[c], own.at[c], across, (4 + c) * steps, pl.ds(0, lw))
        scatters.append(chain.gather(own.at[c], outs[c], across, (7 + c) * steps, pl.ds(0, lw)))

    def scatter_step(step):
        with scope(f"scatter{step}"):
            for chain in scatters:
                chain.scatter_end(step)
                if step + 1 < steps:
                    chain.scatter_start(step + 1)
                else:
                    chain.gather_open()
                    chain.gather_start(0)

    def gather_step(chains, step):
        with scope(f"gather{len(chains)}_{step}"):
            for chain in chains:
                chain.gather_end(step)
                chain.gather_start(step + 1)

    loads[0].wait()
    for c in range(3):
        with scope("weights"):
            src[c] = dot_tn(low[...], grads[c][...]).astype(BF16)
        scatters[c].scatter_start(0)
    gather_step(gathers, 0)
    loads[1].wait()

    def gn_part(at, cols):
        r = block_rows(at, block)
        total = dot_nt(dq[r, :], w[0, cols, :])
        total += dot_nt(dk[r, :], w[1, cols, :])
        return total + dot_nt(dv[r, :], w[2, cols, :])

    def gn_copy(j):
        r = pl.ds(j * block, block)
        return remote(gn_send.at[r], gn_got.at[r], narrow, j, peer)

    for j in range(each):
        at = (1 - n) * half + j * block
        for c in range(2):
            cols = slice(c * cw, (c + 1) * cw)
            gn_send[j * block : (j + 1) * block, cols] = gn_part(at, cols).astype(BF16)
        gn_copy(j).start()
    scatter_step(0)
    for j in range(each):
        at = n * half + j * block
        for c in range(2):
            cols = slice(c * cw, (c + 1) * cw)
            gn_own[j * block : (j + 1) * block, cols] = gn_part(at, cols)
    gather_step(gathers, 1)
    loads[2].wait()

    sums[...] = jnp.zeros_like(sums)

    def put(at, value):
        for i in range(value.shape[1] // 128):
            sums[at + i : at + i + 1, :] = value[:, i * 128 : (i + 1) * 128]

    dr, fr, lr = d // 128, s_ub.shape[1] // 128, lw // 128
    shared = -(-6 * dr // 8) * 8
    put(2 * dr, s_g2[...])
    put(3 * dr, s_s2[...])
    put(4 * dr, s_pb[...])
    put(5 * dr, s_db[...])
    put(shared, s_ub[...])
    put(shared + fr, jnp.sum(dq[...].astype(F32), axis=0, keepdims=True))
    put(shared + fr + lr, jnp.sum(dv[...].astype(F32), axis=0, keepdims=True))

    mine, other = lane_part(n, cw), lane_part(1 - n, cw)
    g1 = s1 = 0.0

    def ig_copy(j):
        r = block_rows(n * half + j * block, block)
        return remote(ig_send.at[pl.ds(j * block, block)], ig.at[r], narrow, each + j, peer)

    for j in range(each):
        with scope("gn_wait"):
            gn_copy(j).wait()
        rh = pl.ds(j * block, block)
        r = block_rows(n * half + j * block, block)
        g = gn_own[rh, :] + gn_got[rh, :].astype(F32)
        xhat, scale = norm_rows(xf[r, :].astype(F32))
        gg = g * vec(gain)
        m1 = jnp.mean(gg, axis=-1, keepdims=True)
        m2 = jnp.mean(gg * xhat, axis=-1, keepdims=True)
        ig_own[...] = gm[rh, :] + scale * (gg - m1 - xhat * m2)
        ig_send[rh, :] = ig_own[:, other].astype(BF16)
        ig_copy(j).start()
        ig[r, :] = ig_own[:, mine].astype(BF16)
        g1 += jnp.sum(g * xhat, axis=0, keepdims=True)
        s1 += jnp.sum(g, axis=0, keepdims=True)
    put(0, g1)
    put(dr, s1)

    def vec_copy(step):
        if step == 0:
            top = pl.ds(0, shared)
            return remote(sums.at[top], sums_box.at[0, top], narrow, 2 * each, peer)
        return remote(sums, sums_box.at[step], across, 10 * steps + step - 1, {"wide": flip(me, step - 1)})

    def vec_end(step):
        vec_copy(step).wait()
        if step == 0:
            sums[0:shared, :] += sums_box[0, 0:shared, :]
        else:
            sums[...] += sums_box[step]
        if step < steps:
            vec_copy(step + 1).start()

    vec_copy(0).start()
    for step in range(1, steps):
        scatter_step(step)
        vec_end(step - 1)
    for step in range(2, steps):
        gather_step(gathers, step)
    vec_end(steps - 1)
    for step in range(steps):
        gather_step(scatters, step)
    vec_end(steps)
    small[...] = sums[...]
    for j in range(each):
        ig_copy(j).wait()


def last_call(dq, dk, dv, low, w, xf, gm, gain, up_own, gp_sum, s_ub, s_db, s_g2, s_s2, s_pb, wide):
    rows, lw = dq.shape
    d, f = xf.shape[1], s_ub.shape[1]
    cw, half = d // 2, rows // 2
    block = min(256, half)
    each, steps = half // block, bits(wide)
    sd, vm = jax.ShapeDtypeStruct, pltpu.VMEM
    chain = Chain(0, order_of(wide, 0), d)
    vec_rows = -(-6 * d // 1024) * 8 + -(-(f + 2 * lw) // 1024) * 8
    return pl.pallas_call(
        functools.partial(last_body, wide=wide),
        out_shape=(sd((rows, cw), BF16), sd((d, f), BF16), sd((2 * lw, cw), BF16))
        + (sd((d, lw), BF16),) * 3 + (sd((vec_rows, 128), F32),),
        in_specs=[vmem()] * 3 + [anywhere()] * 3 + [vmem()] * 9,
        out_specs=(vmem(),) * 7,
        scratch_shapes=[
            vm((rows, d), BF16), vm(w.shape, BF16), vm((rows, d), BF16), vm((half, d), BF16), vm((half, d), BF16),
            vm((half, d), F32), vm((block, d), F32), vm((half, cw), BF16), vm((3, d, lw), BF16),
            vm((3, chain.box_rows, lw), BF16), vm((3, d // 2, lw), BF16), vm((3, chain.size, lw), BF16),
            vm((vec_rows, 128), F32), vm((steps + 1, vec_rows, 128), F32),
        ]
        + sems(3, 2 * each + 1, 2 * each + 1, 11 * steps, 11 * steps),
        compiler_params=params(collective_id=5, has_side_effects=True),
        cost_estimate=cost(2 * rows * d * 6 * lw, 2 * rows * d * 8),
        name="last",
    )(dq, dk, dv, low, w, xf, gm, gain, up_own, gp_sum, s_ub, s_db, s_g2, s_s2, s_pb)


def finish_body(
    lo, lo_got, bias, ig, up, down, q, k, v, p0, p1, small,
    out, ig_out, o_qkv, o_qvb, o_proj, o_pb, o_up, o_ub, o_down, o_db, o_g1, o_s1, o_g2, o_s2,
    *, factor, dr, shared,
):
    n = lax.axis_index("narrow")
    cw = lo.shape[1]
    out[...] = (lo[...] + lo_got[...].astype(F32) + bias[:, lane_part(n, cw)]).astype(BF16)
    ig_out[...] = ig[...]
    for c, ref in enumerate((q, k, v)):
        o_qkv[c] = ref[...].astype(F32) * factor
    o_proj[:, :cw] = p0[...].astype(F32) * factor
    o_proj[:, cw:] = p1[...].astype(F32) * factor
    o_up[...] = up[...].astype(F32) * factor
    o_down[...] = down[...].astype(F32) * factor

    @pl.when(pl.program_id(0) == 0)
    def _():
        for i, ref in enumerate((o_g1, o_s1, o_g2, o_s2, o_pb, o_db)):
            ref[...] = small[i * dr : (i + 1) * dr, :] * factor
        fr = o_ub.shape[0]
        o_ub[...] = small[shared : shared + fr, :] * factor
        lr = o_qvb.shape[1] // 128
        for c in range(2):
            for i in range(lr):
                at = shared + fr + c * lr + i
                o_qvb[c : c + 1, i * 128 : (i + 1) * 128] = small[at : at + 1, :] * factor


def finish_call(lo, lo_got, bias, ig, up, down, q, k, v, p, small, factor, grid=8):
    rows, cw = lo.shape
    (d, f), lw = up.shape, q.shape[1]
    dr, shared = d // 128, -(-6 * d // 1024) * 8
    sd = jax.ShapeDtypeStruct
    tiny = [sd((dr, 128), F32)] * 2
    shapes = (
        [sd((rows, cw), BF16), sd((rows, cw), BF16), sd((3, d, lw), F32), sd((2, lw), F32), sd((lw, d), F32)]
        + [sd((dr, 128), F32), sd((d, f), F32), sd((f // 128, 128), F32), sd((f, d), F32)]
        + [sd((dr, 128), F32)] * 5
    )
    big = lambda a: rows_spec(a.shape[0] // grid, a.shape[1])
    pb = lw // grid
    specs = []
    for i, s in enumerate(shapes):
        if len(s.shape) == 3:
            specs.append(pl.BlockSpec((3, d // grid, lw), lambda i, *_: (0, i, 0)))
        elif i in (0, 1, 4, 6, 8):
            specs.append(big(s))
        else:
            specs.append(whole_spec(s.shape))
    return pl.pallas_call(
        functools.partial(finish_body, factor=factor, dr=dr, shared=shared),
        out_shape=tuple(shapes),
        grid=(grid,),
        in_specs=[big(lo), big(lo_got), whole_spec(bias.shape), big(ig), big(up), big(down), big(q), big(k), big(v)]
        + [rows_spec(pb, cw), rows_spec(pb, cw, grid), whole_spec(small.shape)],
        out_specs=tuple(specs),
        compiler_params=params(),
        cost_estimate=cost(up.size * 8, up.size * 24),
        name="finish",
    )(lo, lo_got, bias, ig, up, down, q, k, v, p, p, small)


def on_device(
    tokens, lengths, qkv_weight, qv_bias, proj_weight, proj_bias, up_weight, up_bias,
    down_weight, down_bias, first_gain, first_shift, second_gain, second_shift, cotangent,
):
    cw = tokens.shape[1]
    d, ff, lw = 2 * cw, up_weight.shape[1], proj_weight.shape[0]
    wide = lax.axis_size("wide")
    w3 = jnp.transpose(qkv_weight, (1, 0, 2))

    xf, low, q, k, v = qkv_call(tokens, w3, qv_bias, first_gain, first_shift)
    mixed, qa, mixed_got, proj_got = attend_forward(lengths, q, k, v, proj_weight)
    lo, lo_send, gmix, gm, gup, down_own, gp_own, gp_other, s_ub, s_db, s_g2, s_s2, s_pb = mlp_call(
        lengths, xf, mixed, mixed_got, proj_weight, proj_got, proj_bias, second_gain, second_shift,
        up_weight, up_bias, down_weight, cotangent, wide,
    )
    dq, dk, dv, lo_got, gdown, up_own, gp_sum = attend_backward(
        lengths, qa, k, v, gmix, mixed, lo_send, gup, down_own, gp_own, gp_other, wide
    )
    ig, gup, gp, gq, gk, gv, small = last_call(
        dq, dk, dv, low, w3, xf, gm, first_gain, up_own, gp_sum, s_ub, s_db, s_g2, s_s2, s_pb, wide
    )
    out, ig, o_qkv, o_qvb, o_proj, *rest = finish_call(
        lo, lo_got, down_bias.astype(F32).reshape(1, -1), ig, gup, gdown, gq, gk, gv, gp, small,
        1.0 / (lengths.shape[0] * wide),
    )
    pb, up, ubs, down, dbs, g1, s1, g2, s2 = rest
    flat = lambda a: a.reshape(-1)
    return (
        out, ig, jnp.transpose(o_qkv, (1, 0, 2)), o_qvb, o_proj, flat(pb), up, flat(ubs), down, flat(dbs),
        flat(g1), flat(s1), flat(g2), flat(s2),
    )


def solution(mesh):
    split = P("wide", "narrow")
    none3, cols, rows1 = P(None, None, "narrow"), P(None, "narrow"), P("narrow", None)
    return jax.shard_map(
        on_device,
        mesh=mesh,
        in_specs=(
            split, P("wide"), none3, cols, rows1, P(), cols, P("narrow"), rows1, P(), P(), P(), P(), P(), split,
        ),
        out_specs=(
            split, split, none3, cols, rows1, P(), cols, P("narrow"), rows1, P(), P(), P(), P(), P(),
        ),
        check_vma=False,
    )
```

```python
import functools

import jax
import jax.numpy as jnp
from jax import lax
from jax.experimental import pallas as pl
from jax.experimental.pallas import tpu as pltpu
from jax.sharding import PartitionSpec as P

EPS = 1e-05
HEAD = 64
F32, BF16 = jnp.float32, jnp.bfloat16
NT = (((1,), (1,)), ((), ()))
TN = (((0,), (0,)), ((), ()))
GELU_A, GELU_B = 0.7978845608028654, 0.044715
VMEM_LIMIT = 63 * 1024 * 1024


def dot(a, b):
    return jnp.dot(a, b, preferred_element_type=F32)


def dot_nt(a, b):
    return lax.dot_general(a, b, NT, preferred_element_type=F32)


def dot_tn(a, b):
    return lax.dot_general(a, b, TN, preferred_element_type=F32)


def params(**more):
    return pltpu.CompilerParams(vmem_limit_bytes=VMEM_LIMIT, **more)


def cost(flops, size, trans=0):
    return pl.CostEstimate(flops=int(flops), bytes_accessed=int(size), transcendentals=int(trans))


def lane_part(which, width):
    return pl.ds(pl.multiple_of(which * width, 128), width)


def norm_rows(x):
    mean = jnp.mean(x, axis=-1, keepdims=True)
    cen = x - mean
    var = jnp.mean(cen * cen, axis=-1, keepdims=True)
    r = lax.rsqrt(var + EPS)
    return cen * r, r


def rows_spec(rows, cols, base=0):
    return pl.BlockSpec((rows, cols), lambda i, *_: (i + base, 0))


def whole_spec(shape):
    zeros = (0,) * len(shape)
    return pl.BlockSpec(shape, lambda i, *_: zeros)


MESH = pl.DeviceIdType.MESH
scope = jax.named_scope


def vec(ref):
    return ref[...].astype(F32).reshape(1, -1)


def bit_of(index, bit):
    return (index // (1 << bit)) % 2


def flip(index, bit):
    return index + (1 - 2 * bit_of(index, bit)) * (1 << bit)


def greet(peers):
    barrier = pltpu.get_barrier_semaphore()
    for peer in peers:
        pl.semaphore_signal(barrier, inc=1, device_id=peer, device_id_type=MESH)
    pl.semaphore_wait(barrier, len(peers))


def remote(src, dst, sems, at, peer):
    return pltpu.make_async_remote_copy(
        src_ref=src, dst_ref=dst, send_sem=sems[0].at[at], recv_sem=sems[1].at[at],
        device_id=peer, device_id_type=MESH,
    )


def block_rows(start, size, unit=16):
    return pl.ds(start if isinstance(start, int) else pl.multiple_of(start, unit), size)


class Chain:
    def __init__(self, me, order, rows, cols, sems, at):
        self.me, self.cols, self.sems, self.at = me, cols, sems, at
        self.steps, self.splits = [], []
        base, size, box = 0, rows, 0
        for bit in order:
            if size % 32 == 0:
                half = size // 2
                mine = bit_of(me, bit)
                keep, give = base + mine * half, base + (1 - mine) * half
                self.splits.append((bit, keep, half))
            else:
                half, keep, give = size, base, base
            self.steps.append((bit, keep, give, half, box))
            base, size, box = keep, half, box + half
        self.base, self.size, self.box_rows = base, size, box

    def bind(self, src, box, part, own, dst=None, entry=0):
        self.src, self.box, self.part, self.own, self.dst, self.entry = src, box, part, own, dst, entry
        return self

    def _source(self, step):
        off = 0 if step == 0 else self.steps[0][1]
        return (self.src if step == self.entry else self.part), off

    def _scatter_copy(self, step):
        bit, _, give, half, box = self.steps[step]
        source, off = self._source(step)
        return remote(
            source.at[block_rows(give - off, half), self.cols],
            self.box.at[pl.ds(box, half), self.cols],
            self.sems, self.at + step, {"wide": flip(self.me, bit)},
        )

    def scatter_start(self, step):
        self._scatter_copy(step).start()

    def scatter_end(self, step):
        self._scatter_copy(step).wait()
        _, keep, _, half, box = self.steps[step]
        source, off = self._source(step)
        last = step == len(self.steps) - 1
        target, out = (self.own, keep) if last else (self.part, self.steps[0][1])
        unit = next(u for u in (96, 64, 48, 32, 16) if half % u == 0)

        def add(i, carry):
            at = i * unit
            got = self.box[block_rows(box + at, unit), self.cols]
            mine = source[block_rows(keep - off + at, unit), self.cols]
            target[block_rows(keep - out + at, unit), self.cols] = got + mine
            return carry

        lax.fori_loop(0, half // unit, add, 0)

    def gather_open(self, sem):
        region = self.dst.at[block_rows(self.base, self.size), self.cols]
        return pltpu.make_async_copy(self.own.at[:, self.cols], region, sem)

    def _gather_copy(self, step):
        bit, keep, half = self.splits[len(self.splits) - 1 - step]
        region = self.dst.at[block_rows(keep, half), self.cols]
        at = self.at + len(self.steps) + step
        return remote(region, region, self.sems, at, {"wide": flip(self.me, bit)})

    def gather_start(self, step):
        self._gather_copy(step).start()

    def gather_end(self, step):
        self._gather_copy(step).wait()


class Group:
    def __init__(self, chains, open_sem=None, at=0, entry=0, leave=None):
        self.chains, self.open_sem, self.at = chains, open_sem, at
        steps, splits = len(chains[0].steps), len(chains[0].splits)
        self.last = steps
        self.ops = [("scatter", i) for i in range(entry, steps if leave is None else leave)]
        if leave is None:
            self.ops += [("gather", i) for i in range(splits)]
        self.pos = -1

    @property
    def done(self):
        return self.pos >= len(self.ops)

    def next(self):
        pos = self.pos
        self.pos = min(pos + 1, len(self.ops))

        def tick():
            if pos >= len(self.ops):
                return
            if pos >= 0:
                kind, i = self.ops[pos]
                for chain in self.chains:
                    (chain.scatter_end if kind == "scatter" else chain.gather_end)(i)
            if pos + 1 >= len(self.ops):
                return
            kind, i = self.ops[pos + 1]
            if kind == "gather" and i == 0:
                opens = [c.gather_open(self.open_sem.at[self.at + j]) for j, c in enumerate(self.chains)]
                for opened in opens:
                    opened.start()
                for opened in opens:
                    opened.wait()
            for chain in self.chains:
                (chain.scatter_start if kind == "scatter" else chain.gather_start)(i)

        return tick

    def tick(self):
        self.next()()


def bits(wide):
    return wide.bit_length() - 1


def order_of(wide, kind):
    steps = list(range(bits(wide)))
    return steps if kind == 0 else [0] + steps[2:] + steps[1:2]


def lanes_split(cols):
    w = max(128, cols // 6 // 128 * 128)
    return [(0, pl.ds(0, cols - w)), (1, pl.ds(cols - w, w))]


def wide_peers(me, wide):
    return [{"wide": flip(me, b)} for b in range(bits(wide))]


def vmem():
    return pl.BlockSpec(memory_space=pltpu.VMEM)


def anywhere():
    return pl.BlockSpec(memory_space=pl.ANY)


def sems(*counts):
    return [pltpu.SemaphoreType.DMA((c,)) for c in counts]


def qkv_body(own_hbm, own, w, bias, gain, shift, xf, low, q, k, v, got, send_sem, recv_sem):
    n = lax.axis_index("narrow")
    i = pl.program_id(0)
    rows, cw = own.shape
    peer = {"narrow": 1 - n}

    def copy(at):
        block = block_rows(at * rows, rows)
        return remote(own_hbm.at[block], got.at[block], (send_sem, recv_sem), at, peer)

    @pl.when(i == 0)
    def _():
        greet([peer])
        for at in range(got.shape[0] // rows):
            copy(at).start()

    xf[:, lane_part(n, cw)] = own[...]
    with scope("wait"):
        copy(i).wait()
    xf[:, lane_part(1 - n, cw)] = got[block_rows(i * rows, rows), :]
    xhat, _ = norm_rows(xf[...].astype(F32))
    y = (xhat * vec(gain) + vec(shift)).astype(BF16)
    low[...] = y
    q[...] = (dot(y, w[0]) + bias[0:1, :].astype(F32)).astype(BF16) * jnp.asarray(HEAD**-0.5, BF16)
    k[...] = dot(y, w[1]).astype(BF16)
    v[...] = (dot(y, w[2]) + bias[1:2, :].astype(F32)).astype(BF16)


def qkv_call(own, w, bias, gain, shift, block=256):
    rows, cw = own.shape
    d, lw = w.shape[1], w.shape[2]
    sd = jax.ShapeDtypeStruct
    return pl.pallas_call(
        qkv_body,
        out_shape=(sd((rows, d), BF16), sd((rows, d), BF16)) + (sd((rows, lw), BF16),) * 3,
        grid_spec=pltpu.PrefetchScalarGridSpec(
            num_scalar_prefetch=0,
            grid=(rows // block,),
            in_specs=[anywhere(), rows_spec(block, cw)] + [whole_spec(a.shape) for a in (w, bias, gain, shift)],
            out_specs=[rows_spec(block, d)] * 2 + [rows_spec(block, lw)] * 3,
            scratch_shapes=[pltpu.VMEM((rows, cw), BF16)] + sems(rows // block, rows // block),
        ),
        compiler_params=params(collective_id=1, has_side_effects=True),
        cost_estimate=cost(2 * rows * d * 3 * lw, 2 * (rows * d * 5 + w.size)),
        name="norm_qkv",
    )(own, own, w, bias, gain, shift)


def three(x):
    hi = x.astype(BF16).astype(F32)
    mid = (x - hi).astype(BF16).astype(F32)
    return hi, mid, x - hi - mid


def lanes_of(par):
    lane = lax.broadcasted_iota(jnp.int32, (1, 2 * HEAD), 1)
    mine = (lane // HEAD) == par
    return lane, mine, (1 - par) * HEAD


def place(lane, mine, at, base, terms):
    out = jnp.where(mine, base, 0.0)
    for i, term in enumerate(terms):
        out = jnp.where(lane == at + i, term, out)
    return out


def fwd_body(
    len_ref, q, k, v, pw, o, qa_out, o_got, pw_got, ka, va, send_sem, recv_sem, *, bq
):
    head = pl.program_id(0)
    par, pair = head % 2, head // 2
    lane, mine, at = lanes_of(par)
    n, me = lax.axis_index("narrow"), lax.axis_index("wide")
    peer, core = {"narrow": 1 - n}, {"wide": flip(me, 0)}
    pairs = pl.num_programs(0) // 2
    both = (send_sem, recv_sem)
    cols = lane_part(pair, 2 * HEAD)
    part = block_rows((me % 2) * (pw.shape[0] // 2), pw.shape[0] // 2)
    npairs = o.shape[1] // (2 * HEAD)
    weights = remote(pw.at[part], pw_got.at[part], both, npairs, peer)
    shared = remote(pw_got.at[part], pw_got.at[part], both, npairs + 1, core)

    @pl.when(head == 0)
    def _():
        greet([peer, core])
        weights.start()

    keys = k.shape[0]
    kpos = lax.broadcasted_iota(jnp.int32, (keys, 1), 0)
    kbias = jnp.where(kpos < len_ref[0], 0.0, -1e30)
    ka[...] = place(lane, mine, at, k[...].astype(F32), [kbias]).astype(BF16)
    va[...] = place(lane, mine, at, v[...].astype(F32), [1.0]).astype(BF16)
    tri = lax.broadcasted_iota(jnp.int32, (bq, bq), 1) <= lax.broadcasted_iota(jnp.int32, (bq, bq), 0)
    for i in range(q.shape[0] // bq):
        nk = (i + 1) * bq
        rows = pl.ds(i * bq, bq)
        qf = q[rows, :].astype(F32)
        qa = place(lane, mine, at, qf, [1.0])
        s = dot_nt(qa.astype(BF16), ka[0:nk, :])
        edge = jnp.where(tri, s[:, nk - bq :], -1e30)
        m = jnp.max(edge, axis=1, keepdims=True)
        if nk > bq:
            m = jnp.maximum(m, jnp.max(s[:, : nk - bq], axis=1, keepdims=True))
        pv = dot(jnp.exp(edge - m).astype(BF16), va[nk - bq : nk, :])
        if nk > bq:
            pv += dot(jnp.exp(s[:, : nk - bq] - m).astype(BF16), va[0 : nk - bq, :])
        total = jnp.sum(jnp.where(lane == at, pv, 0.0), axis=1, keepdims=True)
        out = (pv / total).astype(BF16).astype(F32)
        old = o[rows, cols].astype(F32)
        o[rows, cols] = jnp.where(mine, out, jnp.where(par == 0, 0.0, old)).astype(BF16)
        lse = m + jnp.log(total)
        qa_out[0, rows, :] = place(lane, mine, at, qf, [1.0, *three(lse)]).astype(BF16)

    def mixed(j):
        c = pl.ds(j * 2 * HEAD, 2 * HEAD)
        return remote(o.at[:, c], o_got.at[:, c], both, j, peer)

    for j in range(npairs):

        @pl.when(head == 2 * j + 1)
        def _():
            mixed(j).start()

    @pl.when(head == 3)
    def _():
        weights.wait()
        shared.start()

    @pl.when(head == 2 * npairs - 1)
    def _():
        shared.wait()
        for j in range(npairs):
            mixed(j).wait()


def attend_forward(length, q, k, v, pw, bq=256):
    rows, width = q.shape
    heads, pair = width // HEAD, 2 * HEAD
    half = lambda h, *_: (0, h // 2)
    sd = jax.ShapeDtypeStruct
    work = 2 * heads * rows * rows * HEAD
    return pl.pallas_call(
        functools.partial(fwd_body, bq=bq),
        out_shape=(
            sd((rows, width), BF16), sd((heads, rows, pair), BF16), sd((rows, width), BF16), sd(pw.shape, BF16),
        ),
        grid_spec=pltpu.PrefetchScalarGridSpec(
            num_scalar_prefetch=1,
            grid=(heads,),
            in_specs=[pl.BlockSpec((rows, pair), half)] * 3 + [anywhere()],
            out_specs=[vmem(), pl.BlockSpec((1, rows, pair), lambda h, *_: (h, 0, 0)), anywhere(), anywhere()],
            scratch_shapes=[pltpu.VMEM((rows, pair), BF16)] * 2 + sems(heads // 2 + 2, heads // 2 + 2),
        ),
        compiler_params=params(collective_id=2, has_side_effects=True),
        cost_estimate=cost(4 * work, 2 * rows * width * 6, work // 256),
        name="attend_fwd",
    )(length, q, k, v, pw)


def mlp_body(
    len_ref, xf_hbm, mo_hbm, mr_hbm, pwo_hbm, pwr_hbm, pb, gain, shift, ub, up_hbm, down_hbm, cot_hbm,
    lo_out, lo_send_out, gmix, gm_out, gup_out, down_part, gp_own, gp_other, sum_ub, sum_db, sum_g, sum_s, sum_pb,
    xf, mo, mr, pwo, pwr, up, down, cot, cot_got, cf, lo, lo_send, mid, second, active, slope, gh,
    gs_send, gs_got, gs_own, gdown, gup, box, gm, glow, gmix_send, load_sem, store_sem, nsend, nrecv, wsend, wrecv,
    *, wide,
):
    n, me = lax.axis_index("narrow"), lax.axis_index("wide")
    peer = {"narrow": 1 - n}
    rows, cw = cot.shape
    d, f = up.shape
    half, block = rows // 2, min(256, rows // 2)
    each = half // block
    mine, other = lane_part(n, cw), lane_part(1 - n, cw)
    narrow, across = (nsend, nrecv), (wsend, wrecv)
    count = iter(range(16))

    def load(src, dst):
        copy = pltpu.make_async_copy(src, dst, load_sem.at[next(count)])
        copy.start()
        return copy

    his, own = block_rows((1 - n) * half, half), block_rows(n * half, half)
    first = [load(a, b) for a, b in ((pwo_hbm, pwo), (pwr_hbm, pwr))]
    first += [load(a.at[his], b.at[his]) for a, b in ((xf_hbm, xf), (mo_hbm, mo), (mr_hbm, mr))]
    up_load = load(up_hbm, up)
    greet([peer] + wide_peers(me, wide))

    def cot_copy(side, j, a):
        r = block_rows(side * half + j * block, block)
        return remote(cot_hbm.at[r], cot_got.at[r], narrow, a * each + j, peer)

    for a, side in enumerate((n, 1 - n)):
        for j in range(each):
            cot_copy(side, j, a).start()
    down_load = load(down_hbm, down)
    cot_load = load(cot_hbm, cot)
    rest = [load(a.at[own], b.at[own]) for a, b in ((xf_hbm, xf), (mo_hbm, mo), (mr_hbm, mr))]

    def project(at):
        r = block_rows(at, block)
        m = xf[r, :].astype(F32) + (dot(mo[r, :], pwo[...]) + dot(mr[r, :], pwr[...])) + vec(pb)
        mid[r, :] = m
        xhat, _ = norm_rows(m)
        second[r, :] = (xhat * vec(gain) + vec(shift)).astype(BF16)

    def forward(at):
        r = block_rows(at, block)
        hid = dot(second[r, :], up[...]) + vec(ub)
        sq = hid * hid
        t = jnp.tanh(GELU_A * (hid + GELU_B * (sq * hid)))
        hf = 0.5 * (1.0 + t)
        act = (hid * hf).astype(BF16)
        active[r, :] = act
        slope[r, :] = hf + (0.5 * hid) * (1.0 - t * t) * (GELU_A + (3.0 * GELU_A * GELU_B) * sq)
        lo[r, :] = mid[r, mine] + dot(act, down[:, mine])
        lo_send[r, :] = dot(act, down[:, other]).astype(BF16)

    def backward(at):
        r = block_rows(at, block)
        pos = at + lax.broadcasted_iota(jnp.int32, (block, 1), 0)
        live = (pos < len_ref[0]).astype(F32)
        cf[r, mine] = (cot[r, :].astype(F32) * live).astype(BF16)
        cf[r, other] = (cot_got[r, :].astype(F32) * live).astype(BF16)
        ghid = (dot_nt(cf[r, :], down[...]) * slope[r, :]).astype(BF16)
        gh[r, :] = ghid
        sum_ub[...] += jnp.sum(ghid.astype(F32), axis=0, keepdims=True)
        return dot_nt(ghid, up[...])

    def every(side, body):
        def step(j, carry):
            body(side * half + j * block)
            return carry

        lax.fori_loop(0, each, step, 0)

    def both(at):
        project(at)
        forward(at)

    for ref in (sum_ub, sum_g, sum_s, sum_pb, sum_db):
        ref[...] = jnp.zeros_like(ref)
    with scope("load"):
        for copy in first:
            copy.wait()
    with scope("project"):
        every(1 - n, project)
    with scope("load2"):
        up_load.wait()
        down_load.wait()
    with scope("fwd_peer"):
        every(1 - n, forward)
    with scope("cot_wait"):
        cot_load.wait()
        for j in range(each):
            cot_copy(n, j, 0).wait()

    def gs_copy(j):
        r = block_rows(j * block, block)
        return remote(gs_send.at[r], gs_got.at[r], narrow, 2 * each + j, peer)

    def for_peer(j, carry):
        gs_send[block_rows(j * block, block), :] = backward((1 - n) * half + j * block).astype(BF16)
        gs_copy(j).start()
        return carry

    def for_own(j, carry):
        gs_own[block_rows(j * block, block), :] = backward(n * half + j * block)
        return carry

    with scope("for_peer"):
        lax.fori_loop(0, each, for_peer, 0)
    for copy in rest:
        copy.wait()
    with scope("fwd_own"):
        every(n, both)
    stores = []

    def store(src, dst):
        copy = pltpu.make_async_copy(src, dst, store_sem.at[len(stores)])
        copy.start()
        stores.append(copy)

    store(lo, lo_out)
    store(lo_send, lo_send_out)
    with scope("cot_wait2"):
        for j in range(each):
            cot_copy(1 - n, j, 1).wait()
    with scope("for_own"):
        lax.fori_loop(0, each, for_own, 0)

    def weight(dst, left, right):
        def step(i, carry):
            c = block_rows(i * 256, 256, 256)
            dst[c, :] = dot_tn(left[:, c], right[...]).astype(BF16)
            return carry

        lax.fori_loop(0, dst.shape[0] // 256, step, 0)

    chains = []
    for kind, cols in lanes_split(d):
        chain = Chain(me, order_of(wide, kind), f, cols, across, len(chains) * bits(wide))
        chains.append(chain.bind(gdown, box, down_part, None))
    reduce_down = Group(chains, leave=2)
    with scope("w_down"):
        weight(gdown, active, cf)
    reduce_down.tick()
    with scope("w_up"):
        weight(gup, second, gh)
    store(gup, gup_out)
    with scope("core"):
        reduce_down.tick()
    with scope("gs_wait"):
        for j in range(each):
            gs_copy(j).wait()

    def gmix_copy(j):
        r = block_rows(n * half + j * block, block)
        return remote(gmix_send.at[block_rows(j * block, block)], gmix.at[r], narrow, 3 * each + j, peer)

    def back_norm(j, carry):
        r, rh = block_rows(n * half + j * block, block), block_rows(j * block, block)
        g = gs_own[rh, :] + gs_got[rh, :].astype(F32)
        xhat, scale = norm_rows(mid[r, :])
        gg = g * vec(gain)
        m1 = jnp.mean(gg, axis=-1, keepdims=True)
        m2 = jnp.mean(gg * xhat, axis=-1, keepdims=True)
        c = cf[r, :].astype(F32)
        grad = c + scale * (gg - m1 - xhat * m2)
        gm[rh, :] = grad
        gl = grad.astype(BF16)
        glow[rh, :] = gl
        gmix_send[rh, :] = dot_nt(gl, pwr[...]).astype(BF16)
        gmix_copy(j).start()
        gmix[r, :] = dot_nt(gl, pwo[...]).astype(BF16)
        sum_g[...] += jnp.sum(g * xhat, axis=0, keepdims=True)
        sum_s[...] += jnp.sum(g, axis=0, keepdims=True)
        sum_pb[...] += jnp.sum(grad, axis=0, keepdims=True)
        sum_db[...] += jnp.sum(c, axis=0, keepdims=True)
        return carry

    with scope("back_norm"):
        lax.fori_loop(0, each, back_norm, 0)
    store(gm, gm_out)
    with scope("proj"):
        lw = mo.shape[1]
        for src, dst in ((mr, gp_other), (mo, gp_own)):
            total = dot_tn(src[own, :], glow[...]).astype(BF16)
            dst[0:lw, :] = total[:, :cw]
            dst[lw : 2 * lw, :] = total[:, cw:]
    with scope("gmix_wait"):
        for j in range(each):
            gmix_copy(j).wait()
    with scope("across"):
        reduce_down.tick()
    with scope("store"):
        for copy in stores:
            copy.wait()


def mlp_call(length, xf, mo, mr, pwo, pwr, pb, gain, shift, up, ub, down, cot, wide):
    rows, d = xf.shape
    f, lw, cw = up.shape[1], mo.shape[1], cot.shape[1]
    half = rows // 2
    sd, vm = jax.ShapeDtypeStruct, pltpu.VMEM
    each = half // min(256, half)
    return pl.pallas_call(
        functools.partial(mlp_body, wide=wide),
        out_shape=(
            sd((rows, cw), F32), sd((rows, cw), BF16), sd((rows, lw), BF16), sd((half, d), F32),
            sd((d, f), BF16), sd((f // 2, d), BF16), sd((2 * lw, cw), BF16), sd((2 * lw, cw), BF16),
            sd((1, f), F32), sd((1, d), F32), sd((1, d), F32), sd((1, d), F32), sd((1, d), F32),
        ),
        in_specs=[pl.BlockSpec(memory_space=pltpu.SMEM)] + [anywhere()] * 5 + [vmem()] * 4 + [anywhere()] * 3,
        out_specs=(anywhere(), anywhere(), vmem(), anywhere(), anywhere()) + (vmem(),) * 8,
        scratch_shapes=[
            vm((rows, d), BF16), vm((rows, lw), BF16), vm((rows, lw), BF16), vm((lw, d), BF16), vm((lw, d), BF16),
            vm((d, f), BF16), vm((f, d), BF16), vm((rows, cw), BF16), vm((rows, cw), BF16), vm((rows, d), BF16),
            vm((rows, cw), F32), vm((rows, cw), BF16), vm((rows, d), F32),
            vm((rows, d), BF16), vm((rows, f), BF16), vm((rows, f), F32), vm((rows, f), BF16),
            vm((half, d), BF16), vm((half, d), BF16), vm((half, d), F32), vm((f, d), BF16), vm((d, f), BF16),
            vm((f - f // 4, d), BF16), vm((half, d), F32), vm((half, d), BF16), vm((half, lw), BF16),
        ]
        + sems(16, 4, 4 * each, 4 * each, 2 * bits(wide), 2 * bits(wide)),
        compiler_params=params(collective_id=3, has_side_effects=True),
        cost_estimate=cost(2 * rows * d * (d + 6 * f), 2 * (rows * d * 8 + 2 * d * f), rows * f),
        name="mlp",
    )(length, xf, mo, mr, pwo, pwr, pb, gain, shift, ub, up, down, cot)


def back_body(
    len_ref, qa_hbm, k_hbm, v_hbm, do_hbm, o_hbm, low_hbm, w_hbm, xf_hbm, gm_hbm, gain, lo_send, gup_hbm,
    down_part_hbm, gp_own_hbm, gp_other_hbm, s_ub, s_db, s_g2, s_s2, s_pb,
    lo_got, down_out, up_out, gp_out, g0_out, g1_out, g2_out, ig, small,
    qa, k, v, do, o, low, wp, xf, gm, gup, down_part, gp_src, gp_got,
    ka, va, dk_acc, dv_acc, dqkv, gpair,
    down_box, down_part2, down_own, up_box, up_part, up_own, gp_box, gp_part, gp_own, pair_box, pair_part, pair_own,
    gn_send, gn_got, gn_own, ig_own, ig_send, sums, sums_box,
    load_sem, open_sem, nsend, nrecv, wsend, wrecv, *, bq, wide,
):
    n, me = lax.axis_index("narrow"), lax.axis_index("wide")
    peer = {"narrow": 1 - n}
    narrow, across = (nsend, nrecv), (wsend, wrecv)
    steps = bits(wide)
    heads, rows = qa.shape[0], qa.shape[1]
    pair_w = 2 * HEAD
    pairs = heads // 2
    d, lw = gain.shape[0], k.shape[1]
    cw = d // 2
    half, block = rows // 2, min(256, rows // 2)
    each = half // block
    count = iter(range(64))

    def load(src, dst):
        copy = pltpu.make_async_copy(src, dst, load_sem.at[next(count)])
        copy.start()
        return copy

    pair_loads = []
    for p in range(pairs):
        c = pl.ds(p * pair_w, pair_w)
        pair_loads.append(
            [load(a.at[:, c], b.at[:, c]) for a, b in ((k_hbm, k), (v_hbm, v), (do_hbm, do), (o_hbm, o))]
            + [load(qa_hbm.at[pl.ds(2 * p, 2)], qa.at[pl.ds(2 * p, 2)])]
        )
    part_load = load(down_part_hbm, down_part)
    up_load = load(gup_hbm, gup)
    gp_load = load(gp_own_hbm, gp_src)
    low_load = load(low_hbm, low)
    greet([peer] + wide_peers(me, wide))
    gp_swap = remote(gp_other_hbm, gp_got, narrow, 0, peer)
    layer = remote(lo_send, lo_got, narrow, 1, peer)
    gp_swap.start()
    late = [
        load(w_hbm.at[c, :, pl.ds(p * pair_w, pair_w)], wp.at[p, :, pl.ds(c * pair_w, pair_w)])
        for p in range(pairs)
        for c in range(3)
    ]
    own_half = block_rows(n * half, half)
    late += [load(xf_hbm.at[own_half], xf), load(gm_hbm, gm)]

    at = iter(range(0, 64 * steps, 2 * steps))
    opening = iter(range(32))

    def group(src, box, part, own, dst, entry=0, cut=True):
        rows_, cols_ = dst.shape
        parts = lanes_split(cols_) if cut else [(0, pl.ds(0, cols_))]
        chains = []
        for kind, cols in parts:
            chain = Chain(me, order_of(wide, kind), rows_, cols, across, next(at))
            chains.append(chain.bind(src, box, part, own, dst, entry))
        first = [next(opening) for _ in chains][0]
        return Group(chains, open_sem, first, entry)

    down = group(down_part, down_box, down_part2, down_own, down_out, entry=2)
    up = group(gup, up_box, up_part, up_own, up_out)
    proj = group(gp_src, gp_box, gp_part, gp_own, gp_out, cut=False)
    qkv = [
        group(gpair.at[p], pair_box.at[p], pair_part.at[p], pair_own.at[p], out, cut=False)
        for p, out in zip(range(pairs), (g0_out, g1_out, g2_out))
    ]

    def tick(name, *groups):
        with scope(name):
            for g in groups:
                g.tick()

    part_load.wait()
    down.tick()
    up_load.wait()
    up.tick()

    kpos = lax.broadcasted_iota(jnp.int32, (rows, 1), 0)
    kbias = jnp.where(kpos < len_ref[0], 0.0, -1e30)
    tri = lax.broadcasted_iota(jnp.int32, (bq, bq), 0) <= lax.broadcasted_iota(jnp.int32, (bq, bq), 1)

    def plan(name, *groups):
        ticks = [g.next() for g in groups]

        def run():
            with scope(name):
                for one in ticks:
                    one()

        return run

    def start_proj(first):
        gp_swap.wait()
        gp_load.wait()
        gp_src[...] = gp_src[...] + gp_got[...]
        first()

    hooks = {
        (0, 1): [plan("t0", up)],
        (1, 1): [plan("t1", down, qkv[0])],
        (2, 1): [plan("t2", down, qkv[0]), layer.start],
        (3, 0): [plan("t3a", up)],
        (3, 1): [plan("t3", down, *qkv[:2]), functools.partial(start_proj, proj.next())],
        (4, 1): [plan("t4", up, down, *qkv[:2], proj)],
        (5, 1): [plan("t5", up, *qkv[:3], proj)],
    }

    def run_hooks(head, place_):
        for (h, where), actions in hooks.items():
            if where == place_:

                @pl.when(head == h)
                def _():
                    for action in actions:
                        action()

    def one_head(head, carry):
        par, pair = head % 2, head // 2
        lane, mine, extra = lanes_of(par)
        cols = lane_part(pair, pair_w)
        for p in range(pairs):

            @pl.when(head == 2 * p)
            def _():
                for copy in pair_loads[p]:
                    copy.wait()

        ka[...] = place(lane, mine, extra, k[:, cols].astype(F32), [kbias, -1.0, -1.0, -1.0]).astype(BF16)
        va[...] = place(lane, mine, extra, v[:, cols].astype(F32), [-1.0, -1.0, -1.0]).astype(BF16)
        dk_acc[...] = jnp.zeros_like(dk_acc)
        dv_acc[...] = jnp.zeros_like(dv_acc)

        def put(c, r, new):
            lanes = pl.ds(c * pair_w, pair_w)
            old = dqkv[pair, r, lanes].astype(F32)
            dqkv[pair, r, lanes] = jnp.where(mine, new, jnp.where(par == 0, 0.0, old)).astype(BF16)

        for i in range(rows // bq):
            r = pl.ds(i * bq, bq)
            qb = qa[head, r, :]
            df = do[r, cols].astype(F32)
            delta = jnp.sum(jnp.where(mine, df * o[r, cols].astype(F32), 0.0), axis=1, keepdims=True)
            db = place(lane, mine, extra, df, three(delta)).astype(BF16)
            dqs = None
            for j in range(i + 1):
                c = pl.ds(j * bq, bq)
                kb, vb = ka[c, :], va[c, :]
                s = dot_nt(kb, qb)
                if j == i:
                    s = jnp.where(tri, s, -1e30)
                p = jnp.exp(s)
                ds = (p * dot_nt(vb, db)).astype(BF16)
                dv_acc[c, :] += dot(p.astype(BF16), db)
                dk_acc[c, :] += dot(ds, qb)
                part = dot_tn(ds, kb)
                dqs = part if dqs is None else dqs + part
            put(0, r, dqs * HEAD**-0.5)
            if i == rows // bq - 2:
                run_hooks(head, 0)
        put(1, pl.ds(0, rows), dk_acc[...])
        put(2, pl.ds(0, rows), dv_acc[...])

        @pl.when(head == 1)
        def _():
            low_load.wait()

        @pl.when(par == 1)
        def _():
            with scope("weights"):
                gpair[pair] = dot_tn(low[...], dqkv[pair]).astype(BF16)

        run_hooks(head, 1)
        return carry

    lax.fori_loop(0, heads, one_head, 0)

    for copy in late:
        copy.wait()

    def gn_part(start):
        r = block_rows(start, block)
        total = dot_nt(dqkv[0, r, :], wp[0])
        for p in range(1, pairs):
            total += dot_nt(dqkv[p, r, :], wp[p])
        return total

    def gn_copy(j):
        r = pl.ds(j * block, block)
        return remote(gn_send.at[r], gn_got.at[r], narrow, 2 + j, peer)

    for j in range(each):
        gn_send[j * block : (j + 1) * block, :] = gn_part((1 - n) * half + j * block).astype(BF16)
        gn_copy(j).start()
        tick(f"p{j}", *qkv[::-1], proj)
    for j in range(each):
        gn_own[j * block : (j + 1) * block, :] = gn_part(n * half + j * block)
    tick("q0", up, down)

    sums[...] = jnp.zeros_like(sums)

    def put_sum(start, value):
        for i in range(value.shape[1] // 128):
            sums[start + i : start + i + 1, :] = value[:, i * 128 : (i + 1) * 128]

    dr, fr, lr = d // 128, s_ub.shape[1] // 128, lw // 128
    shared = -(-6 * dr // 8) * 8
    put_sum(2 * dr, s_g2[...])
    put_sum(3 * dr, s_s2[...])
    put_sum(4 * dr, s_pb[...])
    put_sum(5 * dr, s_db[...])
    put_sum(shared, s_ub[...])
    for p in range(pairs):
        put_sum(shared + fr + p, jnp.sum(dqkv[p, :, 0:pair_w].astype(F32), axis=0, keepdims=True))
        put_sum(shared + fr + lr + p, jnp.sum(dqkv[p, :, 2 * pair_w :].astype(F32), axis=0, keepdims=True))
    tick("q1", *qkv[::-1], proj)

    mine, other = lane_part(n, cw), lane_part(1 - n, cw)
    g1 = s1 = 0.0

    def ig_copy(j):
        r = block_rows(n * half + j * block, block)
        return remote(ig_send.at[pl.ds(j * block, block)], ig.at[r], narrow, 2 + each + j, peer)

    for j in range(each):
        with scope("gn_wait"):
            gn_copy(j).wait()
        rh = pl.ds(j * block, block)
        r = block_rows(n * half + j * block, block)
        g = gn_own[rh, :] + gn_got[rh, :].astype(F32)
        xhat, scale = norm_rows(xf[rh, :].astype(F32))
        gg = g * vec(gain)
        m1 = jnp.mean(gg, axis=-1, keepdims=True)
        m2 = jnp.mean(gg * xhat, axis=-1, keepdims=True)
        ig_own[...] = gm[rh, :] + scale * (gg - m1 - xhat * m2)
        ig_send[rh, :] = ig_own[:, other].astype(BF16)
        ig_copy(j).start()
        ig[r, :] = ig_own[:, mine].astype(BF16)
        g1 += jnp.sum(g * xhat, axis=0, keepdims=True)
        s1 += jnp.sum(g, axis=0, keepdims=True)
        tick(f"r{j}", *qkv[::-1], proj, up, down)
    put_sum(0, g1)
    put_sum(dr, s1)

    def vec_copy(step):
        if step == 0:
            top = pl.ds(0, shared)
            return remote(sums.at[top], sums_box.at[0, top], narrow, 2 + 2 * each, peer)
        slot = 2 * steps * 32 + step - 1
        return remote(sums, sums_box.at[step], across, slot, {"wide": flip(me, step - 1)})

    def vec_end(step):
        vec_copy(step).wait()
        if step == 0:
            sums[0:shared, :] += sums_box[0, 0:shared, :]
        else:
            sums[...] += sums_box[step]
        if step < steps:
            vec_copy(step + 1).start()

    vec_copy(0).start()
    todo = [*qkv[::-1], proj, up, down]
    step = 0
    while step <= steps or not all(g.done for g in todo):
        tick(f"s{step}", *todo)
        if step <= steps:
            vec_end(step)
        step += 1
    small[...] = sums[...]
    with scope("end"):
        layer.wait()
        for j in range(each):
            ig_copy(j).wait()


def back_call(
    length, qa, k, v, do, o, low, w, xf, gm, gain, lo_send, gup, down_part, gp_own, gp_other,
    s_ub, s_db, s_g2, s_s2, s_pb, wide, bq=256,
):
    heads, rows, pair = qa.shape
    d, f, lw = gain.shape[0], gup.shape[1], k.shape[1]
    cw, half = d // 2, rows // 2
    block = min(256, half)
    each, steps, pairs = half // block, bits(wide), heads // 2
    sd, vm = jax.ShapeDtypeStruct, pltpu.VMEM
    shape = lambda r: Chain(0, order_of(wide, 0), r, None, None, 0)
    c_down, c_up, c_gp = shape(f), shape(d), shape(2 * lw)
    vec_rows = -(-6 * d // 1024) * 8 + -(-(f + 2 * lw) // 1024) * 8
    work = 2 * heads * rows * rows * HEAD
    return pl.pallas_call(
        functools.partial(back_body, bq=bq, wide=wide),
        out_shape=(sd((rows, cw), BF16), sd((f, d), BF16), sd((d, f), BF16), sd((2 * lw, cw), BF16))
        + (sd((d, 3 * pair), BF16),) * 3 + (sd((rows, cw), BF16), sd((vec_rows, 128), F32)),
        in_specs=[pl.BlockSpec(memory_space=pltpu.SMEM)] + [anywhere()] * 9 + [vmem()] + [anywhere()] * 5 + [vmem()] * 5,
        out_specs=(anywhere(),) * 7 + (vmem(), vmem()),
        scratch_shapes=[
            vm(qa.shape, BF16), vm((rows, lw), BF16), vm((rows, lw), BF16), vm((rows, lw), BF16), vm((rows, lw), BF16),
            vm((rows, d), BF16), vm((pairs, d, 3 * pair), BF16), vm((half, d), BF16), vm((half, d), F32),
            vm((d, f), BF16), vm((f // 2, d), BF16), vm((2 * lw, cw), BF16), vm((2 * lw, cw), BF16),
            vm((rows, pair), BF16), vm((rows, pair), BF16), vm((rows, pair), F32), vm((rows, pair), F32),
            vm((pairs, rows, 3 * pair), BF16), vm((pairs, d, 3 * pair), BF16),
            vm((c_down.box_rows, d), BF16), vm((f // 2, d), BF16), vm((c_down.size, d), BF16),
            vm((c_up.box_rows, f), BF16), vm((d // 2, f), BF16), vm((c_up.size, f), BF16),
            vm((c_gp.box_rows, cw), BF16), vm((lw, cw), BF16), vm((c_gp.size, cw), BF16),
            vm((pairs, c_up.box_rows, 3 * pair), BF16), vm((pairs, d // 2, 3 * pair), BF16),
            vm((pairs, c_up.size, 3 * pair), BF16),
            vm((half, d), BF16), vm((half, d), BF16), vm((half, d), F32), vm((block, d), F32), vm((half, cw), BF16),
            vm((vec_rows, 128), F32), vm((steps + 1, vec_rows, 128), F32),
        ]
        + sems(64, 32, 3 + 2 * each, 3 + 2 * each, 65 * steps, 65 * steps),
        compiler_params=params(collective_id=4, has_side_effects=True),
        cost_estimate=cost(10 * work + 4 * rows * d * 3 * lw, 2 * rows * d * 20, work // 256),
        name="back",
    )(
        length, qa, k, v, do, o, low, w, xf, gm, gain, lo_send, gup, down_part, gp_own, gp_other,
        s_ub, s_db, s_g2, s_s2, s_pb,
    )


def finish_body(
    lo, lo_got, bias, ig, up, down, q, k, v, p0, p1, small,
    out, ig_out, o_qkv, o_qvb, o_proj, o_pb, o_up, o_ub, o_down, o_db, o_g1, o_s1, o_g2, o_s2,
    *, factor, dr, shared,
):
    n = lax.axis_index("narrow")
    cw = lo.shape[1]
    out[...] = (lo[...] + lo_got[...].astype(F32) + bias[:, lane_part(n, cw)]).astype(BF16)
    ig_out[...] = ig[...]
    for p, ref in enumerate((q, k, v)):
        for c in range(3):
            lanes = slice(c * 128, (c + 1) * 128)
            o_qkv[c, :, p * 128 : (p + 1) * 128] = ref[:, lanes].astype(F32) * factor
    o_proj[:, :cw] = p0[...].astype(F32) * factor
    o_proj[:, cw:] = p1[...].astype(F32) * factor
    o_up[...] = up[...].astype(F32) * factor
    o_down[...] = down[...].astype(F32) * factor

    @pl.when(pl.program_id(0) == 0)
    def _():
        for i, ref in enumerate((o_g1, o_s1, o_g2, o_s2, o_pb, o_db)):
            ref[...] = small[i * dr : (i + 1) * dr, :] * factor
        fr = o_ub.shape[0]
        o_ub[...] = small[shared : shared + fr, :] * factor
        lr = o_qvb.shape[1] // 128
        for c in range(2):
            for i in range(lr):
                at = shared + fr + c * lr + i
                o_qvb[c : c + 1, i * 128 : (i + 1) * 128] = small[at : at + 1, :] * factor


def finish_call(lo, lo_got, bias, ig, up, down, q, k, v, p, small, factor, grid=8):
    rows, cw = lo.shape
    (d, f), lw = up.shape, q.shape[1]
    dr, shared = d // 128, -(-6 * d // 1024) * 8
    sd = jax.ShapeDtypeStruct
    tiny = [sd((dr, 128), F32)] * 2
    shapes = (
        [sd((rows, cw), BF16), sd((rows, cw), BF16), sd((3, d, lw), F32), sd((2, lw), F32), sd((lw, d), F32)]
        + [sd((dr, 128), F32), sd((d, f), F32), sd((f // 128, 128), F32), sd((f, d), F32)]
        + [sd((dr, 128), F32)] * 5
    )
    big = lambda a: rows_spec(a.shape[0] // grid, a.shape[1])
    pb = lw // grid
    specs = []
    for i, s in enumerate(shapes):
        if len(s.shape) == 3:
            specs.append(pl.BlockSpec((3, d // grid, lw), lambda i, *_: (0, i, 0)))
        elif i in (0, 1, 4, 6, 8):
            specs.append(big(s))
        else:
            specs.append(whole_spec(s.shape))
    return pl.pallas_call(
        functools.partial(finish_body, factor=factor, dr=dr, shared=shared),
        out_shape=tuple(shapes),
        grid=(grid,),
        in_specs=[big(lo), big(lo_got), whole_spec(bias.shape), big(ig), big(up), big(down), big(q), big(k), big(v)]
        + [rows_spec(pb, cw), rows_spec(pb, cw, grid), whole_spec(small.shape)],
        out_specs=tuple(specs),
        compiler_params=params(),
        cost_estimate=cost(up.size * 8, up.size * 24),
        name="finish",
    )(lo, lo_got, bias, ig, up, down, q, k, v, p, p, small)


def on_device(
    tokens, lengths, qkv_weight, qv_bias, proj_weight, proj_bias, up_weight, up_bias,
    down_weight, down_bias, first_gain, first_shift, second_gain, second_shift, cotangent,
):
    cw = tokens.shape[1]
    d, ff, lw = 2 * cw, up_weight.shape[1], proj_weight.shape[0]
    wide = lax.axis_size("wide")
    w3 = jnp.transpose(qkv_weight, (1, 0, 2))

    xf, low, q, k, v = qkv_call(tokens, w3, qv_bias, first_gain, first_shift)
    mixed, qa, mixed_got, proj_got = attend_forward(lengths, q, k, v, proj_weight)
    lo, lo_send, gmix, gm, gup, down_part, gp_own, gp_other, s_ub, s_db, s_g2, s_s2, s_pb = mlp_call(
        lengths, xf, mixed, mixed_got, proj_weight, proj_got, proj_bias, second_gain, second_shift,
        up_weight, up_bias, down_weight, cotangent, wide,
    )
    lo_got, gdown, gup, gp, g0, g1, g2, ig, small = back_call(
        lengths, qa, k, v, gmix, mixed, low, w3, xf, gm, first_gain, lo_send, gup, down_part, gp_own, gp_other,
        s_ub, s_db, s_g2, s_s2, s_pb, wide,
    )
    out, ig, o_qkv, o_qvb, o_proj, *rest = finish_call(
        lo, lo_got, down_bias.astype(F32).reshape(1, -1), ig, gup, gdown, g0, g1, g2, gp, small,
        1.0 / (lengths.shape[0] * wide),
    )
    pb, up, ubs, down, dbs, g1, s1, g2, s2 = rest
    flat = lambda a: a.reshape(-1)
    return (
        out, ig, jnp.transpose(o_qkv, (1, 0, 2)), o_qvb, o_proj, flat(pb), up, flat(ubs), down, flat(dbs),
        flat(g1), flat(s1), flat(g2), flat(s2),
    )


def solution(mesh):
    split = P("wide", "narrow")
    none3, cols, rows1 = P(None, None, "narrow"), P(None, "narrow"), P("narrow", None)
    return jax.shard_map(
        on_device,
        mesh=mesh,
        in_specs=(
            split, P("wide"), none3, cols, rows1, P(), cols, P("narrow"), rows1, P(), P(), P(), P(), P(), split,
        ),
        out_specs=(
            split, split, none3, cols, rows1, P(), cols, P("narrow"), rows1, P(), P(), P(), P(), P(),
        ),
        check_vma=False,
    )
```

```python
import functools

import jax
import jax.numpy as jnp
from jax import lax
from jax.experimental import pallas as pl
from jax.experimental.pallas import tpu as pltpu
from jax.sharding import PartitionSpec as P

EPS = 1e-05
HEAD = 64
F32, BF16 = jnp.float32, jnp.bfloat16
NT = (((1,), (1,)), ((), ()))
TN = (((0,), (0,)), ((), ()))
GELU_A, GELU_B = 0.7978845608028654, 0.044715
VMEM_LIMIT = 63 * 1024 * 1024


def dot(a, b):
    return jnp.dot(a, b, preferred_element_type=F32)


def dot_nt(a, b):
    return lax.dot_general(a, b, NT, preferred_element_type=F32)


def dot_tn(a, b):
    return lax.dot_general(a, b, TN, preferred_element_type=F32)


def params(**more):
    return pltpu.CompilerParams(vmem_limit_bytes=VMEM_LIMIT, **more)


def cost(flops, size, trans=0):
    return pl.CostEstimate(flops=int(flops), bytes_accessed=int(size), transcendentals=int(trans))


def lane_part(which, width):
    return pl.ds(pl.multiple_of(which * width, 128), width)


def norm_rows(x):
    mean = jnp.mean(x, axis=-1, keepdims=True)
    cen = x - mean
    var = jnp.mean(cen * cen, axis=-1, keepdims=True)
    r = lax.rsqrt(var + EPS)
    return cen * r, r


def rows_spec(rows, cols, base=0):
    return pl.BlockSpec((rows, cols), lambda i, *_: (i + base, 0))


def whole_spec(shape):
    zeros = (0,) * len(shape)
    return pl.BlockSpec(shape, lambda i, *_: zeros)


MESH = pl.DeviceIdType.MESH
scope = jax.named_scope


def vec(ref):
    return ref[...].astype(F32).reshape(1, -1)


def bit_of(index, bit):
    return (index // (1 << bit)) % 2


def flip(index, bit):
    return index + (1 - 2 * bit_of(index, bit)) * (1 << bit)


def greet(peers):
    barrier = pltpu.get_barrier_semaphore()
    for peer in peers:
        pl.semaphore_signal(barrier, inc=1, device_id=peer, device_id_type=MESH)
    pl.semaphore_wait(barrier, len(peers))


def remote(src, dst, sems, at, peer):
    return pltpu.make_async_remote_copy(
        src_ref=src, dst_ref=dst, send_sem=sems[0].at[at], recv_sem=sems[1].at[at],
        device_id=peer, device_id_type=MESH,
    )


def block_rows(start, size, unit=16):
    return pl.ds(start if isinstance(start, int) else pl.multiple_of(start, unit), size)


LINE = 4


def when(cond, action):
    @pl.when(cond)
    def _():
        action()


def line_peer(me, by):
    q = (me // 4) % LINE
    return me + ((q + by) % LINE - q) * 4


class Chain:
    def __init__(self, me, order, rows, cols, sems, at):
        self.me, self.cols, self.sems, self.at = me, cols, sems, at
        self.phases, self.ops, back = [], [], []
        base, size, box = 0, rows, 0
        for kind, bit in order:
            if kind == "line" and size % (16 * LINE):
                raise ValueError(rows)
            if kind == "line":
                part = size // LINE
                keep, give, boxes = base + (me // 4) % LINE * part, None, 2 * (LINE - 1) * part
                self.ops += [("line", len(self.phases), i) for i in range(1, LINE)]
                back = [("spread", len(self.phases), i) for i in range(1, LINE)] + back
            elif size % 32 == 0:
                part = size // 2
                mine = bit_of(me, bit)
                keep, give, boxes = base + mine * part, base + (1 - mine) * part, part
                self.ops.append(("pair", len(self.phases), 0))
                back = [("join", len(self.phases), 0)] + back
            else:
                part, keep, give, boxes = size, base, base, size
                self.ops.append(("pair", len(self.phases), 0))
            self.phases.append((bit, base, keep, give, part, box))
            base, size, box = keep, part, box + boxes
        self.scatters = len(self.ops)
        self.ops += back
        self.base, self.size, self.box_rows = base, size, box

    def bind(self, src, box, part, own, dst=None, entry=0):
        self.src, self.box, self.part, self.own, self.dst = src, box, part, own, dst
        self.entry = self.ops[entry][1]
        return self

    def _source(self, phase):
        off = 0 if phase == 0 else self.phases[0][2]
        return (self.src if phase == self.entry else self.part), off

    def _target(self, phase):
        if phase == len(self.phases) - 1:
            return self.own, self.phases[phase][2]
        return self.part, self.phases[0][2]

    def _remote(self, op, lane, src, dst, to):
        return remote(src, dst, self.sems, self.at + 2 * op + lane, {"wide": to})

    def _add(self, rows, target, first, *terms):
        unit = next(u for u in (96, 64, 48, 32, 16) if rows % u == 0)

        def add(i, carry):
            total = None
            for ref, start in terms:
                value = ref[block_rows(start + i * unit, unit), self.cols]
                total = value if total is None else total + value
            target[block_rows(first + i * unit, unit), self.cols] = total
            return carry

        lax.fori_loop(0, rows // unit, add, 0)


    def _pair(self, op, phase):
        bit, _, _, give, rows, box = self.phases[phase]
        source, off = self._source(phase)
        src = source.at[block_rows(give - off, rows), self.cols]
        return self._remote(op, 0, src, self.box.at[pl.ds(box, rows), self.cols], flip(self.me, bit))

    def _join(self, op, phase):
        bit, _, keep, _, rows, _ = self.phases[phase]
        region = self.dst.at[block_rows(keep, rows), self.cols]
        return self._remote(op, 0, region, region, flip(self.me, bit))


    def _slot(self, phase, lane, i):
        rows, box = self.phases[phase][4:]
        return box + (lane * (LINE - 1) + i - 1) * rows

    def _line_sends(self, op, phase, i):
        q = (self.me // 4) % LINE
        _, base, _, _, rows, _ = self.phases[phase]
        source, off = self._source(phase)
        sends = []
        for lane, by in ((0, 1), (1, -1)):
            place_ = q if lane == 0 else LINE - 1 - q
            chunk = LINE - i if lane == 0 else i - 1
            dst = self.box.at[pl.ds(self._slot(phase, lane, i), rows), self.cols]
            to = line_peer(self.me, by)
            src = source.at[block_rows(base - off + chunk * rows, rows), self.cols]
            sends.append((place_ == 0, functools.partial(self._remote, op, lane, src, dst, to)))
            if i > 1:
                src = self.box.at[pl.ds(self._slot(phase, lane, i - 1), rows), self.cols]
                moving = jnp.logical_and(place_ >= 1, place_ <= min(i - 1, LINE - 2))
                sends.append((moving, functools.partial(self._remote, op, lane, src, dst, to)))
        return sends

    def _line_end(self, op, phase, i):
        q = (self.me // 4) % LINE
        _, base, keep, _, rows, _ = self.phases[phase]
        source, off = self._source(phase)
        for cond, copy in self._line_sends(op, phase, i):
            when(cond, lambda: copy().wait_send())
        for lane, by in ((0, -1), (1, 1)):
            place_ = q if lane == 0 else LINE - 1 - q
            slot = self._slot(phase, lane, i)
            dst = self.box.at[pl.ds(slot, rows), self.cols]
            arrived = jnp.logical_and(place_ >= 1, place_ <= i)
            chunk = LINE - 1 - i + q if lane == 0 else i + q - (LINE - 1)

            @pl.when(arrived)
            def _():
                self._remote(op, lane, dst, dst, line_peer(self.me, by)).wait_recv()
                if i < LINE - 1:
                    self._add(rows, self.box, slot, (self.box, slot), (source, base - off + chunk * rows))

        if i == LINE - 1:
            target, out = self._target(phase)
            own = (source, keep - off)
            left, right = (self.box, self._slot(phase, 0, i)), (self.box, self._slot(phase, 1, i))

            @pl.when(q == 0)
            def _():
                self._add(rows, target, keep - out, own, right)

            @pl.when(q == LINE - 1)
            def _():
                self._add(rows, target, keep - out, own, left)

            @pl.when(jnp.logical_and(q > 0, q < LINE - 1))
            def _():
                self._add(rows, target, keep - out, left, own, right)

    def _spread(self, op, phase, i):
        q = (self.me // 4) % LINE
        _, base, _, _, rows, _ = self.phases[phase]
        ways = []
        for lane, by in ((0, 1), (1, -1)):
            place_ = q if lane == 0 else LINE - 1 - q
            sent = self.dst.at[block_rows(base + (q - by * (i - 1)) * rows, rows), self.cols]
            came = self.dst.at[block_rows(base + (q - by * i) * rows, rows), self.cols]
            send_if = jnp.logical_and(place_ >= i - 1, place_ <= LINE - 2)
            ways.append(
                (
                    send_if, functools.partial(self._remote, op, lane, sent, sent, line_peer(self.me, by)),
                    place_ >= i, functools.partial(self._remote, op, lane, came, came, line_peer(self.me, -by)),
                )
            )
        return ways

    def start(self, op):
        kind, phase, i = self.ops[op]
        if kind == "pair":
            self._pair(op, phase).start()
        elif kind == "join":
            self._join(op, phase).start()
        elif kind == "line":
            for cond, copy in self._line_sends(op, phase, i):
                when(cond, lambda: copy().start())
        else:
            for cond, copy, _, _ in self._spread(op, phase, i):
                when(cond, lambda: copy().start())

    def end(self, op):
        kind, phase, i = self.ops[op]
        if kind == "pair":
            self._pair(op, phase).wait()
            _, _, keep, _, rows, box = self.phases[phase]
            source, off = self._source(phase)
            target, out = self._target(phase)
            self._add(rows, target, keep - out, (self.box, box), (source, keep - off))
        elif kind == "join":
            self._join(op, phase).wait()
        elif kind == "line":
            self._line_end(op, phase, i)
        else:
            for send_if, send, recv_if, recv in self._spread(op, phase, i):
                when(send_if, lambda: send().wait_send())
                when(recv_if, lambda: recv().wait_recv())

    def gather_open(self, sem):
        region = self.dst.at[block_rows(self.base, self.size), self.cols]
        return pltpu.make_async_copy(self.own.at[:, self.cols], region, sem)


class Group:
    def __init__(self, chain, open_sem=None, at=0, entry=0, leave=None):
        self.chain, self.open_sem, self.at = chain, open_sem, at
        self.ops = list(range(entry, len(chain.ops) if leave is None else leave))
        self.pos = -1

    @property
    def done(self):
        return self.pos >= len(self.ops)

    def next(self):
        pos = self.pos
        self.pos = min(pos + 1, len(self.ops))

        def tick():
            if pos >= len(self.ops):
                return
            if pos >= 0:
                self.chain.end(self.ops[pos])
            if pos + 1 >= len(self.ops):
                return
            if self.ops[pos + 1] == self.chain.scatters:
                opened = self.chain.gather_open(self.open_sem.at[self.at])
                opened.start()
                opened.wait()
            self.chain.start(self.ops[pos + 1])

        return tick

    def tick(self):
        self.next()()


def bits(wide):
    return wide.bit_length() - 1


def order_of(wide, kind):
    first, rest = ("pair", 0), [("pair", b) for b in range(4, bits(wide))]
    pair, line = ("pair", 1), ("line", 2)
    return [first, pair, line, *rest] if kind == 0 else [first, line, pair, *rest]


def lanes_split(cols):
    return [(0, pl.ds(0, cols // 2)), (1, pl.ds(cols // 2, cols // 2))]


def wide_peers(me, wide):
    pairs = [flip(me, b) for b in range(bits(wide)) if b not in (2, 3)]
    return [{"wide": peer} for peer in pairs + [line_peer(me, by) for by in range(1, LINE)]]


def vmem():
    return pl.BlockSpec(memory_space=pltpu.VMEM)


def anywhere():
    return pl.BlockSpec(memory_space=pl.ANY)


def sems(*counts):
    return [pltpu.SemaphoreType.DMA((c,)) for c in counts]


def qkv_body(own_hbm, own, w, bias, gain, shift, xf, low, q, k, v, got, send_sem, recv_sem):
    n = lax.axis_index("narrow")
    i = pl.program_id(0)
    rows, cw = own.shape
    peer = {"narrow": 1 - n}

    def copy(at):
        block = block_rows(at * rows, rows)
        return remote(own_hbm.at[block], got.at[block], (send_sem, recv_sem), at, peer)

    @pl.when(i == 0)
    def _():
        greet([peer])
        for at in range(got.shape[0] // rows):
            copy(at).start()

    xf[:, lane_part(n, cw)] = own[...]
    with scope("wait"):
        copy(i).wait()
    xf[:, lane_part(1 - n, cw)] = got[block_rows(i * rows, rows), :]
    xhat, _ = norm_rows(xf[...].astype(F32))
    y = (xhat * vec(gain) + vec(shift)).astype(BF16)
    low[...] = y
    q[...] = (dot(y, w[0]) + bias[0:1, :].astype(F32)).astype(BF16) * jnp.asarray(HEAD**-0.5, BF16)
    k[...] = dot(y, w[1]).astype(BF16)
    v[...] = (dot(y, w[2]) + bias[1:2, :].astype(F32)).astype(BF16)


def qkv_call(own, w, bias, gain, shift, block=256):
    rows, cw = own.shape
    d, lw = w.shape[1], w.shape[2]
    sd = jax.ShapeDtypeStruct
    return pl.pallas_call(
        qkv_body,
        out_shape=(sd((rows, d), BF16), sd((rows, d), BF16)) + (sd((rows, lw), BF16),) * 3,
        grid_spec=pltpu.PrefetchScalarGridSpec(
            num_scalar_prefetch=0,
            grid=(rows // block,),
            in_specs=[anywhere(), rows_spec(block, cw)] + [whole_spec(a.shape) for a in (w, bias, gain, shift)],
            out_specs=[rows_spec(block, d)] * 2 + [rows_spec(block, lw)] * 3,
            scratch_shapes=[pltpu.VMEM((rows, cw), BF16)] + sems(rows // block, rows // block),
        ),
        compiler_params=params(collective_id=1, has_side_effects=True),
        cost_estimate=cost(2 * rows * d * 3 * lw, 2 * (rows * d * 5 + w.size)),
        name="norm_qkv",
    )(own, own, w, bias, gain, shift)


def three(x):
    hi = x.astype(BF16).astype(F32)
    mid = (x - hi).astype(BF16).astype(F32)
    return hi, mid, x - hi - mid


def lanes_of(par):
    lane = lax.broadcasted_iota(jnp.int32, (1, 2 * HEAD), 1)
    mine = (lane // HEAD) == par
    return lane, mine, (1 - par) * HEAD


def place(lane, mine, at, base, terms):
    out = jnp.where(mine, base, 0.0)
    for i, term in enumerate(terms):
        out = jnp.where(lane == at + i, term, out)
    return out


def fwd_body(
    len_ref, q, k, v, pw, o, qa_out, o_got, pw_got, ka, va, send_sem, recv_sem, *, bq
):
    head = pl.program_id(0)
    par, pair = head % 2, head // 2
    lane, mine, at = lanes_of(par)
    n, me = lax.axis_index("narrow"), lax.axis_index("wide")
    peer, core = {"narrow": 1 - n}, {"wide": flip(me, 0)}
    pairs = pl.num_programs(0) // 2
    both = (send_sem, recv_sem)
    cols = lane_part(pair, 2 * HEAD)
    part = block_rows((me % 2) * (pw.shape[0] // 2), pw.shape[0] // 2)
    npairs = o.shape[1] // (2 * HEAD)
    weights = remote(pw.at[part], pw_got.at[part], both, npairs, peer)
    shared = remote(pw_got.at[part], pw_got.at[part], both, npairs + 1, core)

    @pl.when(head == 0)
    def _():
        greet([peer, core])
        weights.start()

    keys = k.shape[0]
    kpos = lax.broadcasted_iota(jnp.int32, (keys, 1), 0)
    kbias = jnp.where(kpos < len_ref[0], 0.0, -1e30)
    ka[...] = place(lane, mine, at, k[...].astype(F32), [kbias]).astype(BF16)
    va[...] = place(lane, mine, at, v[...].astype(F32), [1.0]).astype(BF16)
    tri = lax.broadcasted_iota(jnp.int32, (bq, bq), 1) <= lax.broadcasted_iota(jnp.int32, (bq, bq), 0)
    for i in range(q.shape[0] // bq):
        nk = (i + 1) * bq
        rows = pl.ds(i * bq, bq)
        qf = q[rows, :].astype(F32)
        qa = place(lane, mine, at, qf, [1.0])
        s = dot_nt(qa.astype(BF16), ka[0:nk, :])
        edge = jnp.where(tri, s[:, nk - bq :], -1e30)
        m = jnp.max(edge, axis=1, keepdims=True)
        if nk > bq:
            m = jnp.maximum(m, jnp.max(s[:, : nk - bq], axis=1, keepdims=True))
        pv = dot(jnp.exp(edge - m).astype(BF16), va[nk - bq : nk, :])
        if nk > bq:
            pv += dot(jnp.exp(s[:, : nk - bq] - m).astype(BF16), va[0 : nk - bq, :])
        total = jnp.sum(jnp.where(lane == at, pv, 0.0), axis=1, keepdims=True)
        out = (pv / total).astype(BF16).astype(F32)
        old = o[rows, cols].astype(F32)
        o[rows, cols] = jnp.where(mine, out, jnp.where(par == 0, 0.0, old)).astype(BF16)
        lse = m + jnp.log(total)
        qa_out[0, rows, :] = place(lane, mine, at, qf, [1.0, *three(lse)]).astype(BF16)

    def mixed(j):
        c = pl.ds(j * 2 * HEAD, 2 * HEAD)
        return remote(o.at[:, c], o_got.at[:, c], both, j, peer)

    for j in range(npairs):

        @pl.when(head == 2 * j + 1)
        def _():
            mixed(j).start()

    @pl.when(head == 3)
    def _():
        weights.wait()
        shared.start()

    @pl.when(head == 2 * npairs - 1)
    def _():
        shared.wait()
        for j in range(npairs):
            mixed(j).wait()


def attend_forward(length, q, k, v, pw, bq=256):
    rows, width = q.shape
    heads, pair = width // HEAD, 2 * HEAD
    half = lambda h, *_: (0, h // 2)
    sd = jax.ShapeDtypeStruct
    work = 2 * heads * rows * rows * HEAD
    return pl.pallas_call(
        functools.partial(fwd_body, bq=bq),
        out_shape=(
            sd((rows, width), BF16), sd((heads, rows, pair), BF16), sd((rows, width), BF16), sd(pw.shape, BF16),
        ),
        grid_spec=pltpu.PrefetchScalarGridSpec(
            num_scalar_prefetch=1,
            grid=(heads,),
            in_specs=[pl.BlockSpec((rows, pair), half)] * 3 + [anywhere()],
            out_specs=[vmem(), pl.BlockSpec((1, rows, pair), lambda h, *_: (h, 0, 0)), anywhere(), anywhere()],
            scratch_shapes=[pltpu.VMEM((rows, pair), BF16)] * 2 + sems(heads // 2 + 2, heads // 2 + 2),
        ),
        compiler_params=params(collective_id=2, has_side_effects=True),
        cost_estimate=cost(4 * work, 2 * rows * width * 6, work // 256),
        name="attend_fwd",
    )(length, q, k, v, pw)


DOWN_ENTRY, UP_ENTRY = (2, 1), (1, 1)


def mlp_body(
    len_ref, xf_hbm, mo_hbm, mr_hbm, pwo_hbm, pwr_hbm, pb, gain, shift, ub, up_hbm, down_hbm, cot_hbm,
    lo_out, lo_send_out, gmix, gm_out, up_part, down_part, gp_own, gp_other, sum_ub, sum_db, sum_g, sum_s, sum_pb,
    xf, mo, mr, pwo, pwr, up, down, cot, cot_got, cf, lo, lo_send, mid, second, active, slope, gh,
    gs_send, gs_got, gs_own, gdown, gup, box, up_box, gm, glow, gmix_send, load_sem, store_sem, nsend, nrecv, wsend, wrecv,
    *, wide,
):
    n, me = lax.axis_index("narrow"), lax.axis_index("wide")
    peer = {"narrow": 1 - n}
    rows, cw = cot.shape
    d, f = up.shape
    half, block = rows // 2, min(256, rows // 2)
    each = half // block
    mine, other = lane_part(n, cw), lane_part(1 - n, cw)
    narrow, across = (nsend, nrecv), (wsend, wrecv)
    count = iter(range(16))

    def load(src, dst):
        copy = pltpu.make_async_copy(src, dst, load_sem.at[next(count)])
        copy.start()
        return copy

    his, own = block_rows((1 - n) * half, half), block_rows(n * half, half)
    first = [load(a, b) for a, b in ((pwo_hbm, pwo), (pwr_hbm, pwr))]
    first += [load(a.at[his], b.at[his]) for a, b in ((xf_hbm, xf), (mo_hbm, mo), (mr_hbm, mr))]
    up_load = load(up_hbm, up)
    greet([peer] + wide_peers(me, wide))

    def cot_copy(side, j, a):
        r = block_rows(side * half + j * block, block)
        return remote(cot_hbm.at[r], cot_got.at[r], narrow, a * each + j, peer)

    for a, side in enumerate((n, 1 - n)):
        for j in range(each):
            cot_copy(side, j, a).start()
    down_load = load(down_hbm, down)
    cot_load = load(cot_hbm, cot)
    rest = [load(a.at[own], b.at[own]) for a, b in ((xf_hbm, xf), (mo_hbm, mo), (mr_hbm, mr))]

    def project(at):
        r = block_rows(at, block)
        m = xf[r, :].astype(F32) + (dot(mo[r, :], pwo[...]) + dot(mr[r, :], pwr[...])) + vec(pb)
        mid[r, :] = m
        xhat, _ = norm_rows(m)
        second[r, :] = (xhat * vec(gain) + vec(shift)).astype(BF16)

    def forward(at):
        r = block_rows(at, block)
        hid = dot(second[r, :], up[...]) + vec(ub)
        sq = hid * hid
        t = jnp.tanh(GELU_A * (hid + GELU_B * (sq * hid)))
        hf = 0.5 * (1.0 + t)
        act = (hid * hf).astype(BF16)
        active[r, :] = act
        slope[r, :] = hf + (0.5 * hid) * (1.0 - t * t) * (GELU_A + (3.0 * GELU_A * GELU_B) * sq)
        lo[r, :] = mid[r, mine] + dot(act, down[:, mine])
        lo_send[r, :] = dot(act, down[:, other]).astype(BF16)

    def backward(at):
        r = block_rows(at, block)
        pos = at + lax.broadcasted_iota(jnp.int32, (block, 1), 0)
        live = (pos < len_ref[0]).astype(F32)
        cf[r, mine] = (cot[r, :].astype(F32) * live).astype(BF16)
        cf[r, other] = (cot_got[r, :].astype(F32) * live).astype(BF16)
        ghid = (dot_nt(cf[r, :], down[...]) * slope[r, :]).astype(BF16)
        gh[r, :] = ghid
        sum_ub[...] += jnp.sum(ghid.astype(F32), axis=0, keepdims=True)
        return dot_nt(ghid, up[...])

    def every(side, body):
        def step(j, carry):
            body(side * half + j * block)
            return carry

        lax.fori_loop(0, each, step, 0)

    def both(at):
        project(at)
        forward(at)

    for ref in (sum_ub, sum_g, sum_s, sum_pb, sum_db):
        ref[...] = jnp.zeros_like(ref)
    with scope("load"):
        for copy in first:
            copy.wait()
    with scope("project"):
        every(1 - n, project)
    with scope("load2"):
        up_load.wait()
        down_load.wait()
    with scope("fwd_peer"):
        every(1 - n, forward)
    for copy in rest:
        copy.wait()
    with scope("fwd_own"):
        every(n, both)
    stores = []

    def store(src, dst):
        copy = pltpu.make_async_copy(src, dst, store_sem.at[len(stores)])
        copy.start()
        stores.append(copy)

    store(lo, lo_out)
    store(lo_send, lo_send_out)
    with scope("cot_wait"):
        cot_load.wait()
        for j in range(each):
            cot_copy(n, j, 0).wait()

    def gs_copy(j):
        r = block_rows(j * block, block)
        return remote(gs_send.at[r], gs_got.at[r], narrow, 2 * each + j, peer)

    def for_peer(j, carry):
        gs_send[block_rows(j * block, block), :] = backward((1 - n) * half + j * block).astype(BF16)
        gs_copy(j).start()
        return carry

    def for_own(j, carry):
        gs_own[block_rows(j * block, block), :] = backward(n * half + j * block)
        return carry

    with scope("for_peer"):
        lax.fori_loop(0, each, for_peer, 0)
    with scope("cot_wait2"):
        for j in range(each):
            cot_copy(1 - n, j, 1).wait()
    with scope("for_own"):
        lax.fori_loop(0, each, for_own, 0)

    def weight(dst, left, right):
        def step(i, carry):
            c = block_rows(i * 256, 256, 256)
            dst[c, :] = dot_tn(left[:, c], right[...]).astype(BF16)
            return carry

        lax.fori_loop(0, dst.shape[0] // 256, step, 0)

    used = iter(range(0, 64, 4))

    def group(src, box_, part, leaves):
        parts = []
        for (kind, cols), leave in zip(lanes_split(src.shape[1]), leaves):
            chain = Chain(me, order_of(wide, kind), src.shape[0], cols, across, next(used))
            parts.append(Group(chain.bind(src, box_, part, None), leave=leave))
        return parts

    reduce_down = group(gdown, box, down_part, DOWN_ENTRY)
    reduce_up = group(gup, up_box, up_part, UP_ENTRY)

    def advance(name, *groups):
        with scope(name):
            for one in groups:
                one.tick()

    with scope("w_down"):
        weight(gdown, active, cf)
    advance("core_d", *reduce_down)
    with scope("w_up"):
        weight(gup, second, gh)
    advance("core_u", *reduce_down, *reduce_up)
    with scope("gs_wait"):
        for j in range(each):
            gs_copy(j).wait()

    def gmix_copy(j):
        r = block_rows(n * half + j * block, block)
        return remote(gmix_send.at[block_rows(j * block, block)], gmix.at[r], narrow, 3 * each + j, peer)

    def back_norm(j, carry):
        r, rh = block_rows(n * half + j * block, block), block_rows(j * block, block)
        g = gs_own[rh, :] + gs_got[rh, :].astype(F32)
        xhat, scale = norm_rows(mid[r, :])
        gg = g * vec(gain)
        m1 = jnp.mean(gg, axis=-1, keepdims=True)
        m2 = jnp.mean(gg * xhat, axis=-1, keepdims=True)
        c = cf[r, :].astype(F32)
        grad = c + scale * (gg - m1 - xhat * m2)
        gm[rh, :] = grad
        gl = grad.astype(BF16)
        glow[rh, :] = gl
        gmix_send[rh, :] = dot_nt(gl, pwr[...]).astype(BF16)
        gmix_copy(j).start()
        gmix[r, :] = dot_nt(gl, pwo[...]).astype(BF16)
        sum_g[...] += jnp.sum(g * xhat, axis=0, keepdims=True)
        sum_s[...] += jnp.sum(g, axis=0, keepdims=True)
        sum_pb[...] += jnp.sum(grad, axis=0, keepdims=True)
        sum_db[...] += jnp.sum(c, axis=0, keepdims=True)
        return carry

    with scope("back_norm"):
        lax.fori_loop(0, each, back_norm, 0)
    store(gm, gm_out)
    advance("across", *reduce_up)
    with scope("proj"):
        lw = mo.shape[1]
        for src, dst in ((mr, gp_other), (mo, gp_own)):
            total = dot_tn(src[own, :], glow[...]).astype(BF16)
            dst[0:lw, :] = total[:, :cw]
            dst[lw : 2 * lw, :] = total[:, cw:]
    with scope("gmix_wait"):
        for j in range(each):
            gmix_copy(j).wait()
    advance("leave", *reduce_down, *reduce_up)
    with scope("store"):
        for copy in stores:
            copy.wait()


def mlp_call(length, xf, mo, mr, pwo, pwr, pb, gain, shift, up, ub, down, cot, wide):
    rows, d = xf.shape
    f, lw, cw = up.shape[1], mo.shape[1], cot.shape[1]
    half = rows // 2
    sd, vm = jax.ShapeDtypeStruct, pltpu.VMEM
    each = half // min(256, half)
    return pl.pallas_call(
        functools.partial(mlp_body, wide=wide),
        out_shape=(
            sd((rows, cw), F32), sd((rows, cw), BF16), sd((rows, lw), BF16), sd((half, d), F32),
            sd((d // 2, f), BF16), sd((f // 2, d), BF16), sd((2 * lw, cw), BF16), sd((2 * lw, cw), BF16),
            sd((1, f), F32), sd((1, d), F32), sd((1, d), F32), sd((1, d), F32), sd((1, d), F32),
        ),
        in_specs=[pl.BlockSpec(memory_space=pltpu.SMEM)] + [anywhere()] * 5 + [vmem()] * 4 + [anywhere()] * 3,
        out_specs=(anywhere(), anywhere(), vmem(), anywhere()) + (vmem(),) * 9,
        scratch_shapes=[
            vm((rows, d), BF16), vm((rows, lw), BF16), vm((rows, lw), BF16), vm((lw, d), BF16), vm((lw, d), BF16),
            vm((d, f), BF16), vm((f, d), BF16), vm((rows, cw), BF16), vm((rows, cw), BF16), vm((rows, d), BF16),
            vm((rows, cw), F32), vm((rows, cw), BF16), vm((rows, d), F32),
            vm((rows, d), BF16), vm((rows, f), BF16), vm((rows, f), F32), vm((rows, f), BF16),
            vm((half, d), BF16), vm((half, d), BF16), vm((half, d), F32), vm((f, d), BF16), vm((d, f), BF16),
            vm((f, d), BF16), vm((d, f), BF16), vm((half, d), F32), vm((half, d), BF16), vm((half, lw), BF16),
        ]
        + sems(16, 4, 4 * each, 4 * each, 16, 16),
        compiler_params=params(collective_id=3, has_side_effects=True),
        cost_estimate=cost(2 * rows * d * (d + 6 * f), 2 * (rows * d * 8 + 2 * d * f), rows * f),
        name="mlp",
    )(length, xf, mo, mr, pwo, pwr, pb, gain, shift, ub, up, down, cot)


HEAD_TICKS = (
    ((0, 3), "D0"),
    ((1, 2), "D1"),
    ((1, 3), "U0U1Q0"),
    ((2, 0), "D0"),
    ((2, 1), "Q0"),
    ((2, 2), "D1"),
    ((2, 3), "U0"),
    ((3, 1), "Q0P0U1"),
    ((3, 2), "D0"),
    ((3, 3), "D1P0D0Q1"),
    ((4, 0), "U0"),
    ((4, 1), "Q0Q1"),
    ((4, 2), "D1D0"),
    ((4, 3), "U1P0"),
    ((5, 0), "U0"),
    ((5, 1), "Q0Q1D0P0D1"),
    ((5, 2), "U0Q0U1Q1"),
    ((5, 3), "D1Q1P0Q2"),
)
PART_TICKS = ("Q0Q2U0Q1U1D0", "D1", "Q0D0P0", "Q2U0Q1", "")
LAST_TICKS = (
    "Q2U1", "norm0", "D1Q2Q0P0U0Q1D1Q2", "U0U1Q0P0Q1", "norm1", "Q0Q2U1Q2",
    "small", "P0U1", "small", "P0Q2Q1", "small", "Q1",
    "small", "Q2", "small", "Q2",
)


def pieces(names):
    return [names[i : i + 2] for i in range(0, len(names), 2)]


def back_body(
    len_ref, qa_hbm, k_hbm, v_hbm, do_hbm, o_hbm, low_hbm, w_hbm, xf_hbm, gm_hbm, gain, lo_send, up_part_hbm,
    down_part_hbm, gp_own_hbm, gp_other_hbm, s_ub, s_db, s_g2, s_s2, s_pb,
    lo_got, down_out, up_out, gp_out, g0_out, g1_out, g2_out, ig, small,
    qa, k, v, do, o, low, wp, xf, gm, up_part, down_part, gp_src, gp_got,
    ka, va, dk_acc, dv_acc, dqkv, gpair,
    down_box, down_part2, down_own, up_box, up_part2, up_own, gp_box, gp_part, gp_own, pair_box, pair_part, pair_own,
    gn_send, gn_got, gn_own, ig_own, ig_send, sums, sums_box,
    load_sem, open_sem, nsend, nrecv, wsend, wrecv, *, bq, wide,
):
    n, me = lax.axis_index("narrow"), lax.axis_index("wide")
    peer = {"narrow": 1 - n}
    narrow, across = (nsend, nrecv), (wsend, wrecv)
    steps = bits(wide)
    heads, rows = qa.shape[0], qa.shape[1]
    pair_w = 2 * HEAD
    pairs = heads // 2
    d, lw = gain.shape[0], k.shape[1]
    cw = d // 2
    half, block = rows // 2, min(256, rows // 2)
    each = half // block
    count = iter(range(64))

    def load(src, dst):
        copy = pltpu.make_async_copy(src, dst, load_sem.at[next(count)])
        copy.start()
        return copy

    pair_loads = []
    for p in range(pairs):
        c = pl.ds(p * pair_w, pair_w)
        pair_loads.append(
            [load(a.at[:, c], b.at[:, c]) for a, b in ((k_hbm, k), (v_hbm, v), (do_hbm, do), (o_hbm, o))]
            + [load(qa_hbm.at[pl.ds(2 * p, 2)], qa.at[pl.ds(2 * p, 2)])]
        )
    part_load = load(down_part_hbm, down_part)
    up_load = load(up_part_hbm, up_part)
    gp_load = load(gp_own_hbm, gp_src)
    low_load = load(low_hbm, low)
    greet([peer] + wide_peers(me, wide))
    gp_swap = remote(gp_other_hbm, gp_got, narrow, 0, peer)
    layer = remote(lo_send, lo_got, narrow, 1, peer)
    gp_swap.start()
    late = [
        load(w_hbm.at[c, :, pl.ds(p * pair_w, pair_w)], wp.at[p, :, pl.ds(c * pair_w, pair_w)])
        for p in range(pairs)
        for c in range(3)
    ]
    own_half = block_rows(n * half, half)
    late += [load(xf_hbm.at[own_half], xf), load(gm_hbm, gm)]

    stride = 2 * len(Chain(0, order_of(wide, 0), d, None, None, 0).ops)
    at = iter(range(0, 64 * stride, stride))
    opening = iter(range(32))

    def group(src, box, part, own, dst, entries=(0,)):
        rows_, cols_ = dst.shape
        made = []
        parts = lanes_split(cols_) if len(entries) == 2 else [(0, pl.ds(0, cols_))]
        for (kind, cols), entry in zip(parts, entries):
            chain = Chain(me, order_of(wide, kind), rows_, cols, across, next(at))
            made.append(Group(chain.bind(src, box, part, own, dst, entry), open_sem, next(opening), entry))
        return made

    groups = {}
    groups["D0"], groups["D1"] = group(down_part, down_box, down_part2, down_own, down_out, DOWN_ENTRY)
    groups["U0"], groups["U1"] = group(up_part, up_box, up_part2, up_own, up_out, UP_ENTRY)
    groups["P0"] = group(gp_src, gp_box, gp_part, gp_own, gp_out)[0]
    for p, out in zip(range(pairs), (g0_out, g1_out, g2_out)):
        groups[f"Q{p}"] = group(gpair.at[p], pair_box.at[p], pair_part.at[p], pair_own.at[p], out)[0]

    def tick(names):
        with scope(names):
            for name in pieces(names):
                groups[name].tick()

    part_load.wait()
    tick("D0D1")
    up_load.wait()
    tick("U0U1")

    kpos = lax.broadcasted_iota(jnp.int32, (rows, 1), 0)
    kbias = jnp.where(kpos < len_ref[0], 0.0, -1e30)
    tri = lax.broadcasted_iota(jnp.int32, (bq, bq), 0) <= lax.broadcasted_iota(jnp.int32, (bq, bq), 1)

    def plan(names):
        ticks = [groups[name].next() for name in pieces(names)]

        def run():
            with scope(names):
                for one in ticks:
                    one()

        return run

    def start_proj():
        first = groups["P0"].next()

        def run():
            gp_swap.wait()
            gp_load.wait()
            gp_src[...] = gp_src[...] + gp_got[...]
            first()

        return run

    hooks = {}
    for at_, names in HEAD_TICKS:
        hooks[at_] = [plan(names)]
        if at_ == (2, 3):
            hooks[at_] += [layer.start, start_proj()]

    def run_hooks(head, block_):
        for (h, where), actions in hooks.items():
            if where == block_:

                @pl.when(head == h)
                def _():
                    for action in actions:
                        action()

    def one_head(head, carry):
        par, pair = head % 2, head // 2
        lane, mine, extra = lanes_of(par)
        cols = lane_part(pair, pair_w)
        for p in range(pairs):

            @pl.when(head == 2 * p)
            def _():
                for copy in pair_loads[p]:
                    copy.wait()

        ka[...] = place(lane, mine, extra, k[:, cols].astype(F32), [kbias, -1.0, -1.0, -1.0]).astype(BF16)
        va[...] = place(lane, mine, extra, v[:, cols].astype(F32), [-1.0, -1.0, -1.0]).astype(BF16)
        dk_acc[...] = jnp.zeros_like(dk_acc)
        dv_acc[...] = jnp.zeros_like(dv_acc)

        def put(c, r, new):
            lanes = pl.ds(c * pair_w, pair_w)
            old = dqkv[pair, r, lanes].astype(F32)
            dqkv[pair, r, lanes] = jnp.where(mine, new, jnp.where(par == 0, 0.0, old)).astype(BF16)

        for i in range(rows // bq):
            r = pl.ds(i * bq, bq)
            qb = qa[head, r, :]
            df = do[r, cols].astype(F32)
            delta = jnp.sum(jnp.where(mine, df * o[r, cols].astype(F32), 0.0), axis=1, keepdims=True)
            db = place(lane, mine, extra, df, three(delta)).astype(BF16)
            dqs = None
            for j in range(i + 1):
                c = pl.ds(j * bq, bq)
                kb, vb = ka[c, :], va[c, :]
                s = dot_nt(kb, qb)
                if j == i:
                    s = jnp.where(tri, s, -1e30)
                p = jnp.exp(s)
                ds = (p * dot_nt(vb, db)).astype(BF16)
                dv_acc[c, :] += dot(p.astype(BF16), db)
                dk_acc[c, :] += dot(ds, qb)
                part = dot_tn(ds, kb)
                dqs = part if dqs is None else dqs + part
            put(0, r, dqs * HEAD**-0.5)
            if i < rows // bq - 1:
                run_hooks(head, i)
        put(1, pl.ds(0, rows), dk_acc[...])
        put(2, pl.ds(0, rows), dv_acc[...])

        @pl.when(head == 1)
        def _():
            low_load.wait()

        @pl.when(par == 1)
        def _():
            with scope("weights"):
                gpair[pair] = dot_tn(low[...], dqkv[pair]).astype(BF16)

        run_hooks(head, rows // bq - 1)
        return carry

    lax.fori_loop(0, heads, one_head, 0)

    for copy in late:
        copy.wait()

    def gn_part(start):
        r = block_rows(start, block)
        total = dot_nt(dqkv[0, r, :], wp[0])
        for p in range(1, pairs):
            total += dot_nt(dqkv[p, r, :], wp[p])
        return total

    def gn_copy(j):
        r = pl.ds(j * block, block)
        return remote(gn_send.at[r], gn_got.at[r], narrow, 2 + j, peer)

    for j in range(each):
        with scope("gn_peer"):
            gn_send[j * block : (j + 1) * block, :] = gn_part((1 - n) * half + j * block).astype(BF16)
        gn_copy(j).start()
        tick(PART_TICKS[j % 2])
    for j in range(each):
        with scope("gn_own"):
            gn_own[j * block : (j + 1) * block, :] = gn_part(n * half + j * block)
        tick(PART_TICKS[2 + j % 2])

    sums[...] = jnp.zeros_like(sums)

    def put_sum(start, value):
        for i in range(value.shape[1] // 128):
            sums[start + i : start + i + 1, :] = value[:, i * 128 : (i + 1) * 128]

    dr, fr, lr = d // 128, s_ub.shape[1] // 128, lw // 128
    shared = -(-6 * dr // 8) * 8
    put_sum(2 * dr, s_g2[...])
    put_sum(3 * dr, s_s2[...])
    put_sum(4 * dr, s_pb[...])
    put_sum(5 * dr, s_db[...])
    put_sum(shared, s_ub[...])
    for p in range(pairs):
        put_sum(shared + fr + p, jnp.sum(dqkv[p, :, 0:pair_w].astype(F32), axis=0, keepdims=True))
        put_sum(shared + fr + lr + p, jnp.sum(dqkv[p, :, 2 * pair_w :].astype(F32), axis=0, keepdims=True))
    tick(PART_TICKS[4])

    mine, other = lane_part(n, cw), lane_part(1 - n, cw)

    def ig_copy(j):
        r = block_rows(n * half + j * block, block)
        return remote(ig_send.at[pl.ds(j * block, block)], ig.at[r], narrow, 2 + each + j, peer)

    def in_norm(j):
        with scope("gn_wait"):
            gn_copy(j).wait()
        rh = pl.ds(j * block, block)
        r = block_rows(n * half + j * block, block)
        g = gn_own[rh, :] + gn_got[rh, :].astype(F32)
        xhat, scale = norm_rows(xf[rh, :].astype(F32))
        gg = g * vec(gain)
        m1 = jnp.mean(gg, axis=-1, keepdims=True)
        m2 = jnp.mean(gg * xhat, axis=-1, keepdims=True)
        ig_own[...] = gm[rh, :] + scale * (gg - m1 - xhat * m2)
        ig_send[rh, :] = ig_own[:, other].astype(BF16)
        ig_copy(j).start()
        ig[r, :] = ig_own[:, mine].astype(BF16)
        return jnp.sum(g * xhat, axis=0, keepdims=True), jnp.sum(g, axis=0, keepdims=True)

    def vec_copy(step):
        if step == 0:
            top = pl.ds(0, shared)
            return remote(sums.at[top], sums_box.at[0, top], narrow, 2 + 2 * each, peer)
        slot = 10 * stride + step - 1
        return remote(sums, sums_box.at[step], across, slot, {"wide": flip(me, step - 1)})

    def vec_end(step):
        vec_copy(step).wait()
        if step == 0:
            sums[0:shared, :] += sums_box[0, 0:shared, :]
        else:
            sums[...] += sums_box[step]
        if step < steps:
            vec_copy(step + 1).start()

    small_step, sums1 = 0, []
    for names in LAST_TICKS:
        if names in ("norm0", "norm1"):
            todo = range(each - 1) if names == "norm0" else range(each - 1, each)
            sums1 += [in_norm(j) for j in todo]
            if names == "norm1":
                put_sum(0, sum(a for a, _ in sums1))
                put_sum(dr, sum(b for _, b in sums1))
                vec_copy(0).start()
        elif names == "small":
            if small_step <= steps:
                with scope("small"):
                    vec_end(small_step)
            small_step += 1
        else:
            tick(names)
    while small_step <= steps or not all(g.done for g in groups.values()):
        for name in groups:
            tick(name)
        if small_step <= steps:
            vec_end(small_step)
        small_step += 1
    small[...] = sums[...]
    with scope("end"):
        layer.wait()
        for j in range(each):
            ig_copy(j).wait()


def back_call(
    length, qa, k, v, do, o, low, w, xf, gm, gain, lo_send, up_part, down_part, gp_own, gp_other,
    s_ub, s_db, s_g2, s_s2, s_pb, wide, bq=256,
):
    heads, rows, pair = qa.shape
    d, f, lw = gain.shape[0], up_part.shape[1], k.shape[1]
    cw, half = d // 2, rows // 2
    block = min(256, half)
    each, steps, pairs = half // block, bits(wide), heads // 2
    sd, vm = jax.ShapeDtypeStruct, pltpu.VMEM
    shape = lambda r: Chain(0, order_of(wide, 0), r, None, None, 0)
    stride = 2 * len(shape(d).ops)
    c_down, c_up, c_gp = shape(f), shape(d), shape(2 * lw)
    other = lambda r: Chain(0, order_of(wide, 1), r, None, None, 0).box_rows
    down_rows, up_rows = max(c_down.box_rows, other(f)), max(c_up.box_rows, other(d))
    vec_rows = -(-6 * d // 1024) * 8 + -(-(f + 2 * lw) // 1024) * 8
    work = 2 * heads * rows * rows * HEAD
    return pl.pallas_call(
        functools.partial(back_body, bq=bq, wide=wide),
        out_shape=(sd((rows, cw), BF16), sd((f, d), BF16), sd((d, f), BF16), sd((2 * lw, cw), BF16))
        + (sd((d, 3 * pair), BF16),) * 3 + (sd((rows, cw), BF16), sd((vec_rows, 128), F32)),
        in_specs=[pl.BlockSpec(memory_space=pltpu.SMEM)] + [anywhere()] * 9 + [vmem()] + [anywhere()] * 5 + [vmem()] * 5,
        out_specs=(anywhere(),) * 7 + (vmem(), vmem()),
        scratch_shapes=[
            vm(qa.shape, BF16), vm((rows, lw), BF16), vm((rows, lw), BF16), vm((rows, lw), BF16), vm((rows, lw), BF16),
            vm((rows, d), BF16), vm((pairs, d, 3 * pair), BF16), vm((half, d), BF16), vm((half, d), F32),
            vm((d // 2, f), BF16), vm((f // 2, d), BF16), vm((2 * lw, cw), BF16), vm((2 * lw, cw), BF16),
            vm((rows, pair), BF16), vm((rows, pair), BF16), vm((rows, pair), F32), vm((rows, pair), F32),
            vm((pairs, rows, 3 * pair), BF16), vm((pairs, d, 3 * pair), BF16),
            vm((down_rows, d), BF16), vm((f // 2, d), BF16), vm((c_down.size, d), BF16),
            vm((up_rows, f), BF16), vm((d // 2, f), BF16), vm((c_up.size, f), BF16),
            vm((c_gp.box_rows, cw), BF16), vm((lw, cw), BF16), vm((c_gp.size, cw), BF16),
            vm((pairs, c_up.box_rows, 3 * pair), BF16), vm((pairs, d // 2, 3 * pair), BF16),
            vm((pairs, c_up.size, 3 * pair), BF16),
            vm((half, d), BF16), vm((half, d), BF16), vm((half, d), F32), vm((block, d), F32), vm((half, cw), BF16),
            vm((vec_rows, 128), F32), vm((steps + 1, vec_rows, 128), F32),
        ]
        + sems(64, 32, 3 + 2 * each, 3 + 2 * each, 11 * stride, 11 * stride),
        compiler_params=params(collective_id=4, has_side_effects=True),
        cost_estimate=cost(10 * work + 4 * rows * d * 3 * lw, 2 * rows * d * 20, work // 256),
        name="back",
    )(
        length, qa, k, v, do, o, low, w, xf, gm, gain, lo_send, up_part, down_part, gp_own, gp_other,
        s_ub, s_db, s_g2, s_s2, s_pb,
    )


def finish_body(
    lo, lo_got, bias, ig, up, down, q, k, v, p0, p1, small,
    out, ig_out, o_qkv, o_qvb, o_proj, o_pb, o_up, o_ub, o_down, o_db, o_g1, o_s1, o_g2, o_s2,
    *, factor, dr, shared,
):
    n = lax.axis_index("narrow")
    cw = lo.shape[1]
    out[...] = (lo[...] + lo_got[...].astype(F32) + bias[:, lane_part(n, cw)]).astype(BF16)
    ig_out[...] = ig[...]
    for p, ref in enumerate((q, k, v)):
        for c in range(3):
            lanes = slice(c * 128, (c + 1) * 128)
            o_qkv[c, :, p * 128 : (p + 1) * 128] = ref[:, lanes].astype(F32) * factor
    o_proj[:, :cw] = p0[...].astype(F32) * factor
    o_proj[:, cw:] = p1[...].astype(F32) * factor
    o_up[...] = up[...].astype(F32) * factor
    o_down[...] = down[...].astype(F32) * factor

    @pl.when(pl.program_id(0) == 0)
    def _():
        for i, ref in enumerate((o_g1, o_s1, o_g2, o_s2, o_pb, o_db)):
            ref[...] = small[i * dr : (i + 1) * dr, :] * factor
        fr = o_ub.shape[0]
        o_ub[...] = small[shared : shared + fr, :] * factor
        lr = o_qvb.shape[1] // 128
        for c in range(2):
            for i in range(lr):
                at = shared + fr + c * lr + i
                o_qvb[c : c + 1, i * 128 : (i + 1) * 128] = small[at : at + 1, :] * factor


def finish_call(lo, lo_got, bias, ig, up, down, q, k, v, p, small, factor, grid=8):
    rows, cw = lo.shape
    (d, f), lw = up.shape, q.shape[1]
    dr, shared = d // 128, -(-6 * d // 1024) * 8
    sd = jax.ShapeDtypeStruct
    tiny = [sd((dr, 128), F32)] * 2
    shapes = (
        [sd((rows, cw), BF16), sd((rows, cw), BF16), sd((3, d, lw), F32), sd((2, lw), F32), sd((lw, d), F32)]
        + [sd((dr, 128), F32), sd((d, f), F32), sd((f // 128, 128), F32), sd((f, d), F32)]
        + [sd((dr, 128), F32)] * 5
    )
    big = lambda a: rows_spec(a.shape[0] // grid, a.shape[1])
    pb = lw // grid
    specs = []
    for i, s in enumerate(shapes):
        if len(s.shape) == 3:
            specs.append(pl.BlockSpec((3, d // grid, lw), lambda i, *_: (0, i, 0)))
        elif i in (0, 1, 4, 6, 8):
            specs.append(big(s))
        else:
            specs.append(whole_spec(s.shape))
    return pl.pallas_call(
        functools.partial(finish_body, factor=factor, dr=dr, shared=shared),
        out_shape=tuple(shapes),
        grid=(grid,),
        in_specs=[big(lo), big(lo_got), whole_spec(bias.shape), big(ig), big(up), big(down), big(q), big(k), big(v)]
        + [rows_spec(pb, cw), rows_spec(pb, cw, grid), whole_spec(small.shape)],
        out_specs=tuple(specs),
        compiler_params=params(),
        cost_estimate=cost(up.size * 8, up.size * 24),
        name="finish",
    )(lo, lo_got, bias, ig, up, down, q, k, v, p, p, small)


def on_device(
    tokens, lengths, qkv_weight, qv_bias, proj_weight, proj_bias, up_weight, up_bias,
    down_weight, down_bias, first_gain, first_shift, second_gain, second_shift, cotangent,
):
    cw = tokens.shape[1]
    d, ff, lw = 2 * cw, up_weight.shape[1], proj_weight.shape[0]
    wide = lax.axis_size("wide")
    w3 = jnp.transpose(qkv_weight, (1, 0, 2))

    xf, low, q, k, v = qkv_call(tokens, w3, qv_bias, first_gain, first_shift)
    mixed, qa, mixed_got, proj_got = attend_forward(lengths, q, k, v, proj_weight)
    lo, lo_send, gmix, gm, up_part, down_part, gp_own, gp_other, s_ub, s_db, s_g2, s_s2, s_pb = mlp_call(
        lengths, xf, mixed, mixed_got, proj_weight, proj_got, proj_bias, second_gain, second_shift,
        up_weight, up_bias, down_weight, cotangent, wide,
    )
    lo_got, gdown, gup, gp, g0, g1, g2, ig, small = back_call(
        lengths, qa, k, v, gmix, mixed, low, w3, xf, gm, first_gain, lo_send, up_part, down_part, gp_own, gp_other,
        s_ub, s_db, s_g2, s_s2, s_pb, wide,
    )
    out, ig, o_qkv, o_qvb, o_proj, *rest = finish_call(
        lo, lo_got, down_bias.astype(F32).reshape(1, -1), ig, gup, gdown, g0, g1, g2, gp, small,
        1.0 / (lengths.shape[0] * wide),
    )
    pb, up, ubs, down, dbs, g1, s1, g2, s2 = rest
    flat = lambda a: a.reshape(-1)
    return (
        out, ig, jnp.transpose(o_qkv, (1, 0, 2)), o_qvb, o_proj, flat(pb), up, flat(ubs), down, flat(dbs),
        flat(g1), flat(s1), flat(g2), flat(s2),
    )


def solution(mesh):
    split = P("wide", "narrow")
    none3, cols, rows1 = P(None, None, "narrow"), P(None, "narrow"), P("narrow", None)
    return jax.shard_map(
        on_device,
        mesh=mesh,
        in_specs=(
            split, P("wide"), none3, cols, rows1, P(), cols, P("narrow"), rows1, P(), P(), P(), P(), P(), split,
        ),
        out_specs=(
            split, split, none3, cols, rows1, P(), cols, P("narrow"), rows1, P(), P(), P(), P(), P(),
        ),
        check_vma=False,
    )
```

```python
import functools

import jax
import jax.numpy as jnp
from jax import lax
from jax.experimental import pallas as pl
from jax.experimental.pallas import tpu as pltpu
from jax.sharding import PartitionSpec as P

EPS = 1e-05
HEAD = 64
F32, BF16 = jnp.float32, jnp.bfloat16
NT = (((1,), (1,)), ((), ()))
TN = (((0,), (0,)), ((), ()))
GELU_A, GELU_B = 0.7978845608028654, 0.044715
VMEM_LIMIT = 63 * 1024 * 1024


def dot(a, b):
    return jnp.dot(a, b, preferred_element_type=F32)


def dot_nt(a, b):
    return lax.dot_general(a, b, NT, preferred_element_type=F32)


def dot_tn(a, b):
    return lax.dot_general(a, b, TN, preferred_element_type=F32)


def params(**more):
    return pltpu.CompilerParams(vmem_limit_bytes=VMEM_LIMIT, **more)


def cost(flops, size, trans=0):
    return pl.CostEstimate(flops=int(flops), bytes_accessed=int(size), transcendentals=int(trans))


def lane_part(which, width):
    return pl.ds(pl.multiple_of(which * width, 128), width)


def norm_rows(x):
    mean = jnp.mean(x, axis=-1, keepdims=True)
    cen = x - mean
    var = jnp.mean(cen * cen, axis=-1, keepdims=True)
    r = lax.rsqrt(var + EPS)
    return cen * r, r


def rows_spec(rows, cols, base=0):
    return pl.BlockSpec((rows, cols), lambda i, *_: (i + base, 0))


def whole_spec(shape):
    zeros = (0,) * len(shape)
    return pl.BlockSpec(shape, lambda i, *_: zeros)


MESH = pl.DeviceIdType.MESH
scope = jax.named_scope


def vec(ref):
    return ref[...].astype(F32).reshape(1, -1)


def bit_of(index, bit):
    return (index // (1 << bit)) % 2


def flip(index, bit):
    return index + (1 - 2 * bit_of(index, bit)) * (1 << bit)


def greet(peers):
    barrier = pltpu.get_barrier_semaphore()
    for peer in peers:
        pl.semaphore_signal(barrier, inc=1, device_id=peer, device_id_type=MESH)
    pl.semaphore_wait(barrier, len(peers))


def remote(src, dst, sems, at, peer, send_at=None):
    return pltpu.make_async_remote_copy(
        src_ref=src, dst_ref=dst, send_sem=sems[0].at[at if send_at is None else send_at], recv_sem=sems[1].at[at],
        device_id=peer, device_id_type=MESH,
    )


def block_rows(start, size, unit=16):
    return pl.ds(start if isinstance(start, int) else pl.multiple_of(start, unit), size)


LINE, CHIPS = 4, 8


def when(cond, action):
    @pl.when(cond)
    def _():
        action()


def line_peer(me, by):
    q = (me // 4) % LINE
    return me + ((q + by) % LINE - q) * 4


class Chain:
    def __init__(self, me, order, rows, cols, sems, send_at, recv_at):
        self.me, self.cols, self.sems, self.send_at = me, cols, sems, send_at
        self.phases, self.ops, back = [], [], []
        base, size, box = 0, rows, 0
        for kind, bit in order:
            if kind == "line" and size % (16 * LINE):
                raise ValueError(rows)
            if kind == "all":
                ways = CHIPS >> (bit - 1)
                part = size // ways
                keep, give, boxes = base + (me // (1 << bit)) % ways * part, None, (ways - 1) * part
                self.ops.append(("send", len(self.phases), ways))
                back = [("share", len(self.phases), ways)] + back
            elif kind == "line":
                part = size // LINE
                keep, give, boxes = base + (me // 4) % LINE * part, None, 2 * (LINE - 1) * part
                self.ops += [("line", len(self.phases), i) for i in range(1, LINE)]
                back = [("spread", len(self.phases), i) for i in range(1, LINE)] + back
            elif size % 32 == 0:
                part = size // 2
                mine = bit_of(me, bit)
                keep, give, boxes = base + mine * part, base + (1 - mine) * part, part
                self.ops.append(("pair", len(self.phases), 0))
                back = [("join", len(self.phases), 0)] + back
            else:
                part, keep, give, boxes = size, base, base, size
                self.ops.append(("pair", len(self.phases), 0))
            self.phases.append((bit, base, keep, give, part, box))
            base, size, box = keep, part, box + boxes
        self.scatters = len(self.ops)
        self.ops += back
        self.base, self.size, self.box_rows = base, size, box
        self.recv_at, widest = [], 1
        for kind, _, i in self.ops:
            width = {"line": 2, "spread": 2, "send": i - 1, "share": i - 1}.get(kind, 1)
            self.recv_at.append(recv_at)
            recv_at, widest = recv_at + width, max(widest, width)
        self.recv_next, self.send_next = recv_at, send_at + widest

    def bind(self, src, box, part, own, dst=None, entry=0):
        self.src, self.box, self.part, self.own, self.dst = src, box, part, own, dst
        self.entry = self.ops[entry][1]
        return self

    def _source(self, phase):
        off = 0 if phase == 0 else self.phases[0][2]
        return (self.src if phase == self.entry else self.part), off

    def _target(self, phase):
        if phase == len(self.phases) - 1:
            return self.own, self.phases[phase][2]
        return self.part, self.phases[0][2]

    def _remote(self, op, lane, src, dst, to):
        return remote(src, dst, self.sems, self.recv_at[op] + lane, {"wide": to}, self.send_at + lane)

    def _add(self, rows, target, first, *terms):
        unit = next(u for u in (96, 64, 48, 32, 16) if rows % u == 0)

        def add(i, carry):
            total = None
            for ref, start in terms:
                value = ref[block_rows(start + i * unit, unit), self.cols]
                value = value.astype(F32) if len(terms) > 2 else value
                total = value if total is None else total + value
            target[block_rows(first + i * unit, unit), self.cols] = total.astype(BF16)
            return carry

        lax.fori_loop(0, rows // unit, add, 0)


    def _pair(self, op, phase):
        bit, _, _, give, rows, box = self.phases[phase]
        source, off = self._source(phase)
        src = source.at[block_rows(give - off, rows), self.cols]
        return self._remote(op, 0, src, self.box.at[pl.ds(box, rows), self.cols], flip(self.me, bit))

    def _join(self, op, phase):
        bit, _, keep, _, rows, _ = self.phases[phase]
        region = self.dst.at[block_rows(keep, rows), self.cols]
        return self._remote(op, 0, region, region, flip(self.me, bit))


    def _others(self, bit, ways):
        for m in range(1, ways):
            yield m - 1, flip_all(self.me, bit, m)

    def _sends(self, op, phase, ways):
        bit, base, _, _, rows, box = self.phases[phase]
        source, off = self._source(phase)
        for m, to in self._others(bit, ways):
            src = source.at[block_rows(base - off + (to // (1 << bit)) % ways * rows, rows), self.cols]
            yield self._remote(op, m, src, self.box.at[pl.ds(box + m * rows, rows), self.cols], to)

    def _shares(self, op, phase, ways, came):
        bit, base, keep, _, rows, _ = self.phases[phase]
        for m, to in self._others(bit, ways):
            at = base + (to // (1 << bit)) % ways * rows if came else keep
            region = self.dst.at[block_rows(at, rows), self.cols]
            yield self._remote(op, m, region, region, to)


    def _slot(self, phase, lane, i):
        rows, box = self.phases[phase][4:]
        return box + (lane * (LINE - 1) + i - 1) * rows

    def _line_sends(self, op, phase, i):
        q = (self.me // 4) % LINE
        _, base, _, _, rows, _ = self.phases[phase]
        source, off = self._source(phase)
        sends = []
        for lane, by in ((0, 1), (1, -1)):
            place_ = q if lane == 0 else LINE - 1 - q
            chunk = LINE - i if lane == 0 else i - 1
            dst = self.box.at[pl.ds(self._slot(phase, lane, i), rows), self.cols]
            to = line_peer(self.me, by)
            src = source.at[block_rows(base - off + chunk * rows, rows), self.cols]
            sends.append((place_ == 0, functools.partial(self._remote, op, lane, src, dst, to)))
            if i > 1:
                src = self.box.at[pl.ds(self._slot(phase, lane, i - 1), rows), self.cols]
                moving = jnp.logical_and(place_ >= 1, place_ <= min(i - 1, LINE - 2))
                sends.append((moving, functools.partial(self._remote, op, lane, src, dst, to)))
        return sends

    def _line_end(self, op, phase, i):
        q = (self.me // 4) % LINE
        _, base, keep, _, rows, _ = self.phases[phase]
        source, off = self._source(phase)
        for cond, copy in self._line_sends(op, phase, i):
            when(cond, lambda: copy().wait_send())
        for lane, by in ((0, -1), (1, 1)):
            place_ = q if lane == 0 else LINE - 1 - q
            slot = self._slot(phase, lane, i)
            dst = self.box.at[pl.ds(slot, rows), self.cols]
            arrived = jnp.logical_and(place_ >= 1, place_ <= i)
            chunk = LINE - 1 - i + q if lane == 0 else i + q - (LINE - 1)

            @pl.when(arrived)
            def _():
                self._remote(op, lane, dst, dst, line_peer(self.me, by)).wait_recv()
                if i < LINE - 1:
                    self._add(rows, self.box, slot, (self.box, slot), (source, base - off + chunk * rows))

        if i == LINE - 1:
            target, out = self._target(phase)
            own = (source, keep - off)
            left, right = (self.box, self._slot(phase, 0, i)), (self.box, self._slot(phase, 1, i))

            @pl.when(q == 0)
            def _():
                self._add(rows, target, keep - out, own, right)

            @pl.when(q == LINE - 1)
            def _():
                self._add(rows, target, keep - out, own, left)

            @pl.when(jnp.logical_and(q > 0, q < LINE - 1))
            def _():
                self._add(rows, target, keep - out, left, own, right)

    def _spread(self, op, phase, i):
        q = (self.me // 4) % LINE
        _, base, _, _, rows, _ = self.phases[phase]
        ways = []
        for lane, by in ((0, 1), (1, -1)):
            place_ = q if lane == 0 else LINE - 1 - q
            sent = self.dst.at[block_rows(base + (q - by * (i - 1)) * rows, rows), self.cols]
            came = self.dst.at[block_rows(base + (q - by * i) * rows, rows), self.cols]
            send_if = jnp.logical_and(place_ >= i - 1, place_ <= LINE - 2)
            ways.append(
                (
                    send_if, functools.partial(self._remote, op, lane, sent, sent, line_peer(self.me, by)),
                    place_ >= i, functools.partial(self._remote, op, lane, came, came, line_peer(self.me, -by)),
                )
            )
        return ways

    def start(self, op):
        kind, phase, i = self.ops[op]
        if kind == "pair":
            self._pair(op, phase).start()
        elif kind == "join":
            self._join(op, phase).start()
        elif kind == "send":
            for copy in self._sends(op, phase, i):
                copy.start()
        elif kind == "share":
            for copy in self._shares(op, phase, i, False):
                copy.start()
        elif kind == "line":
            for cond, copy in self._line_sends(op, phase, i):
                when(cond, lambda: copy().start())
        else:
            for cond, copy, _, _ in self._spread(op, phase, i):
                when(cond, lambda: copy().start())

    def end(self, op):
        kind, phase, i = self.ops[op]
        if kind == "pair":
            self._pair(op, phase).wait()
            _, _, keep, _, rows, box = self.phases[phase]
            source, off = self._source(phase)
            target, out = self._target(phase)
            self._add(rows, target, keep - out, (self.box, box), (source, keep - off))
        elif kind == "join":
            self._join(op, phase).wait()
        elif kind == "send":
            for copy in self._sends(op, phase, i):
                copy.wait()
            _, _, keep, _, rows, box = self.phases[phase]
            source, off = self._source(phase)
            target, out = self._target(phase)
            terms = [(self.box, box + m * rows) for m in range(i - 1)]
            self._add(rows, target, keep - out, (source, keep - off), *terms)
        elif kind == "share":
            for copy in self._shares(op, phase, i, False):
                copy.wait_send()
            for copy in self._shares(op, phase, i, True):
                copy.wait_recv()
        elif kind == "line":
            self._line_end(op, phase, i)
        else:
            for send_if, send, recv_if, recv in self._spread(op, phase, i):
                when(send_if, lambda: send().wait_send())
                when(recv_if, lambda: recv().wait_recv())

    def gather_open(self):
        self._add(self.size, self.dst, self.base, (self.own, 0))


class Group:
    def __init__(self, chain, entry=0, leave=None, out=None):
        self.chain, self.out = chain, out
        self.ops = list(range(entry, len(chain.ops) if leave is None else leave))
        self.pos = -1

    @property
    def done(self):
        return self.pos >= len(self.ops)

    def next(self):
        pos = self.pos
        self.pos = min(pos + 1, len(self.ops))

        def tick():
            if pos >= len(self.ops):
                return
            if pos >= 0:
                self.chain.end(self.ops[pos])
            if pos + 1 >= len(self.ops):
                if self.out is not None:
                    self.store().start()
                return
            if self.ops[pos + 1] == self.chain.scatters:
                self.chain.gather_open()
            self.chain.start(self.ops[pos + 1])

        return tick

    def tick(self):
        self.next()()

    def store(self):
        out, sem = self.out
        return pltpu.make_async_copy(self.chain.dst.at[:, self.chain.cols], out.at[:, self.chain.cols], sem)


def bits(wide):
    return wide.bit_length() - 1


def order_of(wide, kind):
    first, rest = ("pair", 0), [("pair", b) for b in range(4, bits(wide))]
    pair, line = ("pair", 1), ("line", 2)
    return {
        0: [first, pair, line, *rest], 1: [first, line, pair, *rest], 2: [first, ("all", 1), *rest],
        3: [first, pair, ("all", 2), *rest],
    }[kind]


def lanes_split(cols, kinds):
    w = cols // len(kinds)
    return [(kind, pl.ds(i * w, w)) for i, kind in enumerate(kinds)]


def flip_all(me, bit, mask):
    to = me
    for i in range(3):
        if mask >> i & 1:
            to = to + (flip(me, bit + i) - me)
    return to


def chip_peers(me):
    return [flip_all(me, 1, m) for m in range(1, CHIPS)]


def wide_peers(me, wide):
    pairs = [flip(me, b) for b in range(bits(wide)) if b not in (1, 2, 3)]
    return [{"wide": peer} for peer in pairs + chip_peers(me)]


class Small:
    def __init__(self, me, n, wide, total, box, shared, narrow, across, narrow_at, send_at, recv_at):
        self.me, self.n, self.total, self.box, self.shared = me, n, total, box, shared
        self.narrow, self.across = narrow, across
        self.narrow_at, self.send_at, self.recv_at = narrow_at, send_at, recv_at
        self.ops = ["narrow", 0, "chips"] + list(range(4, bits(wide)))
        self.scatters, self.dst = None, None
        self.send_next = send_at + CHIPS - 1
        self.recv_next = recv_at + len(self.ops) + CHIPS - 1

    def _copies(self, op):
        kind = self.ops[op]
        if kind == "narrow":
            top = pl.ds(0, self.shared)
            return [remote(self.total.at[top], self.box.at[0, top], self.narrow, self.narrow_at, {"narrow": 1 - self.n})]
        if kind == "chips":
            return [
                remote(
                    self.total, self.box.at[2 + i], self.across, self.recv_at + len(self.ops) + i, {"wide": to},
                    self.send_at + i,
                )
                for i, to in enumerate(chip_peers(self.me))
            ]
        slot = 1 if kind == 0 else CHIPS + 1 + kind - 4
        peer = {"wide": flip(self.me, kind)}
        return [remote(self.total, self.box.at[slot], self.across, self.recv_at + op, peer, self.send_at)]

    def start(self, op):
        for copy in self._copies(op):
            copy.start()

    def end(self, op):
        for copy in self._copies(op):
            copy.wait()
        kind = self.ops[op]
        if kind == "narrow":
            self.total[0 : self.shared, :] += self.box[0, 0 : self.shared, :]
        elif kind == "chips":
            self.total[...] += sum(self.box[2 + i] for i in range(CHIPS - 1))
        else:
            self.total[...] += self.box[1 if kind == 0 else CHIPS + 1 + kind - 4]


def vmem():
    return pl.BlockSpec(memory_space=pltpu.VMEM)


def anywhere():
    return pl.BlockSpec(memory_space=pl.ANY)


def sems(*counts):
    return [pltpu.SemaphoreType.DMA((c,)) for c in counts]


def qkv_body(own_hbm, own, w, bias, gain, shift, xf, low, q, k, v, got, send_sem, recv_sem):
    n = lax.axis_index("narrow")
    i = pl.program_id(0)
    rows, cw = own.shape
    peer = {"narrow": 1 - n}

    def copy(at):
        block = block_rows(at * rows, rows)
        return remote(own_hbm.at[block], got.at[block], (send_sem, recv_sem), at, peer)

    @pl.when(i == 0)
    def _():
        greet([peer])
        for at in range(got.shape[0] // rows):
            copy(at).start()

    xf[:, lane_part(n, cw)] = own[...]
    with scope("wait"):
        copy(i).wait()
    xf[:, lane_part(1 - n, cw)] = got[block_rows(i * rows, rows), :]
    xhat, _ = norm_rows(xf[...].astype(F32))
    y = (xhat * vec(gain) + vec(shift)).astype(BF16)
    low[...] = y
    q[...] = (dot(y, w[0]) + bias[0:1, :].astype(F32)).astype(BF16) * jnp.asarray(HEAD**-0.5, BF16)
    k[...] = dot(y, w[1]).astype(BF16)
    v[...] = (dot(y, w[2]) + bias[1:2, :].astype(F32)).astype(BF16)


def qkv_call(own, w, bias, gain, shift, block=256):
    rows, cw = own.shape
    d, lw = w.shape[1], w.shape[2]
    sd = jax.ShapeDtypeStruct
    return pl.pallas_call(
        qkv_body,
        out_shape=(sd((rows, d), BF16), sd((rows, d), BF16)) + (sd((rows, lw), BF16),) * 3,
        grid_spec=pltpu.PrefetchScalarGridSpec(
            num_scalar_prefetch=0,
            grid=(rows // block,),
            in_specs=[anywhere(), rows_spec(block, cw)] + [whole_spec(a.shape) for a in (w, bias, gain, shift)],
            out_specs=[rows_spec(block, d)] * 2 + [rows_spec(block, lw)] * 3,
            scratch_shapes=[pltpu.VMEM((rows, cw), BF16)] + sems(rows // block, rows // block),
        ),
        compiler_params=params(collective_id=1, has_side_effects=True),
        cost_estimate=cost(2 * rows * d * 3 * lw, 2 * (rows * d * 5 + w.size)),
        name="norm_qkv",
    )(own, own, w, bias, gain, shift)


def three(x):
    hi = x.astype(BF16).astype(F32)
    mid = (x - hi).astype(BF16).astype(F32)
    return hi, mid, x - hi - mid


def lanes_of(par):
    lane = lax.broadcasted_iota(jnp.int32, (1, 2 * HEAD), 1)
    mine = (lane // HEAD) == par
    return lane, mine, (1 - par) * HEAD


def place(lane, mine, at, base, terms):
    out = jnp.where(mine, base, 0.0)
    for i, term in enumerate(terms):
        out = jnp.where(lane == at + i, term, out)
    return out


def fwd_body(
    len_ref, q, k, v, pw, o, qa_out, o_got, pw_got, ka, va, send_sem, recv_sem, *, bq
):
    head = pl.program_id(0)
    par, pair = head % 2, head // 2
    lane, mine, at = lanes_of(par)
    n, me = lax.axis_index("narrow"), lax.axis_index("wide")
    peer, core = {"narrow": 1 - n}, {"wide": flip(me, 0)}
    pairs = pl.num_programs(0) // 2
    both = (send_sem, recv_sem)
    cols = lane_part(pair, 2 * HEAD)
    part = block_rows((me % 2) * (pw.shape[0] // 2), pw.shape[0] // 2)
    npairs = o.shape[1] // (2 * HEAD)
    weights = remote(pw.at[part], pw_got.at[part], both, npairs, peer)
    shared = remote(pw_got.at[part], pw_got.at[part], both, npairs + 1, core)

    @pl.when(head == 0)
    def _():
        greet([peer, core])
        weights.start()

    keys = k.shape[0]
    kpos = lax.broadcasted_iota(jnp.int32, (keys, 1), 0)
    kbias = jnp.where(kpos < len_ref[0], 0.0, -1e30)
    ka[...] = place(lane, mine, at, k[...].astype(F32), [kbias]).astype(BF16)
    va[...] = place(lane, mine, at, v[...].astype(F32), [1.0]).astype(BF16)
    tri = lax.broadcasted_iota(jnp.int32, (bq, bq), 1) <= lax.broadcasted_iota(jnp.int32, (bq, bq), 0)
    for i in range(q.shape[0] // bq):
        nk = (i + 1) * bq
        rows = pl.ds(i * bq, bq)
        qf = q[rows, :].astype(F32)
        qa = place(lane, mine, at, qf, [1.0])
        s = dot_nt(qa.astype(BF16), ka[0:nk, :])
        edge = jnp.where(tri, s[:, nk - bq :], -1e30)
        m = jnp.max(edge, axis=1, keepdims=True)
        if nk > bq:
            m = jnp.maximum(m, jnp.max(s[:, : nk - bq], axis=1, keepdims=True))
        pv = dot(jnp.exp(edge - m).astype(BF16), va[nk - bq : nk, :])
        if nk > bq:
            pv += dot(jnp.exp(s[:, : nk - bq] - m).astype(BF16), va[0 : nk - bq, :])
        total = jnp.sum(jnp.where(lane == at, pv, 0.0), axis=1, keepdims=True)
        out = (pv / total).astype(BF16).astype(F32)
        old = o[rows, cols].astype(F32)
        o[rows, cols] = jnp.where(mine, out, jnp.where(par == 0, 0.0, old)).astype(BF16)
        lse = m + jnp.log(total)
        qa_out[0, rows, :] = place(lane, mine, at, qf, [1.0, *three(lse)]).astype(BF16)

    def mixed(j):
        c = pl.ds(j * 2 * HEAD, 2 * HEAD)
        return remote(o.at[:, c], o_got.at[:, c], both, j, peer)

    for j in range(npairs):

        @pl.when(head == 2 * j + 1)
        def _():
            mixed(j).start()

    @pl.when(head == 3)
    def _():
        weights.wait()
        shared.start()

    @pl.when(head == 2 * npairs - 1)
    def _():
        shared.wait()
        for j in range(npairs):
            mixed(j).wait()


def attend_forward(length, q, k, v, pw, bq=256):
    rows, width = q.shape
    heads, pair = width // HEAD, 2 * HEAD
    half = lambda h, *_: (0, h // 2)
    sd = jax.ShapeDtypeStruct
    work = 2 * heads * rows * rows * HEAD
    return pl.pallas_call(
        functools.partial(fwd_body, bq=bq),
        out_shape=(
            sd((rows, width), BF16), sd((heads, rows, pair), BF16), sd((rows, width), BF16), sd(pw.shape, BF16),
        ),
        grid_spec=pltpu.PrefetchScalarGridSpec(
            num_scalar_prefetch=1,
            grid=(heads,),
            in_specs=[pl.BlockSpec((rows, pair), half)] * 3 + [anywhere()],
            out_specs=[vmem(), pl.BlockSpec((1, rows, pair), lambda h, *_: (h, 0, 0)), anywhere(), anywhere()],
            scratch_shapes=[pltpu.VMEM((rows, pair), BF16)] * 2 + sems(heads // 2 + 2, heads // 2 + 2),
        ),
        compiler_params=params(collective_id=2, has_side_effects=True),
        cost_estimate=cost(4 * work, 2 * rows * width * 6, work // 256),
        name="attend_fwd",
    )(length, q, k, v, pw)


DOWN_ENTRY, UP_ENTRY = (2, 2), (1, 1)
DOWN_KINDS, UP_KINDS = (0, 0), (0, 1)


def mlp_body(
    len_ref, xf_hbm, mo_hbm, mr_hbm, pwo_hbm, pwr_hbm, pb, gain, shift, ub, up_hbm, down_hbm, cot_hbm,
    lo_out, lo_send_out, gmix, gm_out, up_part, down_part, gp_own, gp_other, sum_ub, sum_db, sum_g, sum_s, sum_pb,
    xf, mo, mr, pwo, pwr, up, down, cot, cot_got, cf, lo, lo_send, mid, second, active, slope, gh,
    gs_send, gs_got, gs_own, gdown, gup, box, up_box, gm, glow, gmix_send, load_sem, store_sem, nsend, nrecv, wsend, wrecv,
    *, wide,
):
    n, me = lax.axis_index("narrow"), lax.axis_index("wide")
    peer = {"narrow": 1 - n}
    rows, cw = cot.shape
    d, f = up.shape
    half, block = rows // 2, min(256, rows // 2)
    each = half // block
    mine, other = lane_part(n, cw), lane_part(1 - n, cw)
    narrow, across = (nsend, nrecv), (wsend, wrecv)
    count = iter(range(16))

    def load(src, dst):
        copy = pltpu.make_async_copy(src, dst, load_sem.at[next(count)])
        copy.start()
        return copy

    his, own = block_rows((1 - n) * half, half), block_rows(n * half, half)
    first = [load(a, b) for a, b in ((pwo_hbm, pwo), (pwr_hbm, pwr))]
    first += [load(a.at[his], b.at[his]) for a, b in ((xf_hbm, xf), (mo_hbm, mo), (mr_hbm, mr))]
    up_load = load(up_hbm, up)
    greet([peer] + wide_peers(me, wide))

    def cot_copy(side, j, a):
        r = block_rows(side * half + j * block, block)
        return remote(cot_hbm.at[r], cot_got.at[r], narrow, a * each + j, peer)

    for a, side in enumerate((n, 1 - n)):
        for j in range(each):
            cot_copy(side, j, a).start()
    down_load = load(down_hbm, down)
    cot_load = load(cot_hbm, cot)
    rest = [load(a.at[own], b.at[own]) for a, b in ((xf_hbm, xf), (mo_hbm, mo), (mr_hbm, mr))]

    def project(at):
        r = block_rows(at, block)
        m = xf[r, :].astype(F32) + (dot(mo[r, :], pwo[...]) + dot(mr[r, :], pwr[...])) + vec(pb)
        mid[r, :] = m
        xhat, _ = norm_rows(m)
        second[r, :] = (xhat * vec(gain) + vec(shift)).astype(BF16)

    def forward(at):
        r = block_rows(at, block)
        hid = dot(second[r, :], up[...]) + vec(ub)
        sq = hid * hid
        t = jnp.tanh(GELU_A * (hid + GELU_B * (sq * hid)))
        hf = 0.5 * (1.0 + t)
        act = (hid * hf).astype(BF16)
        active[r, :] = act
        slope[r, :] = hf + (0.5 * hid) * (1.0 - t * t) * (GELU_A + (3.0 * GELU_A * GELU_B) * sq)
        lo[r, :] = mid[r, mine] + dot(act, down[:, mine])
        lo_send[r, :] = dot(act, down[:, other]).astype(BF16)

    def backward(at):
        r = block_rows(at, block)
        pos = at + lax.broadcasted_iota(jnp.int32, (block, 1), 0)
        live = (pos < len_ref[0]).astype(F32)
        cf[r, mine] = (cot[r, :].astype(F32) * live).astype(BF16)
        cf[r, other] = (cot_got[r, :].astype(F32) * live).astype(BF16)
        ghid = (dot_nt(cf[r, :], down[...]) * slope[r, :]).astype(BF16)
        gh[r, :] = ghid
        sum_ub[...] += jnp.sum(ghid.astype(F32), axis=0, keepdims=True)
        return dot_nt(ghid, up[...])

    def every(side, body):
        def step(j, carry):
            body(side * half + j * block)
            return carry

        lax.fori_loop(0, each, step, 0)

    def both(at):
        project(at)
        forward(at)

    for ref in (sum_ub, sum_g, sum_s, sum_pb, sum_db):
        ref[...] = jnp.zeros_like(ref)
    with scope("load"):
        for copy in first:
            copy.wait()
    with scope("project"):
        every(1 - n, project)
    with scope("load2"):
        up_load.wait()
        down_load.wait()
    with scope("fwd_peer"):
        every(1 - n, forward)
    for copy in rest:
        copy.wait()
    with scope("fwd_own"):
        every(n, both)
    stores = []

    def store(src, dst):
        copy = pltpu.make_async_copy(src, dst, store_sem.at[len(stores)])
        copy.start()
        stores.append(copy)

    store(lo, lo_out)
    store(lo_send, lo_send_out)
    with scope("cot_wait"):
        cot_load.wait()
        for j in range(each):
            cot_copy(n, j, 0).wait()

    def gs_copy(j):
        r = block_rows(j * block, block)
        return remote(gs_send.at[r], gs_got.at[r], narrow, 2 * each + j, peer)

    def for_peer(j, carry):
        gs_send[block_rows(j * block, block), :] = backward((1 - n) * half + j * block).astype(BF16)
        gs_copy(j).start()
        return carry

    def for_own(j, carry):
        gs_own[block_rows(j * block, block), :] = backward(n * half + j * block)
        return carry

    with scope("for_peer"):
        lax.fori_loop(0, each, for_peer, 0)
    with scope("cot_wait2"):
        for j in range(each):
            cot_copy(1 - n, j, 1).wait()
    with scope("for_own"):
        lax.fori_loop(0, each, for_own, 0)

    def weight(dst, left, right):
        def step(i, carry):
            c = block_rows(i * 256, 256, 256)
            dst[c, :] = dot_tn(left[:, c], right[...]).astype(BF16)
            return carry

        lax.fori_loop(0, dst.shape[0] // 256, step, 0)

    used = iter(range(16))

    def group(src, box_, part, kinds, leaves):
        parts = []
        for (kind, cols), leave in zip(lanes_split(src.shape[1], kinds), leaves):
            a = next(used)
            chain = Chain(me, order_of(wide, kind), src.shape[0], cols, across, 2 * a, 2 * a)
            parts.append(Group(chain.bind(src, box_, part, None), leave=leave))
        return parts

    reduce_down = group(gdown, box, down_part, DOWN_KINDS, DOWN_ENTRY)
    reduce_up = group(gup, up_box, up_part, UP_KINDS, UP_ENTRY)

    def advance(name, *groups):
        with scope(name):
            for one in groups:
                one.tick()

    with scope("w_down"):
        weight(gdown, active, cf)
    advance("core_d", *reduce_down)
    with scope("w_up"):
        weight(gup, second, gh)
    advance("core_u", *reduce_down, *reduce_up)
    with scope("gs_wait"):
        for j in range(each):
            gs_copy(j).wait()

    def gmix_copy(j):
        r = block_rows(n * half + j * block, block)
        return remote(gmix_send.at[block_rows(j * block, block)], gmix.at[r], narrow, 3 * each + j, peer)

    def back_norm(j, carry):
        r, rh = block_rows(n * half + j * block, block), block_rows(j * block, block)
        g = gs_own[rh, :] + gs_got[rh, :].astype(F32)
        xhat, scale = norm_rows(mid[r, :])
        gg = g * vec(gain)
        m1 = jnp.mean(gg, axis=-1, keepdims=True)
        m2 = jnp.mean(gg * xhat, axis=-1, keepdims=True)
        c = cf[r, :].astype(F32)
        grad = c + scale * (gg - m1 - xhat * m2)
        gm[rh, :] = grad
        gl = grad.astype(BF16)
        glow[rh, :] = gl
        gmix_send[rh, :] = dot_nt(gl, pwr[...]).astype(BF16)
        gmix_copy(j).start()
        gmix[r, :] = dot_nt(gl, pwo[...]).astype(BF16)
        sum_g[...] += jnp.sum(g * xhat, axis=0, keepdims=True)
        sum_s[...] += jnp.sum(g, axis=0, keepdims=True)
        sum_pb[...] += jnp.sum(grad, axis=0, keepdims=True)
        sum_db[...] += jnp.sum(c, axis=0, keepdims=True)
        return carry

    with scope("back_norm"):
        lax.fori_loop(0, each, back_norm, 0)
    store(gm, gm_out)
    advance("across", *reduce_up)
    with scope("proj"):
        lw = mo.shape[1]
        for src, dst in ((mr, gp_other), (mo, gp_own)):
            total = dot_tn(src[own, :], glow[...]).astype(BF16)
            dst[0:lw, :] = total[:, :cw]
            dst[lw : 2 * lw, :] = total[:, cw:]
    with scope("gmix_wait"):
        for j in range(each):
            gmix_copy(j).wait()
    advance("leave", *reduce_down, *reduce_up)
    with scope("store"):
        for copy in stores:
            copy.wait()


def mlp_call(length, xf, mo, mr, pwo, pwr, pb, gain, shift, up, ub, down, cot, wide):
    rows, d = xf.shape
    f, lw, cw = up.shape[1], mo.shape[1], cot.shape[1]
    half = rows // 2
    sd, vm = jax.ShapeDtypeStruct, pltpu.VMEM
    each = half // min(256, half)
    return pl.pallas_call(
        functools.partial(mlp_body, wide=wide),
        out_shape=(
            sd((rows, cw), F32), sd((rows, cw), BF16), sd((rows, lw), BF16), sd((half, d), F32),
            sd((d // 2, f), BF16), sd((f // 2, d), BF16), sd((2 * lw, cw), BF16), sd((2 * lw, cw), BF16),
            sd((1, f), F32), sd((1, d), F32), sd((1, d), F32), sd((1, d), F32), sd((1, d), F32),
        ),
        in_specs=[pl.BlockSpec(memory_space=pltpu.SMEM)] + [anywhere()] * 5 + [vmem()] * 4 + [anywhere()] * 3,
        out_specs=(anywhere(), anywhere(), vmem(), anywhere()) + (vmem(),) * 9,
        scratch_shapes=[
            vm((rows, d), BF16), vm((rows, lw), BF16), vm((rows, lw), BF16), vm((lw, d), BF16), vm((lw, d), BF16),
            vm((d, f), BF16), vm((f, d), BF16), vm((rows, cw), BF16), vm((rows, cw), BF16), vm((rows, d), BF16),
            vm((rows, cw), F32), vm((rows, cw), BF16), vm((rows, d), F32),
            vm((rows, d), BF16), vm((rows, f), BF16), vm((rows, f), F32), vm((rows, f), BF16),
            vm((half, d), BF16), vm((half, d), BF16), vm((half, d), F32), vm((f, d), BF16), vm((d, f), BF16),
            vm((f, d), BF16), vm((d, f), BF16), vm((half, d), F32), vm((half, d), BF16), vm((half, lw), BF16),
        ]
        + sems(12, 4, 4 * each, 4 * each, 8, 8),
        compiler_params=params(collective_id=3, has_side_effects=True),
        cost_estimate=cost(2 * rows * d * (d + 6 * f), 2 * (rows * d * 8 + 2 * d * f), rows * f),
        name="mlp",
    )(length, xf, mo, mr, pwo, pwr, pb, gain, shift, ub, up, down, cot)


HEAD_TICKS = (
    ((1, 2), "U1"),
    ((1, 3), "D1U0D0Q0"),
    ((2, 2), "Q0U1"),
    ((2, 3), "D1"),
    ((3, 1), "U0SA"),
    ((3, 2), "D0P0"),
    ((3, 3), "SAQ0U1Q1"),
    ((4, 1), "D1"),
    ((4, 2), "U0Q1"),
    ((4, 3), "D0"),
    ((5, 0), "P0"),
    ((5, 3), "Q0D1U1Q2"),
)
PART_TICKS = ("U0D0SAQ1P0Q2", "Q0D1U1", "Q1U0", "D0P0", "Q0Q2")
LAST_TICKS = (
    "D1Q1P0U1Q2Q1", "norm0", "U0Q2D0Q0D1Q2P0U1", "D1Q1U0", "norm1", "Q0Q2P0D0D0U1Q1Q0",
    "U1Q2SBU0SBP0Q1U0", "Q2Q0Q0P0SBQ1P0Q1", "Q2Q2",
)


def pieces(names):
    return [names[i : i + 2] for i in range(0, len(names), 2)]


def back_body(
    len_ref, qa_hbm, k_hbm, v_hbm, do_hbm, o_hbm, low_hbm, w_hbm, xf_hbm, gm_hbm, gain, lo_send, up_part_hbm,
    down_part_hbm, gp_own_hbm, gp_other_hbm, s_ub, s_db, s_g2, s_s2, s_pb,
    lo_got, down_out, up_out, gp_out, g0_out, g1_out, g2_out, ig, small_a, small_b,
    qa, k, v, do, o, low, wp, xf, gm, up_part, down_part, gp_src, gp_got,
    ka, va, dk_acc, dv_acc, dqkv, gpair,
    down_box, down_part2, down_own, up_box, up_part2, up_own, gp_box, gp_part, gp_own, pair_box, pair_part, pair_own,
    down_sum, up_sum, gp_sum, pair_sum,
    gn_send, gn_got, gn_own, ig_own, ig_send, early, early_box, late_sums, late_box,
    load_sem, open_sem, nsend, nrecv, wsend, wrecv, *, bq, wide,
):
    n, me = lax.axis_index("narrow"), lax.axis_index("wide")
    peer = {"narrow": 1 - n}
    narrow, across = (nsend, nrecv), (wsend, wrecv)
    steps = bits(wide)
    heads, rows = qa.shape[0], qa.shape[1]
    pair_w = 2 * HEAD
    pairs = heads // 2
    d, lw = gain.shape[0], k.shape[1]
    cw = d // 2
    half, block = rows // 2, min(256, rows // 2)
    each = half // block
    count = iter(range(64))

    def load(src, dst):
        copy = pltpu.make_async_copy(src, dst, load_sem.at[next(count)])
        copy.start()
        return copy

    pair_loads = []
    for p in range(pairs):
        c = pl.ds(p * pair_w, pair_w)
        pair_loads.append(
            [load(a.at[:, c], b.at[:, c]) for a, b in ((k_hbm, k), (v_hbm, v), (do_hbm, do), (o_hbm, o))]
            + [load(qa_hbm.at[pl.ds(2 * p, 2)], qa.at[pl.ds(2 * p, 2)])]
        )
    part_load = load(down_part_hbm, down_part)
    up_load = load(up_part_hbm, up_part)
    gp_load = load(gp_own_hbm, gp_src)
    low_load = load(low_hbm, low)
    greet([peer] + wide_peers(me, wide))
    gp_swap = remote(gp_other_hbm, gp_got, narrow, 0, peer)
    layer = remote(lo_send, lo_got, narrow, 1, peer)
    gp_swap.start()
    late = [
        load(w_hbm.at[c, :, pl.ds(p * pair_w, pair_w)], wp.at[p, :, pl.ds(c * pair_w, pair_w)])
        for p in range(pairs)
        for c in range(3)
    ]
    own_half = block_rows(n * half, half)
    late += [load(xf_hbm.at[own_half], xf), load(gm_hbm, gm)]

    at = [0, 0]
    opening = iter(range(16))

    def group(src, box, part, own, dst, out, kinds=(0,), entries=(0,)):
        rows_, cols_ = dst.shape
        made = []
        for (kind, cols), entry in zip(lanes_split(cols_, kinds), entries):
            chain = Chain(me, order_of(wide, kind), rows_, cols, across, *at)
            at[:] = chain.send_next, chain.recv_next
            made.append(Group(chain.bind(src, box, part, own, dst, entry), entry, out=(out, open_sem.at[next(opening)])))
        return made

    groups = {}
    groups["D0"], groups["D1"] = group(down_part, down_box, down_part2, down_own, down_sum, down_out, DOWN_KINDS, DOWN_ENTRY)
    groups["U0"], groups["U1"] = group(up_part, up_box, up_part2, up_own, up_sum, up_out, UP_KINDS, UP_ENTRY)
    groups["P0"] = group(gp_src, gp_box, gp_part, gp_own, gp_sum, gp_out, kinds=(1,))[0]
    for p, out in zip(range(pairs), (g0_out, g1_out, g2_out)):
        groups[f"Q{p}"] = group(
            gpair.at[p], pair_box.at[p], pair_part.at[p], pair_own.at[p], pair_sum.at[p], out,
        )[0]

    dr, fr, lr = d // 128, s_ub.shape[1] // 128, lw // 128
    for i, (name, total, box, shared) in enumerate(
        (("SA", early, early_box, 4 * dr), ("SB", late_sums, late_box, -(-2 * dr // 8) * 8))
    ):
        one = Small(me, n, wide, total, box, shared, narrow, across, 2 + 2 * each + i, *at)
        at[:] = one.send_next, one.recv_next
        groups[name] = Group(one)

    def put_sum(ref, start, value):
        for i in range(value.shape[1] // 128):
            ref[start + i : start + i + 1, :] = value[:, i * 128 : (i + 1) * 128]

    early[...] = jnp.zeros_like(early)
    late_sums[...] = jnp.zeros_like(late_sums)
    for i, ref in enumerate((s_g2, s_s2, s_pb, s_db, s_ub)):
        put_sum(early, i * dr, ref[...])

    def tick(names):
        for name in pieces(names):
            with scope(name):
                groups[name].tick()

    part_load.wait()
    tick("D0D1")
    up_load.wait()
    tick("U0U1SA")

    kpos = lax.broadcasted_iota(jnp.int32, (rows, 1), 0)
    kbias = jnp.where(kpos < len_ref[0], 0.0, -1e30)
    tri = lax.broadcasted_iota(jnp.int32, (bq, bq), 0) <= lax.broadcasted_iota(jnp.int32, (bq, bq), 1)

    def plan(names):
        ticks = [groups[name].next() for name in pieces(names)]

        def run():
            for name, one in zip(pieces(names), ticks):
                with scope(name):
                    one()

        return run

    def start_proj():
        first = groups["P0"].next()

        def run():
            gp_swap.wait()
            gp_load.wait()
            gp_src[...] = gp_src[...] + gp_got[...]
            first()

        return run

    hooks = {}
    for at_, names in HEAD_TICKS:
        hooks[at_] = [plan(names)]
        if at_ == (2, 3):
            hooks[at_] += [layer.start, start_proj()]

    def run_hooks(head, block_):
        for (h, where), actions in hooks.items():
            if where == block_:

                @pl.when(head == h)
                def _():
                    for action in actions:
                        action()

    def one_head(head, carry):
        par, pair = head % 2, head // 2
        lane, mine, extra = lanes_of(par)
        cols = lane_part(pair, pair_w)
        for p in range(pairs):

            @pl.when(head == 2 * p)
            def _():
                for copy in pair_loads[p]:
                    copy.wait()

        ka[...] = place(lane, mine, extra, k[:, cols].astype(F32), [kbias, -1.0, -1.0, -1.0]).astype(BF16)
        va[...] = place(lane, mine, extra, v[:, cols].astype(F32), [-1.0, -1.0, -1.0]).astype(BF16)
        dk_acc[...] = jnp.zeros_like(dk_acc)
        dv_acc[...] = jnp.zeros_like(dv_acc)

        def put(c, r, new):
            lanes = pl.ds(c * pair_w, pair_w)
            old = dqkv[pair, r, lanes].astype(F32)
            dqkv[pair, r, lanes] = jnp.where(mine, new, jnp.where(par == 0, 0.0, old)).astype(BF16)

        for i in range(rows // bq):
            r = pl.ds(i * bq, bq)
            qb = qa[head, r, :]
            df = do[r, cols].astype(F32)
            delta = jnp.sum(jnp.where(mine, df * o[r, cols].astype(F32), 0.0), axis=1, keepdims=True)
            db = place(lane, mine, extra, df, three(delta)).astype(BF16)
            dqs = None
            for j in range(i + 1):
                c = pl.ds(j * bq, bq)
                kb, vb = ka[c, :], va[c, :]
                s = dot_nt(kb, qb)
                if j == i:
                    s = jnp.where(tri, s, -1e30)
                p = jnp.exp(s)
                ds = (p * dot_nt(vb, db)).astype(BF16)
                dv_acc[c, :] += dot(p.astype(BF16), db)
                dk_acc[c, :] += dot(ds, qb)
                part = dot_tn(ds, kb)
                dqs = part if dqs is None else dqs + part
            put(0, r, dqs * HEAD**-0.5)
            if i < rows // bq - 1:
                run_hooks(head, i)
        put(1, pl.ds(0, rows), dk_acc[...])
        put(2, pl.ds(0, rows), dv_acc[...])

        @pl.when(head == 1)
        def _():
            low_load.wait()

        @pl.when(par == 1)
        def _():
            with scope("weights"):
                gpair[pair] = dot_tn(low[...], dqkv[pair]).astype(BF16)

        run_hooks(head, rows // bq - 1)
        return carry

    lax.fori_loop(0, heads, one_head, 0)

    for copy in late:
        copy.wait()

    def gn_part(start):
        r = block_rows(start, block)
        total = dot_nt(dqkv[0, r, :], wp[0])
        for p in range(1, pairs):
            total += dot_nt(dqkv[p, r, :], wp[p])
        return total

    def gn_copy(j):
        r = pl.ds(j * block, block)
        return remote(gn_send.at[r], gn_got.at[r], narrow, 2 + j, peer)

    for j in range(each):
        with scope("gn_peer"):
            gn_send[j * block : (j + 1) * block, :] = gn_part((1 - n) * half + j * block).astype(BF16)
        gn_copy(j).start()
        tick(PART_TICKS[j % 2])
    for j in range(each):
        with scope("gn_own"):
            gn_own[j * block : (j + 1) * block, :] = gn_part(n * half + j * block)
        tick(PART_TICKS[2 + j % 2])

    shared = -(-2 * dr // 8) * 8
    for p in range(pairs):
        put_sum(late_sums, shared + p, jnp.sum(dqkv[p, :, 0:pair_w].astype(F32), axis=0, keepdims=True))
        put_sum(late_sums, shared + lr + p, jnp.sum(dqkv[p, :, 2 * pair_w :].astype(F32), axis=0, keepdims=True))
    tick(PART_TICKS[4])

    mine, other = lane_part(n, cw), lane_part(1 - n, cw)

    def ig_copy(j):
        r = block_rows(n * half + j * block, block)
        return remote(ig_send.at[pl.ds(j * block, block)], ig.at[r], narrow, 2 + each + j, peer)

    def in_norm(j):
        with scope("gn_wait"):
            gn_copy(j).wait()
        rh = pl.ds(j * block, block)
        r = block_rows(n * half + j * block, block)
        g = gn_own[rh, :] + gn_got[rh, :].astype(F32)
        xhat, scale = norm_rows(xf[rh, :].astype(F32))
        gg = g * vec(gain)
        m1 = jnp.mean(gg, axis=-1, keepdims=True)
        m2 = jnp.mean(gg * xhat, axis=-1, keepdims=True)
        ig_own[...] = gm[rh, :] + scale * (gg - m1 - xhat * m2)
        ig_send[rh, :] = ig_own[:, other].astype(BF16)
        ig_copy(j).start()
        ig[r, :] = ig_own[:, mine].astype(BF16)
        return jnp.sum(g * xhat, axis=0, keepdims=True), jnp.sum(g, axis=0, keepdims=True)

    sums1 = []
    for names in LAST_TICKS:
        if names in ("norm0", "norm1"):
            todo = range(each - 1) if names == "norm0" else range(each - 1, each)
            sums1 += [in_norm(j) for j in todo]
            if names == "norm1":
                put_sum(late_sums, 0, sum(a for a, _ in sums1))
                put_sum(late_sums, dr, sum(b for _, b in sums1))
                tick("SB")
        else:
            tick(names)
    while not all(g.done for g in groups.values()):
        for name in groups:
            tick(name)
    small_a[...] = early[...]
    small_b[...] = late_sums[...]
    with scope("end"):
        for one in groups.values():
            if one.out is not None:
                one.store().wait()
        layer.wait()
        for j in range(each):
            ig_copy(j).wait()


def back_call(
    length, qa, k, v, do, o, low, w, xf, gm, gain, lo_send, up_part, down_part, gp_own, gp_other,
    s_ub, s_db, s_g2, s_s2, s_pb, wide, bq=256,
):
    heads, rows, pair = qa.shape
    d, f, lw = gain.shape[0], up_part.shape[1], k.shape[1]
    cw, half = d // 2, rows // 2
    block = min(256, half)
    each, steps, pairs = half // block, bits(wide), heads // 2
    sd, vm = jax.ShapeDtypeStruct, pltpu.VMEM
    shape = lambda r, kind=0: Chain(0, order_of(wide, kind), r, None, None, 0, 0)
    c_down, c_up, c_gp = shape(f), shape(d), shape(2 * lw)
    down_rows, up_rows, pair_rows = (max(shape(r, k).box_rows for k in range(4)) for r in (f, d, d))
    small = lambda shared, rest: -(-(shared + rest) // 8) * 8
    rows_a = small(4 * d // 128, f // 128)
    rows_b = small(-(-2 * d // 1024) * 8, 2 * lw // 128)
    slots = CHIPS + 1 + max(0, bits(wide) - 4)
    semaphores = (len(DOWN_KINDS) + len(UP_KINDS) + 1 + pairs) * shape(d).recv_next + 2 * (bits(wide) + CHIPS)
    work = 2 * heads * rows * rows * HEAD
    return pl.pallas_call(
        functools.partial(back_body, bq=bq, wide=wide),
        out_shape=(sd((rows, cw), BF16), sd((f, d), BF16), sd((d, f), BF16), sd((2 * lw, cw), BF16))
        + (sd((d, 3 * pair), BF16),) * 3
        + (sd((rows, cw), BF16), sd((rows_a, 128), F32), sd((rows_b, 128), F32)),
        in_specs=[pl.BlockSpec(memory_space=pltpu.SMEM)] + [anywhere()] * 9 + [vmem()] + [anywhere()] * 5 + [vmem()] * 5,
        out_specs=(anywhere(),) * 7 + (vmem(), vmem(), vmem()),
        scratch_shapes=[
            vm(qa.shape, BF16), vm((rows, lw), BF16), vm((rows, lw), BF16), vm((rows, lw), BF16), vm((rows, lw), BF16),
            vm((rows, d), BF16), vm((pairs, d, 3 * pair), BF16), vm((half, d), BF16), vm((half, d), F32),
            vm((d // 2, f), BF16), vm((f // 2, d), BF16), vm((2 * lw, cw), BF16), vm((2 * lw, cw), BF16),
            vm((rows, pair), BF16), vm((rows, pair), BF16), vm((rows, pair), F32), vm((rows, pair), F32),
            vm((pairs, rows, 3 * pair), BF16), vm((pairs, d, 3 * pair), BF16),
            vm((down_rows, d), BF16), vm((f // 2, d), BF16), vm((c_down.size, d), BF16),
            vm((up_rows, f), BF16), vm((d // 2, f), BF16), vm((c_up.size, f), BF16),
            vm((pair_rows, cw), BF16), vm((lw, cw), BF16), vm((c_gp.size, cw), BF16),
            vm((pairs, pair_rows, 3 * pair), BF16), vm((pairs, d // 2, 3 * pair), BF16),
            vm((pairs, c_up.size, 3 * pair), BF16),
            vm((f, d), BF16), vm((d, f), BF16), vm((2 * lw, cw), BF16), vm((pairs, d, 3 * pair), BF16),
            vm((half, d), BF16), vm((half, d), BF16), vm((half, d), F32), vm((block, d), F32), vm((half, cw), BF16),
            vm((rows_a, 128), F32), vm((slots, rows_a, 128), F32), vm((rows_b, 128), F32), vm((slots, rows_b, 128), F32),
        ]
        + sems(8 * pairs + 8, 8, 4 + 2 * each, 4 + 2 * each, 17 + 3 * CHIPS, semaphores),
        compiler_params=params(collective_id=4, has_side_effects=True),
        cost_estimate=cost(10 * work + 4 * rows * d * 3 * lw, 2 * rows * d * 20, work // 256),
        name="back",
    )(
        length, qa, k, v, do, o, low, w, xf, gm, gain, lo_send, up_part, down_part, gp_own, gp_other,
        s_ub, s_db, s_g2, s_s2, s_pb,
    )


def finish_body(
    lo, lo_got, bias, ig, up, down, q, k, v, p0, p1, small_a, small_b,
    out, ig_out, o_qkv, o_qvb, o_proj, o_pb, o_up, o_ub, o_down, o_db, o_g1, o_s1, o_g2, o_s2,
    *, factor,
):
    n = lax.axis_index("narrow")
    cw = lo.shape[1]
    out[...] = (lo[...] + lo_got[...].astype(F32) + bias[:, lane_part(n, cw)]).astype(BF16)
    ig_out[...] = ig[...]
    for p, ref in enumerate((q, k, v)):
        for c in range(3):
            lanes = slice(c * 128, (c + 1) * 128)
            o_qkv[c, :, p * 128 : (p + 1) * 128] = ref[:, lanes].astype(F32) * factor
    o_proj[:, :cw] = p0[...].astype(F32) * factor
    o_proj[:, cw:] = p1[...].astype(F32) * factor
    o_up[...] = up[...].astype(F32) * factor
    o_down[...] = down[...].astype(F32) * factor

    @pl.when(pl.program_id(0) == 0)
    def _():
        dr, fr = o_g1.shape[0], o_ub.shape[0]
        for i, ref in enumerate((o_g2, o_s2, o_pb, o_db)):
            ref[...] = small_a[i * dr : (i + 1) * dr, :] * factor
        o_ub[...] = small_a[4 * dr : 4 * dr + fr, :] * factor
        o_g1[...] = small_b[0:dr, :] * factor
        o_s1[...] = small_b[dr : 2 * dr, :] * factor
        lr, shared = o_qvb.shape[1] // 128, -(-2 * dr // 8) * 8
        for c in range(2):
            for i in range(lr):
                at = shared + c * lr + i
                o_qvb[c : c + 1, i * 128 : (i + 1) * 128] = small_b[at : at + 1, :] * factor


def finish_call(lo, lo_got, bias, ig, up, down, q, k, v, p, small_a, small_b, factor, grid=8):
    rows, cw = lo.shape
    (d, f), lw = up.shape, q.shape[1]
    dr, sd = d // 128, jax.ShapeDtypeStruct
    shapes = (
        [sd((rows, cw), BF16), sd((rows, cw), BF16), sd((3, d, lw), F32), sd((2, lw), F32), sd((lw, d), F32)]
        + [sd((dr, 128), F32), sd((d, f), F32), sd((f // 128, 128), F32), sd((f, d), F32)]
        + [sd((dr, 128), F32)] * 5
    )
    big = lambda a: rows_spec(a.shape[0] // grid, a.shape[1])
    pb = lw // grid
    specs = []
    for i, s in enumerate(shapes):
        if len(s.shape) == 3:
            specs.append(pl.BlockSpec((3, d // grid, lw), lambda i, *_: (0, i, 0)))
        elif i in (0, 1, 4, 6, 8):
            specs.append(big(s))
        else:
            specs.append(whole_spec(s.shape))
    return pl.pallas_call(
        functools.partial(finish_body, factor=factor),
        out_shape=tuple(shapes),
        grid=(grid,),
        in_specs=[big(lo), big(lo_got), whole_spec(bias.shape), big(ig), big(up), big(down), big(q), big(k), big(v)]
        + [rows_spec(pb, cw), rows_spec(pb, cw, grid), whole_spec(small_a.shape), whole_spec(small_b.shape)],
        out_specs=tuple(specs),
        compiler_params=params(),
        cost_estimate=cost(up.size * 8, up.size * 24),
        name="finish",
    )(lo, lo_got, bias, ig, up, down, q, k, v, p, p, small_a, small_b)


def on_device(
    tokens, lengths, qkv_weight, qv_bias, proj_weight, proj_bias, up_weight, up_bias,
    down_weight, down_bias, first_gain, first_shift, second_gain, second_shift, cotangent,
):
    cw = tokens.shape[1]
    d, ff, lw = 2 * cw, up_weight.shape[1], proj_weight.shape[0]
    wide = lax.axis_size("wide")
    w3 = jnp.transpose(qkv_weight, (1, 0, 2))

    xf, low, q, k, v = qkv_call(tokens, w3, qv_bias, first_gain, first_shift)
    mixed, qa, mixed_got, proj_got = attend_forward(lengths, q, k, v, proj_weight)
    lo, lo_send, gmix, gm, up_part, down_part, gp_own, gp_other, s_ub, s_db, s_g2, s_s2, s_pb = mlp_call(
        lengths, xf, mixed, mixed_got, proj_weight, proj_got, proj_bias, second_gain, second_shift,
        up_weight, up_bias, down_weight, cotangent, wide,
    )
    lo_got, gdown, gup, gp, g0, g1, g2, ig, small_a, small_b = back_call(
        lengths, qa, k, v, gmix, mixed, low, w3, xf, gm, first_gain, lo_send, up_part, down_part, gp_own, gp_other,
        s_ub, s_db, s_g2, s_s2, s_pb, wide,
    )
    out, ig, o_qkv, o_qvb, o_proj, *rest = finish_call(
        lo, lo_got, down_bias.astype(F32).reshape(1, -1), ig, gup, gdown, g0, g1, g2, gp, small_a, small_b,
        1.0 / (lengths.shape[0] * wide),
    )
    pb, up, ubs, down, dbs, g1, s1, g2, s2 = rest
    flat = lambda a: a.reshape(-1)
    return (
        out, ig, jnp.transpose(o_qkv, (1, 0, 2)), o_qvb, o_proj, flat(pb), up, flat(ubs), down, flat(dbs),
        flat(g1), flat(s1), flat(g2), flat(s2),
    )


def solution(mesh):
    split = P("wide", "narrow")
    none3, cols, rows1 = P(None, None, "narrow"), P(None, "narrow"), P("narrow", None)
    return jax.shard_map(
        on_device,
        mesh=mesh,
        in_specs=(
            split, P("wide"), none3, cols, rows1, P(), cols, P("narrow"), rows1, P(), P(), P(), P(), P(), split,
        ),
        out_specs=(
            split, split, none3, cols, rows1, P(), cols, P("narrow"), rows1, P(), P(), P(), P(), P(),
        ),
        check_vma=False,
    )
```

```python
import functools

import jax
import jax.numpy as jnp
from jax import lax
from jax.experimental import pallas as pl
from jax.experimental.pallas import tpu as pltpu
from jax.sharding import PartitionSpec as P

EPS = 1e-05
HEAD = 64
F32, BF16 = jnp.float32, jnp.bfloat16
NT = (((1,), (1,)), ((), ()))
TN = (((0,), (0,)), ((), ()))
GELU_A, GELU_B = 0.7978845608028654, 0.044715
VMEM_LIMIT = 63 * 1024 * 1024


def dot(a, b):
    return jnp.dot(a, b, preferred_element_type=F32)


def dot_nt(a, b):
    return lax.dot_general(a, b, NT, preferred_element_type=F32)


def dot_tn(a, b):
    return lax.dot_general(a, b, TN, preferred_element_type=F32)


def params(**more):
    return pltpu.CompilerParams(vmem_limit_bytes=VMEM_LIMIT, **more)


def cost(flops, size, trans=0):
    return pl.CostEstimate(flops=int(flops), bytes_accessed=int(size), transcendentals=int(trans))


def lane_part(which, width):
    return pl.ds(pl.multiple_of(which * width, 128), width)


def norm_rows(x):
    mean = jnp.mean(x, axis=-1, keepdims=True)
    cen = x - mean
    var = jnp.mean(cen * cen, axis=-1, keepdims=True)
    r = lax.rsqrt(var + EPS)
    return cen * r, r


def rows_spec(rows, cols, base=0):
    return pl.BlockSpec((rows, cols), lambda i, *_: (i + base, 0))


def whole_spec(shape):
    zeros = (0,) * len(shape)
    return pl.BlockSpec(shape, lambda i, *_: zeros)


MESH = pl.DeviceIdType.MESH
scope = jax.named_scope


def vec(ref):
    return ref[...].astype(F32).reshape(1, -1)


def bit_of(index, bit):
    return (index // (1 << bit)) % 2


def flip(index, bit):
    return index + (1 - 2 * bit_of(index, bit)) * (1 << bit)


def greet(peers):
    barrier = pltpu.get_barrier_semaphore()
    for peer in peers:
        pl.semaphore_signal(barrier, inc=1, device_id=peer, device_id_type=MESH)
    pl.semaphore_wait(barrier, len(peers))


def remote(src, dst, sems, at, peer, send_at=None):
    return pltpu.make_async_remote_copy(
        src_ref=src, dst_ref=dst, send_sem=sems[0].at[at if send_at is None else send_at], recv_sem=sems[1].at[at],
        device_id=peer, device_id_type=MESH,
    )


def block_rows(start, size, unit=16):
    return pl.ds(start if isinstance(start, int) else pl.multiple_of(start, unit), size)


LINE, CHIPS = 4, 8


def when(cond, action):
    @pl.when(cond)
    def _():
        action()


def line_peer(me, by):
    q = (me // 4) % LINE
    return me + ((q + by) % LINE - q) * 4


class Chain:
    def __init__(self, me, order, rows, cols, sems, send_at, recv_at):
        self.me, self.cols, self.sems, self.send_at = me, cols, sems, send_at
        self.phases, self.ops, back = [], [], []
        base, size, box = 0, rows, 0
        for kind, bit in order:
            if kind == "line" and size % (16 * LINE):
                raise ValueError(rows)
            if kind == "all":
                ways = CHIPS >> (bit - 1)
                part = size // ways
                keep, give, boxes = base + (me // (1 << bit)) % ways * part, None, (ways - 1) * part
                self.ops.append(("send", len(self.phases), ways))
                back = [("share", len(self.phases), ways)] + back
            elif kind == "line":
                part = size // LINE
                keep, give, boxes = base + (me // 4) % LINE * part, None, 2 * (LINE - 1) * part
                self.ops += [("line", len(self.phases), i) for i in range(1, LINE)]
                back = [("spread", len(self.phases), i) for i in range(1, LINE)] + back
            elif size % 32 == 0:
                part = size // 2
                mine = bit_of(me, bit)
                keep, give, boxes = base + mine * part, base + (1 - mine) * part, part
                self.ops.append(("pair", len(self.phases), 0))
                back = [("join", len(self.phases), 0)] + back
            else:
                part, keep, give, boxes = size, base, base, size
                self.ops.append(("pair", len(self.phases), 0))
            self.phases.append((bit, base, keep, give, part, box))
            base, size, box = keep, part, box + boxes
        self.scatters = len(self.ops)
        self.ops += back
        self.base, self.size, self.box_rows = base, size, box
        self.recv_at, widest = [], 1
        for kind, _, i in self.ops:
            width = {"line": 2, "spread": 2, "send": i - 1, "share": i - 1}.get(kind, 1)
            self.recv_at.append(recv_at)
            recv_at, widest = recv_at + width, max(widest, width)
        self.recv_next, self.send_next = recv_at, send_at + widest

    def bind(self, src, box, part, own, dst=None, entry=0):
        self.src, self.box, self.part, self.own, self.dst = src, box, part, own, dst
        self.entry = self.ops[entry][1]
        return self

    def _source(self, phase):
        off = 0 if phase == 0 else self.phases[0][2]
        return (self.src if phase == self.entry else self.part), off

    def _target(self, phase):
        if phase == len(self.phases) - 1:
            return self.own, self.phases[phase][2]
        return self.part, self.phases[0][2]

    def _remote(self, op, lane, src, dst, to):
        return remote(src, dst, self.sems, self.recv_at[op] + lane, {"wide": to}, self.send_at + lane)

    def _add(self, rows, target, first, *terms):
        unit = next(u for u in (96, 64, 48, 32, 16) if rows % u == 0)

        def add(i, carry):
            total = None
            for ref, start in terms:
                value = ref[block_rows(start + i * unit, unit), self.cols]
                value = value.astype(F32) if len(terms) > 2 else value
                total = value if total is None else total + value
            target[block_rows(first + i * unit, unit), self.cols] = total.astype(BF16)
            return carry

        lax.fori_loop(0, rows // unit, add, 0)


    def _pair(self, op, phase):
        bit, _, _, give, rows, box = self.phases[phase]
        source, off = self._source(phase)
        src = source.at[block_rows(give - off, rows), self.cols]
        return self._remote(op, 0, src, self.box.at[pl.ds(box, rows), self.cols], flip(self.me, bit))

    def _join(self, op, phase):
        bit, _, keep, _, rows, _ = self.phases[phase]
        region = self.dst.at[block_rows(keep, rows), self.cols]
        return self._remote(op, 0, region, region, flip(self.me, bit))


    def _others(self, bit, ways):
        for m in range(1, ways):
            yield m - 1, flip_all(self.me, bit, m)

    def _sends(self, op, phase, ways):
        bit, base, _, _, rows, box = self.phases[phase]
        source, off = self._source(phase)
        for m, to in self._others(bit, ways):
            src = source.at[block_rows(base - off + (to // (1 << bit)) % ways * rows, rows), self.cols]
            yield self._remote(op, m, src, self.box.at[pl.ds(box + m * rows, rows), self.cols], to)

    def _shares(self, op, phase, ways, came):
        bit, base, keep, _, rows, _ = self.phases[phase]
        for m, to in self._others(bit, ways):
            at = base + (to // (1 << bit)) % ways * rows if came else keep
            region = self.dst.at[block_rows(at, rows), self.cols]
            yield self._remote(op, m, region, region, to)


    def _slot(self, phase, lane, i):
        rows, box = self.phases[phase][4:]
        return box + (lane * (LINE - 1) + i - 1) * rows

    def _line_sends(self, op, phase, i):
        q = (self.me // 4) % LINE
        _, base, _, _, rows, _ = self.phases[phase]
        source, off = self._source(phase)
        sends = []
        for lane, by in ((0, 1), (1, -1)):
            place_ = q if lane == 0 else LINE - 1 - q
            chunk = LINE - i if lane == 0 else i - 1
            dst = self.box.at[pl.ds(self._slot(phase, lane, i), rows), self.cols]
            to = line_peer(self.me, by)
            src = source.at[block_rows(base - off + chunk * rows, rows), self.cols]
            sends.append((place_ == 0, functools.partial(self._remote, op, lane, src, dst, to)))
            if i > 1:
                src = self.box.at[pl.ds(self._slot(phase, lane, i - 1), rows), self.cols]
                moving = jnp.logical_and(place_ >= 1, place_ <= min(i - 1, LINE - 2))
                sends.append((moving, functools.partial(self._remote, op, lane, src, dst, to)))
        return sends

    def _line_end(self, op, phase, i):
        q = (self.me // 4) % LINE
        _, base, keep, _, rows, _ = self.phases[phase]
        source, off = self._source(phase)
        for cond, copy in self._line_sends(op, phase, i):
            when(cond, lambda: copy().wait_send())
        for lane, by in ((0, -1), (1, 1)):
            place_ = q if lane == 0 else LINE - 1 - q
            slot = self._slot(phase, lane, i)
            dst = self.box.at[pl.ds(slot, rows), self.cols]
            arrived = jnp.logical_and(place_ >= 1, place_ <= i)
            chunk = LINE - 1 - i + q if lane == 0 else i + q - (LINE - 1)

            @pl.when(arrived)
            def _():
                self._remote(op, lane, dst, dst, line_peer(self.me, by)).wait_recv()
                if i < LINE - 1:
                    self._add(rows, self.box, slot, (self.box, slot), (source, base - off + chunk * rows))

        if i == LINE - 1:
            target, out = self._target(phase)
            own = (source, keep - off)
            left, right = (self.box, self._slot(phase, 0, i)), (self.box, self._slot(phase, 1, i))

            @pl.when(q == 0)
            def _():
                self._add(rows, target, keep - out, own, right)

            @pl.when(q == LINE - 1)
            def _():
                self._add(rows, target, keep - out, own, left)

            @pl.when(jnp.logical_and(q > 0, q < LINE - 1))
            def _():
                self._add(rows, target, keep - out, left, own, right)

    def _spread(self, op, phase, i):
        q = (self.me // 4) % LINE
        _, base, _, _, rows, _ = self.phases[phase]
        ways = []
        for lane, by in ((0, 1), (1, -1)):
            place_ = q if lane == 0 else LINE - 1 - q
            sent = self.dst.at[block_rows(base + (q - by * (i - 1)) * rows, rows), self.cols]
            came = self.dst.at[block_rows(base + (q - by * i) * rows, rows), self.cols]
            send_if = jnp.logical_and(place_ >= i - 1, place_ <= LINE - 2)
            ways.append(
                (
                    send_if, functools.partial(self._remote, op, lane, sent, sent, line_peer(self.me, by)),
                    place_ >= i, functools.partial(self._remote, op, lane, came, came, line_peer(self.me, -by)),
                )
            )
        return ways

    def start(self, op):
        kind, phase, i = self.ops[op]
        if kind == "pair":
            self._pair(op, phase).start()
        elif kind == "join":
            self._join(op, phase).start()
        elif kind == "send":
            for copy in self._sends(op, phase, i):
                copy.start()
        elif kind == "share":
            for copy in self._shares(op, phase, i, False):
                copy.start()
        elif kind == "line":
            for cond, copy in self._line_sends(op, phase, i):
                when(cond, lambda: copy().start())
        else:
            for cond, copy, _, _ in self._spread(op, phase, i):
                when(cond, lambda: copy().start())

    def end(self, op):
        kind, phase, i = self.ops[op]
        if kind == "pair":
            self._pair(op, phase).wait()
            _, _, keep, _, rows, box = self.phases[phase]
            source, off = self._source(phase)
            target, out = self._target(phase)
            self._add(rows, target, keep - out, (self.box, box), (source, keep - off))
        elif kind == "join":
            self._join(op, phase).wait()
        elif kind == "send":
            for copy in self._sends(op, phase, i):
                copy.wait()
            _, _, keep, _, rows, box = self.phases[phase]
            source, off = self._source(phase)
            target, out = self._target(phase)
            terms = [(self.box, box + m * rows) for m in range(i - 1)]
            self._add(rows, target, keep - out, (source, keep - off), *terms)
        elif kind == "share":
            for copy in self._shares(op, phase, i, False):
                copy.wait_send()
            for copy in self._shares(op, phase, i, True):
                copy.wait_recv()
        elif kind == "line":
            self._line_end(op, phase, i)
        else:
            for send_if, send, recv_if, recv in self._spread(op, phase, i):
                when(send_if, lambda: send().wait_send())
                when(recv_if, lambda: recv().wait_recv())

    def gather_open(self):
        self._add(self.size, self.dst, self.base, (self.own, 0))


class Group:
    def __init__(self, chain, entry=0, leave=None, out=None):
        self.chain, self.out = chain, out
        self.ops = list(range(entry, len(chain.ops) if leave is None else leave))
        self.pos = -1

    @property
    def done(self):
        return self.pos >= len(self.ops)

    def next(self):
        pos = self.pos
        self.pos = min(pos + 1, len(self.ops))

        def tick():
            if pos >= len(self.ops):
                return
            if pos >= 0:
                self.chain.end(self.ops[pos])
            if pos + 1 >= len(self.ops):
                if self.out is not None:
                    self.store().start()
                return
            if self.ops[pos + 1] == self.chain.scatters:
                self.chain.gather_open()
            self.chain.start(self.ops[pos + 1])

        return tick

    def tick(self):
        self.next()()

    def store(self):
        out, sem = self.out
        return pltpu.make_async_copy(self.chain.dst.at[:, self.chain.cols], out.at[:, self.chain.cols], sem)


def bits(wide):
    return wide.bit_length() - 1


def order_of(wide, kind):
    first, rest = ("pair", 0), [("pair", b) for b in range(4, bits(wide))]
    pair, line = ("pair", 1), ("line", 2)
    return {
        0: [first, pair, line, *rest], 1: [first, line, pair, *rest], 2: [first, ("all", 1), *rest],
        3: [first, pair, ("all", 2), *rest],
    }[kind]


def lanes_split(cols, kinds):
    w = cols // len(kinds)
    return [(kind, pl.ds(i * w, w)) for i, kind in enumerate(kinds)]


def flip_all(me, bit, mask):
    to = me
    for i in range(3):
        if mask >> i & 1:
            to = to + (flip(me, bit + i) - me)
    return to


def chip_peers(me):
    return [flip_all(me, 1, m) for m in range(1, CHIPS)]


def wide_peers(me, wide):
    pairs = [flip(me, b) for b in range(bits(wide)) if b not in (1, 2, 3)]
    return [{"wide": peer} for peer in pairs + chip_peers(me)]


class Small:
    def __init__(self, me, n, wide, total, box, shared, narrow, across, narrow_at, send_at, recv_at):
        self.me, self.n, self.total, self.box, self.shared = me, n, total, box, shared
        self.narrow, self.across = narrow, across
        self.narrow_at, self.send_at, self.recv_at = narrow_at, send_at, recv_at
        self.ops = ["narrow", 0, "chips"] + list(range(4, bits(wide)))
        self.scatters, self.dst = None, None
        self.send_next = send_at + CHIPS - 1
        self.recv_next = recv_at + len(self.ops) + CHIPS - 1

    def _copies(self, op):
        kind = self.ops[op]
        if kind == "narrow":
            top = pl.ds(0, self.shared)
            return [remote(self.total.at[top], self.box.at[0, top], self.narrow, self.narrow_at, {"narrow": 1 - self.n})]
        if kind == "chips":
            return [
                remote(
                    self.total, self.box.at[2 + i], self.across, self.recv_at + len(self.ops) + i, {"wide": to},
                    self.send_at + i,
                )
                for i, to in enumerate(chip_peers(self.me))
            ]
        slot = 1 if kind == 0 else CHIPS + 1 + kind - 4
        peer = {"wide": flip(self.me, kind)}
        return [remote(self.total, self.box.at[slot], self.across, self.recv_at + op, peer, self.send_at)]

    def start(self, op):
        for copy in self._copies(op):
            copy.start()

    def end(self, op):
        for copy in self._copies(op):
            copy.wait()
        kind = self.ops[op]
        if kind == "narrow":
            self.total[0 : self.shared, :] += self.box[0, 0 : self.shared, :]
        elif kind == "chips":
            self.total[...] += sum(self.box[2 + i] for i in range(CHIPS - 1))
        else:
            self.total[...] += self.box[1 if kind == 0 else CHIPS + 1 + kind - 4]


def vmem():
    return pl.BlockSpec(memory_space=pltpu.VMEM)


def anywhere():
    return pl.BlockSpec(memory_space=pl.ANY)


def sems(*counts):
    return [pltpu.SemaphoreType.DMA((c,)) for c in counts]


def three(x):
    hi = x.astype(BF16).astype(F32)
    mid = (x - hi).astype(BF16).astype(F32)
    return hi, mid, x - hi - mid


def lanes_of(par):
    lane = lax.broadcasted_iota(jnp.int32, (1, 2 * HEAD), 1)
    mine = (lane // HEAD) == par
    return lane, mine, (1 - par) * HEAD


def place(lane, mine, at, base, terms):
    out = jnp.where(mine, base, 0.0)
    for i, term in enumerate(terms):
        out = jnp.where(lane == at + i, term, out)
    return out


def front_body(
    len_ref, tokens, w_hbm, bias, gain, shift, pw,
    xf_out, low_out, k_out, v_out, o_out, qa_out, o_got, pw_got,
    own, got, w, xf, low, q, k, v, o, qa, ka, va, load_sem, store_sem, send_sem, recv_sem, *, bq,
):
    n, me = lax.axis_index("narrow"), lax.axis_index("wide")
    peer, core = {"narrow": 1 - n}, {"wide": flip(me, 0)}
    both = (send_sem, recv_sem)
    rows, cw = own.shape
    pair_w, heads = 2 * HEAD, qa.shape[0]
    blocks = rows // bq
    loads = [pltpu.make_async_copy(a, b, load_sem.at[i]) for i, (a, b) in enumerate(((tokens, own), (w_hbm, w)))]
    for load in loads:
        load.start()
    greet([peer, core])

    def token_copy(i):
        r = block_rows(i * bq, bq)
        return remote(tokens.at[r], got.at[r], both, i, peer)

    for i in range(blocks):
        token_copy(i).start()
    part = block_rows((me % 2) * (pw.shape[0] // 2), pw.shape[0] // 2)
    used = blocks + blocks * (heads // 2)
    weights = remote(pw.at[part], pw_got.at[part], both, used, peer)
    shared = remote(pw_got.at[part], pw_got.at[part], both, used + 1, core)
    weights.start()
    for load in loads:
        load.wait()

    def project(i, carry):
        r = block_rows(i * bq, bq)
        xf[r, lane_part(n, cw)] = own[r, :]
        with scope("wait"):
            token_copy(i).wait()
        xf[r, lane_part(1 - n, cw)] = got[r, :]
        xhat, _ = norm_rows(xf[r, :].astype(F32))
        y = (xhat * vec(gain) + vec(shift)).astype(BF16)
        low[r, :] = y
        q[r, :] = (dot(y, w[0]) + bias[0:1, :].astype(F32)).astype(BF16) * jnp.asarray(HEAD**-0.5, BF16)
        k[r, :] = dot(y, w[1]).astype(BF16)
        v[r, :] = (dot(y, w[2]) + bias[1:2, :].astype(F32)).astype(BF16)
        return carry

    lax.fori_loop(0, blocks, project, 0)
    stores = [
        pltpu.make_async_copy(a, b, store_sem.at[i])
        for i, (a, b) in enumerate(((xf, xf_out), (low, low_out), (k, k_out), (v, v_out)))
    ]
    for store in stores:
        store.start()

    kpos = lax.broadcasted_iota(jnp.int32, (rows, 1), 0)
    kbias = jnp.where(kpos < len_ref[0], 0.0, -1e30)
    tri = lax.broadcasted_iota(jnp.int32, (bq, bq), 1) <= lax.broadcasted_iota(jnp.int32, (bq, bq), 0)

    def mixed(pair, i):
        r, c = pl.ds(i * bq, bq), lane_part(pair, pair_w)
        return remote(o.at[r, c], o_got.at[r, c], both, blocks + pair * blocks + i, peer)

    def mixed_store(pair):
        c = lane_part(pair, pair_w)
        return pltpu.make_async_copy(o.at[:, c], o_out.at[:, c], store_sem.at[4 + pair])

    def qa_store(head):
        return pltpu.make_async_copy(qa.at[head], qa_out.at[head], store_sem.at[4 + heads // 2 + head])

    def one_head(head, carry):
        par, pair = head % 2, head // 2
        lane, mine, at = lanes_of(par)
        cols = lane_part(pair, pair_w)
        ka[...] = place(lane, mine, at, k[:, cols].astype(F32), [kbias]).astype(BF16)
        va[...] = place(lane, mine, at, v[:, cols].astype(F32), [1.0]).astype(BF16)
        for i in range(blocks):
            nk = (i + 1) * bq
            r = pl.ds(i * bq, bq)
            qf = q[r, cols].astype(F32)
            s = dot_nt(place(lane, mine, at, qf, [1.0]).astype(BF16), ka[0:nk, :])
            edge = jnp.where(tri, s[:, nk - bq :], -1e30)
            m = jnp.max(edge, axis=1, keepdims=True)
            if nk > bq:
                m = jnp.maximum(m, jnp.max(s[:, : nk - bq], axis=1, keepdims=True))
            pv = dot(jnp.exp(edge - m).astype(BF16), va[nk - bq : nk, :])
            if nk > bq:
                pv += dot(jnp.exp(s[:, : nk - bq] - m).astype(BF16), va[0 : nk - bq, :])
            total = jnp.sum(jnp.where(lane == at, pv, 0.0), axis=1, keepdims=True)
            out = (pv / total).astype(BF16).astype(F32)
            old = o[r, cols].astype(F32)
            o[r, cols] = jnp.where(mine, out, jnp.where(par == 0, 0.0, old)).astype(BF16)
            lse = m + jnp.log(total)
            qa[head, r, :] = place(lane, mine, at, qf, [1.0, *three(lse)]).astype(BF16)
            when(par == 1, lambda: mixed(pair, i).start())
        when(par == 1, lambda: mixed_store(pair).start())
        qa_store(head).start()

        @pl.when(head == 3)
        def _():
            weights.wait()
            shared.start()

        return carry

    with scope("heads"):
        lax.fori_loop(0, heads, one_head, 0)
    for store in stores:
        store.wait()
    for head in range(heads):
        qa_store(head).wait()
    shared.wait()
    with scope("mixed"):
        for pair in range(heads // 2):
            mixed_store(pair).wait()
            for i in range(blocks):
                mixed(pair, i).wait()


def front_call(length, own, w, bias, gain, shift, pw, bq=256):
    rows, cw = own.shape
    d, lw = w.shape[1], w.shape[2]
    heads, pair = lw // HEAD, 2 * HEAD
    sd, vm = jax.ShapeDtypeStruct, pltpu.VMEM
    copies = rows // bq * (1 + heads // 2) + 2
    shapes = [(rows, d), (rows, d), (rows, lw), (rows, lw), (rows, lw), (heads, rows, pair), (rows, lw), pw.shape]
    scratch = [(rows, cw), (rows, cw), w.shape, (rows, d), (rows, d)] + [(rows, lw)] * 4
    work = 2 * heads * rows * rows * HEAD
    return pl.pallas_call(
        functools.partial(front_body, bq=bq),
        out_shape=tuple(sd(a, BF16) for a in shapes),
        in_specs=[pl.BlockSpec(memory_space=pltpu.SMEM), anywhere(), anywhere(), vmem(), vmem(), vmem(), anywhere()],
        out_specs=(anywhere(),) * 8,
        scratch_shapes=[vm(a, BF16) for a in scratch]
        + [vm((heads, rows, pair), BF16), vm((rows, pair), BF16), vm((rows, pair), BF16)]
        + sems(2, 4 + heads // 2 + heads, copies, copies),
        compiler_params=params(collective_id=1, has_side_effects=True),
        cost_estimate=cost(2 * rows * d * 3 * lw + 4 * work, 2 * rows * d * 8, work // 256),
        name="front",
    )(length, own, w, bias, gain, shift, pw)


DOWN_ENTRY, UP_ENTRY = (2, 2), (1, 1)
DOWN_KINDS, UP_KINDS = (0, 0), (0, 1)


def mlp_body(
    len_ref, xf_hbm, mo_hbm, mr_hbm, pwo_hbm, pwr_hbm, pb, gain, shift, ub, up_hbm, down_hbm, cot_hbm,
    lo_out, lo_send_out, gmix, gm_out, up_part, down_part, gp_own, gp_other, sum_ub, sum_db, sum_g, sum_s, sum_pb,
    xf, mo, mr, pwo, pwr, up, down, cot, cot_got, cf, lo, lo_send, mid, second, active, slope, gh,
    gs_send, gs_got, gs_own, gdown, gup, box, up_box, gm, glow, gmix_send, load_sem, store_sem, nsend, nrecv, wsend, wrecv,
    *, wide,
):
    n, me = lax.axis_index("narrow"), lax.axis_index("wide")
    peer = {"narrow": 1 - n}
    rows, cw = cot.shape
    d, f = up.shape
    half, block = rows // 2, min(256, rows // 2)
    each = half // block
    mine, other = lane_part(n, cw), lane_part(1 - n, cw)
    narrow, across = (nsend, nrecv), (wsend, wrecv)
    count = iter(range(16))

    def load(src, dst):
        copy = pltpu.make_async_copy(src, dst, load_sem.at[next(count)])
        copy.start()
        return copy

    his, own = block_rows((1 - n) * half, half), block_rows(n * half, half)
    first = [load(a, b) for a, b in ((pwo_hbm, pwo), (pwr_hbm, pwr))]
    first += [load(a.at[his], b.at[his]) for a, b in ((xf_hbm, xf), (mo_hbm, mo), (mr_hbm, mr))]
    up_load = load(up_hbm, up)
    greet([peer] + wide_peers(me, wide))

    def cot_copy(side, j, a):
        r = block_rows(side * half + j * block, block)
        return remote(cot_hbm.at[r], cot_got.at[r], narrow, a * each + j, peer)

    for a, side in enumerate((n, 1 - n)):
        for j in range(each):
            cot_copy(side, j, a).start()
    down_load = load(down_hbm, down)
    cot_load = load(cot_hbm, cot)
    rest = [load(a.at[own], b.at[own]) for a, b in ((xf_hbm, xf), (mo_hbm, mo), (mr_hbm, mr))]

    def project(at):
        r = block_rows(at, block)
        m = xf[r, :].astype(F32) + (dot(mo[r, :], pwo[...]) + dot(mr[r, :], pwr[...])) + vec(pb)
        mid[r, :] = m
        xhat, _ = norm_rows(m)
        second[r, :] = (xhat * vec(gain) + vec(shift)).astype(BF16)

    def forward(at):
        r = block_rows(at, block)
        hid = dot(second[r, :], up[...]) + vec(ub)
        sq = hid * hid
        t = jnp.tanh(GELU_A * (hid + GELU_B * (sq * hid)))
        hf = 0.5 * (1.0 + t)
        act = (hid * hf).astype(BF16)
        active[r, :] = act
        slope[r, :] = hf + (0.5 * hid) * (1.0 - t * t) * (GELU_A + (3.0 * GELU_A * GELU_B) * sq)
        lo[r, :] = mid[r, mine] + dot(act, down[:, mine])
        lo_send[r, :] = dot(act, down[:, other]).astype(BF16)

    def backward(at):
        r = block_rows(at, block)
        pos = at + lax.broadcasted_iota(jnp.int32, (block, 1), 0)
        live = (pos < len_ref[0]).astype(F32)
        cf[r, mine] = (cot[r, :].astype(F32) * live).astype(BF16)
        cf[r, other] = (cot_got[r, :].astype(F32) * live).astype(BF16)
        ghid = (dot_nt(cf[r, :], down[...]) * slope[r, :]).astype(BF16)
        gh[r, :] = ghid
        sum_ub[...] += jnp.sum(ghid.astype(F32), axis=0, keepdims=True)
        return dot_nt(ghid, up[...])

    def every(side, body):
        def step(j, carry):
            body(side * half + j * block)
            return carry

        lax.fori_loop(0, each, step, 0)

    def both(at):
        project(at)
        forward(at)

    for ref in (sum_ub, sum_g, sum_s, sum_pb, sum_db):
        ref[...] = jnp.zeros_like(ref)
    with scope("load"):
        for copy in first:
            copy.wait()
    with scope("project"):
        every(1 - n, project)
    with scope("load2"):
        up_load.wait()
        down_load.wait()
    with scope("fwd_peer"):
        every(1 - n, forward)
    for copy in rest:
        copy.wait()
    with scope("fwd_own"):
        every(n, both)
    stores = []

    def store(src, dst):
        copy = pltpu.make_async_copy(src, dst, store_sem.at[len(stores)])
        copy.start()
        stores.append(copy)

    store(lo, lo_out)
    store(lo_send, lo_send_out)
    with scope("cot_wait"):
        cot_load.wait()
        for j in range(each):
            cot_copy(n, j, 0).wait()

    def gs_copy(j):
        r = block_rows(j * block, block)
        return remote(gs_send.at[r], gs_got.at[r], narrow, 2 * each + j, peer)

    def for_peer(j, carry):
        gs_send[block_rows(j * block, block), :] = backward((1 - n) * half + j * block).astype(BF16)
        gs_copy(j).start()
        return carry

    def for_own(j, carry):
        gs_own[block_rows(j * block, block), :] = backward(n * half + j * block)
        return carry

    with scope("for_peer"):
        lax.fori_loop(0, each, for_peer, 0)
    with scope("cot_wait2"):
        for j in range(each):
            cot_copy(1 - n, j, 1).wait()
    with scope("for_own"):
        lax.fori_loop(0, each, for_own, 0)

    def weight(dst, left, right):
        def step(i, carry):
            c = block_rows(i * 256, 256, 256)
            dst[c, :] = dot_tn(left[:, c], right[...]).astype(BF16)
            return carry

        lax.fori_loop(0, dst.shape[0] // 256, step, 0)

    used = iter(range(16))

    def group(src, box_, part, kinds, leaves):
        parts = []
        for (kind, cols), leave in zip(lanes_split(src.shape[1], kinds), leaves):
            a = next(used)
            chain = Chain(me, order_of(wide, kind), src.shape[0], cols, across, 2 * a, 2 * a)
            parts.append(Group(chain.bind(src, box_, part, None), leave=leave))
        return parts

    reduce_down = group(gdown, box, down_part, DOWN_KINDS, DOWN_ENTRY)
    reduce_up = group(gup, up_box, up_part, UP_KINDS, UP_ENTRY)

    def advance(name, *groups):
        with scope(name):
            for one in groups:
                one.tick()

    with scope("w_down"):
        weight(gdown, active, cf)
    advance("core_d", *reduce_down)
    with scope("w_up"):
        weight(gup, second, gh)
    advance("core_u", *reduce_down, *reduce_up)
    with scope("gs_wait"):
        for j in range(each):
            gs_copy(j).wait()

    def gmix_copy(j):
        r = block_rows(n * half + j * block, block)
        return remote(gmix_send.at[block_rows(j * block, block)], gmix.at[r], narrow, 3 * each + j, peer)

    def back_norm(j, carry):
        r, rh = block_rows(n * half + j * block, block), block_rows(j * block, block)
        g = gs_own[rh, :] + gs_got[rh, :].astype(F32)
        xhat, scale = norm_rows(mid[r, :])
        gg = g * vec(gain)
        m1 = jnp.mean(gg, axis=-1, keepdims=True)
        m2 = jnp.mean(gg * xhat, axis=-1, keepdims=True)
        c = cf[r, :].astype(F32)
        grad = c + scale * (gg - m1 - xhat * m2)
        gm[rh, :] = grad
        gl = grad.astype(BF16)
        glow[rh, :] = gl
        gmix_send[rh, :] = dot_nt(gl, pwr[...]).astype(BF16)
        gmix_copy(j).start()
        gmix[r, :] = dot_nt(gl, pwo[...]).astype(BF16)
        sum_g[...] += jnp.sum(g * xhat, axis=0, keepdims=True)
        sum_s[...] += jnp.sum(g, axis=0, keepdims=True)
        sum_pb[...] += jnp.sum(grad, axis=0, keepdims=True)
        sum_db[...] += jnp.sum(c, axis=0, keepdims=True)
        return carry

    with scope("back_norm"):
        lax.fori_loop(0, each, back_norm, 0)
    store(gm, gm_out)
    advance("across", *reduce_up)
    with scope("proj"):
        lw = mo.shape[1]
        for src, dst in ((mr, gp_other), (mo, gp_own)):
            total = dot_tn(src[own, :], glow[...]).astype(BF16)
            dst[0:lw, :] = total[:, :cw]
            dst[lw : 2 * lw, :] = total[:, cw:]
    with scope("gmix_wait"):
        for j in range(each):
            gmix_copy(j).wait()
    advance("leave", *reduce_down, *reduce_up)
    with scope("store"):
        for copy in stores:
            copy.wait()


def mlp_call(length, xf, mo, mr, pwo, pwr, pb, gain, shift, up, ub, down, cot, wide):
    rows, d = xf.shape
    f, lw, cw = up.shape[1], mo.shape[1], cot.shape[1]
    half = rows // 2
    sd, vm = jax.ShapeDtypeStruct, pltpu.VMEM
    each = half // min(256, half)
    return pl.pallas_call(
        functools.partial(mlp_body, wide=wide),
        out_shape=(
            sd((rows, cw), F32), sd((rows, cw), BF16), sd((rows, lw), BF16), sd((half, d), F32),
            sd((d // 2, f), BF16), sd((f // 2, d), BF16), sd((2 * lw, cw), BF16), sd((2 * lw, cw), BF16),
            sd((1, f), F32), sd((1, d), F32), sd((1, d), F32), sd((1, d), F32), sd((1, d), F32),
        ),
        in_specs=[pl.BlockSpec(memory_space=pltpu.SMEM)] + [anywhere()] * 5 + [vmem()] * 4 + [anywhere()] * 3,
        out_specs=(anywhere(), anywhere(), vmem(), anywhere()) + (vmem(),) * 9,
        scratch_shapes=[
            vm((rows, d), BF16), vm((rows, lw), BF16), vm((rows, lw), BF16), vm((lw, d), BF16), vm((lw, d), BF16),
            vm((d, f), BF16), vm((f, d), BF16), vm((rows, cw), BF16), vm((rows, cw), BF16), vm((rows, d), BF16),
            vm((rows, cw), F32), vm((rows, cw), BF16), vm((rows, d), F32),
            vm((rows, d), BF16), vm((rows, f), BF16), vm((rows, f), F32), vm((rows, f), BF16),
            vm((half, d), BF16), vm((half, d), BF16), vm((half, d), F32), vm((f, d), BF16), vm((d, f), BF16),
            vm((f, d), BF16), vm((d, f), BF16), vm((half, d), F32), vm((half, d), BF16), vm((half, lw), BF16),
        ]
        + sems(12, 4, 4 * each, 4 * each, 8, 8),
        compiler_params=params(collective_id=3, has_side_effects=True),
        cost_estimate=cost(2 * rows * d * (d + 6 * f), 2 * (rows * d * 8 + 2 * d * f), rows * f),
        name="mlp",
    )(length, xf, mo, mr, pwo, pwr, pb, gain, shift, ub, up, down, cot)


HEAD_TICKS = (
    ((1, 2), "U1"),
    ((1, 3), "D1U0D0Q0"),
    ((2, 2), "Q0U1"),
    ((2, 3), "D1"),
    ((3, 1), "U0SA"),
    ((3, 2), "D0P0"),
    ((3, 3), "SAQ0U1Q1"),
    ((4, 1), "D1"),
    ((4, 2), "U0Q1"),
    ((4, 3), "D0"),
    ((5, 0), "P0"),
    ((5, 3), "Q0D1U1Q2"),
)
PART_TICKS = ("U0D0SAQ1P0Q2", "Q0D1U1", "Q1U0", "D0P0", "Q0Q2")
LAST_TICKS = (
    "D1Q1P0U1Q2Q1", "norm0", "U0Q2D0Q0D1Q2P0U1", "D1Q1U0", "norm1", "Q0Q2P0D0D0U1Q1Q0",
    "U1Q2SBU0SBP0Q1U0", "Q2Q0Q0P0SBQ1P0Q1", "Q2Q2",
)


def pieces(names):
    return [names[i : i + 2] for i in range(0, len(names), 2)]


def back_body(
    len_ref, qa_hbm, k_hbm, v_hbm, do_hbm, o_hbm, low_hbm, w_hbm, xf_hbm, gm_hbm, gain, lo_send, up_part_hbm,
    down_part_hbm, gp_own_hbm, gp_other_hbm, s_ub, s_db, s_g2, s_s2, s_pb,
    lo_got, down_out, up_out, gp_out, g0_out, g1_out, g2_out, ig, small_a, small_b,
    qa, k, v, do, o, low, wp, xf, gm, up_part, down_part, gp_src, gp_got,
    ka, va, kt, dk_acc, dv_acc, dqkv, gpair,
    down_box, down_part2, down_own, up_box, up_part2, up_own, gp_box, gp_part, gp_own, pair_box, pair_part, pair_own,
    down_sum, up_sum, gp_sum, pair_sum,
    gn_send, gn_got, gn_own, ig_own, ig_send, early, early_box, late_sums, late_box,
    load_sem, open_sem, nsend, nrecv, wsend, wrecv, *, bq, wide,
):
    n, me = lax.axis_index("narrow"), lax.axis_index("wide")
    peer = {"narrow": 1 - n}
    narrow, across = (nsend, nrecv), (wsend, wrecv)
    steps = bits(wide)
    heads, rows = qa.shape[0], qa.shape[1]
    pair_w = 2 * HEAD
    pairs = heads // 2
    d, lw = gain.shape[0], k.shape[1]
    cw = d // 2
    half, block = rows // 2, min(256, rows // 2)
    each = half // block
    count = iter(range(64))

    def load(src, dst):
        copy = pltpu.make_async_copy(src, dst, load_sem.at[next(count)])
        copy.start()
        return copy

    pair_loads = []
    for p in range(pairs):
        c = pl.ds(p * pair_w, pair_w)
        pair_loads.append(
            [load(a.at[:, c], b.at[:, c]) for a, b in ((k_hbm, k), (v_hbm, v), (do_hbm, do), (o_hbm, o))]
            + [load(qa_hbm.at[pl.ds(2 * p, 2)], qa.at[pl.ds(2 * p, 2)])]
        )
    part_load = load(down_part_hbm, down_part)
    up_load = load(up_part_hbm, up_part)
    gp_load = load(gp_own_hbm, gp_src)
    low_load = load(low_hbm, low)
    greet([peer] + wide_peers(me, wide))
    gp_swap = remote(gp_other_hbm, gp_got, narrow, 0, peer)
    layer = remote(lo_send, lo_got, narrow, 1, peer)
    gp_swap.start()
    late = [
        load(w_hbm.at[c, :, pl.ds(p * pair_w, pair_w)], wp.at[p, :, pl.ds(c * pair_w, pair_w)])
        for p in range(pairs)
        for c in range(3)
    ]
    own_half = block_rows(n * half, half)
    late += [load(xf_hbm.at[own_half], xf), load(gm_hbm, gm)]

    at = [0, 0]
    opening = iter(range(16))

    def group(src, box, part, own, dst, out, kinds=(0,), entries=(0,)):
        rows_, cols_ = dst.shape
        made = []
        for (kind, cols), entry in zip(lanes_split(cols_, kinds), entries):
            chain = Chain(me, order_of(wide, kind), rows_, cols, across, *at)
            at[:] = chain.send_next, chain.recv_next
            made.append(Group(chain.bind(src, box, part, own, dst, entry), entry, out=(out, open_sem.at[next(opening)])))
        return made

    groups = {}
    groups["D0"], groups["D1"] = group(down_part, down_box, down_part2, down_own, down_sum, down_out, DOWN_KINDS, DOWN_ENTRY)
    groups["U0"], groups["U1"] = group(up_part, up_box, up_part2, up_own, up_sum, up_out, UP_KINDS, UP_ENTRY)
    groups["P0"] = group(gp_src, gp_box, gp_part, gp_own, gp_sum, gp_out, kinds=(1,))[0]
    for p, out in zip(range(pairs), (g0_out, g1_out, g2_out)):
        groups[f"Q{p}"] = group(
            gpair.at[p], pair_box.at[p], pair_part.at[p], pair_own.at[p], pair_sum.at[p], out,
        )[0]

    dr, fr, lr = d // 128, s_ub.shape[1] // 128, lw // 128
    for i, (name, total, box, shared) in enumerate(
        (("SA", early, early_box, 4 * dr), ("SB", late_sums, late_box, -(-2 * dr // 8) * 8))
    ):
        one = Small(me, n, wide, total, box, shared, narrow, across, 2 + 2 * each + i, *at)
        at[:] = one.send_next, one.recv_next
        groups[name] = Group(one)

    def put_sum(ref, start, value):
        for i in range(value.shape[1] // 128):
            ref[start + i : start + i + 1, :] = value[:, i * 128 : (i + 1) * 128]

    early[...] = jnp.zeros_like(early)
    late_sums[...] = jnp.zeros_like(late_sums)
    for i, ref in enumerate((s_g2, s_s2, s_pb, s_db, s_ub)):
        put_sum(early, i * dr, ref[...])

    def tick(names):
        for name in pieces(names):
            with scope(name):
                groups[name].tick()

    part_load.wait()
    tick("D0D1")
    up_load.wait()
    tick("U0U1SA")

    kpos = lax.broadcasted_iota(jnp.int32, (rows, 1), 0)
    kbias = jnp.where(kpos < len_ref[0], 0.0, -1e30)
    tri = lax.broadcasted_iota(jnp.int32, (bq, bq), 0) <= lax.broadcasted_iota(jnp.int32, (bq, bq), 1)

    def plan(names):
        ticks = [groups[name].next() for name in pieces(names)]

        def run():
            for name, one in zip(pieces(names), ticks):
                with scope(name):
                    one()

        return run

    def start_proj():
        first = groups["P0"].next()

        def run():
            gp_swap.wait()
            gp_load.wait()
            gp_src[...] = gp_src[...] + gp_got[...]
            first()

        return run

    hooks = {}
    for at_, names in HEAD_TICKS:
        hooks[at_] = [plan(names)]
        if at_ == (2, 3):
            hooks[at_] += [layer.start, start_proj()]

    def run_hooks(head, block_):
        for (h, where), actions in hooks.items():
            if where == block_:

                @pl.when(head == h)
                def _():
                    for action in actions:
                        action()

    def one_head(head, carry):
        par, pair = head % 2, head // 2
        lane, mine, extra = lanes_of(par)
        cols = lane_part(pair, pair_w)
        for p in range(pairs):

            @pl.when(head == 2 * p)
            def _():
                for copy in pair_loads[p]:
                    copy.wait()

        ka[...] = place(lane, mine, extra, k[:, cols].astype(F32), [kbias, -1.0, -1.0, -1.0]).astype(BF16)
        va[...] = place(lane, mine, extra, v[:, cols].astype(F32), [-1.0, -1.0, -1.0]).astype(BF16)
        kt[...] = ka[...].T
        dk_acc[...] = jnp.zeros_like(dk_acc)
        dv_acc[...] = jnp.zeros_like(dv_acc)

        def put(c, r, new):
            lanes = pl.ds(c * pair_w, pair_w)
            old = dqkv[pair, r, lanes].astype(F32)
            dqkv[pair, r, lanes] = jnp.where(mine, new, jnp.where(par == 0, 0.0, old)).astype(BF16)

        for i in range(rows // bq):
            r = pl.ds(i * bq, bq)
            qb = qa[head, r, :]
            df = do[r, cols].astype(F32)
            delta = jnp.sum(jnp.where(mine, df * o[r, cols].astype(F32), 0.0), axis=1, keepdims=True)
            db = place(lane, mine, extra, df, three(delta)).astype(BF16)
            dqs = None
            chunks = [(0, i * bq), (i * bq, bq)] if i else [(0, bq)]
            for start, size in chunks:
                c = pl.ds(start, size)
                kb, vb = ka[c, :], va[c, :]
                s = dot_nt(kb, qb)
                if start == i * bq:
                    s = jnp.where(tri, s, -1e30)
                p = jnp.exp(s)
                ds = (p * dot_nt(vb, db)).astype(BF16)
                dv_acc[c, :] += dot(p.astype(BF16), db)
                dk_acc[c, :] += dot(ds, qb)
                part = dot(kt[:, c], ds)
                dqs = part if dqs is None else dqs + part
            put(0, r, dqs.T * HEAD**-0.5)
            if i < rows // bq - 1:
                run_hooks(head, i)
        put(1, pl.ds(0, rows), dk_acc[...])
        put(2, pl.ds(0, rows), dv_acc[...])

        @pl.when(head == 1)
        def _():
            low_load.wait()

        @pl.when(par == 1)
        def _():
            with scope("weights"):
                gpair[pair] = dot_tn(low[...], dqkv[pair]).astype(BF16)

        run_hooks(head, rows // bq - 1)
        return carry

    lax.fori_loop(0, heads, one_head, 0)

    for copy in late:
        copy.wait()

    def gn_part(start):
        r = block_rows(start, block)
        total = dot_nt(dqkv[0, r, :], wp[0])
        for p in range(1, pairs):
            total += dot_nt(dqkv[p, r, :], wp[p])
        return total

    def gn_copy(j):
        r = pl.ds(j * block, block)
        return remote(gn_send.at[r], gn_got.at[r], narrow, 2 + j, peer)

    for j in range(each):
        with scope("gn_peer"):
            gn_send[j * block : (j + 1) * block, :] = gn_part((1 - n) * half + j * block).astype(BF16)
        gn_copy(j).start()
        tick(PART_TICKS[j % 2])
    for j in range(each):
        with scope("gn_own"):
            gn_own[j * block : (j + 1) * block, :] = gn_part(n * half + j * block)
        tick(PART_TICKS[2 + j % 2])

    shared = -(-2 * dr // 8) * 8
    for p in range(pairs):
        put_sum(late_sums, shared + p, jnp.sum(dqkv[p, :, 0:pair_w].astype(F32), axis=0, keepdims=True))
        put_sum(late_sums, shared + lr + p, jnp.sum(dqkv[p, :, 2 * pair_w :].astype(F32), axis=0, keepdims=True))
    tick(PART_TICKS[4])

    mine, other = lane_part(n, cw), lane_part(1 - n, cw)

    def ig_copy(j):
        r = block_rows(n * half + j * block, block)
        return remote(ig_send.at[pl.ds(j * block, block)], ig.at[r], narrow, 2 + each + j, peer)

    def in_norm(j):
        with scope("gn_wait"):
            gn_copy(j).wait()
        rh = pl.ds(j * block, block)
        r = block_rows(n * half + j * block, block)
        g = gn_own[rh, :] + gn_got[rh, :].astype(F32)
        xhat, scale = norm_rows(xf[rh, :].astype(F32))
        gg = g * vec(gain)
        m1 = jnp.mean(gg, axis=-1, keepdims=True)
        m2 = jnp.mean(gg * xhat, axis=-1, keepdims=True)
        ig_own[...] = gm[rh, :] + scale * (gg - m1 - xhat * m2)
        ig_send[rh, :] = ig_own[:, other].astype(BF16)
        ig_copy(j).start()
        ig[r, :] = ig_own[:, mine].astype(BF16)
        return jnp.sum(g * xhat, axis=0, keepdims=True), jnp.sum(g, axis=0, keepdims=True)

    sums1 = []
    for names in LAST_TICKS:
        if names in ("norm0", "norm1"):
            todo = range(each - 1) if names == "norm0" else range(each - 1, each)
            sums1 += [in_norm(j) for j in todo]
            if names == "norm1":
                put_sum(late_sums, 0, sum(a for a, _ in sums1))
                put_sum(late_sums, dr, sum(b for _, b in sums1))
                tick("SB")
        else:
            tick(names)
    while not all(g.done for g in groups.values()):
        for name in groups:
            tick(name)
    small_a[...] = early[...]
    small_b[...] = late_sums[...]
    with scope("end"):
        for one in groups.values():
            if one.out is not None:
                one.store().wait()
        layer.wait()
        for j in range(each):
            ig_copy(j).wait()


def back_call(
    length, qa, k, v, do, o, low, w, xf, gm, gain, lo_send, up_part, down_part, gp_own, gp_other,
    s_ub, s_db, s_g2, s_s2, s_pb, wide, bq=256,
):
    heads, rows, pair = qa.shape
    d, f, lw = gain.shape[0], up_part.shape[1], k.shape[1]
    cw, half = d // 2, rows // 2
    block = min(256, half)
    each, steps, pairs = half // block, bits(wide), heads // 2
    sd, vm = jax.ShapeDtypeStruct, pltpu.VMEM
    shape = lambda r, kind=0: Chain(0, order_of(wide, kind), r, None, None, 0, 0)
    c_down, c_up, c_gp = shape(f), shape(d), shape(2 * lw)
    down_rows, up_rows, pair_rows = (max(shape(r, k).box_rows for k in range(4)) for r in (f, d, d))
    small = lambda shared, rest: -(-(shared + rest) // 8) * 8
    rows_a = small(4 * d // 128, f // 128)
    rows_b = small(-(-2 * d // 1024) * 8, 2 * lw // 128)
    slots = CHIPS + 1 + max(0, bits(wide) - 4)
    semaphores = (len(DOWN_KINDS) + len(UP_KINDS) + 1 + pairs) * shape(d).recv_next + 2 * (bits(wide) + CHIPS)
    work = 2 * heads * rows * rows * HEAD
    return pl.pallas_call(
        functools.partial(back_body, bq=bq, wide=wide),
        out_shape=(sd((rows, cw), BF16), sd((f, d), BF16), sd((d, f), BF16), sd((2 * lw, cw), BF16))
        + (sd((d, 3 * pair), BF16),) * 3
        + (sd((rows, cw), BF16), sd((rows_a, 128), F32), sd((rows_b, 128), F32)),
        in_specs=[pl.BlockSpec(memory_space=pltpu.SMEM)] + [anywhere()] * 9 + [vmem()] + [anywhere()] * 5 + [vmem()] * 5,
        out_specs=(anywhere(),) * 7 + (vmem(), vmem(), vmem()),
        scratch_shapes=[
            vm(qa.shape, BF16), vm((rows, lw), BF16), vm((rows, lw), BF16), vm((rows, lw), BF16), vm((rows, lw), BF16),
            vm((rows, d), BF16), vm((pairs, d, 3 * pair), BF16), vm((half, d), BF16), vm((half, d), F32),
            vm((d // 2, f), BF16), vm((f // 2, d), BF16), vm((2 * lw, cw), BF16), vm((2 * lw, cw), BF16),
            vm((rows, pair), BF16), vm((rows, pair), BF16), vm((pair, rows), BF16), vm((rows, pair), F32), vm((rows, pair), F32),
            vm((pairs, rows, 3 * pair), BF16), vm((pairs, d, 3 * pair), BF16),
            vm((down_rows, d), BF16), vm((f // 2, d), BF16), vm((c_down.size, d), BF16),
            vm((up_rows, f), BF16), vm((d // 2, f), BF16), vm((c_up.size, f), BF16),
            vm((pair_rows, cw), BF16), vm((lw, cw), BF16), vm((c_gp.size, cw), BF16),
            vm((pairs, pair_rows, 3 * pair), BF16), vm((pairs, d // 2, 3 * pair), BF16),
            vm((pairs, c_up.size, 3 * pair), BF16),
            vm((f, d), BF16), vm((d, f), BF16), vm((2 * lw, cw), BF16), vm((pairs, d, 3 * pair), BF16),
            vm((half, d), BF16), vm((half, d), BF16), vm((half, d), F32), vm((block, d), F32), vm((half, cw), BF16),
            vm((rows_a, 128), F32), vm((slots, rows_a, 128), F32), vm((rows_b, 128), F32), vm((slots, rows_b, 128), F32),
        ]
        + sems(8 * pairs + 8, 8, 4 + 2 * each, 4 + 2 * each, 17 + 3 * CHIPS, semaphores),
        compiler_params=params(collective_id=4, has_side_effects=True),
        cost_estimate=cost(10 * work + 4 * rows * d * 3 * lw, 2 * rows * d * 20, work // 256),
        name="back",
    )(
        length, qa, k, v, do, o, low, w, xf, gm, gain, lo_send, up_part, down_part, gp_own, gp_other,
        s_ub, s_db, s_g2, s_s2, s_pb,
    )


def finish_body(
    lo, lo_got, bias, ig, up, down, q, k, v, p0, p1, small_a, small_b,
    out, ig_out, o_qkv, o_qvb, o_proj, o_pb, o_up, o_ub, o_down, o_db, o_g1, o_s1, o_g2, o_s2,
    *, factor,
):
    n = lax.axis_index("narrow")
    cw = lo.shape[1]
    b = vec(bias)
    out[...] = (lo[...] + lo_got[...].astype(F32) + jnp.where(n == 0, b[:, :cw], b[:, cw:])).astype(BF16)
    ig_out[...] = ig[...]
    for p, ref in enumerate((q, k, v)):
        for c in range(3):
            lanes = slice(c * 128, (c + 1) * 128)
            o_qkv[c, :, p * 128 : (p + 1) * 128] = ref[:, lanes].astype(F32) * factor
    o_proj[:, :cw] = p0[...].astype(F32) * factor
    o_proj[:, cw:] = p1[...].astype(F32) * factor
    o_up[...] = up[...].astype(F32) * factor
    o_down[...] = down[...].astype(F32) * factor

    @pl.when(pl.program_id(0) == 0)
    def _():
        dr, fr = o_g1.shape[0], o_ub.shape[0]
        for i, ref in enumerate((o_g2, o_s2, o_pb, o_db)):
            ref[...] = small_a[i * dr : (i + 1) * dr, :] * factor
        o_ub[...] = small_a[4 * dr : 4 * dr + fr, :] * factor
        o_g1[...] = small_b[0:dr, :] * factor
        o_s1[...] = small_b[dr : 2 * dr, :] * factor
        lr, shared = o_qvb.shape[1] // 128, -(-2 * dr // 8) * 8
        for c in range(2):
            for i in range(lr):
                at = shared + c * lr + i
                o_qvb[c : c + 1, i * 128 : (i + 1) * 128] = small_b[at : at + 1, :] * factor


def finish_call(lo, lo_got, bias, ig, up, down, q, k, v, p, small_a, small_b, factor, grid=8):
    rows, cw = lo.shape
    (d, f), lw = up.shape, q.shape[1]
    dr, sd = d // 128, jax.ShapeDtypeStruct
    shapes = (
        [sd((rows, cw), BF16), sd((rows, cw), BF16), sd((3, d, lw), F32), sd((2, lw), F32), sd((lw, d), F32)]
        + [sd((dr, 128), F32), sd((d, f), F32), sd((f // 128, 128), F32), sd((f, d), F32)]
        + [sd((dr, 128), F32)] * 5
    )
    big = lambda a: rows_spec(a.shape[0] // grid, a.shape[1])
    pb = lw // grid
    specs = []
    for i, s in enumerate(shapes):
        if len(s.shape) == 3:
            specs.append(pl.BlockSpec((3, d // grid, lw), lambda i, *_: (0, i, 0)))
        elif i in (0, 1, 4, 6, 8):
            specs.append(big(s))
        else:
            specs.append(whole_spec(s.shape))
    return pl.pallas_call(
        functools.partial(finish_body, factor=factor),
        out_shape=tuple(shapes),
        grid=(grid,),
        in_specs=[big(lo), big(lo_got), whole_spec(bias.shape), big(ig), big(up), big(down), big(q), big(k), big(v)]
        + [rows_spec(pb, cw), rows_spec(pb, cw, grid), whole_spec(small_a.shape), whole_spec(small_b.shape)],
        out_specs=tuple(specs),
        compiler_params=params(),
        cost_estimate=cost(up.size * 8, up.size * 24),
        name="finish",
    )(lo, lo_got, bias, ig, up, down, q, k, v, p, p, small_a, small_b)


def on_device(
    tokens, lengths, qkv_weight, qv_bias, proj_weight, proj_bias, up_weight, up_bias,
    down_weight, down_bias, first_gain, first_shift, second_gain, second_shift, cotangent,
):
    cw = tokens.shape[1]
    d, ff, lw = 2 * cw, up_weight.shape[1], proj_weight.shape[0]
    wide = lax.axis_size("wide")
    w3 = jnp.transpose(qkv_weight, (1, 0, 2))

    xf, low, k, v, mixed, qa, mixed_got, proj_got = front_call(
        lengths, tokens, w3, qv_bias, first_gain, first_shift, proj_weight
    )
    lo, lo_send, gmix, gm, up_part, down_part, gp_own, gp_other, s_ub, s_db, s_g2, s_s2, s_pb = mlp_call(
        lengths, xf, mixed, mixed_got, proj_weight, proj_got, proj_bias, second_gain, second_shift,
        up_weight, up_bias, down_weight, cotangent, wide,
    )
    lo_got, gdown, gup, gp, g0, g1, g2, ig, small_a, small_b = back_call(
        lengths, qa, k, v, gmix, mixed, low, w3, xf, gm, first_gain, lo_send, up_part, down_part, gp_own, gp_other,
        s_ub, s_db, s_g2, s_s2, s_pb, wide,
    )
    out, ig, o_qkv, o_qvb, o_proj, *rest = finish_call(
        lo, lo_got, down_bias, ig, gup, gdown, g0, g1, g2, gp, small_a, small_b,
        1.0 / (lengths.shape[0] * wide),
    )
    pb, up, ubs, down, dbs, g1, s1, g2, s2 = rest
    flat = lambda a: a.reshape(-1)
    return (
        out, ig, jnp.transpose(o_qkv, (1, 0, 2)), o_qvb, o_proj, flat(pb), up, flat(ubs), down, flat(dbs),
        flat(g1), flat(s1), flat(g2), flat(s2),
    )


def solution(mesh):
    split = P("wide", "narrow")
    none3, cols, rows1 = P(None, None, "narrow"), P(None, "narrow"), P("narrow", None)
    return jax.shard_map(
        on_device,
        mesh=mesh,
        in_specs=(
            split, P("wide"), none3, cols, rows1, P(), cols, P("narrow"), rows1, P(), P(), P(), P(), P(), split,
        ),
        out_specs=(
            split, split, none3, cols, rows1, P(), cols, P("narrow"), rows1, P(), P(), P(), P(), P(),
        ),
        check_vma=False,
    )
```

```python
import functools

import jax
import jax.numpy as jnp
from jax import lax
from jax.experimental import pallas as pl
from jax.experimental.pallas import tpu as pltpu
from jax.sharding import PartitionSpec as P

EPS = 1e-05
HEAD = 64
F32, BF16 = jnp.float32, jnp.bfloat16
NT = (((1,), (1,)), ((), ()))
TN = (((0,), (0,)), ((), ()))
GELU_A, GELU_B = 0.7978845608028654, 0.044715
VMEM_LIMIT = 63 * 1024 * 1024


def dot(a, b):
    return jnp.dot(a, b, preferred_element_type=F32)


def dot_nt(a, b):
    return lax.dot_general(a, b, NT, preferred_element_type=F32)


def dot_tn(a, b):
    return lax.dot_general(a, b, TN, preferred_element_type=F32)


def params(**more):
    return pltpu.CompilerParams(vmem_limit_bytes=VMEM_LIMIT, **more)


def cost(flops, size, trans=0):
    return pl.CostEstimate(flops=int(flops), bytes_accessed=int(size), transcendentals=int(trans))


def lane_part(which, width):
    return pl.ds(pl.multiple_of(which * width, 128), width)


def norm_rows(x):
    mean = jnp.mean(x, axis=-1, keepdims=True)
    cen = x - mean
    var = jnp.mean(cen * cen, axis=-1, keepdims=True)
    r = lax.rsqrt(var + EPS)
    return cen * r, r


def rows_spec(rows, cols, base=0):
    return pl.BlockSpec((rows, cols), lambda i, *_: (i + base, 0))


def whole_spec(shape):
    zeros = (0,) * len(shape)
    return pl.BlockSpec(shape, lambda i, *_: zeros)


MESH = pl.DeviceIdType.MESH
scope = jax.named_scope


def vec(ref):
    return ref[...].astype(F32).reshape(1, -1)


def bit_of(index, bit):
    return (index // (1 << bit)) % 2


def flip(index, bit):
    return index + (1 - 2 * bit_of(index, bit)) * (1 << bit)


def greet(peers):
    barrier = pltpu.get_barrier_semaphore()
    for peer in peers:
        pl.semaphore_signal(barrier, inc=1, device_id=peer, device_id_type=MESH)
    pl.semaphore_wait(barrier, len(peers))


def remote(src, dst, sems, at, peer, send_at=None):
    return pltpu.make_async_remote_copy(
        src_ref=src, dst_ref=dst, send_sem=sems[0].at[at if send_at is None else send_at], recv_sem=sems[1].at[at],
        device_id=peer, device_id_type=MESH,
    )


def block_rows(start, size, unit=16):
    return pl.ds(start if isinstance(start, int) else pl.multiple_of(start, unit), size)


LINE, CHIPS = 4, 8


def when(cond, action):
    @pl.when(cond)
    def _():
        action()


def line_peer(me, by):
    q = (me // 4) % LINE
    return me + ((q + by) % LINE - q) * 4


class Chain:
    def __init__(self, me, order, rows, cols, sems, send_at, recv_at):
        self.me, self.cols, self.sems, self.send_at = me, cols, sems, send_at
        self.phases, self.ops, back = [], [], []
        base, size, box = 0, rows, 0
        for kind, bit in order:
            if kind == "line" and size % (16 * LINE):
                raise ValueError(rows)
            if kind == "all":
                ways = CHIPS >> (bit - 1)
                part = size // ways
                keep, give, boxes = base + (me // (1 << bit)) % ways * part, None, (ways - 1) * part
                self.ops.append(("send", len(self.phases), ways))
                back = [("share", len(self.phases), ways)] + back
            elif kind == "line":
                part = size // LINE
                keep, give, boxes = base + (me // 4) % LINE * part, None, 2 * (LINE - 1) * part
                self.ops += [("line", len(self.phases), i) for i in range(1, LINE)]
                back = [("spread", len(self.phases), i) for i in range(1, LINE)] + back
            elif size % 32 == 0:
                part = size // 2
                mine = bit_of(me, bit)
                keep, give, boxes = base + mine * part, base + (1 - mine) * part, part
                self.ops.append(("pair", len(self.phases), 0))
                back = [("join", len(self.phases), 0)] + back
            else:
                part, keep, give, boxes = size, base, base, size
                self.ops.append(("pair", len(self.phases), 0))
            self.phases.append((bit, base, keep, give, part, box))
            base, size, box = keep, part, box + boxes
        self.scatters = len(self.ops)
        self.ops += back
        self.base, self.size, self.box_rows = base, size, box
        self.recv_at, widest = [], 1
        for kind, _, i in self.ops:
            width = {"line": 2, "spread": 2, "send": i - 1, "share": i - 1}.get(kind, 1)
            self.recv_at.append(recv_at)
            recv_at, widest = recv_at + width, max(widest, width)
        self.recv_next, self.send_next = recv_at, send_at + widest

    def bind(self, src, box, part, own, dst=None, entry=0):
        self.src, self.box, self.part, self.own, self.dst = src, box, part, own, dst
        self.entry = self.ops[entry][1]
        return self

    def _source(self, phase):
        off = 0 if phase == 0 else self.phases[0][2]
        return (self.src if phase == self.entry else self.part), off

    def _target(self, phase):
        if phase == len(self.phases) - 1:
            return self.own, self.phases[phase][2]
        return self.part, self.phases[0][2]

    def _remote(self, op, lane, src, dst, to):
        return remote(src, dst, self.sems, self.recv_at[op] + lane, {"wide": to}, self.send_at + lane)

    def _add(self, rows, target, first, *terms):
        unit = next(u for u in (96, 64, 48, 32, 16) if rows % u == 0)

        def add(i, carry):
            total = None
            for ref, start in terms:
                value = ref[block_rows(start + i * unit, unit), self.cols]
                value = value.astype(F32) if len(terms) > 2 else value
                total = value if total is None else total + value
            target[block_rows(first + i * unit, unit), self.cols] = total.astype(BF16)
            return carry

        lax.fori_loop(0, rows // unit, add, 0)


    def _pair(self, op, phase):
        bit, _, _, give, rows, box = self.phases[phase]
        source, off = self._source(phase)
        src = source.at[block_rows(give - off, rows), self.cols]
        return self._remote(op, 0, src, self.box.at[pl.ds(box, rows), self.cols], flip(self.me, bit))

    def _join(self, op, phase):
        bit, _, keep, _, rows, _ = self.phases[phase]
        region = self.dst.at[block_rows(keep, rows), self.cols]
        return self._remote(op, 0, region, region, flip(self.me, bit))


    def _others(self, bit, ways):
        for m in range(1, ways):
            yield m - 1, flip_all(self.me, bit, m)

    def _sends(self, op, phase, ways):
        bit, base, _, _, rows, box = self.phases[phase]
        source, off = self._source(phase)
        for m, to in self._others(bit, ways):
            src = source.at[block_rows(base - off + (to // (1 << bit)) % ways * rows, rows), self.cols]
            yield self._remote(op, m, src, self.box.at[pl.ds(box + m * rows, rows), self.cols], to)

    def _shares(self, op, phase, ways, came):
        bit, base, keep, _, rows, _ = self.phases[phase]
        for m, to in self._others(bit, ways):
            at = base + (to // (1 << bit)) % ways * rows if came else keep
            region = self.dst.at[block_rows(at, rows), self.cols]
            yield self._remote(op, m, region, region, to)


    def _slot(self, phase, lane, i):
        rows, box = self.phases[phase][4:]
        return box + (lane * (LINE - 1) + i - 1) * rows

    def _line_sends(self, op, phase, i):
        q = (self.me // 4) % LINE
        _, base, _, _, rows, _ = self.phases[phase]
        source, off = self._source(phase)
        sends = []
        for lane, by in ((0, 1), (1, -1)):
            place_ = q if lane == 0 else LINE - 1 - q
            chunk = LINE - i if lane == 0 else i - 1
            dst = self.box.at[pl.ds(self._slot(phase, lane, i), rows), self.cols]
            to = line_peer(self.me, by)
            src = source.at[block_rows(base - off + chunk * rows, rows), self.cols]
            sends.append((place_ == 0, functools.partial(self._remote, op, lane, src, dst, to)))
            if i > 1:
                src = self.box.at[pl.ds(self._slot(phase, lane, i - 1), rows), self.cols]
                moving = jnp.logical_and(place_ >= 1, place_ <= min(i - 1, LINE - 2))
                sends.append((moving, functools.partial(self._remote, op, lane, src, dst, to)))
        return sends

    def _line_end(self, op, phase, i):
        q = (self.me // 4) % LINE
        _, base, keep, _, rows, _ = self.phases[phase]
        source, off = self._source(phase)
        for cond, copy in self._line_sends(op, phase, i):
            when(cond, lambda: copy().wait_send())
        for lane, by in ((0, -1), (1, 1)):
            place_ = q if lane == 0 else LINE - 1 - q
            slot = self._slot(phase, lane, i)
            dst = self.box.at[pl.ds(slot, rows), self.cols]
            arrived = jnp.logical_and(place_ >= 1, place_ <= i)
            chunk = LINE - 1 - i + q if lane == 0 else i + q - (LINE - 1)

            @pl.when(arrived)
            def _():
                self._remote(op, lane, dst, dst, line_peer(self.me, by)).wait_recv()
                if i < LINE - 1:
                    self._add(rows, self.box, slot, (self.box, slot), (source, base - off + chunk * rows))

        if i == LINE - 1:
            target, out = self._target(phase)
            own = (source, keep - off)
            left, right = (self.box, self._slot(phase, 0, i)), (self.box, self._slot(phase, 1, i))

            @pl.when(q == 0)
            def _():
                self._add(rows, target, keep - out, own, right)

            @pl.when(q == LINE - 1)
            def _():
                self._add(rows, target, keep - out, own, left)

            @pl.when(jnp.logical_and(q > 0, q < LINE - 1))
            def _():
                self._add(rows, target, keep - out, left, own, right)

    def _spread(self, op, phase, i):
        q = (self.me // 4) % LINE
        _, base, _, _, rows, _ = self.phases[phase]
        ways = []
        for lane, by in ((0, 1), (1, -1)):
            place_ = q if lane == 0 else LINE - 1 - q
            sent = self.dst.at[block_rows(base + (q - by * (i - 1)) * rows, rows), self.cols]
            came = self.dst.at[block_rows(base + (q - by * i) * rows, rows), self.cols]
            send_if = jnp.logical_and(place_ >= i - 1, place_ <= LINE - 2)
            ways.append(
                (
                    send_if, functools.partial(self._remote, op, lane, sent, sent, line_peer(self.me, by)),
                    place_ >= i, functools.partial(self._remote, op, lane, came, came, line_peer(self.me, -by)),
                )
            )
        return ways

    def start(self, op):
        kind, phase, i = self.ops[op]
        if kind == "pair":
            self._pair(op, phase).start()
        elif kind == "join":
            self._join(op, phase).start()
        elif kind == "send":
            for copy in self._sends(op, phase, i):
                copy.start()
        elif kind == "share":
            for copy in self._shares(op, phase, i, False):
                copy.start()
        elif kind == "line":
            for cond, copy in self._line_sends(op, phase, i):
                when(cond, lambda: copy().start())
        else:
            for cond, copy, _, _ in self._spread(op, phase, i):
                when(cond, lambda: copy().start())

    def end(self, op):
        kind, phase, i = self.ops[op]
        if kind == "pair":
            self._pair(op, phase).wait()
            _, _, keep, _, rows, box = self.phases[phase]
            source, off = self._source(phase)
            target, out = self._target(phase)
            self._add(rows, target, keep - out, (self.box, box), (source, keep - off))
        elif kind == "join":
            self._join(op, phase).wait()
        elif kind == "send":
            for copy in self._sends(op, phase, i):
                copy.wait()
            _, _, keep, _, rows, box = self.phases[phase]
            source, off = self._source(phase)
            target, out = self._target(phase)
            terms = [(self.box, box + m * rows) for m in range(i - 1)]
            self._add(rows, target, keep - out, (source, keep - off), *terms)
        elif kind == "share":
            for copy in self._shares(op, phase, i, False):
                copy.wait_send()
            for copy in self._shares(op, phase, i, True):
                copy.wait_recv()
        elif kind == "line":
            self._line_end(op, phase, i)
        else:
            for send_if, send, recv_if, recv in self._spread(op, phase, i):
                when(send_if, lambda: send().wait_send())
                when(recv_if, lambda: recv().wait_recv())

    def gather_open(self):
        self._add(self.size, self.dst, self.base, (self.own, 0))


class Group:
    def __init__(self, chain, entry=0, leave=None, out=None):
        self.chain, self.out = chain, out
        self.ops = list(range(entry, len(chain.ops) if leave is None else leave))
        self.pos = -1

    @property
    def done(self):
        return self.pos >= len(self.ops)

    def next(self):
        pos = self.pos
        self.pos = min(pos + 1, len(self.ops))

        def tick():
            if pos >= len(self.ops):
                return
            if pos >= 0:
                self.chain.end(self.ops[pos])
            if pos + 1 >= len(self.ops):
                if self.out is not None:
                    self.store().start()
                return
            if self.ops[pos + 1] == self.chain.scatters:
                self.chain.gather_open()
            self.chain.start(self.ops[pos + 1])

        return tick

    def tick(self):
        self.next()()

    def store(self):
        out, sem = self.out
        return pltpu.make_async_copy(self.chain.dst.at[:, self.chain.cols], out.at[:, self.chain.cols], sem)


def bits(wide):
    return wide.bit_length() - 1


def order_of(wide, kind):
    first, rest = ("pair", 0), [("pair", b) for b in range(4, bits(wide))]
    pair, line = ("pair", 1), ("line", 2)
    return {
        0: [first, pair, line, *rest], 1: [first, line, pair, *rest], 2: [first, ("all", 1), *rest],
        3: [first, pair, ("all", 2), *rest],
    }[kind]


def lanes_split(cols, kinds):
    w = cols // len(kinds)
    return [(kind, pl.ds(i * w, w)) for i, kind in enumerate(kinds)]


def flip_all(me, bit, mask):
    to = me
    for i in range(3):
        if mask >> i & 1:
            to = to + (flip(me, bit + i) - me)
    return to


def chip_peers(me):
    return [flip_all(me, 1, m) for m in range(1, CHIPS)]


def wide_peers(me, wide):
    pairs = [flip(me, b) for b in range(bits(wide)) if b not in (1, 2, 3)]
    return [{"wide": peer} for peer in pairs + chip_peers(me)]


class Small:
    def __init__(self, me, n, wide, total, box, shared, narrow, across, narrow_at, send_at, recv_at):
        self.me, self.n, self.total, self.box, self.shared = me, n, total, box, shared
        self.narrow, self.across = narrow, across
        self.narrow_at, self.send_at, self.recv_at = narrow_at, send_at, recv_at
        self.ops = ["narrow", 0, "chips"] + list(range(4, bits(wide)))
        self.scatters, self.dst = None, None
        self.send_next = send_at + CHIPS - 1
        self.recv_next = recv_at + len(self.ops) + CHIPS - 1

    def _copies(self, op):
        kind = self.ops[op]
        if kind == "narrow":
            top = pl.ds(0, self.shared)
            return [remote(self.total.at[top], self.box.at[0, top], self.narrow, self.narrow_at, {"narrow": 1 - self.n})]
        if kind == "chips":
            return [
                remote(
                    self.total, self.box.at[2 + i], self.across, self.recv_at + len(self.ops) + i, {"wide": to},
                    self.send_at + i,
                )
                for i, to in enumerate(chip_peers(self.me))
            ]
        slot = 1 if kind == 0 else CHIPS + 1 + kind - 4
        peer = {"wide": flip(self.me, kind)}
        return [remote(self.total, self.box.at[slot], self.across, self.recv_at + op, peer, self.send_at)]

    def start(self, op):
        for copy in self._copies(op):
            copy.start()

    def end(self, op):
        for copy in self._copies(op):
            copy.wait()
        kind = self.ops[op]
        if kind == "narrow":
            self.total[0 : self.shared, :] += self.box[0, 0 : self.shared, :]
        elif kind == "chips":
            self.total[...] += sum(self.box[2 + i] for i in range(CHIPS - 1))
        else:
            self.total[...] += self.box[1 if kind == 0 else CHIPS + 1 + kind - 4]


def vmem():
    return pl.BlockSpec(memory_space=pltpu.VMEM)


def anywhere():
    return pl.BlockSpec(memory_space=pl.ANY)


def sems(*counts):
    return [pltpu.SemaphoreType.DMA((c,)) for c in counts]


def three(x):
    hi = x.astype(BF16).astype(F32)
    mid = (x - hi).astype(BF16).astype(F32)
    return hi, mid, x - hi - mid


def lanes_of(par):
    lane = lax.broadcasted_iota(jnp.int32, (1, 2 * HEAD), 1)
    mine = (lane // HEAD) == par
    return lane, mine, (1 - par) * HEAD


def place(lane, mine, at, base, terms):
    out = jnp.where(mine, base, 0.0)
    for i, term in enumerate(terms):
        out = jnp.where(lane == at + i, term, out)
    return out


def front_body(
    len_ref, tokens, w_hbm, bias, gain, shift, pw, cot,
    xf_out, low_out, k_out, v_out, o_out, qa_out, o_got, pw_got, cot_head,
    own, got, w, xf, low, q, k, v, o, qa, ka, va, load_sem, store_sem, send_sem, recv_sem, *, bq,
):
    n, me = lax.axis_index("narrow"), lax.axis_index("wide")
    peer, core = {"narrow": 1 - n}, {"wide": flip(me, 0)}
    both = (send_sem, recv_sem)
    rows, cw = own.shape
    pair_w, heads = 2 * HEAD, qa.shape[0]
    blocks = rows // bq
    loads = [pltpu.make_async_copy(a, b, load_sem.at[i]) for i, (a, b) in enumerate(((tokens, own), (w_hbm, w)))]
    for load in loads:
        load.start()
    greet([peer, core] + [{"wide": to} for to in chip_peers(me)])

    def token_copy(i):
        r = block_rows(i * bq, bq)
        return remote(tokens.at[r], got.at[r], both, i, peer)

    for i in range(blocks):
        token_copy(i).start()
    used = blocks + blocks * (heads // 2)
    slab, mine_lanes = pw.shape[0] // CHIPS, lane_part(me % 2, pw.shape[1] // 2)

    def slab_of(device):
        return pw_got.at[block_rows((device // 2) % CHIPS * slab, slab), mine_lanes]

    source = pw.at[block_rows((me // 2) % CHIPS * slab, slab), mine_lanes]
    weights = remote(source, slab_of(me), both, used, peer)
    core_share = remote(pw_got.at[:, mine_lanes], pw_got.at[:, mine_lanes], both, used + 1, core)
    head_copy = remote(cot.at[block_rows(n * (rows // 2), bq)], cot_head, both, used + 2, peer)

    def chip_shares(came):
        return [
            remote(slab_of(to if came else me), slab_of(to if came else me), both, used + 3 + i, {"wide": to})
            for i, to in enumerate(chip_peers(me))
        ]

    weights.start()
    head_copy.start()
    for load in loads:
        load.wait()

    def project(i, carry):
        r = block_rows(i * bq, bq)
        xf[r, lane_part(n, cw)] = own[r, :]
        with scope("wait"):
            token_copy(i).wait()
        xf[r, lane_part(1 - n, cw)] = got[r, :]
        xhat, _ = norm_rows(xf[r, :].astype(F32))
        y = (xhat * vec(gain) + vec(shift)).astype(BF16)
        low[r, :] = y
        q[r, :] = (dot(y, w[0]) + bias[0:1, :].astype(F32)).astype(BF16) * jnp.asarray(HEAD**-0.5, BF16)
        k[r, :] = dot(y, w[1]).astype(BF16)
        v[r, :] = (dot(y, w[2]) + bias[1:2, :].astype(F32)).astype(BF16)
        return carry

    lax.fori_loop(0, blocks, project, 0)
    stores = [
        pltpu.make_async_copy(a, b, store_sem.at[i])
        for i, (a, b) in enumerate(((xf, xf_out), (low, low_out), (k, k_out), (v, v_out)))
    ]
    for store in stores:
        store.start()

    kpos = lax.broadcasted_iota(jnp.int32, (rows, 1), 0)
    kbias = jnp.where(kpos < len_ref[0], 0.0, -1e30)
    tri = lax.broadcasted_iota(jnp.int32, (bq, bq), 1) <= lax.broadcasted_iota(jnp.int32, (bq, bq), 0)

    def mixed(pair, i):
        r, c = pl.ds(i * bq, bq), lane_part(pair, pair_w)
        return remote(o.at[r, c], o_got.at[r, c], both, blocks + pair * blocks + i, peer)

    def mixed_store(pair):
        c = lane_part(pair, pair_w)
        return pltpu.make_async_copy(o.at[:, c], o_out.at[:, c], store_sem.at[4 + pair])

    def qa_store(head):
        return pltpu.make_async_copy(qa.at[head], qa_out.at[head], store_sem.at[4 + heads // 2 + head])

    def one_head(head, carry):
        par, pair = head % 2, head // 2
        lane, mine, at = lanes_of(par)
        cols = lane_part(pair, pair_w)
        ka[...] = place(lane, mine, at, k[:, cols].astype(F32), [kbias]).astype(BF16)
        va[...] = place(lane, mine, at, v[:, cols].astype(F32), [1.0]).astype(BF16)
        for i in range(blocks):
            nk = (i + 1) * bq
            r = pl.ds(i * bq, bq)
            qf = q[r, cols].astype(F32)
            s = dot_nt(place(lane, mine, at, qf, [1.0]).astype(BF16), ka[0:nk, :])
            edge = jnp.where(tri, s[:, nk - bq :], -1e30)
            m = jnp.max(edge, axis=1, keepdims=True)
            if nk > bq:
                m = jnp.maximum(m, jnp.max(s[:, : nk - bq], axis=1, keepdims=True))
            pv = dot(jnp.exp(edge - m).astype(BF16), va[nk - bq : nk, :])
            if nk > bq:
                pv += dot(jnp.exp(s[:, : nk - bq] - m).astype(BF16), va[0 : nk - bq, :])
            total = jnp.sum(jnp.where(lane == at, pv, 0.0), axis=1, keepdims=True)
            out = (pv / total).astype(BF16).astype(F32)
            old = o[r, cols].astype(F32)
            o[r, cols] = jnp.where(mine, out, jnp.where(par == 0, 0.0, old)).astype(BF16)
            lse = m + jnp.log(total)
            qa[head, r, :] = place(lane, mine, at, qf, [1.0, *three(lse)]).astype(BF16)
            when(par == 1, lambda: mixed(pair, i).start())
        when(par == 1, lambda: mixed_store(pair).start())
        qa_store(head).start()

        @pl.when(head == 0)
        def _():
            weights.wait()
            for share in chip_shares(False):
                share.start()

        @pl.when(head == 3)
        def _():
            for share in chip_shares(False):
                share.wait_send()
            for share in chip_shares(True):
                share.wait_recv()
            core_share.start()

        return carry

    with scope("heads"):
        lax.fori_loop(0, heads, one_head, 0)
    for store in stores:
        store.wait()
    for head in range(heads):
        qa_store(head).wait()
    core_share.wait()
    head_copy.wait()
    with scope("mixed"):
        for pair in range(heads // 2):
            mixed_store(pair).wait()
            for i in range(blocks):
                mixed(pair, i).wait()


def front_call(length, own, w, bias, gain, shift, pw, cot, bq=256):
    rows, cw = own.shape
    d, lw = w.shape[1], w.shape[2]
    heads, pair = lw // HEAD, 2 * HEAD
    sd, vm = jax.ShapeDtypeStruct, pltpu.VMEM
    copies = rows // bq * (1 + heads // 2) + 3 + CHIPS
    shapes = [(rows, d), (rows, d), (rows, lw), (rows, lw), (rows, lw), (heads, rows, pair), (rows, lw), pw.shape, (bq, cw)]
    scratch = [(rows, cw), (rows, cw), w.shape, (rows, d), (rows, d)] + [(rows, lw)] * 4
    work = 2 * heads * rows * rows * HEAD
    return pl.pallas_call(
        functools.partial(front_body, bq=bq),
        out_shape=tuple(sd(a, BF16) for a in shapes),
        in_specs=[pl.BlockSpec(memory_space=pltpu.SMEM), anywhere(), anywhere(), vmem(), vmem(), vmem(), anywhere(), anywhere()],
        out_specs=(anywhere(),) * 9,
        scratch_shapes=[vm(a, BF16) for a in scratch]
        + [vm((heads, rows, pair), BF16), vm((rows, pair), BF16), vm((rows, pair), BF16)]
        + sems(2, 4 + heads // 2 + heads, copies, copies),
        compiler_params=params(collective_id=1, has_side_effects=True),
        cost_estimate=cost(2 * rows * d * 3 * lw + 4 * work, 2 * rows * d * 8, work // 256),
        name="front",
    )(length, own, w, bias, gain, shift, pw, cot)


DOWN_ENTRY, UP_ENTRY = (2, 2), (1, 1)
DOWN_KINDS, UP_KINDS, PAIR_KINDS = (0, 0), (0, 1), (0, 0, 3)


def mlp_body(
    len_ref, xf_hbm, mo_hbm, mr_hbm, pwo_hbm, pwr_hbm, pb, gain, shift, ub, up_hbm, down_hbm, cot_hbm, cot_head,
    lo_out, lo_send_out, gmix, gm_out, up_part, down_part, gp_own, gp_other, sum_ub, sum_db, sum_g, sum_s, sum_pb,
    xf, mo, mr, pwo, pwr, up, down, cot, cot_got, cf, lo, lo_send, mid, second, active, slope, gh,
    gs_send, gs_got, gs_own, gdown, gup, box, up_box, gm, glow, gmix_send, load_sem, store_sem, nsend, nrecv, wsend, wrecv,
    *, wide,
):
    n, me = lax.axis_index("narrow"), lax.axis_index("wide")
    peer = {"narrow": 1 - n}
    rows, cw = cot.shape
    d, f = up.shape
    half, block = rows // 2, min(256, rows // 2)
    each = half // block
    mine, other = lane_part(n, cw), lane_part(1 - n, cw)
    narrow, across = (nsend, nrecv), (wsend, wrecv)
    count = iter(range(16))

    def load(src, dst):
        copy = pltpu.make_async_copy(src, dst, load_sem.at[next(count)])
        copy.start()
        return copy

    his, own = block_rows((1 - n) * half, half), block_rows(n * half, half)
    first = [load(a, b) for a, b in ((pwo_hbm, pwo), (pwr_hbm, pwr))]
    first += [load(a.at[his], b.at[his]) for a, b in ((xf_hbm, xf), (mo_hbm, mo), (mr_hbm, mr))]
    up_load = load(up_hbm, up)
    greet([peer] + wide_peers(me, wide))

    def cot_copy(side, j, a):
        r = block_rows(side * half + j * block, block)
        return remote(cot_hbm.at[r], cot_got.at[r], narrow, a * each + j, peer)

    for a, side in enumerate((n, 1 - n)):
        for j in range(each):
            if (a, j) != (0, 0):
                cot_copy(side, j, a).start()
    head_load = load(cot_head, cot_got.at[block_rows((1 - n) * half, block)])
    down_load = load(down_hbm, down)
    cot_load = load(cot_hbm, cot)
    rest = [load(a.at[own], b.at[own]) for a, b in ((xf_hbm, xf), (mo_hbm, mo), (mr_hbm, mr))]

    def project(at):
        r = block_rows(at, block)
        m = xf[r, :].astype(F32) + (dot(mo[r, :], pwo[...]) + dot(mr[r, :], pwr[...])) + vec(pb)
        mid[r, :] = m
        xhat, _ = norm_rows(m)
        second[r, :] = (xhat * vec(gain) + vec(shift)).astype(BF16)

    def forward(at):
        r = block_rows(at, block)
        hid = dot(second[r, :], up[...]) + vec(ub)
        sq = hid * hid
        t = jnp.tanh(GELU_A * (hid + GELU_B * (sq * hid)))
        hf = 0.5 * (1.0 + t)
        act = (hid * hf).astype(BF16)
        active[r, :] = act
        slope[r, :] = hf + (0.5 * hid) * (1.0 - t * t) * (GELU_A + (3.0 * GELU_A * GELU_B) * sq)
        lo[r, :] = mid[r, mine] + dot(act, down[:, mine])
        lo_send[r, :] = dot(act, down[:, other]).astype(BF16)

    def backward(at):
        r = block_rows(at, block)
        pos = at + lax.broadcasted_iota(jnp.int32, (block, 1), 0)
        live = (pos < len_ref[0]).astype(F32)
        cf[r, mine] = (cot[r, :].astype(F32) * live).astype(BF16)
        cf[r, other] = (cot_got[r, :].astype(F32) * live).astype(BF16)
        ghid = (dot_nt(cf[r, :], down[...]) * slope[r, :]).astype(BF16)
        gh[r, :] = ghid
        sum_ub[...] += jnp.sum(ghid.astype(F32), axis=0, keepdims=True)
        return dot_nt(ghid, up[...])

    def every(side, body):
        def step(j, carry):
            body(side * half + j * block)
            return carry

        lax.fori_loop(0, each, step, 0)

    def both(at):
        project(at)
        forward(at)

    for ref in (sum_ub, sum_g, sum_s, sum_pb, sum_db):
        ref[...] = jnp.zeros_like(ref)
    with scope("load"):
        for copy in first:
            copy.wait()
    with scope("project"):
        every(1 - n, project)
    with scope("load2"):
        up_load.wait()
        down_load.wait()
    with scope("fwd_peer"):
        every(1 - n, forward)
    with scope("cot_wait"):
        cot_load.wait()
        head_load.wait()
        for j in range(1, each):
            cot_copy(n, j, 0).wait()

    def gs_copy(j):
        r = block_rows(j * block, block)
        return remote(gs_send.at[r], gs_got.at[r], narrow, 2 * each + j, peer)

    def for_peer(j, carry):
        gs_send[block_rows(j * block, block), :] = backward((1 - n) * half + j * block).astype(BF16)
        gs_copy(j).start()
        return carry

    def for_own(j, carry):
        gs_own[block_rows(j * block, block), :] = backward(n * half + j * block)
        return carry

    with scope("for_peer"):
        lax.fori_loop(0, each, for_peer, 0)
    for copy in rest:
        copy.wait()
    with scope("fwd_own"):
        every(n, both)
    stores = []

    def store(src, dst):
        copy = pltpu.make_async_copy(src, dst, store_sem.at[len(stores)])
        copy.start()
        stores.append(copy)

    store(lo, lo_out)
    store(lo_send, lo_send_out)
    with scope("cot_wait2"):
        for j in range(each):
            cot_copy(1 - n, j, 1).wait()
    with scope("for_own"):
        lax.fori_loop(0, each, for_own, 0)

    def weight(dst, left, right):
        def step(i, carry):
            c = block_rows(i * 256, 256, 256)
            dst[c, :] = dot_tn(left[:, c], right[...]).astype(BF16)
            return carry

        lax.fori_loop(0, dst.shape[0] // 256, step, 0)

    used = iter(range(16))

    def group(src, box_, part, kinds, leaves):
        parts = []
        for (kind, cols), leave in zip(lanes_split(src.shape[1], kinds), leaves):
            a = next(used)
            chain = Chain(me, order_of(wide, kind), src.shape[0], cols, across, 2 * a, 2 * a)
            parts.append(Group(chain.bind(src, box_, part, None), leave=leave))
        return parts

    reduce_down = group(gdown, box, down_part, DOWN_KINDS, DOWN_ENTRY)
    reduce_up = group(gup, up_box, up_part, UP_KINDS, UP_ENTRY)

    def advance(name, *groups):
        with scope(name):
            for one in groups:
                one.tick()

    with scope("w_down"):
        weight(gdown, active, cf)
    advance("core_d", *reduce_down)
    with scope("w_up"):
        weight(gup, second, gh)
    advance("core_u", *reduce_down, *reduce_up)
    with scope("gs_wait"):
        for j in range(each):
            gs_copy(j).wait()

    def gmix_copy(j):
        r = block_rows(n * half + j * block, block)
        return remote(gmix_send.at[block_rows(j * block, block)], gmix.at[r], narrow, 3 * each + j, peer)

    def back_norm(j, carry):
        r, rh = block_rows(n * half + j * block, block), block_rows(j * block, block)
        g = gs_own[rh, :] + gs_got[rh, :].astype(F32)
        xhat, scale = norm_rows(mid[r, :])
        gg = g * vec(gain)
        m1 = jnp.mean(gg, axis=-1, keepdims=True)
        m2 = jnp.mean(gg * xhat, axis=-1, keepdims=True)
        c = cf[r, :].astype(F32)
        grad = c + scale * (gg - m1 - xhat * m2)
        gm[rh, :] = grad
        gl = grad.astype(BF16)
        glow[rh, :] = gl
        gmix_send[rh, :] = dot_nt(gl, pwr[...]).astype(BF16)
        gmix_copy(j).start()
        gmix[r, :] = dot_nt(gl, pwo[...]).astype(BF16)
        sum_g[...] += jnp.sum(g * xhat, axis=0, keepdims=True)
        sum_s[...] += jnp.sum(g, axis=0, keepdims=True)
        sum_pb[...] += jnp.sum(grad, axis=0, keepdims=True)
        sum_db[...] += jnp.sum(c, axis=0, keepdims=True)
        return carry

    with scope("back_norm"):
        lax.fori_loop(0, each, back_norm, 0)
    store(gm, gm_out)
    advance("across", *reduce_up)
    with scope("proj"):
        lw = mo.shape[1]
        for src, dst in ((mr, gp_other), (mo, gp_own)):
            total = dot_tn(src[own, :], glow[...]).astype(BF16)
            dst[0:lw, :] = total[:, :cw]
            dst[lw : 2 * lw, :] = total[:, cw:]
    with scope("gmix_wait"):
        for j in range(each):
            gmix_copy(j).wait()
    advance("leave", *reduce_down, *reduce_up)
    with scope("store"):
        for copy in stores:
            copy.wait()


def mlp_call(length, xf, mo, mr, pwo, pwr, pb, gain, shift, up, ub, down, cot, cot_head, wide):
    rows, d = xf.shape
    f, lw, cw = up.shape[1], mo.shape[1], cot.shape[1]
    half = rows // 2
    sd, vm = jax.ShapeDtypeStruct, pltpu.VMEM
    each = half // min(256, half)
    return pl.pallas_call(
        functools.partial(mlp_body, wide=wide),
        out_shape=(
            sd((rows, cw), F32), sd((rows, cw), BF16), sd((rows, lw), BF16), sd((half, d), F32),
            sd((d // 2, f), BF16), sd((f // 2, d), BF16), sd((2 * lw, cw), BF16), sd((2 * lw, cw), BF16),
            sd((1, f), F32), sd((1, d), F32), sd((1, d), F32), sd((1, d), F32), sd((1, d), F32),
        ),
        in_specs=[pl.BlockSpec(memory_space=pltpu.SMEM)] + [anywhere()] * 5 + [vmem()] * 4 + [anywhere()] * 4,
        out_specs=(anywhere(), anywhere(), vmem(), anywhere()) + (vmem(),) * 9,
        scratch_shapes=[
            vm((rows, d), BF16), vm((rows, lw), BF16), vm((rows, lw), BF16), vm((lw, d), BF16), vm((lw, d), BF16),
            vm((d, f), BF16), vm((f, d), BF16), vm((rows, cw), BF16), vm((rows, cw), BF16), vm((rows, d), BF16),
            vm((rows, cw), F32), vm((rows, cw), BF16), vm((rows, d), F32),
            vm((rows, d), BF16), vm((rows, f), BF16), vm((rows, f), F32), vm((rows, f), BF16),
            vm((half, d), BF16), vm((half, d), BF16), vm((half, d), F32), vm((f, d), BF16), vm((d, f), BF16),
            vm((f, d), BF16), vm((d, f), BF16), vm((half, d), F32), vm((half, d), BF16), vm((half, lw), BF16),
        ]
        + sems(12, 4, 4 * each, 4 * each, 8, 8),
        compiler_params=params(collective_id=3, has_side_effects=True),
        cost_estimate=cost(2 * rows * d * (d + 6 * f), 2 * (rows * d * 8 + 2 * d * f), rows * f),
        name="mlp",
    )(length, xf, mo, mr, pwo, pwr, pb, gain, shift, ub, up, down, cot, cot_head)


START_TICKS = "U0D1D0U1"
HEAD_TICKS = (
    ((0, 3), "SA"),
    ((1, 2), "D1"),
    ((1, 3), "D0Q0"),
    ((2, 0), "U0U1"),
    ((2, 2), "D1Q0"),
    ((2, 3), ""),
    ((3, 0), "D0"),
    ((3, 1), "SA"),
    ((3, 2), "P0U0"),
    ((3, 3), "Q0SAD1U1Q1"),
    ((4, 1), "D0"),
    ((4, 2), "P0Q1"),
    ((4, 3), "U0Q0"),
    ((5, 3), "D1Q1SAQ2"),
)
PART_TICKS = ("D0U1P0", "Q2U0", "Q1Q0D1", "", "D0P0U1")
LAST_TICKS = (
    "U0Q1Q2Q0D1P0D0", "norm0", "Q1U1U0Q0Q2Q1D1P0", "norm1", "U1D1U0Q0D0Q1Q2SB", "D0P0SBU1U0Q0Q1U0",
    "P0Q2Q2Q0SBU1Q0P0", "Q1U1P0Q1",
)


def pieces(names):
    return [names[i : i + 2] for i in range(0, len(names), 2)]


def back_body(
    len_ref, qa_hbm, k_hbm, v_hbm, do_hbm, o_hbm, low_hbm, w_hbm, xf_hbm, gm_hbm, gain, lo_send, up_part_hbm,
    down_part_hbm, gp_own_hbm, gp_other_hbm, s_ub, s_db, s_g2, s_s2, s_pb,
    lo_got, down_out, up_out, gp_out, g0_out, g1_out, g2_out, ig, small_a, small_b,
    qa, k, v, do, o, low, wp, xf, gm, up_part, down_part, gp_src, gp_got,
    ka, va, kt, dk_acc, dv_acc, dqkv, gpair,
    down_box, down_part2, down_own, up_box, up_part2, up_own, gp_box, gp_part, gp_own, pair_box, pair_part, pair_own,
    down_sum, up_sum, gp_sum, pair_sum,
    gn_send, gn_got, gn_own, ig_own, ig_send, early, early_box, late_sums, late_box,
    load_sem, open_sem, nsend, nrecv, wsend, wrecv, *, bq, wide,
):
    n, me = lax.axis_index("narrow"), lax.axis_index("wide")
    peer = {"narrow": 1 - n}
    narrow, across = (nsend, nrecv), (wsend, wrecv)
    steps = bits(wide)
    heads, rows = qa.shape[0], qa.shape[1]
    pair_w = 2 * HEAD
    pairs = heads // 2
    d, lw = gain.shape[0], k.shape[1]
    cw = d // 2
    half, block = rows // 2, min(256, rows // 2)
    each = half // block
    count = iter(range(64))

    def load(src, dst):
        copy = pltpu.make_async_copy(src, dst, load_sem.at[next(count)])
        copy.start()
        return copy

    pair_loads = []
    for p in range(pairs):
        c = pl.ds(p * pair_w, pair_w)
        pair_loads.append(
            [load(a.at[:, c], b.at[:, c]) for a, b in ((k_hbm, k), (v_hbm, v), (do_hbm, do), (o_hbm, o))]
            + [load(qa_hbm.at[pl.ds(2 * p, 2)], qa.at[pl.ds(2 * p, 2)])]
        )
    part_load = load(down_part_hbm, down_part)
    up_load = load(up_part_hbm, up_part)
    gp_load = load(gp_own_hbm, gp_src)
    low_load = load(low_hbm, low)
    greet([peer] + wide_peers(me, wide))
    gp_swap = remote(gp_other_hbm, gp_got, narrow, 0, peer)
    layer = remote(lo_send, lo_got, narrow, 1, peer)
    gp_swap.start()
    late = [
        load(w_hbm.at[c, :, pl.ds(p * pair_w, pair_w)], wp.at[p, :, pl.ds(c * pair_w, pair_w)])
        for p in range(pairs)
        for c in range(3)
    ]
    own_half = block_rows(n * half, half)
    late += [load(xf_hbm.at[own_half], xf), load(gm_hbm, gm)]

    at = [0, 0]
    opening = iter(range(16))

    def group(src, box, part, own, dst, out, kinds=(0,), entries=(0,)):
        rows_, cols_ = dst.shape
        made = []
        for (kind, cols), entry in zip(lanes_split(cols_, kinds), entries):
            chain = Chain(me, order_of(wide, kind), rows_, cols, across, *at)
            at[:] = chain.send_next, chain.recv_next
            made.append(Group(chain.bind(src, box, part, own, dst, entry), entry, out=(out, open_sem.at[next(opening)])))
        return made

    groups = {}
    groups["D0"], groups["D1"] = group(down_part, down_box, down_part2, down_own, down_sum, down_out, DOWN_KINDS, DOWN_ENTRY)
    groups["U0"], groups["U1"] = group(up_part, up_box, up_part2, up_own, up_sum, up_out, UP_KINDS, UP_ENTRY)
    groups["P0"] = group(gp_src, gp_box, gp_part, gp_own, gp_sum, gp_out, kinds=(1,))[0]
    for p, out in zip(range(pairs), (g0_out, g1_out, g2_out)):
        groups[f"Q{p}"] = group(
            gpair.at[p], pair_box.at[p], pair_part.at[p], pair_own.at[p], pair_sum.at[p], out,
            kinds=(PAIR_KINDS[p],),
        )[0]

    dr, fr, lr = d // 128, s_ub.shape[1] // 128, lw // 128
    for i, (name, total, box, shared) in enumerate(
        (("SA", early, early_box, 4 * dr), ("SB", late_sums, late_box, -(-2 * dr // 8) * 8))
    ):
        one = Small(me, n, wide, total, box, shared, narrow, across, 2 + 2 * each + i, *at)
        at[:] = one.send_next, one.recv_next
        groups[name] = Group(one)

    def put_sum(ref, start, value):
        for i in range(value.shape[1] // 128):
            ref[start + i : start + i + 1, :] = value[:, i * 128 : (i + 1) * 128]

    early[...] = jnp.zeros_like(early)
    late_sums[...] = jnp.zeros_like(late_sums)
    for i, ref in enumerate((s_g2, s_s2, s_pb, s_db, s_ub)):
        put_sum(early, i * dr, ref[...])

    def tick(names):
        for name in pieces(names):
            with scope(name):
                groups[name].tick()

    part_load.wait()
    up_load.wait()
    tick(START_TICKS)

    kpos = lax.broadcasted_iota(jnp.int32, (rows, 1), 0)
    kbias = jnp.where(kpos < len_ref[0], 0.0, -1e30)
    tri = lax.broadcasted_iota(jnp.int32, (bq, bq), 0) <= lax.broadcasted_iota(jnp.int32, (bq, bq), 1)

    def plan(names):
        ticks = [groups[name].next() for name in pieces(names)]

        def run():
            for name, one in zip(pieces(names), ticks):
                with scope(name):
                    one()

        return run

    def start_proj():
        first = groups["P0"].next()

        def run():
            gp_swap.wait()
            gp_load.wait()
            gp_src[...] = gp_src[...] + gp_got[...]
            first()

        return run

    hooks = {}
    for at_, names in HEAD_TICKS:
        hooks[at_] = [plan(names)]
        if at_ == (2, 3):
            hooks[at_] += [layer.start, start_proj()]

    def run_hooks(head, block_):
        for (h, where), actions in hooks.items():
            if where == block_:

                @pl.when(head == h)
                def _():
                    for action in actions:
                        action()

    def one_head(head, carry):
        par, pair = head % 2, head // 2
        lane, mine, extra = lanes_of(par)
        cols = lane_part(pair, pair_w)
        for p in range(pairs):

            @pl.when(head == 2 * p)
            def _():
                for copy in pair_loads[p]:
                    copy.wait()

        ka[...] = place(lane, mine, extra, k[:, cols].astype(F32), [kbias, -1.0, -1.0, -1.0]).astype(BF16)
        va[...] = place(lane, mine, extra, v[:, cols].astype(F32), [-1.0, -1.0, -1.0]).astype(BF16)
        kt[...] = ka[...].T
        dk_acc[...] = jnp.zeros_like(dk_acc)
        dv_acc[...] = jnp.zeros_like(dv_acc)

        def put(c, r, new):
            lanes = pl.ds(c * pair_w, pair_w)
            old = dqkv[pair, r, lanes].astype(F32)
            dqkv[pair, r, lanes] = jnp.where(mine, new, jnp.where(par == 0, 0.0, old)).astype(BF16)

        for i in range(rows // bq):
            r = pl.ds(i * bq, bq)
            qb = qa[head, r, :]
            df = do[r, cols].astype(F32)
            delta = jnp.sum(jnp.where(mine, df * o[r, cols].astype(F32), 0.0), axis=1, keepdims=True)
            db = place(lane, mine, extra, df, three(delta)).astype(BF16)
            dqs = None
            chunks = [(0, i * bq), (i * bq, bq)] if i else [(0, bq)]
            for start, size in chunks:
                c = pl.ds(start, size)
                kb, vb = ka[c, :], va[c, :]
                s = dot_nt(kb, qb)
                if start == i * bq:
                    s = jnp.where(tri, s, -1e30)
                p = jnp.exp(s)
                ds = (p * dot_nt(vb, db)).astype(BF16)
                dv_acc[c, :] += dot(p.astype(BF16), db)
                dk_acc[c, :] += dot(ds, qb)
                part = dot(kt[:, c], ds)
                dqs = part if dqs is None else dqs + part
            put(0, r, dqs.T * HEAD**-0.5)
            if i < rows // bq - 1:
                run_hooks(head, i)
        put(1, pl.ds(0, rows), dk_acc[...])
        put(2, pl.ds(0, rows), dv_acc[...])

        @pl.when(head == 1)
        def _():
            low_load.wait()

        @pl.when(par == 1)
        def _():
            with scope("weights"):
                gpair[pair] = dot_tn(low[...], dqkv[pair]).astype(BF16)

        run_hooks(head, rows // bq - 1)
        return carry

    lax.fori_loop(0, heads, one_head, 0)

    for copy in late:
        copy.wait()

    def gn_part(start):
        r = block_rows(start, block)
        total = dot_nt(dqkv[0, r, :], wp[0])
        for p in range(1, pairs):
            total += dot_nt(dqkv[p, r, :], wp[p])
        return total

    def gn_copy(j):
        r = pl.ds(j * block, block)
        return remote(gn_send.at[r], gn_got.at[r], narrow, 2 + j, peer)

    for j in range(each):
        with scope("gn_peer"):
            gn_send[j * block : (j + 1) * block, :] = gn_part((1 - n) * half + j * block).astype(BF16)
        gn_copy(j).start()
        tick(PART_TICKS[j % 2])
    for j in range(each):
        with scope("gn_own"):
            gn_own[j * block : (j + 1) * block, :] = gn_part(n * half + j * block)
        tick(PART_TICKS[2 + j % 2])

    shared = -(-2 * dr // 8) * 8
    for p in range(pairs):
        put_sum(late_sums, shared + p, jnp.sum(dqkv[p, :, 0:pair_w].astype(F32), axis=0, keepdims=True))
        put_sum(late_sums, shared + lr + p, jnp.sum(dqkv[p, :, 2 * pair_w :].astype(F32), axis=0, keepdims=True))
    tick(PART_TICKS[4])

    mine, other = lane_part(n, cw), lane_part(1 - n, cw)

    def ig_copy(j):
        r = block_rows(n * half + j * block, block)
        return remote(ig_send.at[pl.ds(j * block, block)], ig.at[r], narrow, 2 + each + j, peer)

    def in_norm(j):
        with scope("gn_wait"):
            gn_copy(j).wait()
        rh = pl.ds(j * block, block)
        r = block_rows(n * half + j * block, block)
        g = gn_own[rh, :] + gn_got[rh, :].astype(F32)
        xhat, scale = norm_rows(xf[rh, :].astype(F32))
        gg = g * vec(gain)
        m1 = jnp.mean(gg, axis=-1, keepdims=True)
        m2 = jnp.mean(gg * xhat, axis=-1, keepdims=True)
        ig_own[...] = gm[rh, :] + scale * (gg - m1 - xhat * m2)
        ig_send[rh, :] = ig_own[:, other].astype(BF16)
        ig_copy(j).start()
        ig[r, :] = ig_own[:, mine].astype(BF16)
        return jnp.sum(g * xhat, axis=0, keepdims=True), jnp.sum(g, axis=0, keepdims=True)

    sums1 = []
    for names in LAST_TICKS:
        if names in ("norm0", "norm1"):
            todo = range(each - 1) if names == "norm0" else range(each - 1, each)
            sums1 += [in_norm(j) for j in todo]
            if names == "norm1":
                put_sum(late_sums, 0, sum(a for a, _ in sums1))
                put_sum(late_sums, dr, sum(b for _, b in sums1))
                tick("SB")
        else:
            tick(names)
    while not all(g.done for g in groups.values()):
        for name in groups:
            tick(name)
    small_a[...] = early[...]
    small_b[...] = late_sums[...]
    with scope("end"):
        for one in groups.values():
            if one.out is not None:
                one.store().wait()
        layer.wait()
        for j in range(each):
            ig_copy(j).wait()


def back_call(
    length, qa, k, v, do, o, low, w, xf, gm, gain, lo_send, up_part, down_part, gp_own, gp_other,
    s_ub, s_db, s_g2, s_s2, s_pb, wide, bq=256,
):
    heads, rows, pair = qa.shape
    d, f, lw = gain.shape[0], up_part.shape[1], k.shape[1]
    cw, half = d // 2, rows // 2
    block = min(256, half)
    each, steps, pairs = half // block, bits(wide), heads // 2
    sd, vm = jax.ShapeDtypeStruct, pltpu.VMEM
    shape = lambda r, kind=0: Chain(0, order_of(wide, kind), r, None, None, 0, 0)
    c_down, c_up, c_gp = shape(f), shape(d), shape(2 * lw)
    down_rows, up_rows, pair_rows = (max(shape(r, k).box_rows for k in range(4)) for r in (f, d, d))
    small = lambda shared, rest: -(-(shared + rest) // 8) * 8
    rows_a = small(4 * d // 128, f // 128)
    rows_b = small(-(-2 * d // 1024) * 8, 2 * lw // 128)
    slots = CHIPS + 1 + max(0, bits(wide) - 4)
    semaphores = (len(DOWN_KINDS) + len(UP_KINDS) + 1 + pairs) * shape(d).recv_next + 2 * (bits(wide) + CHIPS)
    work = 2 * heads * rows * rows * HEAD
    return pl.pallas_call(
        functools.partial(back_body, bq=bq, wide=wide),
        out_shape=(sd((rows, cw), BF16), sd((f, d), BF16), sd((d, f), BF16), sd((2 * lw, cw), BF16))
        + (sd((d, 3 * pair), BF16),) * 3
        + (sd((rows, cw), BF16), sd((rows_a, 128), F32), sd((rows_b, 128), F32)),
        in_specs=[pl.BlockSpec(memory_space=pltpu.SMEM)] + [anywhere()] * 9 + [vmem()] + [anywhere()] * 5 + [vmem()] * 5,
        out_specs=(anywhere(),) * 7 + (vmem(), vmem(), vmem()),
        scratch_shapes=[
            vm(qa.shape, BF16), vm((rows, lw), BF16), vm((rows, lw), BF16), vm((rows, lw), BF16), vm((rows, lw), BF16),
            vm((rows, d), BF16), vm((pairs, d, 3 * pair), BF16), vm((half, d), BF16), vm((half, d), F32),
            vm((d // 2, f), BF16), vm((f // 2, d), BF16), vm((2 * lw, cw), BF16), vm((2 * lw, cw), BF16),
            vm((rows, pair), BF16), vm((rows, pair), BF16), vm((pair, rows), BF16), vm((rows, pair), F32), vm((rows, pair), F32),
            vm((pairs, rows, 3 * pair), BF16), vm((pairs, d, 3 * pair), BF16),
            vm((down_rows, d), BF16), vm((f // 2, d), BF16), vm((c_down.size, d), BF16),
            vm((up_rows, f), BF16), vm((d // 2, f), BF16), vm((c_up.size, f), BF16),
            vm((pair_rows, cw), BF16), vm((lw, cw), BF16), vm((c_gp.size, cw), BF16),
            vm((pairs, pair_rows, 3 * pair), BF16), vm((pairs, d // 2, 3 * pair), BF16),
            vm((pairs, c_up.size, 3 * pair), BF16),
            vm((f, d), BF16), vm((d, f), BF16), vm((2 * lw, cw), BF16), vm((pairs, d, 3 * pair), BF16),
            vm((half, d), BF16), vm((half, d), BF16), vm((half, d), F32), vm((block, d), F32), vm((half, cw), BF16),
            vm((rows_a, 128), F32), vm((slots, rows_a, 128), F32), vm((rows_b, 128), F32), vm((slots, rows_b, 128), F32),
        ]
        + sems(8 * pairs + 8, 8, 4 + 2 * each, 4 + 2 * each, 17 + 3 * CHIPS, semaphores),
        compiler_params=params(collective_id=4, has_side_effects=True),
        cost_estimate=cost(10 * work + 4 * rows * d * 3 * lw, 2 * rows * d * 20, work // 256),
        name="back",
    )(
        length, qa, k, v, do, o, low, w, xf, gm, gain, lo_send, up_part, down_part, gp_own, gp_other,
        s_ub, s_db, s_g2, s_s2, s_pb,
    )


def finish_body(
    lo, lo_got, bias, ig, up, down, q, k, v, p0, p1, small_a, small_b,
    out, ig_out, o_qkv, o_qvb, o_proj, o_pb, o_up, o_ub, o_down, o_db, o_g1, o_s1, o_g2, o_s2,
    *, factor,
):
    n = lax.axis_index("narrow")
    cw = lo.shape[1]
    b = vec(bias)
    out[...] = (lo[...] + lo_got[...].astype(F32) + jnp.where(n == 0, b[:, :cw], b[:, cw:])).astype(BF16)
    ig_out[...] = ig[...]
    for p, ref in enumerate((q, k, v)):
        for c in range(3):
            lanes = slice(c * 128, (c + 1) * 128)
            o_qkv[c, :, p * 128 : (p + 1) * 128] = ref[:, lanes].astype(F32) * factor
    o_proj[:, :cw] = p0[...].astype(F32) * factor
    o_proj[:, cw:] = p1[...].astype(F32) * factor
    o_up[...] = up[...].astype(F32) * factor
    o_down[...] = down[...].astype(F32) * factor

    @pl.when(pl.program_id(0) == 0)
    def _():
        dr, fr = o_g1.shape[0], o_ub.shape[0]
        for i, ref in enumerate((o_g2, o_s2, o_pb, o_db)):
            ref[...] = small_a[i * dr : (i + 1) * dr, :] * factor
        o_ub[...] = small_a[4 * dr : 4 * dr + fr, :] * factor
        o_g1[...] = small_b[0:dr, :] * factor
        o_s1[...] = small_b[dr : 2 * dr, :] * factor
        lr, shared = o_qvb.shape[1] // 128, -(-2 * dr // 8) * 8
        for c in range(2):
            for i in range(lr):
                at = shared + c * lr + i
                o_qvb[c : c + 1, i * 128 : (i + 1) * 128] = small_b[at : at + 1, :] * factor


def finish_call(lo, lo_got, bias, ig, up, down, q, k, v, p, small_a, small_b, factor, grid=8):
    rows, cw = lo.shape
    (d, f), lw = up.shape, q.shape[1]
    dr, sd = d // 128, jax.ShapeDtypeStruct
    shapes = (
        [sd((rows, cw), BF16), sd((rows, cw), BF16), sd((3, d, lw), F32), sd((2, lw), F32), sd((lw, d), F32)]
        + [sd((dr, 128), F32), sd((d, f), F32), sd((f // 128, 128), F32), sd((f, d), F32)]
        + [sd((dr, 128), F32)] * 5
    )
    big = lambda a: rows_spec(a.shape[0] // grid, a.shape[1])
    pb = lw // grid
    specs = []
    for i, s in enumerate(shapes):
        if len(s.shape) == 3:
            specs.append(pl.BlockSpec((3, d // grid, lw), lambda i, *_: (0, i, 0)))
        elif i in (0, 1, 4, 6, 8):
            specs.append(big(s))
        else:
            specs.append(whole_spec(s.shape))
    return pl.pallas_call(
        functools.partial(finish_body, factor=factor),
        out_shape=tuple(shapes),
        grid=(grid,),
        in_specs=[big(lo), big(lo_got), whole_spec(bias.shape), big(ig), big(up), big(down), big(q), big(k), big(v)]
        + [rows_spec(pb, cw), rows_spec(pb, cw, grid), whole_spec(small_a.shape), whole_spec(small_b.shape)],
        out_specs=tuple(specs),
        compiler_params=params(),
        cost_estimate=cost(up.size * 8, up.size * 24),
        name="finish",
    )(lo, lo_got, bias, ig, up, down, q, k, v, p, p, small_a, small_b)


def on_device(
    tokens, lengths, qkv_weight, qv_bias, proj_weight, proj_bias, up_weight, up_bias,
    down_weight, down_bias, first_gain, first_shift, second_gain, second_shift, cotangent,
):
    cw = tokens.shape[1]
    d, ff, lw = 2 * cw, up_weight.shape[1], proj_weight.shape[0]
    wide = lax.axis_size("wide")
    w3 = jnp.transpose(qkv_weight, (1, 0, 2))

    xf, low, k, v, mixed, qa, mixed_got, proj_got, cot_head = front_call(
        lengths, tokens, w3, qv_bias, first_gain, first_shift, proj_weight, cotangent
    )
    lo, lo_send, gmix, gm, up_part, down_part, gp_own, gp_other, s_ub, s_db, s_g2, s_s2, s_pb = mlp_call(
        lengths, xf, mixed, mixed_got, proj_weight, proj_got, proj_bias, second_gain, second_shift,
        up_weight, up_bias, down_weight, cotangent, cot_head, wide,
    )
    lo_got, gdown, gup, gp, g0, g1, g2, ig, small_a, small_b = back_call(
        lengths, qa, k, v, gmix, mixed, low, w3, xf, gm, first_gain, lo_send, up_part, down_part, gp_own, gp_other,
        s_ub, s_db, s_g2, s_s2, s_pb, wide,
    )
    out, ig, o_qkv, o_qvb, o_proj, *rest = finish_call(
        lo, lo_got, down_bias, ig, gup, gdown, g0, g1, g2, gp, small_a, small_b,
        1.0 / (lengths.shape[0] * wide),
    )
    pb, up, ubs, down, dbs, g1, s1, g2, s2 = rest
    flat = lambda a: a.reshape(-1)
    return (
        out, ig, jnp.transpose(o_qkv, (1, 0, 2)), o_qvb, o_proj, flat(pb), up, flat(ubs), down, flat(dbs),
        flat(g1), flat(s1), flat(g2), flat(s2),
    )


def solution(mesh):
    split = P("wide", "narrow")
    none3, cols, rows1 = P(None, None, "narrow"), P(None, "narrow"), P("narrow", None)
    return jax.shard_map(
        on_device,
        mesh=mesh,
        in_specs=(
            split, P("wide"), none3, cols, rows1, P(), cols, P("narrow"), rows1, P(), P(), P(), P(), P(), split,
        ),
        out_specs=(
            split, split, none3, cols, rows1, P(), cols, P("narrow"), rows1, P(), P(), P(), P(), P(),
        ),
        check_vma=False,
    )
```

```python
import functools

import jax
import jax.numpy as jnp
from jax import lax
from jax.experimental import pallas as pl
from jax.experimental.pallas import tpu as pltpu
from jax.sharding import PartitionSpec as P

EPS = 1e-05
HEAD = 64
F32, BF16 = jnp.float32, jnp.bfloat16
NT = (((1,), (1,)), ((), ()))
TN = (((0,), (0,)), ((), ()))
GELU_A, GELU_B = 0.7978845608028654, 0.044715
VMEM_LIMIT = 63 * 1024 * 1024


def dot(a, b):
    return jnp.dot(a, b, preferred_element_type=F32)


def dot_nt(a, b):
    return lax.dot_general(a, b, NT, preferred_element_type=F32)


def dot_tn(a, b):
    return lax.dot_general(a, b, TN, preferred_element_type=F32)


def params(**more):
    return pltpu.CompilerParams(vmem_limit_bytes=VMEM_LIMIT, **more)


def cost(flops, size, trans=0):
    return pl.CostEstimate(flops=int(flops), bytes_accessed=int(size), transcendentals=int(trans))


def lane_part(which, width):
    return pl.ds(pl.multiple_of(which * width, 128), width)


def norm_rows(x):
    mean = jnp.mean(x, axis=-1, keepdims=True)
    cen = x - mean
    var = jnp.mean(cen * cen, axis=-1, keepdims=True)
    r = lax.rsqrt(var + EPS)
    return cen * r, r


def rows_spec(rows, cols, base=0):
    return pl.BlockSpec((rows, cols), lambda i, *_: (i + base, 0))


def whole_spec(shape):
    zeros = (0,) * len(shape)
    return pl.BlockSpec(shape, lambda i, *_: zeros)


MESH = pl.DeviceIdType.MESH
scope = jax.named_scope


def vec(ref):
    return ref[...].astype(F32).reshape(1, -1)


def bit_of(index, bit):
    return (index // (1 << bit)) % 2


def flip(index, bit):
    return index + (1 - 2 * bit_of(index, bit)) * (1 << bit)


def greet(peers):
    barrier = pltpu.get_barrier_semaphore()
    for peer in peers:
        pl.semaphore_signal(barrier, inc=1, device_id=peer, device_id_type=MESH)
    pl.semaphore_wait(barrier, len(peers))


def remote(src, dst, sems, at, peer, send_at=None):
    return pltpu.make_async_remote_copy(
        src_ref=src, dst_ref=dst, send_sem=sems[0].at[at if send_at is None else send_at], recv_sem=sems[1].at[at],
        device_id=peer, device_id_type=MESH,
    )


def block_rows(start, size, unit=16):
    return pl.ds(start if isinstance(start, int) else pl.multiple_of(start, unit), size)


LINE, CHIPS = 4, 8


def when(cond, action):
    @pl.when(cond)
    def _():
        action()


def line_peer(me, by):
    q = (me // 4) % LINE
    return me + ((q + by) % LINE - q) * 4


class Chain:
    def __init__(self, me, order, rows, cols, sems, send_at, recv_at):
        self.me, self.cols, self.sems, self.send_at = me, cols, sems, send_at
        self.phases, self.ops, back = [], [], []
        base, size, box = 0, rows, 0
        for kind, bit in order:
            if kind == "line" and size % (16 * LINE):
                raise ValueError(rows)
            if kind == "all":
                ways = CHIPS >> (bit - 1)
                part = size // ways
                keep, give, boxes = base + (me // (1 << bit)) % ways * part, None, (ways - 1) * part
                self.ops.append(("send", len(self.phases), ways))
                back = [("share", len(self.phases), ways)] + back
            elif kind == "line":
                part = size // LINE
                keep, give, boxes = base + (me // 4) % LINE * part, None, 2 * (LINE - 1) * part
                self.ops += [("line", len(self.phases), i) for i in range(1, LINE)]
                back = [("spread", len(self.phases), i) for i in range(1, LINE)] + back
            elif size % 32 == 0:
                part = size // 2
                mine = bit_of(me, bit)
                keep, give, boxes = base + mine * part, base + (1 - mine) * part, part
                self.ops.append(("pair", len(self.phases), 0))
                back = [("join", len(self.phases), 0)] + back
            else:
                part, keep, give, boxes = size, base, base, size
                self.ops.append(("pair", len(self.phases), 0))
            self.phases.append((bit, base, keep, give, part, box))
            base, size, box = keep, part, box + boxes
        self.scatters = len(self.ops)
        self.ops += back
        self.base, self.size, self.box_rows = base, size, box
        self.recv_at, widest = [], 1
        for kind, _, i in self.ops:
            width = {"line": 2, "spread": 2, "send": i - 1, "share": i - 1}.get(kind, 1)
            self.recv_at.append(recv_at)
            recv_at, widest = recv_at + width, max(widest, width)
        self.recv_next, self.send_next = recv_at, send_at + widest

    def bind(self, src, box, part, own, dst=None, entry=0):
        self.src, self.box, self.part, self.own, self.dst = src, box, part, own, dst
        self.entry = self.ops[entry][1]
        return self

    def _source(self, phase):
        off = 0 if phase == 0 else self.phases[0][2]
        return (self.src if phase == self.entry else self.part), off

    def _target(self, phase):
        if phase == len(self.phases) - 1:
            return self.own, self.phases[phase][2]
        return self.part, self.phases[0][2]

    def _remote(self, op, lane, src, dst, to):
        return remote(src, dst, self.sems, self.recv_at[op] + lane, {"wide": to}, self.send_at + lane)

    def _add(self, rows, target, first, *terms):
        unit = next(u for u in (96, 64, 48, 32, 16) if rows % u == 0)

        def add(i, carry):
            total = None
            for ref, start in terms:
                value = ref[block_rows(start + i * unit, unit), self.cols]
                value = value.astype(F32) if len(terms) > 2 else value
                total = value if total is None else total + value
            target[block_rows(first + i * unit, unit), self.cols] = total.astype(BF16)
            return carry

        lax.fori_loop(0, rows // unit, add, 0)


    def _pair(self, op, phase):
        bit, _, _, give, rows, box = self.phases[phase]
        source, off = self._source(phase)
        src = source.at[block_rows(give - off, rows), self.cols]
        return self._remote(op, 0, src, self.box.at[pl.ds(box, rows), self.cols], flip(self.me, bit))

    def _join(self, op, phase):
        bit, _, keep, _, rows, _ = self.phases[phase]
        region = self.dst.at[block_rows(keep, rows), self.cols]
        return self._remote(op, 0, region, region, flip(self.me, bit))


    def _others(self, bit, ways):
        for m in range(1, ways):
            yield m - 1, flip_all(self.me, bit, m)

    def _sends(self, op, phase, ways):
        bit, base, _, _, rows, box = self.phases[phase]
        source, off = self._source(phase)
        for m, to in self._others(bit, ways):
            src = source.at[block_rows(base - off + (to // (1 << bit)) % ways * rows, rows), self.cols]
            yield self._remote(op, m, src, self.box.at[pl.ds(box + m * rows, rows), self.cols], to)

    def _shares(self, op, phase, ways, came):
        bit, base, keep, _, rows, _ = self.phases[phase]
        for m, to in self._others(bit, ways):
            at = base + (to // (1 << bit)) % ways * rows if came else keep
            region = self.dst.at[block_rows(at, rows), self.cols]
            yield self._remote(op, m, region, region, to)


    def _slot(self, phase, lane, i):
        rows, box = self.phases[phase][4:]
        return box + (lane * (LINE - 1) + i - 1) * rows

    def _line_sends(self, op, phase, i):
        q = (self.me // 4) % LINE
        _, base, _, _, rows, _ = self.phases[phase]
        source, off = self._source(phase)
        sends = []
        for lane, by in ((0, 1), (1, -1)):
            place_ = q if lane == 0 else LINE - 1 - q
            chunk = LINE - i if lane == 0 else i - 1
            dst = self.box.at[pl.ds(self._slot(phase, lane, i), rows), self.cols]
            to = line_peer(self.me, by)
            src = source.at[block_rows(base - off + chunk * rows, rows), self.cols]
            sends.append((place_ == 0, functools.partial(self._remote, op, lane, src, dst, to)))
            if i > 1:
                src = self.box.at[pl.ds(self._slot(phase, lane, i - 1), rows), self.cols]
                moving = jnp.logical_and(place_ >= 1, place_ <= min(i - 1, LINE - 2))
                sends.append((moving, functools.partial(self._remote, op, lane, src, dst, to)))
        return sends

    def _line_end(self, op, phase, i):
        q = (self.me // 4) % LINE
        _, base, keep, _, rows, _ = self.phases[phase]
        source, off = self._source(phase)
        for cond, copy in self._line_sends(op, phase, i):
            when(cond, lambda: copy().wait_send())
        for lane, by in ((0, -1), (1, 1)):
            place_ = q if lane == 0 else LINE - 1 - q
            slot = self._slot(phase, lane, i)
            dst = self.box.at[pl.ds(slot, rows), self.cols]
            arrived = jnp.logical_and(place_ >= 1, place_ <= i)
            chunk = LINE - 1 - i + q if lane == 0 else i + q - (LINE - 1)

            @pl.when(arrived)
            def _():
                self._remote(op, lane, dst, dst, line_peer(self.me, by)).wait_recv()
                if i < LINE - 1:
                    self._add(rows, self.box, slot, (self.box, slot), (source, base - off + chunk * rows))

        if i == LINE - 1:
            target, out = self._target(phase)
            own = (source, keep - off)
            left, right = (self.box, self._slot(phase, 0, i)), (self.box, self._slot(phase, 1, i))

            @pl.when(q == 0)
            def _():
                self._add(rows, target, keep - out, own, right)

            @pl.when(q == LINE - 1)
            def _():
                self._add(rows, target, keep - out, own, left)

            @pl.when(jnp.logical_and(q > 0, q < LINE - 1))
            def _():
                self._add(rows, target, keep - out, left, own, right)

    def _spread(self, op, phase, i):
        q = (self.me // 4) % LINE
        _, base, _, _, rows, _ = self.phases[phase]
        ways = []
        for lane, by in ((0, 1), (1, -1)):
            place_ = q if lane == 0 else LINE - 1 - q
            sent = self.dst.at[block_rows(base + (q - by * (i - 1)) * rows, rows), self.cols]
            came = self.dst.at[block_rows(base + (q - by * i) * rows, rows), self.cols]
            send_if = jnp.logical_and(place_ >= i - 1, place_ <= LINE - 2)
            ways.append(
                (
                    send_if, functools.partial(self._remote, op, lane, sent, sent, line_peer(self.me, by)),
                    place_ >= i, functools.partial(self._remote, op, lane, came, came, line_peer(self.me, -by)),
                )
            )
        return ways

    def start(self, op):
        kind, phase, i = self.ops[op]
        if kind == "pair":
            self._pair(op, phase).start()
        elif kind == "join":
            self._join(op, phase).start()
        elif kind == "send":
            for copy in self._sends(op, phase, i):
                copy.start()
        elif kind == "share":
            for copy in self._shares(op, phase, i, False):
                copy.start()
        elif kind == "line":
            for cond, copy in self._line_sends(op, phase, i):
                when(cond, lambda: copy().start())
        else:
            for cond, copy, _, _ in self._spread(op, phase, i):
                when(cond, lambda: copy().start())

    def end(self, op):
        kind, phase, i = self.ops[op]
        if kind == "pair":
            self._pair(op, phase).wait()
            _, _, keep, _, rows, box = self.phases[phase]
            source, off = self._source(phase)
            target, out = self._target(phase)
            self._add(rows, target, keep - out, (self.box, box), (source, keep - off))
        elif kind == "join":
            self._join(op, phase).wait()
        elif kind == "send":
            for copy in self._sends(op, phase, i):
                copy.wait()
            _, _, keep, _, rows, box = self.phases[phase]
            source, off = self._source(phase)
            target, out = self._target(phase)
            terms = [(self.box, box + m * rows) for m in range(i - 1)]
            self._add(rows, target, keep - out, (source, keep - off), *terms)
        elif kind == "share":
            for copy in self._shares(op, phase, i, False):
                copy.wait_send()
            for copy in self._shares(op, phase, i, True):
                copy.wait_recv()
        elif kind == "line":
            self._line_end(op, phase, i)
        else:
            for send_if, send, recv_if, recv in self._spread(op, phase, i):
                when(send_if, lambda: send().wait_send())
                when(recv_if, lambda: recv().wait_recv())

    def gather_open(self):
        self._add(self.size, self.dst, self.base, (self.own, 0))


class Group:
    def __init__(self, chain, entry=0, leave=None, out=None):
        self.chain, self.out = chain, out
        self.ops = list(range(entry, len(chain.ops) if leave is None else leave))
        self.pos = -1

    @property
    def done(self):
        return self.pos >= len(self.ops)

    def next(self):
        pos = self.pos
        self.pos = min(pos + 1, len(self.ops))

        def tick():
            if pos >= len(self.ops):
                return
            if pos >= 0:
                self.chain.end(self.ops[pos])
            if pos + 1 >= len(self.ops):
                if self.out is not None:
                    self.store().start()
                return
            if self.ops[pos + 1] == self.chain.scatters:
                self.chain.gather_open()
            self.chain.start(self.ops[pos + 1])

        return tick

    def tick(self):
        self.next()()

    def store(self):
        out, sem = self.out
        return pltpu.make_async_copy(self.chain.dst.at[:, self.chain.cols], out.at[:, self.chain.cols], sem)


def bits(wide):
    return wide.bit_length() - 1


def order_of(wide, kind):
    first, rest = ("pair", 0), [("pair", b) for b in range(4, bits(wide))]
    pair, line = ("pair", 1), ("line", 2)
    return {
        0: [first, pair, line, *rest], 1: [first, line, pair, *rest], 2: [first, ("all", 1), *rest],
        3: [first, pair, ("all", 2), *rest],
    }[kind]


def lanes_split(cols, kinds):
    w = cols // len(kinds)
    return [(kind, pl.ds(i * w, w)) for i, kind in enumerate(kinds)]


def flip_all(me, bit, mask):
    to = me
    for i in range(3):
        if mask >> i & 1:
            to = to + (flip(me, bit + i) - me)
    return to


def chip_peers(me):
    return [flip_all(me, 1, m) for m in range(1, CHIPS)]


def wide_peers(me, wide):
    pairs = [flip(me, b) for b in range(bits(wide)) if b not in (1, 2, 3)]
    return [{"wide": peer} for peer in pairs + chip_peers(me)]


class Small:
    def __init__(self, me, n, wide, total, box, shared, narrow, across, narrow_at, send_at, recv_at):
        self.me, self.n, self.total, self.box, self.shared = me, n, total, box, shared
        self.narrow, self.across = narrow, across
        self.narrow_at, self.send_at, self.recv_at = narrow_at, send_at, recv_at
        self.ops = ["narrow", 0, "chips"] + list(range(4, bits(wide)))
        self.scatters, self.dst = None, None
        self.send_next = send_at + CHIPS - 1
        self.recv_next = recv_at + len(self.ops) + CHIPS - 1

    def _copies(self, op):
        kind = self.ops[op]
        if kind == "narrow":
            top = pl.ds(0, self.shared)
            return [remote(self.total.at[top], self.box.at[0, top], self.narrow, self.narrow_at, {"narrow": 1 - self.n})]
        if kind == "chips":
            return [
                remote(
                    self.total, self.box.at[2 + i], self.across, self.recv_at + len(self.ops) + i, {"wide": to},
                    self.send_at + i,
                )
                for i, to in enumerate(chip_peers(self.me))
            ]
        slot = 1 if kind == 0 else CHIPS + 1 + kind - 4
        peer = {"wide": flip(self.me, kind)}
        return [remote(self.total, self.box.at[slot], self.across, self.recv_at + op, peer, self.send_at)]

    def start(self, op):
        for copy in self._copies(op):
            copy.start()

    def end(self, op):
        for copy in self._copies(op):
            copy.wait()
        kind = self.ops[op]
        if kind == "narrow":
            self.total[0 : self.shared, :] += self.box[0, 0 : self.shared, :]
        elif kind == "chips":
            self.total[...] += sum(self.box[2 + i] for i in range(CHIPS - 1))
        else:
            self.total[...] += self.box[1 if kind == 0 else CHIPS + 1 + kind - 4]


def vmem():
    return pl.BlockSpec(memory_space=pltpu.VMEM)


def anywhere():
    return pl.BlockSpec(memory_space=pl.ANY)


def sems(*counts):
    return [pltpu.SemaphoreType.DMA((c,)) for c in counts]


def three(x):
    hi = x.astype(BF16).astype(F32)
    mid = (x - hi).astype(BF16).astype(F32)
    return hi, mid, x - hi - mid


def lanes_of(par):
    lane = lax.broadcasted_iota(jnp.int32, (1, 2 * HEAD), 1)
    mine = (lane // HEAD) == par
    return lane, mine, (1 - par) * HEAD


def place(lane, mine, at, base, terms):
    out = jnp.where(mine, base, 0.0)
    for i, term in enumerate(terms):
        out = jnp.where(lane == at + i, term, out)
    return out


def front_body(
    len_ref, tokens, w_hbm, bias, gain, shift, pw, cot,
    xf_out, low_out, k_out, v_out, o_out, qa_out, o_got, pw_got, cot_head,
    own, got, w, xf, low, q, k, v, o, qa, ka, va, load_sem, store_sem, send_sem, recv_sem, *, bq,
):
    n, me = lax.axis_index("narrow"), lax.axis_index("wide")
    peer, core = {"narrow": 1 - n}, {"wide": flip(me, 0)}
    both = (send_sem, recv_sem)
    rows, cw = own.shape
    pair_w, heads = 2 * HEAD, qa.shape[0]
    blocks = rows // bq
    loads = [pltpu.make_async_copy(a, b, load_sem.at[i]) for i, (a, b) in enumerate(((tokens, own), (w_hbm, w)))]
    for load in loads:
        load.start()
    greet([peer, core] + [{"wide": to} for to in chip_peers(me)])

    def token_copy(i):
        r = block_rows(i * bq, bq)
        return remote(tokens.at[r], got.at[r], both, i, peer)

    for i in range(blocks):
        token_copy(i).start()
    used = blocks + blocks * (heads // 2)
    slab, mine_lanes = pw.shape[0] // CHIPS, lane_part(me % 2, pw.shape[1] // 2)

    def slab_of(device):
        return pw_got.at[block_rows((device // 2) % CHIPS * slab, slab), mine_lanes]

    source = pw.at[block_rows((me // 2) % CHIPS * slab, slab), mine_lanes]
    weights = remote(source, slab_of(me), both, used, peer)
    core_share = remote(pw_got.at[:, mine_lanes], pw_got.at[:, mine_lanes], both, used + 1, core)
    head_copy = remote(cot.at[block_rows(n * (rows // 2), bq)], cot_head, both, used + 2, peer)

    def chip_shares(came):
        return [
            remote(slab_of(to if came else me), slab_of(to if came else me), both, used + 3 + i, {"wide": to})
            for i, to in enumerate(chip_peers(me))
        ]

    weights.start()
    head_copy.start()
    for load in loads:
        load.wait()

    def project(i, carry):
        r = block_rows(i * bq, bq)
        xf[r, lane_part(n, cw)] = own[r, :]
        with scope("wait"):
            token_copy(i).wait()
        xf[r, lane_part(1 - n, cw)] = got[r, :]
        xhat, _ = norm_rows(xf[r, :].astype(F32))
        y = (xhat * vec(gain) + vec(shift)).astype(BF16)
        low[r, :] = y
        q[r, :] = (dot(y, w[0]) + bias[0:1, :].astype(F32)).astype(BF16) * jnp.asarray(HEAD**-0.5, BF16)
        k[r, :] = dot(y, w[1]).astype(BF16)
        v[r, :] = (dot(y, w[2]) + bias[1:2, :].astype(F32)).astype(BF16)
        return carry

    lax.fori_loop(0, blocks, project, 0)
    stores = [
        pltpu.make_async_copy(a, b, store_sem.at[i])
        for i, (a, b) in enumerate(((xf, xf_out), (low, low_out), (k, k_out), (v, v_out)))
    ]
    for store in stores:
        store.start()

    kpos = lax.broadcasted_iota(jnp.int32, (rows, 1), 0)
    kbias = jnp.where(kpos < len_ref[0], 0.0, -1e30)
    tri = lax.broadcasted_iota(jnp.int32, (bq, bq), 1) <= lax.broadcasted_iota(jnp.int32, (bq, bq), 0)

    def mixed(pair, i):
        r, c = pl.ds(i * bq, bq), lane_part(pair, pair_w)
        return remote(o.at[r, c], o_got.at[r, c], both, blocks + pair * blocks + i, peer)

    def mixed_store(pair):
        c = lane_part(pair, pair_w)
        return pltpu.make_async_copy(o.at[:, c], o_out.at[:, c], store_sem.at[4 + pair])

    def qa_store(head):
        return pltpu.make_async_copy(qa.at[head], qa_out.at[head], store_sem.at[4 + heads // 2 + head])

    def one_head(head, carry):
        par, pair = head % 2, head // 2
        lane, mine, at = lanes_of(par)
        cols = lane_part(pair, pair_w)
        ka[...] = place(lane, mine, at, k[:, cols].astype(F32), [kbias]).astype(BF16)
        va[...] = place(lane, mine, at, v[:, cols].astype(F32), [1.0]).astype(BF16)
        for i in range(blocks):
            nk = (i + 1) * bq
            r = pl.ds(i * bq, bq)
            qf = q[r, cols].astype(F32)
            s = dot_nt(place(lane, mine, at, qf, [1.0]).astype(BF16), ka[0:nk, :])
            edge = jnp.where(tri, s[:, nk - bq :], -1e30)
            m = jnp.max(edge, axis=1, keepdims=True)
            if nk > bq:
                m = jnp.maximum(m, jnp.max(s[:, : nk - bq], axis=1, keepdims=True))
            pv = dot(jnp.exp(edge - m).astype(BF16), va[nk - bq : nk, :])
            if nk > bq:
                pv += dot(jnp.exp(s[:, : nk - bq] - m).astype(BF16), va[0 : nk - bq, :])
            total = jnp.sum(jnp.where(lane == at, pv, 0.0), axis=1, keepdims=True)
            out = (pv / total).astype(BF16).astype(F32)
            old = o[r, cols].astype(F32)
            o[r, cols] = jnp.where(mine, out, jnp.where(par == 0, 0.0, old)).astype(BF16)
            lse = m + jnp.log(total)
            qa[head, r, :] = place(lane, mine, at, qf, [1.0, *three(lse)]).astype(BF16)
            when(par == 1, lambda: mixed(pair, i).start())
        when(par == 1, lambda: mixed_store(pair).start())
        qa_store(head).start()

        @pl.when(head == 0)
        def _():
            weights.wait()
            for share in chip_shares(False):
                share.start()

        @pl.when(head == 3)
        def _():
            for share in chip_shares(False):
                share.wait_send()
            for share in chip_shares(True):
                share.wait_recv()
            core_share.start()

        return carry

    with scope("heads"):
        lax.fori_loop(0, heads, one_head, 0)
    for store in stores:
        store.wait()
    for head in range(heads):
        qa_store(head).wait()
    core_share.wait()
    head_copy.wait()
    with scope("mixed"):
        for pair in range(heads // 2):
            mixed_store(pair).wait()
            for i in range(blocks):
                mixed(pair, i).wait()


def front_call(length, own, w, bias, gain, shift, pw, cot, bq=256):
    rows, cw = own.shape
    d, lw = w.shape[1], w.shape[2]
    heads, pair = lw // HEAD, 2 * HEAD
    sd, vm = jax.ShapeDtypeStruct, pltpu.VMEM
    copies = rows // bq * (1 + heads // 2) + 3 + CHIPS
    shapes = [(rows, d), (rows, d), (rows, lw), (rows, lw), (rows, lw), (heads, rows, pair), (rows, lw), pw.shape, (bq, cw)]
    scratch = [(rows, cw), (rows, cw), w.shape, (rows, d), (rows, d)] + [(rows, lw)] * 4
    work = 2 * heads * rows * rows * HEAD
    return pl.pallas_call(
        functools.partial(front_body, bq=bq),
        out_shape=tuple(sd(a, BF16) for a in shapes),
        in_specs=[pl.BlockSpec(memory_space=pltpu.SMEM), anywhere(), anywhere(), vmem(), vmem(), vmem(), anywhere(), anywhere()],
        out_specs=(anywhere(),) * 9,
        scratch_shapes=[vm(a, BF16) for a in scratch]
        + [vm((heads, rows, pair), BF16), vm((rows, pair), BF16), vm((rows, pair), BF16)]
        + sems(2, 4 + heads // 2 + heads, copies, copies),
        compiler_params=params(collective_id=1, has_side_effects=True),
        cost_estimate=cost(2 * rows * d * 3 * lw + 4 * work, 2 * rows * d * 8, work // 256),
        name="front",
    )(length, own, w, bias, gain, shift, pw, cot)


DOWN_ENTRY, UP_ENTRY = (2, 2), (1, 1)
DOWN_KINDS, UP_KINDS, PAIR_KINDS = (0, 0), (0, 1), (0, 0, 3)


def mlp_body(
    len_ref, xf_hbm, mo_hbm, mr_hbm, pwo_hbm, pwr_hbm, pb, gain, shift, ub, up_hbm, down_hbm, cot_hbm, cot_head,
    lo_out, lo_send_out, gmix, gm_out, up_part, down_part, gp_own, gp_other, sum_ub, sum_db, sum_g, sum_s, sum_pb,
    xf, mo, mr, pwo, pwr, up, down, cot, cot_got, cf, lo, lo_send, mid, second, active, slope, gh,
    gs_send, gs_got, gs_own, gdown, gup, box, up_box, gm, glow, gmix_send, load_sem, store_sem, nsend, nrecv, wsend, wrecv,
    *, wide,
):
    n, me = lax.axis_index("narrow"), lax.axis_index("wide")
    peer = {"narrow": 1 - n}
    rows, cw = cot.shape
    d, f = up.shape
    half, block = rows // 2, min(256, rows // 2)
    each = half // block
    mine, other = lane_part(n, cw), lane_part(1 - n, cw)
    narrow, across = (nsend, nrecv), (wsend, wrecv)
    count = iter(range(16))

    def load(src, dst):
        copy = pltpu.make_async_copy(src, dst, load_sem.at[next(count)])
        copy.start()
        return copy

    his, own = block_rows((1 - n) * half, half), block_rows(n * half, half)
    first = [load(a, b) for a, b in ((pwo_hbm, pwo), (pwr_hbm, pwr))]
    first += [load(a.at[his], b.at[his]) for a, b in ((xf_hbm, xf), (mo_hbm, mo), (mr_hbm, mr))]
    up_load = load(up_hbm, up)
    greet([peer] + wide_peers(me, wide))

    def cot_copy(side, j, a):
        r = block_rows(side * half + j * block, block)
        return remote(cot_hbm.at[r], cot_got.at[r], narrow, a * each + j, peer)

    for a, side in enumerate((n, 1 - n)):
        for j in range(each):
            if (a, j) != (0, 0):
                cot_copy(side, j, a).start()
    head_load = load(cot_head, cot_got.at[block_rows((1 - n) * half, block)])
    down_load = load(down_hbm, down)
    cot_load = load(cot_hbm, cot)
    rest = [load(a.at[own], b.at[own]) for a, b in ((xf_hbm, xf), (mo_hbm, mo), (mr_hbm, mr))]

    def project(at):
        r = block_rows(at, block)
        m = xf[r, :].astype(F32) + (dot(mo[r, :], pwo[...]) + dot(mr[r, :], pwr[...])) + vec(pb)
        mid[r, :] = m
        xhat, _ = norm_rows(m)
        second[r, :] = (xhat * vec(gain) + vec(shift)).astype(BF16)

    def forward(at):
        r = block_rows(at, block)
        hid = dot(second[r, :], up[...]) + vec(ub)
        sq = hid * hid
        t = jnp.tanh(GELU_A * (hid + GELU_B * (sq * hid)))
        hf = 0.5 * (1.0 + t)
        act = (hid * hf).astype(BF16)
        active[r, :] = act
        slope[r, :] = hf + (0.5 * hid) * (1.0 - t * t) * (GELU_A + (3.0 * GELU_A * GELU_B) * sq)
        lo[r, :] = mid[r, mine] + dot(act, down[:, mine])
        lo_send[r, :] = dot(act, down[:, other]).astype(BF16)

    def backward(at):
        r = block_rows(at, block)
        pos = at + lax.broadcasted_iota(jnp.int32, (block, 1), 0)
        live = (pos < len_ref[0]).astype(F32)
        cf[r, mine] = (cot[r, :].astype(F32) * live).astype(BF16)
        cf[r, other] = (cot_got[r, :].astype(F32) * live).astype(BF16)
        ghid = (dot_nt(cf[r, :], down[...]) * slope[r, :]).astype(BF16)
        gh[r, :] = ghid
        sum_ub[...] += jnp.sum(ghid.astype(F32), axis=0, keepdims=True)
        return dot_nt(ghid, up[...])

    def every(side, body):
        def step(j, carry):
            body(side * half + j * block)
            return carry

        lax.fori_loop(0, each, step, 0)

    def both(at):
        project(at)
        forward(at)

    for ref in (sum_ub, sum_g, sum_s, sum_pb, sum_db):
        ref[...] = jnp.zeros_like(ref)
    with scope("load"):
        for copy in first:
            copy.wait()
    with scope("project"):
        every(1 - n, project)
    with scope("load2"):
        up_load.wait()
        down_load.wait()
    with scope("fwd_peer"):
        every(1 - n, forward)
    with scope("cot_wait"):
        cot_load.wait()
        head_load.wait()
        for j in range(1, each):
            cot_copy(n, j, 0).wait()

    def gs_copy(j):
        r = block_rows(j * block, block)
        return remote(gs_send.at[r], gs_got.at[r], narrow, 2 * each + j, peer)

    def for_peer(j, carry):
        gs_send[block_rows(j * block, block), :] = backward((1 - n) * half + j * block).astype(BF16)
        gs_copy(j).start()
        return carry

    def for_own(j, carry):
        gs_own[block_rows(j * block, block), :] = backward(n * half + j * block)
        return carry

    with scope("for_peer"):
        lax.fori_loop(0, each, for_peer, 0)
    for copy in rest:
        copy.wait()
    with scope("fwd_own"):
        every(n, both)
    stores = []

    def store(src, dst):
        copy = pltpu.make_async_copy(src, dst, store_sem.at[len(stores)])
        copy.start()
        stores.append(copy)

    store(lo, lo_out)
    store(lo_send, lo_send_out)
    with scope("cot_wait2"):
        for j in range(each):
            cot_copy(1 - n, j, 1).wait()
    with scope("for_own"):
        lax.fori_loop(0, each, for_own, 0)

    def weight(dst, left, right):
        def step(i, carry):
            c = block_rows(i * 256, 256, 256)
            dst[c, :] = dot_tn(left[:, c], right[...]).astype(BF16)
            return carry

        lax.fori_loop(0, dst.shape[0] // 256, step, 0)

    used = iter(range(16))

    def group(src, box_, part, kinds, leaves):
        parts = []
        for (kind, cols), leave in zip(lanes_split(src.shape[1], kinds), leaves):
            a = next(used)
            chain = Chain(me, order_of(wide, kind), src.shape[0], cols, across, 2 * a, 2 * a)
            parts.append(Group(chain.bind(src, box_, part, None), leave=leave))
        return parts

    reduce_down = group(gdown, box, down_part, DOWN_KINDS, DOWN_ENTRY)
    reduce_up = group(gup, up_box, up_part, UP_KINDS, UP_ENTRY)

    def advance(name, *groups):
        with scope(name):
            for one in groups:
                one.tick()

    with scope("w_down"):
        weight(gdown, active, cf)
    advance("core_d", *reduce_down)
    with scope("w_up"):
        weight(gup, second, gh)
    advance("core_u", *reduce_down, *reduce_up)
    with scope("gs_wait"):
        for j in range(each):
            gs_copy(j).wait()

    fine = min(128, half)

    def gmix_copy(j):
        r = block_rows(n * half + j * fine, fine)
        return remote(gmix_send.at[block_rows(j * fine, fine)], gmix.at[r], narrow, 3 * each + j, peer)

    def back_norm(j, carry):
        r, rh = block_rows(n * half + j * fine, fine), block_rows(j * fine, fine)
        g = gs_own[rh, :] + gs_got[rh, :].astype(F32)
        xhat, scale = norm_rows(mid[r, :])
        gg = g * vec(gain)
        m1 = jnp.mean(gg, axis=-1, keepdims=True)
        m2 = jnp.mean(gg * xhat, axis=-1, keepdims=True)
        c = cf[r, :].astype(F32)
        grad = c + scale * (gg - m1 - xhat * m2)
        gm[rh, :] = grad
        gl = grad.astype(BF16)
        glow[rh, :] = gl
        gmix_send[rh, :] = dot_nt(gl, pwr[...]).astype(BF16)
        gmix_copy(j).start()
        gmix[r, :] = dot_nt(gl, pwo[...]).astype(BF16)
        sum_g[...] += jnp.sum(g * xhat, axis=0, keepdims=True)
        sum_s[...] += jnp.sum(g, axis=0, keepdims=True)
        sum_pb[...] += jnp.sum(grad, axis=0, keepdims=True)
        sum_db[...] += jnp.sum(c, axis=0, keepdims=True)
        return carry

    with scope("back_norm"):
        lax.fori_loop(0, half // fine, back_norm, 0)
    store(gm, gm_out)
    advance("across", *reduce_up)
    with scope("proj"):
        lw = mo.shape[1]
        for src, dst in ((mr, gp_other), (mo, gp_own)):
            total = dot_tn(src[own, :], glow[...]).astype(BF16)
            dst[0:lw, :] = total[:, :cw]
            dst[lw : 2 * lw, :] = total[:, cw:]
    with scope("gmix_wait"):
        for j in range(half // fine):
            gmix_copy(j).wait()
    advance("leave", *reduce_down, *reduce_up)
    with scope("store"):
        for copy in stores:
            copy.wait()


def mlp_call(length, xf, mo, mr, pwo, pwr, pb, gain, shift, up, ub, down, cot, cot_head, wide):
    rows, d = xf.shape
    f, lw, cw = up.shape[1], mo.shape[1], cot.shape[1]
    half = rows // 2
    sd, vm = jax.ShapeDtypeStruct, pltpu.VMEM
    each = half // min(256, half)
    return pl.pallas_call(
        functools.partial(mlp_body, wide=wide),
        out_shape=(
            sd((rows, cw), F32), sd((rows, cw), BF16), sd((rows, lw), BF16), sd((half, d), F32),
            sd((d // 2, f), BF16), sd((f // 2, d), BF16), sd((2 * lw, cw), BF16), sd((2 * lw, cw), BF16),
            sd((1, f), F32), sd((1, d), F32), sd((1, d), F32), sd((1, d), F32), sd((1, d), F32),
        ),
        in_specs=[pl.BlockSpec(memory_space=pltpu.SMEM)] + [anywhere()] * 5 + [vmem()] * 4 + [anywhere()] * 4,
        out_specs=(anywhere(), anywhere(), vmem(), anywhere()) + (vmem(),) * 9,
        scratch_shapes=[
            vm((rows, d), BF16), vm((rows, lw), BF16), vm((rows, lw), BF16), vm((lw, d), BF16), vm((lw, d), BF16),
            vm((d, f), BF16), vm((f, d), BF16), vm((rows, cw), BF16), vm((rows, cw), BF16), vm((rows, d), BF16),
            vm((rows, cw), F32), vm((rows, cw), BF16), vm((rows, d), F32),
            vm((rows, d), BF16), vm((rows, f), BF16), vm((rows, f), F32), vm((rows, f), BF16),
            vm((half, d), BF16), vm((half, d), BF16), vm((half, d), F32), vm((f, d), BF16), vm((d, f), BF16),
            vm((f, d), BF16), vm((d, f), BF16), vm((half, d), F32), vm((half, d), BF16), vm((half, lw), BF16),
        ]
        + sems(12, 4, 3 * each + half // min(128, half), 3 * each + half // min(128, half), 8, 8),
        compiler_params=params(collective_id=3, has_side_effects=True),
        cost_estimate=cost(2 * rows * d * (d + 6 * f), 2 * (rows * d * 8 + 2 * d * f), rows * f),
        name="mlp",
    )(length, xf, mo, mr, pwo, pwr, pb, gain, shift, ub, up, down, cot, cot_head)


START_TICKS = "U0D1D0U1"
HEAD_TICKS = (
    ((0, 3), "SA"),
    ((1, 2), "D1"),
    ((1, 3), "D0Q0"),
    ((2, 0), "U0U1"),
    ((2, 2), "D1Q0"),
    ((2, 3), ""),
    ((3, 0), "D0"),
    ((3, 1), "SA"),
    ((3, 2), "P0U0"),
    ((3, 3), "Q0SAD1U1Q1"),
    ((4, 1), "D0"),
    ((4, 2), "P0Q1"),
    ((4, 3), "U0Q0"),
    ((5, 3), "D1Q1SAQ2"),
)
PART_TICKS = ("D0U1P0", "Q2U0", "Q1Q0D1", "", "D0P0U1")
LAST_TICKS = (
    "U0Q1Q2Q0D1P0D0", "norm0", "Q1U1U0Q0Q2Q1D1P0", "norm1", "U1D1U0Q0D0Q1Q2SB", "D0P0SBU1U0Q0Q1U0",
    "P0Q2Q2Q0SBU1Q0P0", "Q1U1P0Q1",
)


def pieces(names):
    return [names[i : i + 2] for i in range(0, len(names), 2)]


def back_body(
    len_ref, qa_hbm, k_hbm, v_hbm, do_hbm, o_hbm, low_hbm, w_hbm, xf_hbm, gm_hbm, gain, lo_send, up_part_hbm,
    down_part_hbm, gp_own_hbm, gp_other_hbm, s_ub, s_db, s_g2, s_s2, s_pb,
    lo_got, down_out, up_out, gp_out, g0_out, g1_out, g2_out, ig, small_a, small_b,
    qa, k, v, do, o, low, wp, xf, gm, up_part, down_part, gp_src, gp_got,
    ka, va, kt, dk_acc, dv_acc, dqkv, gpair,
    down_box, down_part2, down_own, up_box, up_part2, up_own, gp_box, gp_part, gp_own, pair_box, pair_part, pair_own,
    down_sum, up_sum, gp_sum, pair_sum,
    gn_send, gn_got, gn_own, ig_own, ig_send, early, early_box, late_sums, late_box,
    load_sem, open_sem, nsend, nrecv, wsend, wrecv, *, bq, wide,
):
    n, me = lax.axis_index("narrow"), lax.axis_index("wide")
    peer = {"narrow": 1 - n}
    narrow, across = (nsend, nrecv), (wsend, wrecv)
    steps = bits(wide)
    heads, rows = qa.shape[0], qa.shape[1]
    pair_w = 2 * HEAD
    pairs = heads // 2
    d, lw = gain.shape[0], k.shape[1]
    cw = d // 2
    half, block = rows // 2, min(256, rows // 2)
    each = half // block
    count = iter(range(64))

    def load(src, dst):
        copy = pltpu.make_async_copy(src, dst, load_sem.at[next(count)])
        copy.start()
        return copy

    pair_loads = []
    for p in range(pairs):
        c = pl.ds(p * pair_w, pair_w)
        pair_loads.append(
            [load(a.at[:, c], b.at[:, c]) for a, b in ((k_hbm, k), (v_hbm, v), (do_hbm, do), (o_hbm, o))]
            + [load(qa_hbm.at[pl.ds(2 * p, 2)], qa.at[pl.ds(2 * p, 2)])]
        )
    part_load = load(down_part_hbm, down_part)
    up_load = load(up_part_hbm, up_part)
    gp_load = load(gp_own_hbm, gp_src)
    low_load = load(low_hbm, low)
    greet([peer] + wide_peers(me, wide))
    gp_swap = remote(gp_other_hbm, gp_got, narrow, 0, peer)
    layer = remote(lo_send, lo_got, narrow, 1, peer)
    gp_swap.start()
    late = [
        load(w_hbm.at[c, :, pl.ds(p * pair_w, pair_w)], wp.at[p, :, pl.ds(c * pair_w, pair_w)])
        for p in range(pairs)
        for c in range(3)
    ]
    own_half = block_rows(n * half, half)
    late += [load(xf_hbm.at[own_half], xf), load(gm_hbm, gm)]

    at = [0, 0]
    opening = iter(range(16))

    def group(src, box, part, own, dst, out, kinds=(0,), entries=(0,)):
        rows_, cols_ = dst.shape
        made = []
        for (kind, cols), entry in zip(lanes_split(cols_, kinds), entries):
            chain = Chain(me, order_of(wide, kind), rows_, cols, across, *at)
            at[:] = chain.send_next, chain.recv_next
            made.append(Group(chain.bind(src, box, part, own, dst, entry), entry, out=(out, open_sem.at[next(opening)])))
        return made

    groups = {}
    groups["D0"], groups["D1"] = group(down_part, down_box, down_part2, down_own, down_sum, down_out, DOWN_KINDS, DOWN_ENTRY)
    groups["U0"], groups["U1"] = group(up_part, up_box, up_part2, up_own, up_sum, up_out, UP_KINDS, UP_ENTRY)
    groups["P0"] = group(gp_src, gp_box, gp_part, gp_own, gp_sum, gp_out, kinds=(1,))[0]
    for p, out in zip(range(pairs), (g0_out, g1_out, g2_out)):
        groups[f"Q{p}"] = group(
            gpair.at[p], pair_box.at[p], pair_part.at[p], pair_own.at[p], pair_sum.at[p], out,
            kinds=(PAIR_KINDS[p],),
        )[0]

    dr, fr, lr = d // 128, s_ub.shape[1] // 128, lw // 128
    for i, (name, total, box, shared) in enumerate(
        (("SA", early, early_box, 4 * dr), ("SB", late_sums, late_box, -(-2 * dr // 8) * 8))
    ):
        one = Small(me, n, wide, total, box, shared, narrow, across, 2 + 2 * each + i, *at)
        at[:] = one.send_next, one.recv_next
        groups[name] = Group(one)

    def put_sum(ref, start, value):
        for i in range(value.shape[1] // 128):
            ref[start + i : start + i + 1, :] = value[:, i * 128 : (i + 1) * 128]

    early[...] = jnp.zeros_like(early)
    late_sums[...] = jnp.zeros_like(late_sums)
    for i, ref in enumerate((s_g2, s_s2, s_pb, s_db, s_ub)):
        put_sum(early, i * dr, ref[...])

    def tick(names):
        for name in pieces(names):
            with scope(name):
                groups[name].tick()

    part_load.wait()
    up_load.wait()
    tick(START_TICKS)

    kpos = lax.broadcasted_iota(jnp.int32, (rows, 1), 0)
    kbias = jnp.where(kpos < len_ref[0], 0.0, -1e30)
    tri = lax.broadcasted_iota(jnp.int32, (bq, bq), 0) <= lax.broadcasted_iota(jnp.int32, (bq, bq), 1)

    def plan(names):
        ticks = [groups[name].next() for name in pieces(names)]

        def run():
            for name, one in zip(pieces(names), ticks):
                with scope(name):
                    one()

        return run

    def start_proj():
        first = groups["P0"].next()

        def run():
            gp_swap.wait()
            gp_load.wait()
            gp_src[...] = gp_src[...] + gp_got[...]
            first()

        return run

    hooks = {}
    for at_, names in HEAD_TICKS:
        hooks[at_] = [plan(names)]
        if at_ == (2, 3):
            hooks[at_] += [layer.start, start_proj()]

    def run_hooks(head, block_):
        for (h, where), actions in hooks.items():
            if where == block_:

                @pl.when(head == h)
                def _():
                    for action in actions:
                        action()

    def one_head(head, carry):
        par, pair = head % 2, head // 2
        lane, mine, extra = lanes_of(par)
        cols = lane_part(pair, pair_w)
        for p in range(pairs):

            @pl.when(head == 2 * p)
            def _():
                for copy in pair_loads[p]:
                    copy.wait()

        ka[...] = place(lane, mine, extra, k[:, cols].astype(F32), [kbias, -1.0, -1.0, -1.0]).astype(BF16)
        va[...] = place(lane, mine, extra, v[:, cols].astype(F32), [-1.0, -1.0, -1.0]).astype(BF16)
        kt[...] = ka[...].T
        dk_acc[...] = jnp.zeros_like(dk_acc)
        dv_acc[...] = jnp.zeros_like(dv_acc)

        def put(c, r, new):
            lanes = pl.ds(c * pair_w, pair_w)
            old = dqkv[pair, r, lanes].astype(F32)
            dqkv[pair, r, lanes] = jnp.where(mine, new, jnp.where(par == 0, 0.0, old)).astype(BF16)

        for i in range(rows // bq):
            r = pl.ds(i * bq, bq)
            qb = qa[head, r, :]
            df = do[r, cols].astype(F32)
            delta = jnp.sum(jnp.where(mine, df * o[r, cols].astype(F32), 0.0), axis=1, keepdims=True)
            db = place(lane, mine, extra, df, three(delta)).astype(BF16)
            dqs = None
            chunks = [(0, i * bq), (i * bq, bq)] if i else [(0, bq)]
            for start, size in chunks:
                c = pl.ds(start, size)
                kb, vb = ka[c, :], va[c, :]
                s = dot_nt(kb, qb)
                if start == i * bq:
                    s = jnp.where(tri, s, -1e30)
                p = jnp.exp(s)
                ds = (p * dot_nt(vb, db)).astype(BF16)
                dv_acc[c, :] += dot(p.astype(BF16), db)
                dk_acc[c, :] += dot(ds, qb)
                part = dot(kt[:, c], ds)
                dqs = part if dqs is None else dqs + part
            put(0, r, dqs.T * HEAD**-0.5)
            if i < rows // bq - 1:
                run_hooks(head, i)
        put(1, pl.ds(0, rows), dk_acc[...])
        put(2, pl.ds(0, rows), dv_acc[...])

        @pl.when(head == 1)
        def _():
            low_load.wait()

        @pl.when(par == 1)
        def _():
            with scope("weights"):
                gpair[pair] = dot_tn(low[...], dqkv[pair]).astype(BF16)

        run_hooks(head, rows // bq - 1)
        return carry

    lax.fori_loop(0, heads, one_head, 0)

    for copy in late:
        copy.wait()

    def gn_part(start):
        r = block_rows(start, block)
        total = dot_nt(dqkv[0, r, :], wp[0])
        for p in range(1, pairs):
            total += dot_nt(dqkv[p, r, :], wp[p])
        return total

    def gn_copy(j):
        r = pl.ds(j * block, block)
        return remote(gn_send.at[r], gn_got.at[r], narrow, 2 + j, peer)

    for j in range(each):
        with scope("gn_peer"):
            gn_send[j * block : (j + 1) * block, :] = gn_part((1 - n) * half + j * block).astype(BF16)
        gn_copy(j).start()
        tick(PART_TICKS[j % 2])
    for j in range(each):
        with scope("gn_own"):
            gn_own[j * block : (j + 1) * block, :] = gn_part(n * half + j * block)
        tick(PART_TICKS[2 + j % 2])

    shared = -(-2 * dr // 8) * 8
    for p in range(pairs):
        put_sum(late_sums, shared + p, jnp.sum(dqkv[p, :, 0:pair_w].astype(F32), axis=0, keepdims=True))
        put_sum(late_sums, shared + lr + p, jnp.sum(dqkv[p, :, 2 * pair_w :].astype(F32), axis=0, keepdims=True))
    tick(PART_TICKS[4])

    mine, other = lane_part(n, cw), lane_part(1 - n, cw)

    def ig_copy(j):
        r = block_rows(n * half + j * block, block)
        return remote(ig_send.at[pl.ds(j * block, block)], ig.at[r], narrow, 2 + each + j, peer)

    def in_norm(j):
        with scope("gn_wait"):
            gn_copy(j).wait()
        rh = pl.ds(j * block, block)
        r = block_rows(n * half + j * block, block)
        g = gn_own[rh, :] + gn_got[rh, :].astype(F32)
        xhat, scale = norm_rows(xf[rh, :].astype(F32))
        gg = g * vec(gain)
        m1 = jnp.mean(gg, axis=-1, keepdims=True)
        m2 = jnp.mean(gg * xhat, axis=-1, keepdims=True)
        ig_own[...] = gm[rh, :] + scale * (gg - m1 - xhat * m2)
        ig_send[rh, :] = ig_own[:, other].astype(BF16)
        ig_copy(j).start()
        ig[r, :] = ig_own[:, mine].astype(BF16)
        return jnp.sum(g * xhat, axis=0, keepdims=True), jnp.sum(g, axis=0, keepdims=True)

    sums1 = []
    for names in LAST_TICKS:
        if names in ("norm0", "norm1"):
            todo = range(each - 1) if names == "norm0" else range(each - 1, each)
            sums1 += [in_norm(j) for j in todo]
            if names == "norm1":
                put_sum(late_sums, 0, sum(a for a, _ in sums1))
                put_sum(late_sums, dr, sum(b for _, b in sums1))
                tick("SB")
        else:
            tick(names)
    while not all(g.done for g in groups.values()):
        for name in groups:
            tick(name)
    small_a[...] = early[...]
    small_b[...] = late_sums[...]
    with scope("end"):
        for one in groups.values():
            if one.out is not None:
                one.store().wait()
        layer.wait()
        for j in range(each):
            ig_copy(j).wait()


def back_call(
    length, qa, k, v, do, o, low, w, xf, gm, gain, lo_send, up_part, down_part, gp_own, gp_other,
    s_ub, s_db, s_g2, s_s2, s_pb, wide, bq=256,
):
    heads, rows, pair = qa.shape
    d, f, lw = gain.shape[0], up_part.shape[1], k.shape[1]
    cw, half = d // 2, rows // 2
    block = min(256, half)
    each, steps, pairs = half // block, bits(wide), heads // 2
    sd, vm = jax.ShapeDtypeStruct, pltpu.VMEM
    shape = lambda r, kind=0: Chain(0, order_of(wide, kind), r, None, None, 0, 0)
    c_down, c_up, c_gp = shape(f), shape(d), shape(2 * lw)
    down_rows, up_rows, pair_rows = (max(shape(r, k).box_rows for k in range(4)) for r in (f, d, d))
    small = lambda shared, rest: -(-(shared + rest) // 8) * 8
    rows_a = small(4 * d // 128, f // 128)
    rows_b = small(-(-2 * d // 1024) * 8, 2 * lw // 128)
    slots = CHIPS + 1 + max(0, bits(wide) - 4)
    semaphores = (len(DOWN_KINDS) + len(UP_KINDS) + 1 + pairs) * shape(d).recv_next + 2 * (bits(wide) + CHIPS)
    work = 2 * heads * rows * rows * HEAD
    return pl.pallas_call(
        functools.partial(back_body, bq=bq, wide=wide),
        out_shape=(sd((rows, cw), BF16), sd((f, d), BF16), sd((d, f), BF16), sd((2 * lw, cw), BF16))
        + (sd((d, 3 * pair), BF16),) * 3
        + (sd((rows, cw), BF16), sd((rows_a, 128), F32), sd((rows_b, 128), F32)),
        in_specs=[pl.BlockSpec(memory_space=pltpu.SMEM)] + [anywhere()] * 9 + [vmem()] + [anywhere()] * 5 + [vmem()] * 5,
        out_specs=(anywhere(),) * 7 + (vmem(), vmem(), vmem()),
        scratch_shapes=[
            vm(qa.shape, BF16), vm((rows, lw), BF16), vm((rows, lw), BF16), vm((rows, lw), BF16), vm((rows, lw), BF16),
            vm((rows, d), BF16), vm((pairs, d, 3 * pair), BF16), vm((half, d), BF16), vm((half, d), F32),
            vm((d // 2, f), BF16), vm((f // 2, d), BF16), vm((2 * lw, cw), BF16), vm((2 * lw, cw), BF16),
            vm((rows, pair), BF16), vm((rows, pair), BF16), vm((pair, rows), BF16), vm((rows, pair), F32), vm((rows, pair), F32),
            vm((pairs, rows, 3 * pair), BF16), vm((pairs, d, 3 * pair), BF16),
            vm((down_rows, d), BF16), vm((f // 2, d), BF16), vm((c_down.size, d), BF16),
            vm((up_rows, f), BF16), vm((d // 2, f), BF16), vm((c_up.size, f), BF16),
            vm((pair_rows, cw), BF16), vm((lw, cw), BF16), vm((c_gp.size, cw), BF16),
            vm((pairs, pair_rows, 3 * pair), BF16), vm((pairs, d // 2, 3 * pair), BF16),
            vm((pairs, c_up.size, 3 * pair), BF16),
            vm((f, d), BF16), vm((d, f), BF16), vm((2 * lw, cw), BF16), vm((pairs, d, 3 * pair), BF16),
            vm((half, d), BF16), vm((half, d), BF16), vm((half, d), F32), vm((block, d), F32), vm((half, cw), BF16),
            vm((rows_a, 128), F32), vm((slots, rows_a, 128), F32), vm((rows_b, 128), F32), vm((slots, rows_b, 128), F32),
        ]
        + sems(8 * pairs + 8, 8, 4 + 2 * each, 4 + 2 * each, 9 + 3 * CHIPS, semaphores),
        compiler_params=params(collective_id=4, has_side_effects=True),
        cost_estimate=cost(10 * work + 4 * rows * d * 3 * lw, 2 * rows * d * 20, work // 256),
        name="back",
    )(
        length, qa, k, v, do, o, low, w, xf, gm, gain, lo_send, up_part, down_part, gp_own, gp_other,
        s_ub, s_db, s_g2, s_s2, s_pb,
    )


def finish_body(
    lo, lo_got, bias, ig, up, down, q, k, v, p0, p1, small_a, small_b,
    out, ig_out, o_qkv, o_qvb, o_proj, o_pb, o_up, o_ub, o_down, o_db, o_g1, o_s1, o_g2, o_s2,
    *, factor,
):
    n = lax.axis_index("narrow")
    cw = lo.shape[1]
    b = vec(bias)
    out[...] = (lo[...] + lo_got[...].astype(F32) + jnp.where(n == 0, b[:, :cw], b[:, cw:])).astype(BF16)
    ig_out[...] = ig[...]
    for p, ref in enumerate((q, k, v)):
        for c in range(3):
            lanes = slice(c * 128, (c + 1) * 128)
            o_qkv[c, :, p * 128 : (p + 1) * 128] = ref[:, lanes].astype(F32) * factor
    o_proj[:, :cw] = p0[...].astype(F32) * factor
    o_proj[:, cw:] = p1[...].astype(F32) * factor
    o_up[...] = up[...].astype(F32) * factor
    o_down[...] = down[...].astype(F32) * factor

    @pl.when(pl.program_id(0) == 0)
    def _():
        dr, fr = o_g1.shape[0], o_ub.shape[0]
        for i, ref in enumerate((o_g2, o_s2, o_pb, o_db)):
            ref[...] = small_a[i * dr : (i + 1) * dr, :] * factor
        o_ub[...] = small_a[4 * dr : 4 * dr + fr, :] * factor
        o_g1[...] = small_b[0:dr, :] * factor
        o_s1[...] = small_b[dr : 2 * dr, :] * factor
        lr, shared = o_qvb.shape[1] // 128, -(-2 * dr // 8) * 8
        for c in range(2):
            for i in range(lr):
                at = shared + c * lr + i
                o_qvb[c : c + 1, i * 128 : (i + 1) * 128] = small_b[at : at + 1, :] * factor


def finish_call(lo, lo_got, bias, ig, up, down, q, k, v, p, small_a, small_b, factor, grid=8):
    rows, cw = lo.shape
    (d, f), lw = up.shape, q.shape[1]
    dr, sd = d // 128, jax.ShapeDtypeStruct
    shapes = (
        [sd((rows, cw), BF16), sd((rows, cw), BF16), sd((3, d, lw), F32), sd((2, lw), F32), sd((lw, d), F32)]
        + [sd((dr, 128), F32), sd((d, f), F32), sd((f // 128, 128), F32), sd((f, d), F32)]
        + [sd((dr, 128), F32)] * 5
    )
    big = lambda a: rows_spec(a.shape[0] // grid, a.shape[1])
    pb = lw // grid
    specs = []
    for i, s in enumerate(shapes):
        if len(s.shape) == 3:
            specs.append(pl.BlockSpec((3, d // grid, lw), lambda i, *_: (0, i, 0)))
        elif i in (0, 1, 4, 6, 8):
            specs.append(big(s))
        else:
            specs.append(whole_spec(s.shape))
    return pl.pallas_call(
        functools.partial(finish_body, factor=factor),
        out_shape=tuple(shapes),
        grid=(grid,),
        in_specs=[big(lo), big(lo_got), whole_spec(bias.shape), big(ig), big(up), big(down), big(q), big(k), big(v)]
        + [rows_spec(pb, cw), rows_spec(pb, cw, grid), whole_spec(small_a.shape), whole_spec(small_b.shape)],
        out_specs=tuple(specs),
        compiler_params=params(),
        cost_estimate=cost(up.size * 8, up.size * 24),
        name="finish",
    )(lo, lo_got, bias, ig, up, down, q, k, v, p, p, small_a, small_b)


def on_device(
    tokens, lengths, qkv_weight, qv_bias, proj_weight, proj_bias, up_weight, up_bias,
    down_weight, down_bias, first_gain, first_shift, second_gain, second_shift, cotangent,
):
    cw = tokens.shape[1]
    d, ff, lw = 2 * cw, up_weight.shape[1], proj_weight.shape[0]
    wide = lax.axis_size("wide")
    w3 = jnp.transpose(qkv_weight, (1, 0, 2))

    xf, low, k, v, mixed, qa, mixed_got, proj_got, cot_head = front_call(
        lengths, tokens, w3, qv_bias, first_gain, first_shift, proj_weight, cotangent
    )
    lo, lo_send, gmix, gm, up_part, down_part, gp_own, gp_other, s_ub, s_db, s_g2, s_s2, s_pb = mlp_call(
        lengths, xf, mixed, mixed_got, proj_weight, proj_got, proj_bias, second_gain, second_shift,
        up_weight, up_bias, down_weight, cotangent, cot_head, wide,
    )
    lo_got, gdown, gup, gp, g0, g1, g2, ig, small_a, small_b = back_call(
        lengths, qa, k, v, gmix, mixed, low, w3, xf, gm, first_gain, lo_send, up_part, down_part, gp_own, gp_other,
        s_ub, s_db, s_g2, s_s2, s_pb, wide,
    )
    out, ig, o_qkv, o_qvb, o_proj, *rest = finish_call(
        lo, lo_got, down_bias, ig, gup, gdown, g0, g1, g2, gp, small_a, small_b,
        1.0 / (lengths.shape[0] * wide),
    )
    pb, up, ubs, down, dbs, g1, s1, g2, s2 = rest
    flat = lambda a: a.reshape(-1)
    return (
        out, ig, jnp.transpose(o_qkv, (1, 0, 2)), o_qvb, o_proj, flat(pb), up, flat(ubs), down, flat(dbs),
        flat(g1), flat(s1), flat(g2), flat(s2),
    )


def solution(mesh):
    split = P("wide", "narrow")
    none3, cols, rows1 = P(None, None, "narrow"), P(None, "narrow"), P("narrow", None)
    return jax.shard_map(
        on_device,
        mesh=mesh,
        in_specs=(
            split, P("wide"), none3, cols, rows1, P(), cols, P("narrow"), rows1, P(), P(), P(), P(), P(), split,
        ),
        out_specs=(
            split, split, none3, cols, rows1, P(), cols, P("narrow"), rows1, P(), P(), P(), P(), P(),
        ),
        check_vma=False,
    )
```
